32 devices in a mesh: tp: 8 (over z, y), dp: 4 (over x, core).
Axes of the slice: x: 2, y: 2, z: 4, core: 2. Of those that a mesh axis runs over, the one named last changes fastest.
Arguments:
- x: bfloat16 [8192, 2048], P(('dp', 'tp'))
- w_gate: bfloat16 [2048, 8192], P('dp', 'tp')
- w_up: bfloat16 [2048, 8192], P('dp', 'tp')
- w_down: bfloat16 [8192, 2048], P('tp', 'dp')
- dy: bfloat16 [8192, 2048], P(('dp', 'tp'))
Outputs:
- output 1: bfloat16 [8192, 2048], P(('dp', 'tp'))
- output 2: bfloat16 [8192, 2048], P(('dp', 'tp'))
- output 3: float32 [2048, 8192], P('dp', 'tp')
- output 4: float32 [2048, 8192], P('dp', 'tp')
- output 5: float32 [8192, 2048], P('tp', 'dp')
All inputs are finite; a program needn't handle non-finite values.
Results may differ from the reference program's by a relative error of at most 0.00111.
Values are sent between devices in bfloat16 or wider.
A program may use at most 1 GiB of HBM per device.

```python
import jax
import jax.numpy as jnp
from jax import lax

ROWS = 8192
D = 2048
FF = 8192


def setup_inputs(seed: int = 0) -> dict:
    ks = jax.random.split(jax.random.key(seed), 5)
    x = jax.random.normal(ks[0], (ROWS, D), jnp.float32)
    w_gate = jax.random.normal(ks[1], (D, FF), jnp.float32) * (D ** -0.5)
    w_up = jax.random.normal(ks[2], (D, FF), jnp.float32) * (D ** -0.5)
    w_down = jax.random.normal(ks[3], (FF, D), jnp.float32) * (1.5 * FF ** -0.5)
    dy = jax.random.normal(ks[4], (ROWS, D), jnp.float32)
    return dict(x=x.astype(jnp.bfloat16), w_gate=w_gate.astype(jnp.bfloat16), w_up=w_up.astype(jnp.bfloat16), w_down=w_down.astype(jnp.bfloat16), dy=dy.astype(jnp.bfloat16))


def reference(x, w_gate, w_up, w_down, dy):
    nb = ROWS // 256
    xs = x.reshape(nb, ROWS // nb, D)
    dys = dy.reshape(nb, ROWS // nb, D)

    def body(carry, inp):
        gw, uw, dw = carry
        xb, dyb = inp
        a = jnp.dot(xb, w_gate, preferred_element_type=jnp.float32)
        b = jnp.dot(xb, w_up, preferred_element_type=jnp.float32)
        sig = jax.nn.sigmoid(a)
        sa = a * sig
        h = (sa * b).astype(jnp.bfloat16)
        y = (xb.astype(jnp.float32) + jnp.dot(h, w_down, preferred_element_type=jnp.float32)).astype(jnp.bfloat16)
        g = jnp.dot(dyb, w_down.T, preferred_element_type=jnp.float32)
        da = (g * b * sig * (1.0 + a * (1.0 - sig))).astype(jnp.bfloat16)
        db = (g * sa).astype(jnp.bfloat16)
        dx = (dyb.astype(jnp.float32) + jnp.dot(da, w_gate.T, preferred_element_type=jnp.float32) + jnp.dot(db, w_up.T, preferred_element_type=jnp.float32)).astype(jnp.bfloat16)
        gw = gw + jnp.dot(xb.T, da, preferred_element_type=jnp.float32)
        uw = uw + jnp.dot(xb.T, db, preferred_element_type=jnp.float32)
        dw = dw + jnp.dot(h.T, dyb, preferred_element_type=jnp.float32)
        return (gw, uw, dw), (y, dx)

    init = (jnp.zeros((D, FF), jnp.float32), jnp.zeros((D, FF), jnp.float32), jnp.zeros((FF, D), jnp.float32))
    (gw, uw, dw), (ys, dxs) = lax.scan(body, init, (xs, dys))
    return ys.reshape(ROWS, D), dxs.reshape(ROWS, D), gw, uw, dw
```

```python
import jax
import jax.numpy as jnp
from jax import lax
from jax.experimental import pallas as pl
from jax.experimental.pallas import tpu as pltpu
from jax.sharding import PartitionSpec as P

MESH = pl.DeviceIdType.MESH
f32 = jnp.float32
bf = jnp.bfloat16


NEXT = (1, 3, 0, 2)


def gather_kernel(x_in, dy_in, wg_in, wu_in, wd_in, xa, dya, wg, wu, wd, ssem, rsem, lsem):
    tp = lax.axis_index("tp")
    dp = lax.axis_index("dp")
    z, y = tp // 2, tp % 2
    nxt = 2 * z + 1 - 5 * (z // 2)
    prv = z // 2 + 2 * (1 - z % 2)
    dev_x = {"tp": tp, "dp": (dp + 2) % 4}
    dev_y = {"tp": 2 * z + 1 - y, "dp": dp}
    dev_c = {"tp": tp, "dp": 2 * (dp // 2) + 1 - dp % 2}
    dev_n = {"tp": 2 * nxt + y, "dp": dp}
    dev_p = {"tp": 2 * prv + y, "dp": dp}

    bar = pltpu.get_barrier_semaphore()
    for d in (dev_x, dev_y, dev_c, dev_n, dev_p):
        pl.semaphore_signal(bar, inc=1, device_id=d, device_id_type=MESH)
    pl.semaphore_wait(bar, 5)

    kd, kf = wg_in.shape

    def blk(k, rx, rc, ry, h=None):
        d0 = (2 * rc + rx) * kd
        if k < 2:
            ref = (wg, wu)[k]
            if h is None:
                return ref.at[pl.ds(d0, kd), pl.ds(ry * kf, kf)]
            return ref.at[pl.ds(d0 + h * (kd // 2), kd // 2), pl.ds(ry * kf, kf)]
        if h is None:
            return wd.at[pl.ds(ry * kf, kf), pl.ds(d0, kd)]
        return wd.at[pl.ds(ry * kf + h * (kf // 2), kf // 2), pl.ds(d0, kd)]

    count = [0]
    sends = []

    def send(src, dst, dev):
        i = count[0]
        count[0] += 1
        c = pltpu.make_async_remote_copy(
            src_ref=src, dst_ref=dst, send_sem=ssem.at[i], recv_sem=rsem.at[i], device_id=dev, device_id_type=MESH
        )
        c.start()
        sends.append(c)
        return c

    own = (wg_in, wu_in, wd_in)
    zc = [[None, None] for _ in range(3)]
    xc, yc, cc = [None] * 3, [None] * 3, []
    zc[0][0] = send(x_in, xa.at[1], dev_n)
    for k in range(3):
        xc[k] = send(own[k], blk(k, 1, 0, 0), dev_x)
        yc[k] = send(own[k], blk(k, 0, 0, 1), dev_y)
        cc.append(send(own[k], blk(k, 0, 1, 0), dev_c))
        if k == 0:
            zc[0][1] = send(dy_in, dya.at[1], dev_n)
    local = [(x_in, xa.at[0]), (dy_in, dya.at[0])] + [(own[k], blk(k, 0, 0, 0)) for k in range(3)]
    local = [pltpu.make_async_copy(s, d, lsem.at[i]) for i, (s, d) in enumerate(local)]
    for c in local:
        c.start()

    def zstep(s, j):
        ref = (xa, dya)[j]
        zc[s - 1][j].wait_recv()
        if s < 3:
            zc[s][j] = send(ref.at[s], ref.at[s + 1], dev_n)

    ra, rb = [None] * 3, [None] * 3
    zorder = [(1, 0), (1, 1), (2, 0), (2, 1), (3, 0), (3, 1)]
    for k in range(3):
        xc[k].wait_recv()
        ra[k] = send(blk(k, 1, 0, 0, 0), blk(k, 1, 0, 1, 0), dev_y)
        yc[k].wait_recv()
        rb[k] = send(blk(k, 0, 0, 1, 1), blk(k, 1, 0, 1, 1), dev_x)
        cc.append(send(blk(k, 1, 0, 0), blk(k, 1, 1, 0), dev_c))
        cc.append(send(blk(k, 0, 0, 1), blk(k, 0, 1, 1), dev_c))
        zstep(*zorder[k])
    for k in range(3):
        if k == 2:
            zstep(*zorder[3])
        ra[k].wait_recv()
        cc.append(send(blk(k, 1, 0, 1, 0), blk(k, 1, 1, 1, 0), dev_c))
        rb[k].wait_recv()
        cc.append(send(blk(k, 1, 0, 1, 1), blk(k, 1, 1, 1, 1), dev_c))
    zstep(*zorder[4])
    zstep(*zorder[5])
    for c in cc:
        c.wait_recv()
    for c in sends:
        c.wait_send()
    for c in local:
        c.wait()


def gather(x, dy, wg, wu, wd):
    rows, d = x.shape
    kd, kf = wg.shape
    vm = pl.BlockSpec(memory_space=pltpu.VMEM)
    hbm = pl.BlockSpec(memory_space=pl.ANY)
    n = 6 + 9 + 6 + 12
    return pl.pallas_call(
        gather_kernel,
        name="gather",
        out_shape=(
            jax.ShapeDtypeStruct((4, rows, d), bf),
            jax.ShapeDtypeStruct((4, rows, d), bf),
            jax.ShapeDtypeStruct((4 * kd, 2 * kf), bf),
            jax.ShapeDtypeStruct((4 * kd, 2 * kf), bf),
            jax.ShapeDtypeStruct((2 * kf, 4 * kd), bf),
        ),
        in_specs=[vm] * 5,
        out_specs=(hbm,) * 5,
        scratch_shapes=[pltpu.SemaphoreType.DMA((n,)), pltpu.SemaphoreType.DMA((n,)), pltpu.SemaphoreType.DMA((5,))],
        compiler_params=pltpu.CompilerParams(collective_id=0, has_side_effects=True),
    )(x, dy, wg, wu, wd)


def solution(mesh):
    rows = P(("dp", "tp"), None)
    wsp = P("dp", "tp")
    dsp = P("tp", "dp")

    def px(v):
        return lax.ppermute(v, "dp", [(i, i ^ 2) for i in range(4)])

    def pc(v):
        return lax.ppermute(v, "dp", [(i, i ^ 1) for i in range(4)])

    def py(v):
        return lax.ppermute(v, "tp", [(i, i ^ 1) for i in range(8)])

    def pz(v):
        return lax.ppermute(v, "tp", [(2 * z + y, 2 * NEXT[z] + y) for z in range(4) for y in range(2)])

    def dot(a, b):
        return jnp.dot(a, b, preferred_element_type=f32)

    def relative(v):
        dp = lax.axis_index("dp")
        t = v.reshape(v.shape[0], 2, 2, -1)
        t = jnp.where(dp >= 2, t[:, ::-1], t)
        t = jnp.where(dp % 2 == 1, t[:, :, ::-1], t)
        return t

    def to_rel(v):
        return relative(v).transpose(0, 2, 1, 3).reshape(v.shape)

    def from_rel(v):
        return relative(v.reshape(v.shape[0], 2, 2, -1).transpose(0, 2, 1, 3).reshape(v.shape)).reshape(v.shape)

    def local(x, w_gate, w_up, w_down, dy):
        nr, d = x.shape
        kd, kf = w_gate.shape
        xr, dyr = to_rel(x), to_rel(dy)
        xa, dya, wg, wu, wd = gather(xr, dyr, w_gate, w_up, w_down)

        def front(xs, dys):
            a = dot(xs, wg)
            b = dot(xs, wu)
            g = dot(dys, wd.T)
            sig = jax.nn.sigmoid(a)
            sa = a * sig
            h = (sa * b).astype(bf)
            da = (g * b * sig * (1.0 + a * (1.0 - sig))).astype(bf)
            db = (g * sa).astype(bf)
            return h, da, db

        def back(h, da, db):
            return dot(h, wd), dot(da, wg.T) + dot(db, wu.T)

        h1, da1, db1 = front(xa[1], dya[1])
        y, dx = back(h1, da1, db1)
        y, dx = pz(y), pz(dx)
        xs = jnp.concatenate([xa[1:], xa[:1]]).reshape(4 * nr, d)
        dys = jnp.concatenate([dya[1:], dya[:1]]).reshape(4 * nr, d)
        h3, da3, db3 = front(xs[nr:], dys[nr:])
        h = jnp.concatenate([h1, h3])
        da = jnp.concatenate([da1, da3])
        db = jnp.concatenate([db1, db3])
        for s in range(3):
            o = slice(s * nr, (s + 1) * nr)
            oy, odx = back(h3[o], da3[o], db3[o])
            y = y + oy
            dx = dx + odx
            if s < 2:
                y, dx = pz(y), pz(dx)
        y = from_rel((xr.astype(f32) + y).astype(bf))
        dx = from_rel((dyr.astype(f32) + dx).astype(bf))

        def reduce_dw(far, near, half):
            s = near + pc(far)
            m = s.shape[1] // 2
            a, b = s[:, :m], s[:, m:]
            sa = a[0] + px(a[1])
            sb = b[:, :, 0] + py(b[:, :, 1])
            ra = sa[:, 0] + py(sa[:, 1])
            rb = sb[0] + px(sb[1])
            return jnp.concatenate([ra, rb])

        hd = 2 * kd
        def dw_cols(t, v):
            far = dot(t[:, hd:].T, v).reshape(2, kd, 2, kf)
            near = dot(t[:, :hd].T, v).reshape(2, kd, 2, kf)
            return reduce_dw(far, near, kd)

        dwg = dw_cols(xs, da)
        dwu = dw_cols(xs, db)
        far = dot(h.T, dys[:, hd:]).reshape(2, kf, 2, kd).transpose(2, 1, 0, 3)
        near = dot(h.T, dys[:, :hd]).reshape(2, kf, 2, kd).transpose(2, 1, 0, 3)
        dwd = reduce_dw(far, near, kf)
        return y, dx, dwg, dwu, dwd

    return jax.shard_map(local, mesh=mesh, in_specs=(rows, wsp, wsp, dsp, rows), out_specs=(rows, rows, wsp, wsp, dsp), check_vma=False)
```

```python
import jax
import jax.numpy as jnp
from jax import lax
from jax.experimental import pallas as pl
from jax.experimental.pallas import tpu as pltpu
from jax.sharding import PartitionSpec as P

MESH = pl.DeviceIdType.MESH
f32 = jnp.float32
bf = jnp.bfloat16
VMEM_LIMIT = 67043328


def mm(a, b):
    return lax.dot_general(a, b, (((1,), (0,)), ((), ())), preferred_element_type=f32)


def mmt(a, b):
    return lax.dot_general(a, b, (((1,), (1,)), ((), ())), preferred_element_type=f32)


def kernel(
    x_in, dy_in, wg_in, wu_in, wd_in,
    y_out, dx_out, dw_out, zl, far_r, near, xr1, yr1, xr2, yr2,
    wg, wu, wd, xa, dya, act, zs, zin, lt, fst, nst, cst, ost,
    gs, gr, lsem, zsend, zrecv, zload, fsend, frecv, nstore, cload, xs1, xq1, ys1, yq1, xs2, xq2, ys2, yq2, cin, osem,
):
    tp = lax.axis_index("tp")
    dp = lax.axis_index("dp")
    z, y = tp // 2, tp % 2
    x, c = dp // 2, dp % 2
    nxt = 2 * z + 1 - 5 * (z // 2)
    prv = z // 2 + 2 * (1 - z % 2)
    dev_x = {"tp": tp, "dp": 2 * (1 - x) + c}
    dev_y = {"tp": 2 * z + 1 - y, "dp": dp}
    dev_c = {"tp": tp, "dp": 2 * x + 1 - c}
    dev_n = {"tp": 2 * nxt + y, "dp": dp}
    dev_p = {"tp": 2 * prv + y, "dp": dp}

    nr, d = x_in.shape
    kd, kf = wg_in.shape
    f = 2 * kf
    hd = kd // 2

    def nat(r):
        rc, rx = r // 2, r % 2
        return 2 * (x + rx - 2 * x * rx) + c + rc - 2 * c * rc

    def ncol(r):
        return pl.ds(pl.multiple_of(nat(r) * kd, kd), kd)

    def remote(src, dst, ss, rs, dev):
        return pltpu.make_async_remote_copy(
            src_ref=src, dst_ref=dst, send_sem=ss, recv_sem=rs, device_id=dev, device_id_type=MESH
        )

    local = []
    for r in range(4):
        local.append((x_in.at[:, ncol(r)], xa.at[0, :, pl.ds(r * kd, kd)]))
        local.append((dy_in.at[:, ncol(r)], dya.at[0, :, pl.ds(r * kd, kd)]))
    own = (wg_in, wu_in, wd_in)

    def blk(k, rx, rc, ry, h=None):
        d0 = (2 * rc + rx) * kd
        if k < 2:
            ref = (wg, wu)[k]
            if h is None:
                return ref.at[pl.ds(d0, kd), pl.ds(ry * kf, kf)]
            return ref.at[pl.ds(d0 + h * hd, hd), pl.ds(ry * kf, kf)]
        if h is None:
            return wd.at[pl.ds(ry * kf, kf), pl.ds(d0, kd)]
        return wd.at[pl.ds(ry * kf + h * (kf // 2), kf // 2), pl.ds(d0, kd)]

    for k in range(3):
        local.append((own[k], blk(k, 0, 0, 0)))
    local = [pltpu.make_async_copy(s, t, lsem.at[i]) for i, (s, t) in enumerate(local)]
    for cp in local:
        cp.start()

    bar = pltpu.get_barrier_semaphore()
    for dev in (dev_x, dev_y, dev_c, dev_n, dev_p):
        pl.semaphore_signal(bar, inc=1, device_id=dev, device_id_type=MESH)
    pl.semaphore_wait(bar, 5)

    count = [0]
    sends = []

    def send(src, dst, dev):
        i = count[0]
        count[0] += 1
        cp = remote(src, dst, gs.at[i], gr.at[i], dev)
        cp.start()
        sends.append(cp)
        return cp

    zc = [[None, None] for _ in range(3)]
    xc, yc, cc = [None] * 3, [None] * 3, []
    for k in range(3):
        xc[k] = send(own[k], blk(k, 1, 0, 0), dev_x)
        yc[k] = send(own[k], blk(k, 0, 0, 1), dev_y)
        cc.append(send(own[k], blk(k, 0, 1, 0), dev_c))
    for cp in local[:8]:
        cp.wait()
    zc[0][0] = send(xa.at[0], xa.at[1], dev_n)
    zc[0][1] = send(dya.at[0], dya.at[1], dev_n)

    def zstep(s, j):
        ref = (xa, dya)[j]
        zc[s - 1][j].wait_recv()
        if s < 3:
            zc[s][j] = send(ref.at[s], ref.at[s + 1], dev_n)

    ra, rb = [None] * 3, [None] * 3
    for k in range(3):
        xc[k].wait_recv()
        ra[k] = send(blk(k, 1, 0, 0, 0), blk(k, 1, 0, 1, 0), dev_y)
        yc[k].wait_recv()
        rb[k] = send(blk(k, 0, 0, 1, 1), blk(k, 1, 0, 1, 1), dev_x)
        cc.append(send(blk(k, 1, 0, 0), blk(k, 1, 1, 0), dev_c))
        cc.append(send(blk(k, 0, 0, 1), blk(k, 0, 1, 1), dev_c))
        zstep(*((1, 0), (1, 1), (2, 0))[k])
    for k in range(3):
        if k == 2:
            zstep(2, 1)
        ra[k].wait_recv()
        cc.append(send(blk(k, 1, 0, 1, 0), blk(k, 1, 1, 1, 0), dev_c))
        rb[k].wait_recv()
        cc.append(send(blk(k, 1, 0, 1, 1), blk(k, 1, 1, 1, 1), dev_c))
    for cp in local[8:]:
        cp.wait()
    for cp in cc:
        cp.wait_recv()

    ft = min(256, f)

    def rows(s):
        return pl.ds(s * nr, nr)

    def front(s):
        @pl.loop(0, f // ft)
        def _(i):
            col = pl.ds(pl.multiple_of(i * ft, ft), ft)
            a = mm(xa[s], wg[:, col])
            b = mm(xa[s], wu[:, col])
            g = mmt(dya[s], wd[col, :])
            sig = jax.nn.sigmoid(a)
            sa = a * sig
            act[2, rows(s), col] = (sa * b).astype(bf)
            act[0, rows(s), col] = (g * b * sig * (1.0 + a * (1.0 - sig))).astype(bf)
            act[1, rows(s), col] = (g * sa).astype(bf)

    def back_y(s, r):
        return mm(act[2, rows(s), :], wd[:, pl.ds(pl.multiple_of(r * kd, kd), kd)])

    def back_dx(s, r):
        row = pl.ds(pl.multiple_of(r * kd, kd), kd)
        return mmt(act[0, rows(s), :], wg[row, :]) + mmt(act[1, rows(s), :], wu[row, :])

    def zcopy(step, i):
        return remote(zs.at[i], zl.at[step, i], zsend.at[i], zrecv.at[step, i], dev_n)

    def zinload(step, i):
        return pltpu.make_async_copy(zl.at[step, i], zin.at[i % 2], zload.at[i % 2])

    def zpart(s, kind):
        calc = (back_y, back_dx)[kind]

        @pl.loop(0, 4)
        def _(r):
            i = 4 * kind + r
            if s > 1:
                zcopy(s - 2, i).wait_recv()
                zinload(s - 2, i).start()
            v = calc(s, r)
            if s > 1:
                zinload(s - 2, i).wait()
                v = v + zin[i % 2]
                zcopy(s - 2, i).wait_send()
            zs[i] = v

            @pl.when(r > 0)
            def _():
                zcopy(s - 1, i - 1).start()

    def zlast(s, kind):
        zcopy(s - 1, 4 * kind + 3).start()

    def zend(kind):
        calc = (back_y, back_dx)[kind]
        src, out = ((xa, y_out), (dya, dx_out))[kind]

        def store(r):
            return pltpu.make_async_copy(ost.at[r % 2], out.at[:, ncol(r)], osem.at[r % 2])

        @pl.loop(0, 4)
        def _(r):
            i = 4 * kind + r
            v = calc(0, r)
            zcopy(2, i).wait_recv()
            zinload(2, i).start()
            v = v + src[0, :, pl.ds(pl.multiple_of(r * kd, kd), kd)].astype(f32)
            zinload(2, i).wait()

            @pl.when(r > 1)
            def _():
                store(r).wait()

            ost[r % 2] = (v + zin[i % 2]).astype(bf)
            store(r).start()

        store(2).wait()
        store(3).wait()

    def transpose(rc, rx):
        c0 = (2 * rc + rx) * kd
        for l, ref in ((0, xa), (1, dya)):
            for s in range(4):
                lt[l, :, rows(s)] = ref[s, :, pl.ds(c0, kd)].T

    def unit(j):
        ryi, k, half = j // 6, (j // 2) % 3, j % 2
        a = lt[k // 2, pl.ds(pl.multiple_of(half * hd, hd), hd), :]
        b = act[k, :, pl.ds(pl.multiple_of((1 - ryi) * kf, kf), kf)]
        return mm(a, b)

    def fcopy(u):
        return remote(fst.at[u % 2], far_r.at[u], fsend.at[u % 2], frecv.at[u], dev_c)

    def far(rx):
        base = 12 * (1 - rx)
        transpose(1, rx)

        @pl.loop(0, 12)
        def _(j):
            u = base + j
            v = unit(j)

            @pl.when(u > 1)
            def _():
                fcopy(u).wait_send()

            fst[u % 2] = v

            @pl.when(j > 0)
            def _():
                fcopy(u - 1).start()

        fcopy(base + 11).start()

    def ncopy(u):
        return pltpu.make_async_copy(nst.at[u % 2], near.at[u], nstore.at[u % 2])

    def xcopy1(i, u):
        return remote(near.at[u], xr1.at[i], xs1.at[i], xq1.at[i], dev_x)

    def ycopy1(i, u):
        return remote(near.at[u], yr1.at[i], ys1.at[i], yq1.at[i], dev_y)

    def nsend(rx, j):
        ryi, k, half = j // 6, (j // 2) % 3, j % 2
        u = 12 * (1 - rx) + j
        if rx:
            @pl.when(half == 0)
            def _():
                xcopy1(ryi * 3 + k, u).start()

        @pl.when((half == 1) & (ryi == 0))
        def _():
            ycopy1(3 * (1 - rx) + k, u).start()

    def nearg(rx):
        base = 12 * (1 - rx)
        transpose(0, rx)

        @pl.loop(0, 12)
        def _(j):
            u = base + j
            fcopy(u).wait_recv()
            cp = pltpu.make_async_copy(far_r.at[u], cst, cload)
            cp.start()
            v = unit(j)
            cp.wait()
            nst[u % 2] = v + cst[...]

            @pl.when(j > 0)
            def _():
                ncopy(u - 1).wait()
                nsend(rx, j - 1)

            ncopy(u).start()

        ncopy(base + 11).wait()
        nsend(rx, 11)

    def gather_sum(srcs, dst):
        bufs = (fst.at[0], fst.at[1], cst)
        cps = [pltpu.make_async_copy(s, b, cin.at[i]) for i, (s, b) in enumerate(zip(srcs, bufs))]
        for cp in cps:
            cp.start()
        for cp in cps:
            cp.wait()

        st = min(64, hd)

        @pl.loop(0, hd // st)
        def _(i):
            row = pl.ds(pl.multiple_of(i * st, st), st)
            v = fst[0, row, :] + fst[1, row, :]
            if len(srcs) == 3:
                v = v + cst[row, :]
            nst[0, row, :] = v

        cp = pltpu.make_async_copy(nst.at[0], dst, nstore.at[0])
        cp.start()
        cp.wait()

    def uid(rx, ry, k, half):
        return 12 * (1 - rx) + 6 * (1 - ry) + 2 * k + half

    def second(k):
        ua, ub = uid(0, 1, k, 0), uid(1, 0, k, 1)
        xcopy1(k, 0).wait_recv()
        gather_sum((near.at[ua], xr1.at[k]), near.at[ua])
        ca = remote(near.at[ua], yr2.at[k], ys2.at[k], yq2.at[k], dev_y)
        ca.start()
        ycopy1(k, 0).wait_recv()
        gather_sum((near.at[ub], yr1.at[k]), near.at[ub])
        cb = remote(near.at[ub], xr2.at[k], xs2.at[k], xq2.at[k], dev_x)
        cb.start()
        return ca, cb

    def last(k, ca, cb):
        xcopy1(3 + k, 0).wait_recv()
        ca.wait_recv()
        gather_sum((near.at[uid(0, 0, k, 0)], xr1.at[3 + k], yr2.at[k]), dw_out.at[k, pl.ds(0, hd)])
        ycopy1(3 + k, 0).wait_recv()
        cb.wait_recv()
        gather_sum((near.at[uid(0, 0, k, 1)], yr1.at[3 + k], xr2.at[k]), dw_out.at[k, pl.ds(hd, hd)])

    front(1)
    zpart(1, 0)
    zlast(1, 0)
    zpart(1, 1)
    zlast(1, 1)
    front(0)
    front(2)
    zstep(3, 0)
    zstep(3, 1)
    front(3)
    far(1)
    nearg(1)
    far(0)
    nearg(0)
    fcopy(0).wait_send()
    fcopy(1).wait_send()
    zpart(2, 0)
    zlast(2, 0)
    zpart(2, 1)
    zlast(2, 1)
    pairs = [second(k) for k in range(3)]
    zpart(3, 0)
    zlast(3, 0)
    zpart(3, 1)
    zlast(3, 1)
    zend(0)
    for k in range(3):
        last(k, *pairs[k])
    zend(1)

    for cp in sends:
        cp.wait_send()
    for i in range(8):
        zcopy(2, i).wait_send()
    for i in range(6):
        xcopy1(i, 0).wait_send()
        ycopy1(i, 0).wait_send()
    for ca, cb in pairs:
        ca.wait_send()
        cb.wait_send()


def fused(x, dy, wg, wu, wd):
    nr, d = x.shape
    kd, kf = wg.shape
    f, hd = 2 * kf, kd // 2
    hbm = pl.BlockSpec(memory_space=pl.ANY)
    sds = jax.ShapeDtypeStruct
    ng = 33
    out_shape = (
        sds((nr, d), bf), sds((nr, d), bf), sds((3, kd, kf), f32),
        sds((3, 8, nr, kd), f32), sds((24, hd, kf), f32), sds((24, hd, kf), f32),
        sds((6, hd, kf), f32), sds((6, hd, kf), f32), sds((3, hd, kf), f32), sds((3, hd, kf), f32),
    )
    dma = pltpu.SemaphoreType.DMA
    return pl.pallas_call(
        kernel,
        name="fused",
        out_shape=out_shape,
        in_specs=[hbm] * 5,
        out_specs=(hbm,) * len(out_shape),
        scratch_shapes=[
            pltpu.VMEM((d, f), bf), pltpu.VMEM((d, f), bf), pltpu.VMEM((f, d), bf),
            pltpu.VMEM((4, nr, d), bf), pltpu.VMEM((4, nr, d), bf), pltpu.VMEM((3, 4 * nr, f), bf),
            pltpu.VMEM((8, nr, kd), f32), pltpu.VMEM((2, nr, kd), f32), pltpu.VMEM((2, kd, 4 * nr), bf),
            pltpu.VMEM((2, hd, kf), f32), pltpu.VMEM((2, hd, kf), f32), pltpu.VMEM((hd, kf), f32),
            pltpu.VMEM((2, nr, kd), bf),
            dma((ng,)), dma((ng,)), dma((11,)), dma((8,)), dma((3, 8)), dma((2,)), dma((2,)), dma((24,)), dma((2,)), dma,
            dma((6,)), dma((6,)), dma((6,)), dma((6,)), dma((3,)), dma((3,)), dma((3,)), dma((3,)), dma((3,)), dma((2,)),
        ],
        compiler_params=pltpu.CompilerParams(collective_id=0, has_side_effects=True, vmem_limit_bytes=VMEM_LIMIT),
    )(x, dy, wg, wu, wd)


def solution(mesh):
    rows = P(("dp", "tp"), None)
    wsp = P("dp", "tp")
    dsp = P("tp", "dp")

    def local(x, w_gate, w_up, w_down, dy):
        y, dx, dw = fused(x, dy, w_gate, w_up, w_down)[:3]
        return y, dx, dw[0], dw[1], dw[2].T

    return jax.shard_map(local, mesh=mesh, in_specs=(rows, wsp, wsp, dsp, rows), out_specs=(rows, rows, wsp, wsp, dsp), check_vma=False)
```

```python
import jax
import jax.numpy as jnp
from jax import lax
from jax.experimental import pallas as pl
from jax.experimental.pallas import tpu as pltpu
from jax.sharding import PartitionSpec as P

MESH = pl.DeviceIdType.MESH
f32 = jnp.float32
bf = jnp.bfloat16
VMEM_LIMIT = 67043328
sc = jax.named_scope
LAG = 2


def mm(a, b):
    return lax.dot_general(a, b, (((1,), (0,)), ((), ())), preferred_element_type=f32)


def mmt(a, b):
    return lax.dot_general(a, b, (((1,), (1,)), ((), ())), preferred_element_type=f32)


def kernel(
    x_in, dy_in, wg_in, wu_in, wd_in,
    y_out, dx_out, n00, r2, zl, far_r, near, xr1, yr1,
    wg, wu, wd, xa, dya, act, zs, zin, lt, eye, fst, nst, cst, ost,
    gs, gr, lsem, zsend, zrecv, zload, fsend, frecv, nstore, cload, xs1, xq1, ys1, yq1, s2, q2, cin, osem,
):
    tp = lax.axis_index("tp")
    dp = lax.axis_index("dp")
    z, y = tp // 2, tp % 2
    x, c = dp // 2, dp % 2
    is_end = (z == 0) | (z == 3)
    is_mid = (z == 1) | (z == 2)
    dev_x = {"tp": tp, "dp": 2 * (1 - x) + c}
    dev_y = {"tp": 2 * z + 1 - y, "dp": dp}
    dev_c = {"tp": tp, "dp": 2 * x + 1 - c}
    dev_a = {"tp": 2 * (z + 1 - 2 * (z % 2)) + y, "dp": dp}
    dev_b = {"tp": 2 * (3 - z) + y, "dp": dp}

    nr, d = x_in.shape
    kd, kf = wg_in.shape
    f = 2 * kf
    hd = kd // 2
    hf = kf // 2

    def end(fn):
        pl.when(is_end)(fn)

    def mid(fn):
        pl.when(is_mid)(fn)

    def nat(r):
        rc, rx = r // 2, r % 2
        return 2 * (x + rx - 2 * x * rx) + c + rc - 2 * c * rc

    def ncol(r):
        return pl.ds(pl.multiple_of(nat(r) * kd, kd), kd)

    def remote(src, dst, ss, rs, dev):
        return pltpu.make_async_remote_copy(
            src_ref=src, dst_ref=dst, send_sem=ss, recv_sem=rs, device_id=dev, device_id_type=MESH
        )

    own = (wg_in, wu_in, wd_in)

    def blk(k, rx, rc, ry, h=None):
        d0 = (2 * rc + rx) * kd
        if k < 2:
            ref = (wg, wu)[k]
            if h is None:
                return ref.at[pl.ds(d0, kd), pl.ds(ry * kf, kf)]
            return ref.at[pl.ds(d0 + h * hd, hd), pl.ds(ry * kf, kf)]
        if h is None:
            return wd.at[pl.ds(ry * kf, kf), pl.ds(d0, kd)]
        return wd.at[pl.ds(ry * kf + h * hf, hf), pl.ds(d0, kd)]

    local = []
    for r in range(4):
        local.append((x_in.at[:, ncol(r)], xa.at[0, :, pl.ds(r * kd, kd)]))
    for r in range(4):
        local.append((dy_in.at[:, ncol(r)], dya.at[0, :, pl.ds(r * kd, kd)]))
    for k in range(3):
        local.append((own[k], blk(k, 0, 0, 0)))
    local = [pltpu.make_async_copy(s, t, lsem.at[i]) for i, (s, t) in enumerate(local)]
    for cp in local:
        cp.start()

    bar = pltpu.get_barrier_semaphore()
    for dev in (dev_x, dev_y, dev_c, dev_a, dev_b):
        pl.semaphore_signal(bar, inc=1, device_id=dev, device_id_type=MESH)

    with sc("barrier"):
        pl.semaphore_wait(bar, 5)

    def wcopy(i, src, dst, dev):
        return remote(src, dst, gs.at[i], gr.at[i], dev)

    xo = [wcopy(k, own[k], blk(k, 1, 0, 0), dev_x) for k in range(2)]
    yo = [wcopy(2 + k, own[k], blk(k, 0, 0, 1), dev_y) for k in range(2)]
    co = [wcopy(4 + k, own[k], blk(k, 0, 1, 0), dev_c) for k in range(3)]

    def dhalf(h):
        return wd_in.at[pl.ds(h * hf, hf), :]

    xd = [wcopy(7 + h, dhalf(h), blk(2, 1, 0, 0, h), dev_x) for h in range(2)]
    yd = [wcopy(9 + h, dhalf(h), blk(2, 0, 0, 1, h), dev_y) for h in range(2)]
    ra = [wcopy(11 + k, blk(k, 1, 0, 0, 0), blk(k, 1, 0, 1, 0), dev_y) for k in range(3)]
    rb = [wcopy(14 + k, blk(k, 0, 0, 1, 1), blk(k, 1, 0, 1, 1), dev_x) for k in range(3)]
    cx = [wcopy(17 + k, blk(k, 1, 0, 0), blk(k, 1, 1, 0), dev_c) for k in range(2)]
    cy = [wcopy(19 + k, blk(k, 0, 0, 1), blk(k, 0, 1, 1), dev_c) for k in range(2)]
    cxd = [wcopy(21 + h, blk(2, 1, 0, 0, h), blk(2, 1, 1, 0, h), dev_c) for h in range(2)]
    cyd = [wcopy(23 + h, blk(2, 0, 0, 1, h), blk(2, 0, 1, 1, h), dev_c) for h in range(2)]
    cra = [wcopy(25 + k, blk(k, 1, 0, 1, 0), blk(k, 1, 1, 1, 0), dev_c) for k in range(3)]
    crb = [wcopy(28 + k, blk(k, 1, 0, 1, 1), blk(k, 1, 1, 1, 1), dev_c) for k in range(3)]
    nw = 31

    rows_ = (xa, dya)

    def acopy(src, dst, j):
        return remote(
            rows_[j].at[src], rows_[j].at[dst], gs.at[nw + 2 * dst + j], gr.at[nw + 2 * dst + j], dev_a
        )

    def bcopy(src, dst, j):
        return remote(
            rows_[j].at[src], rows_[j].at[dst], gs.at[nw + 8 + 2 * dst + j], gr.at[nw + 2 * dst + j], dev_b
        )

    def got(s, j):
        acopy(s, s, j).wait_recv()

    for k in range(2):
        xo[k].start()
        yo[k].start()
    with sc("rows_in"):
        for cp in local[:8]:
            cp.wait()
    for j in range(2):
        acopy(0, 1, j).start()

    @mid
    def _():
        for j in range(2):
            bcopy(0, 2, j).start()

    for k in range(3):
        co[k].start()

    def pass_on(s, j):
        with sc(f"rows{s}_{j}"):
            got(s, j)
        if s == 1:
            bcopy(1, 3, j).start()
        else:
            acopy(s, s, j).start()

    for k in range(2):
        with sc(f"gx{k}"):
            xo[k].wait_recv()
        ra[k].start()
        cx[k].start()
        with sc(f"gy{k}"):
            yo[k].wait_recv()
        rb[k].start()
        cy[k].start()
        if k == 1:
            xd[0].start()
            yd[1].start()
            xd[1].start()
            yd[0].start()

        @mid
        def _():
            pass_on(1, k)
            pass_on(2, k)

    for k in range(2):
        with sc(f"gr{k}"):
            ra[k].wait_recv()
            cra[k].start()
            rb[k].wait_recv()
            crb[k].start()
    for cp in local[8:]:
        cp.wait()
    with sc("gc01"):
        for cp in (*co[:2], *cx, *cy, *cra[:2], *crb[:2]):
            cp.wait_recv()

    ft = min(256, f)

    def rows(s):
        return pl.ds(s * nr, nr)

    def front_h(s):
        @pl.loop(0, f // ft)
        def _(i):
            col = pl.ds(pl.multiple_of(i * ft, ft), ft)
            a = mm(xa[s], wg[:, col])
            b = mm(xa[s], wu[:, col])
            act[2, rows(s), col] = (a * jax.nn.sigmoid(a) * b).astype(bf)

    def front(s):
        @pl.loop(0, f // ft)
        def _(i):
            col = pl.ds(pl.multiple_of(i * ft, ft), ft)
            a = mm(xa[s], wg[:, col])
            b = mm(xa[s], wu[:, col])
            g = mmt(dya[s], wd[col, :])
            sig = jax.nn.sigmoid(a)
            sa = a * sig
            act[2, rows(s), col] = (sa * b).astype(bf)
            act[0, rows(s), col] = (g * b * sig * (1.0 + a * (1.0 - sig))).astype(bf)
            act[1, rows(s), col] = (g * sa).astype(bf)

    def back(kind, s, r):
        col = pl.ds(pl.multiple_of(r * kd, kd), kd)
        if kind == 0:
            return mm(act[2, rows(s), :], wd[:, col])
        return mmt(act[0, rows(s), :], wg[col, :]) + mmt(act[1, rows(s), :], wu[col, :])

    def zcopy(q, kind, r, half, dev):
        i = 4 * kind + r
        return remote(zs.at[4 * half + r], zl.at[q, i], zsend.at[4 * half + r], zrecv.at[q, i], dev)

    def zload_(q, kind, r, slot):
        return pltpu.make_async_copy(zl.at[q, 4 * kind + r], zin.at[slot], zload.at[slot])

    def chunk(kind, s, r, half, q_add, first):
        if q_add is not None:
            with sc("zrecv"):
                zcopy(q_add, kind, r, half, dev_a).wait_recv()
            zload_(q_add, kind, r, r % 2).start()
        v = back(kind, s, r)
        if q_add is not None:
            zload_(q_add, kind, r, r % 2).wait()
            v = v + zin[r % 2]
        if not first:
            with sc("zsend"):
                zcopy(0, kind, r, half, dev_a).wait_send()
        zs[4 * half + r] = v

    def job(kind, s, half, q_add, q_dst, dev, first=False):
        with sc(f"job{kind}_{s}"):
            @pl.loop(0, 4)
            def _(r):
                chunk(kind, s, r, half, q_add, first)

                @pl.when(r > 0)
                def _():
                    zcopy(q_dst, kind, r - 1, half, dev).start()

        zcopy(q_dst, kind, 3, half, dev).start()

    def finish(kind, adds):
        src, out = ((x_in, y_out), (dy_in, dx_out))[kind]
        res = (xa, dya)[kind]

        def store(r):
            return pltpu.make_async_copy(ost.at[r % 2], out.at[:, ncol(r)], osem.at[r % 2])

        with sc(f"fin{kind}"):
            @pl.loop(0, 4)
            def _(r):
                v = back(kind, 0, r)
                v = v + res[0, :, pl.ds(pl.multiple_of(r * kd, kd), kd)].astype(f32)
                for n, q in enumerate(adds):
                    with sc("finrecv"):
                        zcopy(q, kind, r, 0, dev_a).wait_recv()
                    zload_(q, kind, r, n).start()
                for n, q in enumerate(adds):
                    zload_(q, kind, r, n).wait()
                    v = v + zin[n]

                @pl.when(r > 1)
                def _():
                    store(r).wait()

                ost[r % 2] = v.astype(bf)
                store(r).start()

            store(2).wait()
            store(3).wait()

    def transpose(rx):
        for rc in range(2):
            c0 = (2 * rc + rx) * kd
            for l, ref in ((0, xa), (1, dya)):
                for s in range(4):
                    for h in range(2):
                        v = mmt(eye[...], ref[s, :, pl.ds(c0 + h * hd, hd)])
                        lt[rc, l, pl.ds(h * hd, hd), rows(s)] = v.astype(bf)

    def unit(rc, j):
        ryi, k, half = j // 6, (j // 2) % 3, j % 2
        a = lt[rc, k // 2, pl.ds(pl.multiple_of(half * hd, hd), hd), :]
        b = act[k, :, pl.ds(pl.multiple_of((1 - ryi) * kf, kf), kf)]
        return mm(a, b)

    def fcopy(u):
        return remote(fst.at[u % 2], far_r.at[u], fsend.at[u % 2], frecv.at[u], dev_c)

    def ncopy(u):
        return pltpu.make_async_copy(nst.at[u % 2], near.at[u], nstore.at[u % 2])

    def ccopy(u):
        return pltpu.make_async_copy(far_r.at[u], cst.at[u % 2], cload.at[u % 2])

    def xcopy1(i, u):
        return remote(near.at[u], xr1.at[i], xs1.at[i], xq1.at[i], dev_x)

    def ycopy1(i, u):
        return remote(near.at[u], yr1.at[i], ys1.at[i], yq1.at[i], dev_y)

    def nsend(rx, j):
        ryi, k, half = j // 6, (j // 2) % 3, j % 2
        u = 12 * (1 - rx) + j
        if rx:
            @pl.when(half == 0)
            def _():
                xcopy1(ryi * 3 + k, u).start()

        @pl.when((half == 1) & (ryi == 0))
        def _():
            ycopy1(3 * (1 - rx) + k, u).start()

    def dw(rx):
        base = 12 * (1 - rx)
        with sc(f"tr{rx}"):
            transpose(rx)

        with sc(f"dw{rx}"):
            @pl.loop(0, 12 + LAG)
            def _(j):
                u = base + j
                w = u - LAG

                @pl.when(j >= LAG)
                def _():
                    with sc("frecv"):
                        fcopy(w).wait_recv()
                    ccopy(w).start()

                @pl.when(j < 12)
                def _():
                    v = unit(1, j)

                    @pl.when(u > 1)
                    def _():
                        fcopy(u).wait_send()

                    fst[u % 2] = v

                @pl.when((j > 0) & (j < 13))
                def _():
                    fcopy(u - 1).start()

                @pl.when(j >= LAG)
                def _():
                    v = unit(0, j - LAG)
                    ccopy(w).wait()
                    nst[w % 2] = v + cst[w % 2]

                    @pl.when(j > LAG)
                    def _():
                        ncopy(w - 1).wait()
                        nsend(rx, j - LAG - 1)

                    ncopy(w).start()

            ncopy(base + 11).wait()
            nsend(rx, 11)

    def add_units(a, b, dst):
        ca = pltpu.make_async_copy(a, fst.at[0], cin.at[0])
        cb = pltpu.make_async_copy(b, fst.at[1], cin.at[1])
        ca.start()
        cb.start()
        ca.wait()
        cb.wait()
        st = min(64, hd)

        @pl.loop(0, hd // st)
        def _(i):
            row = pl.ds(pl.multiple_of(i * st, st), st)
            nst[0, row, :] = fst[0, row, :] + fst[1, row, :]

        cp = pltpu.make_async_copy(nst.at[0], dst, nstore.at[0])
        cp.start()
        cp.wait()

    def uid(rx, ry, k, half):
        return 12 * (1 - rx) + 6 * (1 - ry) + 2 * k + half

    def ycopy2(k):
        return remote(near.at[uid(0, 1, k, 0)], r2.at[2 * k], s2.at[2 * k], q2.at[2 * k], dev_y)

    def xcopy2(k):
        return remote(near.at[uid(1, 0, k, 1)], r2.at[2 * k + 1], s2.at[2 * k + 1], q2.at[2 * k + 1], dev_x)

    def second(k):
        with sc(f"second{k}"):
            ua, ub = uid(0, 1, k, 0), uid(1, 0, k, 1)
            xcopy1(k, 0).wait_recv()
            add_units(near.at[ua], xr1.at[k], near.at[ua])
            ycopy2(k).start()
            ycopy1(k, 0).wait_recv()
            add_units(near.at[ub], yr1.at[k], near.at[ub])
            xcopy2(k).start()

    def third(k):
        with sc(f"third{k}"):
            xcopy1(3 + k, 0).wait_recv()
            add_units(near.at[uid(0, 0, k, 0)], xr1.at[3 + k], n00.at[2 * k])
            ycopy1(3 + k, 0).wait_recv()
            add_units(near.at[uid(0, 0, k, 1)], yr1.at[3 + k], n00.at[2 * k + 1])

    eye[...] = (
        lax.broadcasted_iota(jnp.int32, (hd, hd), 0) == lax.broadcasted_iota(jnp.int32, (hd, hd), 1)
    ).astype(f32).astype(bf)

    @end
    def _():
        with sc("e_rows1"):
            got(1, 0)
        with sc("front_h1"):
            front_h(1)

    with sc("gd0"):
        xd[0].wait_recv()
        ra[2].start()
        cxd[0].start()
        yd[1].wait_recv()
        rb[2].start()
        cyd[1].start()

    @end
    def _():
        with sc("e_rows2"):
            got(2, 0)
        with sc("front_h2"):
            front_h(2)

    with sc("gd1"):
        yd[0].wait_recv()
        cyd[0].start()
        xd[1].wait_recv()
        cxd[1].start()

    @mid
    def _():
        pass_on(3, 0)

    def early(r):
        chunk(0, 1, r, 0, None, True)

    def early_send(r):
        zcopy(0, 0, r, 0, dev_a).start()

    @end
    def _():
        early(0)

    with sc("gc2a"):
        co[2].wait_recv()
        cyd[0].wait_recv()
        cyd[1].wait_recv()

    @end
    def _():
        early(2)
        early_send(0)

    with sc("gr2"):
        ra[2].wait_recv()
        cra[2].start()
        rb[2].wait_recv()
        crb[2].start()

    @mid
    def _():
        pass_on(3, 1)

    @end
    def _():
        early_send(2)
        early(1)

    with sc("gc2b"):
        for cp in (*cxd, cra[2], crb[2]):
            cp.wait_recv()

    @end
    def _():
        early(3)
        early_send(1)
        job(0, 2, 1, None, 1, dev_a, True)
        early_send(3)
        got(1, 1)
        got(2, 1)

    with sc("front1"):
        front(1)
    with sc("front0"):
        front(0)
    with sc("front2"):
        front(2)

    @end
    def _():
        with sc("e_rows3"):
            got(3, 0)
            got(3, 1)

    with sc("front3"):
        front(3)

    @end
    def _():
        job(0, 3, 0, None, 2, dev_a)

    dw(1)
    dw(0)
    fcopy(0).wait_send()
    fcopy(1).wait_send()

    @end
    def _():
        job(1, 3, 1, None, 2, dev_a)

    @mid
    def _():
        job(0, 2, 0, 1, 3, dev_b, True)

    for k in range(3):
        second(k)

    @end
    def _():
        job(1, 2, 0, None, 1, dev_a)

    @mid
    def _():
        job(0, 3, 1, 2, 4, dev_b, True)
        job(0, 1, 0, 4, 0, dev_a)

    third(0)
    third(1)

    @end
    def _():
        job(1, 1, 1, None, 0, dev_a)

    @mid
    def _():
        job(1, 3, 1, 2, 4, dev_b)

    third(2)

    @end
    def _():
        finish(0, (0,))
        finish(1, (0,))

    @mid
    def _():
        job(1, 1, 0, 4, 0, dev_a)
        finish(0, (0, 3))
        job(1, 2, 1, 1, 3, dev_b)
        finish(1, (0, 3))

    with sc("drain"):
        for k in range(3):
            ycopy2(k).wait_recv()
            xcopy2(k).wait_recv()
        for cp in (*xo, *yo, *co, *xd, *yd, *ra, *rb, *cx, *cy, *cxd, *cyd, *cra, *crb):
            cp.wait_send()
        for j in range(2):
            acopy(0, 1, j).wait_send()

        @mid
        def _():
            for j in range(2):
                bcopy(0, 2, j).wait_send()
                bcopy(1, 3, j).wait_send()
                acopy(2, 2, j).wait_send()
                acopy(3, 3, j).wait_send()

        for half in range(2):
            for r in range(4):
                zcopy(0, 0, r, half, dev_a).wait_send()
        for i in range(6):
            xcopy1(i, 0).wait_send()
            ycopy1(i, 0).wait_send()
        for k in range(3):
            ycopy2(k).wait_send()
            xcopy2(k).wait_send()


def fused(x, dy, wg, wu, wd):
    nr, d = x.shape
    kd, kf = wg.shape
    f, hd = 2 * kf, kd // 2
    hbm = pl.BlockSpec(memory_space=pl.ANY)
    sds = jax.ShapeDtypeStruct
    out_shape = (
        sds((nr, d), bf), sds((nr, d), bf), sds((6, hd, kf), f32), sds((6, hd, kf), f32),
        sds((5, 8, nr, kd), f32), sds((24, hd, kf), f32), sds((24, hd, kf), f32),
        sds((6, hd, kf), f32), sds((6, hd, kf), f32),
    )
    dma = pltpu.SemaphoreType.DMA
    return pl.pallas_call(
        kernel,
        name="fused",
        out_shape=out_shape,
        in_specs=[hbm] * 5,
        out_specs=(hbm,) * len(out_shape),
        scratch_shapes=[
            pltpu.VMEM((d, f), bf), pltpu.VMEM((d, f), bf), pltpu.VMEM((f, d), bf),
            pltpu.VMEM((4, nr, d), bf), pltpu.VMEM((4, nr, d), bf), pltpu.VMEM((3, 4 * nr, f), bf),
            pltpu.VMEM((8, nr, kd), f32), pltpu.VMEM((2, nr, kd), f32), pltpu.VMEM((2, 2, kd, 4 * nr), bf),
            pltpu.VMEM((hd, hd), bf),
            pltpu.VMEM((2, hd, kf), f32), pltpu.VMEM((2, hd, kf), f32), pltpu.VMEM((2, hd, kf), f32),
            pltpu.VMEM((2, nr, kd), bf),
            dma((47,)), dma((39,)), dma((11,)), dma((8,)), dma((5, 8)), dma((2,)), dma((2,)), dma((24,)), dma((2,)),
            dma((2,)), dma((6,)), dma((6,)), dma((6,)), dma((6,)), dma((6,)), dma((6,)), dma((2,)), dma((2,)),
        ],
        compiler_params=pltpu.CompilerParams(collective_id=0, has_side_effects=True, vmem_limit_bytes=VMEM_LIMIT),
    )(x, dy, wg, wu, wd)


def solution(mesh):
    rows = P(("dp", "tp"), None)
    wsp = P("dp", "tp")
    dsp = P("tp", "dp")

    def local(x, w_gate, w_up, w_down, dy):
        y, dx, a, b = fused(x, dy, w_gate, w_up, w_down)[:4]
        kd, kf = w_gate.shape

        def dw(k):
            return (a[2 * k : 2 * k + 2] + b[2 * k : 2 * k + 2]).reshape(kd, kf)

        return y, dx, dw(0), dw(1), dw(2).T

    return jax.shard_map(local, mesh=mesh, in_specs=(rows, wsp, wsp, dsp, rows), out_specs=(rows, rows, wsp, wsp, dsp), check_vma=False)
```

```python
import jax
import jax.numpy as jnp
from jax import lax
from jax.experimental import pallas as pl
from jax.experimental.pallas import tpu as pltpu
from jax.sharding import PartitionSpec as P

MESH = pl.DeviceIdType.MESH
f32 = jnp.float32
bf = jnp.bfloat16
VMEM_LIMIT = 67043328
sc = jax.named_scope
LAG = 4


def mm(a, b):
    return lax.dot_general(a, b, (((1,), (0,)), ((), ())), preferred_element_type=f32)


def mmt(a, b):
    return lax.dot_general(a, b, (((1,), (1,)), ((), ())), preferred_element_type=f32)


def kernel(
    x_in, dy_in, wg_in, wu_in, wd_in,
    y_out, dx_out, dwg_out, dwu_out, dwd_out, n00, r2, zl, far_r, near, xr1, yr1,
    wg, wu, wd, xa, dya, act, zs, zin, lt, eye, fst, nst, cst, ost,
    gs, gr, lsem, zsend, zrecv, zload, fsend, frecv, nstore, cload, xs1, xq1, ys1, yq1, s2, q2, cin, osem,
):
    tp = lax.axis_index("tp")
    dp = lax.axis_index("dp")
    z, y = tp // 2, tp % 2
    x, c = dp // 2, dp % 2
    is_end = (z == 0) | (z == 3)
    is_mid = (z == 1) | (z == 2)
    dev_x = {"tp": tp, "dp": 2 * (1 - x) + c}
    dev_y = {"tp": 2 * z + 1 - y, "dp": dp}
    dev_c = {"tp": tp, "dp": 2 * x + 1 - c}
    dev_a = {"tp": 2 * (z + 1 - 2 * (z % 2)) + y, "dp": dp}
    dev_b = {"tp": 2 * (3 - z) + y, "dp": dp}

    nr, d = x_in.shape
    kd, kf = wg_in.shape
    f = 2 * kf
    hd = kd // 2
    hf = kf // 2

    def end(fn):
        pl.when(is_end)(fn)

    def mid(fn):
        pl.when(is_mid)(fn)

    def nat(r):
        rc, rx = r // 2, r % 2
        return 2 * (x + rx - 2 * x * rx) + c + rc - 2 * c * rc

    def ncol(r):
        return pl.ds(pl.multiple_of(nat(r) * kd, kd), kd)

    def remote(src, dst, ss, rs, dev):
        return pltpu.make_async_remote_copy(
            src_ref=src, dst_ref=dst, send_sem=ss, recv_sem=rs, device_id=dev, device_id_type=MESH
        )

    own = (wg_in, wu_in, wd_in)

    def blk(k, rx, rc, ry, h=None):
        d0 = (2 * rc + rx) * kd
        if k < 2:
            ref = (wg, wu)[k]
            if h is None:
                return ref.at[pl.ds(d0, kd), pl.ds(ry * kf, kf)]
            return ref.at[pl.ds(d0 + h * hd, hd), pl.ds(ry * kf, kf)]
        if h is None:
            return wd.at[pl.ds(ry * kf, kf), pl.ds(d0, kd)]
        return wd.at[pl.ds(ry * kf + h * hf, hf), pl.ds(d0, kd)]

    local = []
    for r in range(4):
        local.append((x_in.at[:, ncol(r)], xa.at[0, :, pl.ds(r * kd, kd)]))
    for r in range(4):
        local.append((dy_in.at[:, ncol(r)], dya.at[0, :, pl.ds(r * kd, kd)]))
    for k in range(3):
        local.append((own[k], blk(k, 0, 0, 0)))
    local = [pltpu.make_async_copy(s, t, lsem.at[i]) for i, (s, t) in enumerate(local)]
    for cp in local:
        cp.start()

    bar = pltpu.get_barrier_semaphore()
    for dev in (dev_x, dev_y, dev_c, dev_a, dev_b):
        pl.semaphore_signal(bar, inc=1, device_id=dev, device_id_type=MESH)

    with sc("barrier"):
        pl.semaphore_wait(bar, 5)

    def wcopy(i, src, dst, dev):
        return remote(src, dst, gs.at[i], gr.at[i], dev)

    xo = [wcopy(k, own[k], blk(k, 1, 0, 0), dev_x) for k in range(2)]
    yo = [wcopy(2 + k, own[k], blk(k, 0, 0, 1), dev_y) for k in range(2)]
    co = [wcopy(4 + k, own[k], blk(k, 0, 1, 0), dev_c) for k in range(3)]

    def dhalf(h):
        return wd_in.at[pl.ds(h * hf, hf), :]

    xd = [wcopy(7 + h, dhalf(h), blk(2, 1, 0, 0, h), dev_x) for h in range(2)]
    yd = [wcopy(9 + h, dhalf(h), blk(2, 0, 0, 1, h), dev_y) for h in range(2)]
    ra = [wcopy(11 + k, blk(k, 1, 0, 0, 0), blk(k, 1, 0, 1, 0), dev_y) for k in range(3)]
    rb = [wcopy(14 + k, blk(k, 0, 0, 1, 1), blk(k, 1, 0, 1, 1), dev_x) for k in range(3)]
    cx = [wcopy(17 + k, blk(k, 1, 0, 0), blk(k, 1, 1, 0), dev_c) for k in range(2)]
    cy = [wcopy(19 + k, blk(k, 0, 0, 1), blk(k, 0, 1, 1), dev_c) for k in range(2)]
    cxd = [wcopy(21 + h, blk(2, 1, 0, 0, h), blk(2, 1, 1, 0, h), dev_c) for h in range(2)]
    cyd = [wcopy(23 + h, blk(2, 0, 0, 1, h), blk(2, 0, 1, 1, h), dev_c) for h in range(2)]
    cra = [wcopy(25 + k, blk(k, 1, 0, 1, 0), blk(k, 1, 1, 1, 0), dev_c) for k in range(3)]
    crb = [wcopy(28 + k, blk(k, 1, 0, 1, 1), blk(k, 1, 1, 1, 1), dev_c) for k in range(3)]
    nw = 31

    rows_ = (xa, dya)

    def acopy(src, dst, j):
        return remote(
            rows_[j].at[src], rows_[j].at[dst], gs.at[nw + 2 * dst + j], gr.at[nw + 2 * dst + j], dev_a
        )

    def bcopy(src, dst, j):
        return remote(
            rows_[j].at[src], rows_[j].at[dst], gs.at[nw + 8 + 2 * dst + j], gr.at[nw + 2 * dst + j], dev_b
        )

    def got(s, j):
        acopy(s, s, j).wait_recv()

    for k in range(2):
        xo[k].start()
        yo[k].start()
    with sc("rows_in"):
        for cp in local[:8]:
            cp.wait()
    for j in range(2):
        acopy(0, 1, j).start()

    @mid
    def _():
        for j in range(2):
            bcopy(0, 2, j).start()

    for k in range(3):
        co[k].start()

    def pass_on(s, j):
        with sc(f"rows{s}_{j}"):
            got(s, j)
        if s == 1:
            bcopy(1, 3, j).start()
        else:
            acopy(s, s, j).start()

    for k in range(2):
        with sc(f"gx{k}"):
            xo[k].wait_recv()
        ra[k].start()
        cx[k].start()
        with sc(f"gy{k}"):
            yo[k].wait_recv()
        rb[k].start()
        cy[k].start()
        if k == 1:
            xd[0].start()
            yd[1].start()
            xd[1].start()
            yd[0].start()

        @mid
        def _():
            pass_on(1, k)
            pass_on(2, k)

    for k in range(2):
        with sc(f"gr{k}"):
            ra[k].wait_recv()
            cra[k].start()
            rb[k].wait_recv()
            crb[k].start()
    for cp in local[8:]:
        cp.wait()
    with sc("gc01"):
        for cp in (*co[:2], *cx, *cy, *cra[:2], *crb[:2]):
            cp.wait_recv()

    ft = min(256, f)

    def rows(s):
        return pl.ds(s * nr, nr)

    def front_h(s):
        @pl.loop(0, f // ft)
        def _(i):
            col = pl.ds(pl.multiple_of(i * ft, ft), ft)
            a = mm(xa[s], wg[:, col])
            b = mm(xa[s], wu[:, col])
            act[2, rows(s), col] = (a * jax.nn.sigmoid(a) * b).astype(bf)

    def front(s):
        @pl.loop(0, f // ft)
        def _(i):
            col = pl.ds(pl.multiple_of(i * ft, ft), ft)
            a = mm(xa[s], wg[:, col])
            b = mm(xa[s], wu[:, col])
            g = mmt(dya[s], wd[col, :])
            sig = jax.nn.sigmoid(a)
            sa = a * sig
            act[2, rows(s), col] = (sa * b).astype(bf)
            act[0, rows(s), col] = (g * b * sig * (1.0 + a * (1.0 - sig))).astype(bf)
            act[1, rows(s), col] = (g * sa).astype(bf)

    def back(kind, s, r):
        col = pl.ds(pl.multiple_of(r * kd, kd), kd)
        if kind == 0:
            return mm(act[2, rows(s), :], wd[:, col])
        return mmt(act[0, rows(s), :], wg[col, :]) + mmt(act[1, rows(s), :], wu[col, :])

    def zcopy(q, kind, r, half, dev):
        i = 4 * kind + r
        return remote(zs.at[4 * half + r], zl.at[q, i], zsend.at[4 * half + r], zrecv.at[q, i], dev)

    def zload_(q, kind, r, slot):
        return pltpu.make_async_copy(zl.at[q, 4 * kind + r], zin.at[slot], zload.at[slot])

    def chunk(kind, s, r, half, q_add, first):
        if q_add is not None:
            with sc("zrecv"):
                zcopy(q_add, kind, r, half, dev_a).wait_recv()
            zload_(q_add, kind, r, r % 2).start()
        v = back(kind, s, r)
        if q_add is not None:
            zload_(q_add, kind, r, r % 2).wait()
            v = v + zin[r % 2]
        if not first:
            with sc("zsend"):
                zcopy(0, kind, r, half, dev_a).wait_send()
        zs[4 * half + r] = v

    def job(kind, s, half, q_add, q_dst, dev, first=False):
        with sc(f"job{kind}_{s}"):
            @pl.loop(0, 4)
            def _(r):
                chunk(kind, s, r, half, q_add, first)

                @pl.when(r > 0)
                def _():
                    zcopy(q_dst, kind, r - 1, half, dev).start()

        zcopy(q_dst, kind, 3, half, dev).start()

    def finish(kind, adds):
        src, out = ((x_in, y_out), (dy_in, dx_out))[kind]
        res = (xa, dya)[kind]

        def store(r):
            return pltpu.make_async_copy(ost.at[r % 2], out.at[:, ncol(r)], osem.at[r % 2])

        with sc(f"fin{kind}"):
            @pl.loop(0, 4)
            def _(r):
                v = back(kind, 0, r)
                v = v + res[0, :, pl.ds(pl.multiple_of(r * kd, kd), kd)].astype(f32)
                for n, q in enumerate(adds):
                    with sc("finrecv"):
                        zcopy(q, kind, r, 0, dev_a).wait_recv()
                    zload_(q, kind, r, n).start()
                for n, q in enumerate(adds):
                    zload_(q, kind, r, n).wait()
                    v = v + zin[n]

                @pl.when(r > 1)
                def _():
                    store(r).wait()

                ost[r % 2] = v.astype(bf)
                store(r).start()

            store(2).wait()
            store(3).wait()

    def transpose(rx):
        for rc in range(2):
            c0 = (2 * rc + rx) * kd
            for l, ref in ((0, xa), (1, dya)):
                for s in range(4):
                    for h in range(2):
                        v = mmt(eye[...], ref[s, :, pl.ds(c0 + h * hd, hd)])
                        lt[rc, l, pl.ds(h * hd, hd), rows(s)] = v.astype(bf)

    def unit(rc, j):
        ryi, k, half = j // 6, (j // 2) % 3, j % 2
        a = lt[rc, k // 2, pl.ds(pl.multiple_of(half * hd, hd), hd), :]
        b = act[k, :, pl.ds(pl.multiple_of((1 - ryi) * kf, kf), kf)]
        return mm(a, b)

    def fcopy(u):
        return remote(fst.at[u % 2], far_r.at[u], fsend.at[u % 2], frecv.at[u], dev_c)

    def ncopy(u):
        return pltpu.make_async_copy(nst.at[u % 2], near.at[u], nstore.at[u % 2])

    def ccopy(u):
        return pltpu.make_async_copy(far_r.at[u], cst.at[u % 2], cload.at[u % 2])

    def xcopy1(i, u):
        return remote(near.at[u], xr1.at[i], xs1.at[i], xq1.at[i], dev_x)

    def ycopy1(i, u):
        return remote(near.at[u], yr1.at[i], ys1.at[i], yq1.at[i], dev_y)

    def nsend(rx, j):
        ryi, k, half = j // 6, (j // 2) % 3, j % 2
        u = 12 * (1 - rx) + j
        if rx:
            @pl.when(half == 0)
            def _():
                xcopy1(ryi * 3 + k, u).start()

        @pl.when((half == 1) & (ryi == 0))
        def _():
            ycopy1(3 * (1 - rx) + k, u).start()

    def dw(rx):
        base = 12 * (1 - rx)
        with sc(f"tr{rx}"):
            transpose(rx)

        with sc(f"dw{rx}"):
            @pl.loop(0, 12 + LAG)
            def _(j):
                u = base + j
                w = u - LAG

                @pl.when(j >= LAG)
                def _():
                    with sc("frecv"):
                        fcopy(w).wait_recv()
                    ccopy(w).start()

                @pl.when(j < 12)
                def _():
                    v = unit(1, j)

                    @pl.when(u > 1)
                    def _():
                        fcopy(u).wait_send()

                    fst[u % 2] = v

                @pl.when((j > 0) & (j < 13))
                def _():
                    fcopy(u - 1).start()

                @pl.when(j >= LAG)
                def _():
                    v = unit(0, j - LAG)
                    ccopy(w).wait()
                    nst[w % 2] = v + cst[w % 2]

                    @pl.when(j > LAG)
                    def _():
                        ncopy(w - 1).wait()
                        nsend(rx, j - LAG - 1)

                    ncopy(w).start()

            ncopy(base + 11).wait()
            nsend(rx, 11)

    def add_units(a, b, dst):
        ca = pltpu.make_async_copy(a, fst.at[0], cin.at[0])
        cb = pltpu.make_async_copy(b, fst.at[1], cin.at[1])
        ca.start()
        cb.start()
        ca.wait()
        cb.wait()
        st = min(64, hd)

        @pl.loop(0, hd // st)
        def _(i):
            row = pl.ds(pl.multiple_of(i * st, st), st)
            nst[0, row, :] = fst[0, row, :] + fst[1, row, :]

        cp = pltpu.make_async_copy(nst.at[0], dst, nstore.at[0])
        cp.start()
        cp.wait()

    def uid(rx, ry, k, half):
        return 12 * (1 - rx) + 6 * (1 - ry) + 2 * k + half

    def ycopy2(k):
        return remote(near.at[uid(0, 1, k, 0)], r2.at[2 * k], s2.at[2 * k], q2.at[2 * k], dev_y)

    def xcopy2(k):
        return remote(near.at[uid(1, 0, k, 1)], r2.at[2 * k + 1], s2.at[2 * k + 1], q2.at[2 * k + 1], dev_x)

    def second(k):
        with sc(f"second{k}"):
            ua, ub = uid(0, 1, k, 0), uid(1, 0, k, 1)
            xcopy1(k, 0).wait_recv()
            add_units(near.at[ua], xr1.at[k], near.at[ua])
            ycopy2(k).start()
            ycopy1(k, 0).wait_recv()
            add_units(near.at[ub], yr1.at[k], near.at[ub])
            xcopy2(k).start()

    def third(k):
        with sc(f"third{k}"):
            xcopy1(3 + k, 0).wait_recv()
            add_units(near.at[uid(0, 0, k, 0)], xr1.at[3 + k], n00.at[2 * k])
            ycopy1(3 + k, 0).wait_recv()
            add_units(near.at[uid(0, 0, k, 1)], yr1.at[3 + k], n00.at[2 * k + 1])

    def fourth(k):
        out = (dwg_out, dwu_out, dwd_out)[k]
        cn = [pltpu.make_async_copy(n00.at[2 * k + h], fst.at[h], cin.at[h]) for h in range(2)]
        cr = [pltpu.make_async_copy(r2.at[2 * k + h], cst.at[h], cload.at[h]) for h in range(2)]
        co_ = [pltpu.make_async_copy(nst.at[h], out.at[pl.ds(h * hd, hd)], nstore.at[h]) for h in range(2)]
        with sc(f"fourth{k}"):
            for h in range(2):
                cn[h].start()
            for h in range(2):
                (ycopy2, xcopy2)[h](k).wait_recv()
                cr[h].start()
            st = min(64, hd)
            for h in range(2):
                cn[h].wait()
                cr[h].wait()

                @pl.loop(0, hd // st)
                def _(i):
                    row = pl.ds(pl.multiple_of(i * st, st), st)
                    nst[h, row, :] = fst[h, row, :] + cst[h, row, :]

                co_[h].start()
            for h in range(2):
                co_[h].wait()

    eye[...] = (
        lax.broadcasted_iota(jnp.int32, (hd, hd), 0) == lax.broadcasted_iota(jnp.int32, (hd, hd), 1)
    ).astype(f32).astype(bf)

    @end
    def _():
        with sc("e_rows1"):
            got(1, 0)
        with sc("front_h1"):
            front_h(1)

    with sc("gd0"):
        xd[0].wait_recv()
        ra[2].start()
        cxd[0].start()
        yd[1].wait_recv()
        rb[2].start()
        cyd[1].start()

    @end
    def _():
        with sc("e_rows2"):
            got(2, 0)
        with sc("front_h2"):
            front_h(2)

    with sc("gd1"):
        yd[0].wait_recv()
        cyd[0].start()
        xd[1].wait_recv()
        cxd[1].start()

    @mid
    def _():
        pass_on(3, 0)

    def early(r):
        chunk(0, 1, r, 0, None, True)

    def early_send(r):
        zcopy(0, 0, r, 0, dev_a).start()

    @end
    def _():
        early(0)

    with sc("gc2a"):
        co[2].wait_recv()
        cyd[0].wait_recv()
        cyd[1].wait_recv()

    @end
    def _():
        early(2)
        early_send(0)

    with sc("gr2"):
        ra[2].wait_recv()
        cra[2].start()
        rb[2].wait_recv()
        crb[2].start()

    @mid
    def _():
        pass_on(3, 1)

    @end
    def _():
        early_send(2)
        early(1)

    with sc("gc2b"):
        for cp in (*cxd, cra[2], crb[2]):
            cp.wait_recv()

    @end
    def _():
        early(3)
        early_send(1)
        got(1, 1)
        got(2, 1)
        early_send(3)
        job(0, 2, 1, None, 1, dev_a, True)

    with sc("front1"):
        front(1)
    with sc("front0"):
        front(0)
    with sc("front2"):
        front(2)

    @end
    def _():
        with sc("e_rows3"):
            got(3, 0)
            got(3, 1)

    with sc("front3"):
        front(3)

    @end
    def _():
        job(0, 3, 0, None, 2, dev_a)

    dw(1)
    dw(0)
    fcopy(0).wait_send()
    fcopy(1).wait_send()

    @end
    def _():
        job(1, 3, 1, None, 2, dev_a)

    @mid
    def _():
        job(0, 2, 0, 1, 3, dev_b, True)

    for k in range(3):
        second(k)

    @end
    def _():
        job(1, 2, 0, None, 1, dev_a)

    @mid
    def _():
        job(0, 3, 1, 2, 4, dev_b, True)
        job(0, 1, 0, 4, 0, dev_a)

    third(0)
    third(1)

    @end
    def _():
        job(1, 1, 1, None, 0, dev_a)

    @mid
    def _():
        job(1, 3, 1, 2, 4, dev_b)

    third(2)

    @end
    def _():
        finish(0, (0,))
        finish(1, (0,))

    @mid
    def _():
        job(1, 1, 0, 4, 0, dev_a)
        finish(0, (0, 3))
        job(1, 2, 1, 1, 3, dev_b)

    for k in range(3):
        fourth(k)

    @mid
    def _():
        finish(1, (0, 3))

    with sc("drain"):
        for cp in (*xo, *yo, *co, *xd, *yd, *ra, *rb, *cx, *cy, *cxd, *cyd, *cra, *crb):
            cp.wait_send()
        for j in range(2):
            acopy(0, 1, j).wait_send()

        @mid
        def _():
            for j in range(2):
                bcopy(0, 2, j).wait_send()
                bcopy(1, 3, j).wait_send()
                acopy(2, 2, j).wait_send()
                acopy(3, 3, j).wait_send()

        for half in range(2):
            for r in range(4):
                zcopy(0, 0, r, half, dev_a).wait_send()
        for i in range(6):
            xcopy1(i, 0).wait_send()
            ycopy1(i, 0).wait_send()
        for k in range(3):
            ycopy2(k).wait_send()
            xcopy2(k).wait_send()


def fused(x, dy, wg, wu, wd):
    nr, d = x.shape
    kd, kf = wg.shape
    f, hd = 2 * kf, kd // 2
    hbm = pl.BlockSpec(memory_space=pl.ANY)
    sds = jax.ShapeDtypeStruct
    out_shape = (
        sds((nr, d), bf), sds((nr, d), bf), sds((kd, kf), f32), sds((kd, kf), f32), sds((kd, kf), f32),
        sds((6, hd, kf), f32), sds((6, hd, kf), f32),
        sds((5, 8, nr, kd), f32), sds((24, hd, kf), f32), sds((24, hd, kf), f32),
        sds((6, hd, kf), f32), sds((6, hd, kf), f32),
    )
    dma = pltpu.SemaphoreType.DMA
    return pl.pallas_call(
        kernel,
        name="fused",
        out_shape=out_shape,
        in_specs=[hbm] * 5,
        out_specs=(hbm,) * len(out_shape),
        scratch_shapes=[
            pltpu.VMEM((d, f), bf), pltpu.VMEM((d, f), bf), pltpu.VMEM((f, d), bf),
            pltpu.VMEM((4, nr, d), bf), pltpu.VMEM((4, nr, d), bf), pltpu.VMEM((3, 4 * nr, f), bf),
            pltpu.VMEM((8, nr, kd), f32), pltpu.VMEM((2, nr, kd), f32), pltpu.VMEM((2, 2, kd, 4 * nr), bf),
            pltpu.VMEM((hd, hd), bf),
            pltpu.VMEM((2, hd, kf), f32), pltpu.VMEM((2, hd, kf), f32), pltpu.VMEM((2, hd, kf), f32),
            pltpu.VMEM((2, nr, kd), bf),
            dma((47,)), dma((39,)), dma((11,)), dma((8,)), dma((5, 8)), dma((2,)), dma((2,)), dma((24,)), dma((2,)),
            dma((2,)), dma((6,)), dma((6,)), dma((6,)), dma((6,)), dma((6,)), dma((6,)), dma((2,)), dma((2,)),
        ],
        compiler_params=pltpu.CompilerParams(collective_id=0, has_side_effects=True, vmem_limit_bytes=VMEM_LIMIT),
    )(x, dy, wg, wu, wd)


def solution(mesh):
    rows = P(("dp", "tp"), None)
    wsp = P("dp", "tp")
    dsp = P("tp", "dp")

    def local(x, w_gate, w_up, w_down, dy):
        y, dx, dwg, dwu, dwd = fused(x, dy, w_gate, w_up, w_down)[:5]
        return y, dx, dwg, dwu, dwd.T

    return jax.shard_map(local, mesh=mesh, in_specs=(rows, wsp, wsp, dsp, rows), out_specs=(rows, rows, wsp, wsp, dsp), check_vma=False)
```

```python
import jax
import jax.numpy as jnp
from jax import lax
from jax.experimental import pallas as pl
from jax.experimental.pallas import tpu as pltpu
from jax.sharding import PartitionSpec as P

MESH = pl.DeviceIdType.MESH
f32 = jnp.float32
bf = jnp.bfloat16
VMEM_LIMIT = 67043328
sc = jax.named_scope
LAG = 4


def mm(a, b):
    return lax.dot_general(a, b, (((1,), (0,)), ((), ())), preferred_element_type=f32)


def mmt(a, b):
    return lax.dot_general(a, b, (((1,), (1,)), ((), ())), preferred_element_type=f32)


def kernel(
    x_in, dy_in, wg_in, wu_in, wd_in,
    y_out, dx_out, n00, r2, zl, far_r, near, xr1, yr1,
    wg, wu, wd, xa, dya, act, zs, xt, ht, eye, fst, nst, cst,
    gs, gr, lsem, zsend, zrecv, zload, fsend, frecv, nstore, cload, xs1, xq1, ys1, yq1, s2, q2, cin, osem,
):
    tp = lax.axis_index("tp")
    dp = lax.axis_index("dp")
    z, y = tp // 2, tp % 2
    x, c = dp // 2, dp % 2
    is_end = (z == 0) | (z == 3)
    is_mid = (z == 1) | (z == 2)
    dev_x = {"tp": tp, "dp": 2 * (1 - x) + c}
    dev_y = {"tp": 2 * z + 1 - y, "dp": dp}
    dev_c = {"tp": tp, "dp": 2 * x + 1 - c}
    dev_a = {"tp": 2 * (z + 1 - 2 * (z % 2)) + y, "dp": dp}
    dev_b = {"tp": 2 * (3 - z) + y, "dp": dp}

    nr, d = x_in.shape
    kd, kf = wg_in.shape
    f = 2 * kf
    hd = kd // 2
    hf = kf // 2

    def end(fn):
        pl.when(is_end)(fn)

    def mid(fn):
        pl.when(is_mid)(fn)

    def nat(r):
        rc, rx = r // 2, r % 2
        return 2 * (x + rx - 2 * x * rx) + c + rc - 2 * c * rc

    def ncol(r):
        return pl.ds(pl.multiple_of(nat(r) * kd, kd), kd)

    def remote(src, dst, ss, rs, dev):
        return pltpu.make_async_remote_copy(
            src_ref=src, dst_ref=dst, send_sem=ss, recv_sem=rs, device_id=dev, device_id_type=MESH
        )

    own = (wg_in, wu_in, wd_in)

    def blk(k, rx, rc, ry, h=None):
        d0 = (2 * rc + rx) * kd
        if k < 2:
            ref = (wg, wu)[k]
            if h is None:
                return ref.at[pl.ds(d0, kd), pl.ds(ry * kf, kf)]
            return ref.at[pl.ds(d0 + h * hd, hd), pl.ds(ry * kf, kf)]
        if h is None:
            return wd.at[pl.ds(ry * kf, kf), pl.ds(d0, kd)]
        return wd.at[pl.ds(ry * kf + h * hf, hf), pl.ds(d0, kd)]

    local = []
    for r in range(4):
        local.append((x_in.at[:, ncol(r)], xa.at[pl.ds(0, nr), pl.ds(r * kd, kd)]))
    for r in range(4):
        local.append((dy_in.at[:, ncol(r)], dya.at[pl.ds(0, nr), pl.ds(r * kd, kd)]))
    for k in range(3):
        local.append((own[k], blk(k, 0, 0, 0)))
    local = [pltpu.make_async_copy(s, t, lsem.at[i]) for i, (s, t) in enumerate(local)]
    for cp in local:
        cp.start()

    bar = pltpu.get_barrier_semaphore()
    for dev in (dev_x, dev_y, dev_c, dev_a, dev_b):
        pl.semaphore_signal(bar, inc=1, device_id=dev, device_id_type=MESH)

    with sc("barrier"):
        pl.semaphore_wait(bar, 5)

    def wcopy(i, src, dst, dev):
        return remote(src, dst, gs.at[i], gr.at[i], dev)

    xo = [wcopy(k, own[k], blk(k, 1, 0, 0), dev_x) for k in range(2)]
    yo = [wcopy(2 + k, own[k], blk(k, 0, 0, 1), dev_y) for k in range(2)]
    co = [wcopy(4 + k, own[k], blk(k, 0, 1, 0), dev_c) for k in range(3)]

    def dhalf(h):
        return wd_in.at[pl.ds(h * hf, hf), :]

    xd = [wcopy(7 + h, dhalf(h), blk(2, 1, 0, 0, h), dev_x) for h in range(2)]
    yd = [wcopy(9 + h, dhalf(h), blk(2, 0, 0, 1, h), dev_y) for h in range(2)]
    ra = [wcopy(11 + k, blk(k, 1, 0, 0, 0), blk(k, 1, 0, 1, 0), dev_y) for k in range(3)]
    rb = [wcopy(14 + k, blk(k, 0, 0, 1, 1), blk(k, 1, 0, 1, 1), dev_x) for k in range(3)]
    cx = [wcopy(17 + k, blk(k, 1, 0, 0), blk(k, 1, 1, 0), dev_c) for k in range(2)]
    cy = [wcopy(19 + k, blk(k, 0, 0, 1), blk(k, 0, 1, 1), dev_c) for k in range(2)]
    cxd = [wcopy(21 + h, blk(2, 1, 0, 0, h), blk(2, 1, 1, 0, h), dev_c) for h in range(2)]
    cyd = [wcopy(23 + h, blk(2, 0, 0, 1, h), blk(2, 0, 1, 1, h), dev_c) for h in range(2)]
    cra = [wcopy(25 + k, blk(k, 1, 0, 1, 0), blk(k, 1, 1, 1, 0), dev_c) for k in range(3)]
    crb = [wcopy(28 + k, blk(k, 1, 0, 1, 1), blk(k, 1, 1, 1, 1), dev_c) for k in range(3)]
    nw = 31

    def slot(j, s):
        return (xa, dya)[j].at[pl.ds(s * nr, nr)]

    def acopy(src, dst, j):
        return remote(
            slot(j, src), slot(j, dst), gs.at[nw + 2 * dst + j], gr.at[nw + 2 * dst + j], dev_a
        )

    def bcopy(src, dst, j):
        return remote(
            slot(j, src), slot(j, dst), gs.at[nw + 8 + 2 * dst + j], gr.at[nw + 2 * dst + j], dev_b
        )

    def got(s, j):
        acopy(s, s, j).wait_recv()

    for k in range(2):
        xo[k].start()
        yo[k].start()
    with sc("rows_in"):
        for cp in local[:8]:
            cp.wait()
    for j in range(2):
        acopy(0, 1, j).start()

    @mid
    def _():
        for j in range(2):
            bcopy(0, 2, j).start()

    for k in range(3):
        co[k].start()

    def pass_on(s, j):
        with sc(f"rows{s}_{j}"):
            got(s, j)
        if s == 1:
            bcopy(1, 3, j).start()
        else:
            acopy(s, s, j).start()

    for k in range(2):
        with sc(f"gx{k}"):
            xo[k].wait_recv()
        ra[k].start()
        cx[k].start()
        with sc(f"gy{k}"):
            yo[k].wait_recv()
        rb[k].start()
        cy[k].start()
        if k == 1:
            xd[0].start()
            yd[1].start()
            xd[1].start()
            yd[0].start()

        @mid
        def _():
            pass_on(1, k)
            pass_on(2, k)

    for k in range(2):
        with sc(f"gr{k}"):
            ra[k].wait_recv()
            cra[k].start()
            rb[k].wait_recv()
            crb[k].start()
    for cp in local[8:]:
        cp.wait()
    with sc("gc01"):
        for cp in (*co[:2], *cx, *cy, *cra[:2], *crb[:2]):
            cp.wait_recv()

    ft = min(256, f)

    def rows(s):
        return pl.ds(s * nr, nr)

    def front_h(s):
        @pl.loop(0, f // ft)
        def _(i):
            col = pl.ds(pl.multiple_of(i * ft, ft), ft)
            a = mm(xa[rows(s), :], wg[:, col])
            b = mm(xa[rows(s), :], wu[:, col])
            act[2, rows(s), col] = (a * jax.nn.sigmoid(a) * b).astype(bf)

    def front(s):
        @pl.loop(0, f // ft)
        def _(i):
            col = pl.ds(pl.multiple_of(i * ft, ft), ft)
            a = mm(xa[rows(s), :], wg[:, col])
            b = mm(xa[rows(s), :], wu[:, col])
            g = mmt(dya[rows(s), :], wd[col, :])
            sig = jax.nn.sigmoid(a)
            sa = a * sig
            act[2, rows(s), col] = (sa * b).astype(bf)
            act[0, rows(s), col] = (g * b * sig * (1.0 + a * (1.0 - sig))).astype(bf)
            act[1, rows(s), col] = (g * sa).astype(bf)

    def back(kind, s, r):
        col = pl.ds(pl.multiple_of(r * kd, kd), kd)
        if kind == 0:
            return mm(act[2, rows(s), :], wd[:, col])
        return mmt(act[0, rows(s), :], wg[col, :]) + mmt(act[1, rows(s), :], wu[col, :])

    def zcopy(q, kind, r, half, dev):
        i = 4 * kind + r
        return remote(zs.at[4 * half + r], zl.at[q, i], zsend.at[4 * half + r], zrecv.at[q, i], dev)

    def zload_(q, kind, r, slot):
        return pltpu.make_async_copy(zl.at[q, 4 * kind + r], cst.at[slot, pl.ds(0, nr), pl.ds(0, kd)], zload.at[slot])

    def chunk(kind, s, r, half, q_add, first):
        if q_add is not None:
            with sc("zrecv"):
                zcopy(q_add, kind, r, half, dev_a).wait_recv()
            zload_(q_add, kind, r, r % 2).start()
        v = back(kind, s, r)
        if q_add is not None:
            zload_(q_add, kind, r, r % 2).wait()
            v = v + cst[r % 2, pl.ds(0, nr), pl.ds(0, kd)]
        if not first:
            with sc("zsend"):
                zcopy(0, kind, r, half, dev_a).wait_send()
        zs[4 * half + r] = v

    def job(kind, s, half, q_add, q_dst, dev, first=False):
        with sc(f"job{kind}_{s}"):
            @pl.loop(0, 4)
            def _(r):
                chunk(kind, s, r, half, q_add, first)

                @pl.when(r > 0)
                def _():
                    zcopy(q_dst, kind, r - 1, half, dev).start()

        zcopy(q_dst, kind, 3, half, dev).start()

    def finish(kind, adds):
        res, out = ((xa, y_out), (dya, dx_out))[kind]

        def store(r):
            col = pl.ds(pl.multiple_of(r * kd, kd), kd)
            return pltpu.make_async_copy(res.at[rows(1), col], out.at[:, ncol(r)], osem.at[r])

        with sc(f"fin{kind}"):
            @pl.loop(0, 4)
            def _(r):
                v = back(kind, 0, r)
                v = v + res[rows(0), pl.ds(pl.multiple_of(r * kd, kd), kd)].astype(f32)
                for n, q in enumerate(adds):
                    with sc("finrecv"):
                        zcopy(q, kind, r, 0, dev_a).wait_recv()
                    zload_(q, kind, r, n).start()
                for n, q in enumerate(adds):
                    zload_(q, kind, r, n).wait()
                    v = v + cst[n, pl.ds(0, nr), pl.ds(0, kd)]

                res[rows(1), pl.ds(pl.multiple_of(r * kd, kd), kd)] = v.astype(bf)
                store(r).start()

            for r in range(4):
                store(r).wait()

    def transpose_h():
        for s in range(4):
            @pl.loop(0, f // hd)
            def _(i):
                col = pl.ds(pl.multiple_of(i * hd, hd), hd)
                ht[col, rows(s)] = mmt(eye[...], act[2, rows(s), col]).astype(bf)

    def transpose_x(rx):
        for rc in range(2):
            c0 = (2 * rc + rx) * kd
            for s in range(4):
                for h in range(2):
                    v = mmt(eye[...], xa[rows(s), pl.ds(c0 + h * hd, hd)])
                    xt[rc, pl.ds(h * hd, hd), rows(s)] = v.astype(bf)

    def unit(rc, rx, j, put):
        ryi, k, half = j // 6, (j // 2) % 3, j % 2
        f0 = (1 - ryi) * kf

        @pl.when(k < 2)
        def _():
            a = xt[rc, pl.ds(pl.multiple_of(half * hd, hd), hd), :]
            b = act[k, :, pl.ds(pl.multiple_of(f0, kf), kf)]
            put(pl.ds(0, kf), mm(a, b))

        @pl.when(k == 2)
        def _():
            b = dya[:, pl.ds((2 * rc + rx) * kd, kd)]
            for q in range(2):
                a = ht[pl.ds(pl.multiple_of(f0 + half * hf + q * hd, hd), hd), :]
                put(pl.ds(q * kd, kd), mm(a, b))

    def fcopy(u):
        return remote(fst.at[u % 3], far_r.at[u], fsend.at[u % 3], frecv.at[u], dev_c)

    def ncopy(u):
        return pltpu.make_async_copy(nst.at[u % 2], near.at[u], nstore.at[u % 2])

    def ccopy(u):
        return pltpu.make_async_copy(far_r.at[u], cst.at[u % 2], cload.at[u % 2])

    def xcopy1(i, u):
        return remote(near.at[u], xr1.at[i], xs1.at[i], xq1.at[i], dev_x)

    def ycopy1(i, u):
        return remote(near.at[u], yr1.at[i], ys1.at[i], yq1.at[i], dev_y)

    def nsend(rx, j):
        ryi, k, half = j // 6, (j // 2) % 3, j % 2
        u = 12 * (1 - rx) + j
        if rx:
            @pl.when(half == 0)
            def _():
                xcopy1(ryi * 3 + k, u).start()

        @pl.when((half == 1) & (ryi == 0))
        def _():
            ycopy1(3 * (1 - rx) + k, u).start()

    def dw(rx):
        base = 12 * (1 - rx)
        with sc(f"tr{rx}"):
            transpose_x(rx)

        with sc(f"dw{rx}"):
            @pl.loop(0, 12 + LAG)
            def _(j):
                u = base + j
                w = u - LAG

                @pl.when(j >= LAG)
                def _():
                    with sc("frecv"):
                        fcopy(w).wait_recv()
                    ccopy(w).start()

                @pl.when(j < 12)
                def _():
                    @pl.when(u > 2)
                    def _():
                        fcopy(u).wait_send()

                    def put(col, v):
                        fst[u % 3, :, col] = v

                    unit(1, rx, j, put)

                @pl.when((j > 0) & (j < 13))
                def _():
                    fcopy(u - 1).start()

                @pl.when(j >= LAG)
                def _():
                    ccopy(w).wait()

                    def put(col, v):
                        nst[w % 2, :, col] = v + cst[w % 2, :, col]

                    unit(0, rx, j - LAG, put)

                    @pl.when(j > LAG)
                    def _():
                        ncopy(w - 1).wait()
                        nsend(rx, j - LAG - 1)

                    ncopy(w).start()

            ncopy(base + 11).wait()
            nsend(rx, 11)

    def add_units(a, b, dst):
        ca = pltpu.make_async_copy(a, fst.at[0], cin.at[0])
        cb = pltpu.make_async_copy(b, fst.at[1], cin.at[1])
        ca.start()
        cb.start()
        ca.wait()
        cb.wait()
        st = min(64, hd)

        @pl.loop(0, hd // st)
        def _(i):
            row = pl.ds(pl.multiple_of(i * st, st), st)
            nst[0, row, :] = fst[0, row, :] + fst[1, row, :]

        cp = pltpu.make_async_copy(nst.at[0], dst, nstore.at[0])
        cp.start()
        cp.wait()

    def uid(rx, ry, k, half):
        return 12 * (1 - rx) + 6 * (1 - ry) + 2 * k + half

    def ycopy2(k):
        return remote(near.at[uid(0, 1, k, 0)], r2.at[2 * k], s2.at[2 * k], q2.at[2 * k], dev_y)

    def xcopy2(k):
        return remote(near.at[uid(1, 0, k, 1)], r2.at[2 * k + 1], s2.at[2 * k + 1], q2.at[2 * k + 1], dev_x)

    def second(k):
        with sc(f"second{k}"):
            ua, ub = uid(0, 1, k, 0), uid(1, 0, k, 1)
            xcopy1(k, 0).wait_recv()
            add_units(near.at[ua], xr1.at[k], near.at[ua])
            ycopy2(k).start()
            ycopy1(k, 0).wait_recv()
            add_units(near.at[ub], yr1.at[k], near.at[ub])
            xcopy2(k).start()

    def third(k):
        with sc(f"third{k}"):
            xcopy1(3 + k, 0).wait_recv()
            add_units(near.at[uid(0, 0, k, 0)], xr1.at[3 + k], n00.at[2 * k])
            ycopy1(3 + k, 0).wait_recv()
            add_units(near.at[uid(0, 0, k, 1)], yr1.at[3 + k], n00.at[2 * k + 1])

    eye[...] = (
        lax.broadcasted_iota(jnp.int32, (hd, hd), 0) == lax.broadcasted_iota(jnp.int32, (hd, hd), 1)
    ).astype(f32).astype(bf)

    @end
    def _():
        with sc("e_rows1"):
            got(1, 0)
        with sc("front_h1"):
            front_h(1)

    with sc("gd0"):
        xd[0].wait_recv()
        ra[2].start()
        cxd[0].start()
        yd[1].wait_recv()
        rb[2].start()
        cyd[1].start()

    @end
    def _():
        with sc("e_rows2"):
            got(2, 0)
        with sc("front_h2"):
            front_h(2)

    with sc("gd1"):
        yd[0].wait_recv()
        cyd[0].start()
        xd[1].wait_recv()
        cxd[1].start()

    @mid
    def _():
        pass_on(3, 0)

    def early(r):
        chunk(0, 1, r, 0, None, True)

    def early_send(r):
        zcopy(0, 0, r, 0, dev_a).start()

    @end
    def _():
        early(0)

    with sc("gc2a"):
        co[2].wait_recv()
        cyd[0].wait_recv()
        cyd[1].wait_recv()

    @end
    def _():
        early(2)
        early_send(0)

    with sc("gr2"):
        ra[2].wait_recv()
        cra[2].start()
        rb[2].wait_recv()
        crb[2].start()

    @mid
    def _():
        pass_on(3, 1)

    @end
    def _():
        early_send(2)
        early(1)

    with sc("gc2b"):
        for cp in (*cxd, cra[2], crb[2]):
            cp.wait_recv()

    @end
    def _():
        early(3)
        early_send(1)
        got(1, 1)
        got(2, 1)
        early_send(3)
        job(0, 2, 1, None, 1, dev_a, True)

    with sc("front1"):
        front(1)
    with sc("front0"):
        front(0)
    with sc("front2"):
        front(2)

    @end
    def _():
        with sc("e_rows3"):
            got(3, 0)
            got(3, 1)

    with sc("front3"):
        front(3)

    @end
    def _():
        job(0, 3, 0, None, 2, dev_a)

    with sc("trh"):
        transpose_h()
    dw(1)

    @mid
    def _():
        job(0, 2, 0, 1, 3, dev_b, True)

    dw(0)
    for u in range(3):
        fcopy(u).wait_send()
    for cp in (*xo, *yo, *co, *xd, *yd, *ra, *rb, *cx, *cy, *cxd, *cyd, *cra, *crb):
        cp.wait_send()
    for j in range(2):
        acopy(0, 1, j).wait_send()

    @mid
    def _():
        for j in range(2):
            bcopy(0, 2, j).wait_send()
            bcopy(1, 3, j).wait_send()
            acopy(2, 2, j).wait_send()
            acopy(3, 3, j).wait_send()


    @end
    def _():
        job(1, 3, 1, None, 2, dev_a)
        second(0)
        second(1)
        second(2)
        job(1, 2, 0, None, 1, dev_a)
        third(0)
        third(1)
        job(1, 1, 1, None, 0, dev_a)
        third(2)
        finish(0, (0,))
        finish(1, (0,))

    @mid
    def _():
        job(0, 3, 1, 2, 4, dev_b, True)
        second(0)
        second(1)
        second(2)
        job(0, 1, 0, 4, 0, dev_a)
        job(1, 3, 1, 2, 4, dev_b)
        third(0)
        third(1)
        job(1, 1, 0, 4, 0, dev_a)
        third(2)
        finish(0, (0, 3))
        job(1, 2, 1, 1, 3, dev_b)
        finish(1, (0, 3))

    with sc("drain"):
        for k in range(3):
            ycopy2(k).wait_recv()
            xcopy2(k).wait_recv()
        for half in range(2):
            for r in range(4):
                zcopy(0, 0, r, half, dev_a).wait_send()
        for i in range(6):
            xcopy1(i, 0).wait_send()
            ycopy1(i, 0).wait_send()
        for k in range(3):
            ycopy2(k).wait_send()
            xcopy2(k).wait_send()


def fused(x, dy, wg, wu, wd):
    nr, d = x.shape
    kd, kf = wg.shape
    f, hd = 2 * kf, kd // 2
    hbm = pl.BlockSpec(memory_space=pl.ANY)
    sds = jax.ShapeDtypeStruct
    out_shape = (
        sds((nr, d), bf), sds((nr, d), bf),
        sds((6, hd, kf), f32), sds((6, hd, kf), f32),
        sds((5, 8, nr, kd), f32), sds((24, hd, kf), f32), sds((24, hd, kf), f32),
        sds((6, hd, kf), f32), sds((6, hd, kf), f32),
    )
    dma = pltpu.SemaphoreType.DMA
    return pl.pallas_call(
        kernel,
        name="fused",
        out_shape=out_shape,
        in_specs=[hbm] * 5,
        out_specs=(hbm,) * len(out_shape),
        scratch_shapes=[
            pltpu.VMEM((d, f), bf), pltpu.VMEM((d, f), bf), pltpu.VMEM((f, d), bf),
            pltpu.VMEM((4 * nr, d), bf), pltpu.VMEM((4 * nr, d), bf), pltpu.VMEM((3, 4 * nr, f), bf),
            pltpu.VMEM((8, nr, kd), f32), pltpu.VMEM((2, kd, 4 * nr), bf), pltpu.VMEM((f, 4 * nr), bf),
            pltpu.VMEM((hd, hd), bf),
            pltpu.VMEM((3, hd, kf), f32), pltpu.VMEM((2, hd, kf), f32), pltpu.VMEM((2, hd, kf), f32),
            dma((47,)), dma((39,)), dma((11,)), dma((8,)), dma((5, 8)), dma((2,)), dma((3,)), dma((24,)), dma((2,)),
            dma((2,)), dma((6,)), dma((6,)), dma((6,)), dma((6,)), dma((6,)), dma((6,)), dma((2,)), dma((4,)),
        ],
        compiler_params=pltpu.CompilerParams(collective_id=0, has_side_effects=True, vmem_limit_bytes=VMEM_LIMIT),
    )(x, dy, wg, wu, wd)


def tail_kernel(y_in, dx_in, a_in, b_in, y, dx, dwg, dwu, dwd, va, vb, vo, vy, sa, sb, so, sy, sz):
    hd, kf = va.shape[1:]
    kd = dwd.shape[1]
    ca = [pltpu.make_async_copy(a_in.at[i], va.at[i], sa.at[i]) for i in range(6)]
    cb = [pltpu.make_async_copy(b_in.at[i], vb.at[i], sb.at[i]) for i in range(6)]
    cy = [pltpu.make_async_copy(r, vy.at[i], sy.at[i]) for i, r in enumerate((y_in, dx_in))]
    cz = [pltpu.make_async_copy(vy.at[i], r, sz.at[i]) for i, r in enumerate((y, dx))]
    for c in cy:
        c.start()
    for i in range(6):
        ca[i].start()
        cb[i].start()
    for i in range(2):
        cy[i].wait()
        cz[i].start()
    co = []
    for i in range(6):
        ca[i].wait()
        cb[i].wait()
        st = min(64, hd)

        @pl.loop(0, hd // st)
        def _(j):
            row = pl.ds(pl.multiple_of(j * st, st), st)
            vo[i, row, :] = va[i, row, :] + vb[i, row, :]

        k, h = i // 2, i % 2
        if k < 2:
            out = [((dwg, dwu)[k].at[pl.ds(h * hd, hd)], vo.at[i])]
        else:
            out = [(dwd.at[pl.ds((2 * h + q) * hd, hd)], vo.at[i, :, pl.ds(q * kd, kd)]) for q in range(2)]
        for n, (t, v) in enumerate(out):
            co.append(pltpu.make_async_copy(v, t, so.at[i, n]))
            co[-1].start()
    for c in cz + co:
        c.wait()


def tail(y, dx, a, b, kd, kf):
    hbm = pl.BlockSpec(memory_space=pl.ANY)
    sds = jax.ShapeDtypeStruct
    dma = pltpu.SemaphoreType.DMA
    return pl.pallas_call(
        tail_kernel,
        name="tail",
        out_shape=(sds(y.shape, bf), sds(y.shape, bf), sds((kd, kf), f32), sds((kd, kf), f32), sds((kf, kd), f32)),
        in_specs=[hbm] * 4,
        out_specs=(hbm,) * 5,
        scratch_shapes=[
            pltpu.VMEM(a.shape, f32), pltpu.VMEM(a.shape, f32), pltpu.VMEM(a.shape, f32), pltpu.VMEM((2, *y.shape), bf),
            dma((6,)), dma((6,)), dma((6, 2)), dma((2,)), dma((2,)),
        ],
        compiler_params=pltpu.CompilerParams(vmem_limit_bytes=VMEM_LIMIT),
    )(y, dx, a, b)


def solution(mesh):
    rows = P(("dp", "tp"), None)
    wsp = P("dp", "tp")
    dsp = P("tp", "dp")

    def local(x, w_gate, w_up, w_down, dy):
        y, dx, a, b = fused(x, dy, w_gate, w_up, w_down)[:4]
        return tail(y, dx, a, b, *w_gate.shape)

    return jax.shard_map(local, mesh=mesh, in_specs=(rows, wsp, wsp, dsp, rows), out_specs=(rows, rows, wsp, wsp, dsp), check_vma=False)
```

```python
import jax
import jax.numpy as jnp
from jax import lax
from jax.experimental import pallas as pl
from jax.experimental.pallas import tpu as pltpu
from jax.sharding import PartitionSpec as P

MESH = pl.DeviceIdType.MESH
f32 = jnp.float32
bf = jnp.bfloat16
VMEM_LIMIT = 67043328
sc = jax.named_scope
LAG = 4


def mm(a, b):
    return lax.dot_general(a, b, (((1,), (0,)), ((), ())), preferred_element_type=f32)


def mmt(a, b):
    return lax.dot_general(a, b, (((1,), (1,)), ((), ())), preferred_element_type=f32)


def kernel(
    x_in, dy_in, wg_in, wu_in, wd_in,
    y_out, dx_out, n00, r2, zl, far_r, near, xr1, yr1,
    wg, wu, wd, xa, dya, act, zs, xt, ht, eye, fst, nst, cst,
    gs, gr, lsem, zsend, zrecv, zload, fsend, frecv, nstore, cload, xs1, xq1, ys1, yq1, s2, q2, cin, osem,
):
    tp = lax.axis_index("tp")
    dp = lax.axis_index("dp")
    z, y = tp // 2, tp % 2
    x, c = dp // 2, dp % 2
    is_end = (z == 0) | (z == 3)
    is_mid = (z == 1) | (z == 2)
    dev_x = {"tp": tp, "dp": 2 * (1 - x) + c}
    dev_y = {"tp": 2 * z + 1 - y, "dp": dp}
    dev_c = {"tp": tp, "dp": 2 * x + 1 - c}
    dev_a = {"tp": 2 * (z + 1 - 2 * (z % 2)) + y, "dp": dp}
    dev_b = {"tp": 2 * (3 - z) + y, "dp": dp}

    nr, d = x_in.shape
    kd, kf = wg_in.shape
    f = 2 * kf
    hd = kd // 2
    hf = kf // 2

    def end(fn):
        pl.when(is_end)(fn)

    def mid(fn):
        pl.when(is_mid)(fn)

    def nat(r):
        rc, rx = r // 2, r % 2
        return 2 * (x + rx - 2 * x * rx) + c + rc - 2 * c * rc

    def ncol(r):
        return pl.ds(pl.multiple_of(nat(r) * kd, kd), kd)

    def remote(src, dst, ss, rs, dev):
        return pltpu.make_async_remote_copy(
            src_ref=src, dst_ref=dst, send_sem=ss, recv_sem=rs, device_id=dev, device_id_type=MESH
        )

    own = (wg_in, wu_in, wd_in)

    def blk(k, rx, rc, ry, h=None):
        d0 = (2 * rc + rx) * kd
        if k < 2:
            ref = (wg, wu)[k]
            if h is None:
                return ref.at[pl.ds(d0, kd), pl.ds(ry * kf, kf)]
            return ref.at[pl.ds(d0 + h * hd, hd), pl.ds(ry * kf, kf)]
        if h is None:
            return wd.at[pl.ds(ry * kf, kf), pl.ds(d0, kd)]
        return wd.at[pl.ds(ry * kf + h * hf, hf), pl.ds(d0, kd)]

    local = []
    for r in range(4):
        local.append((x_in.at[:, ncol(r)], xa.at[pl.ds(0, nr), pl.ds(r * kd, kd)]))
    for r in range(4):
        local.append((dy_in.at[:, ncol(r)], dya.at[pl.ds(0, nr), pl.ds(r * kd, kd)]))
    for k in range(3):
        local.append((own[k], blk(k, 0, 0, 0)))
    local = [pltpu.make_async_copy(s, t, lsem.at[i]) for i, (s, t) in enumerate(local)]
    for cp in local:
        cp.start()

    bar = pltpu.get_barrier_semaphore()
    for dev in (dev_x, dev_y, dev_c, dev_a, dev_b):
        pl.semaphore_signal(bar, inc=1, device_id=dev, device_id_type=MESH)

    with sc("barrier"):
        pl.semaphore_wait(bar, 5)

    ft = min(256, f)

    def rows(s):
        return pl.ds(s * nr, nr)

    def transpose_x(rx, slots):
        for s in slots:
            for rc in range(2):
                for h in range(2):
                    v = mmt(eye[...], xa[rows(s), pl.ds((2 * rc + rx) * kd + h * hd, hd)])
                    xt[rc, pl.ds(h * hd, hd), rows(s)] = v.astype(bf)

    def wcopy(i, src, dst, dev):
        return remote(src, dst, gs.at[i], gr.at[i], dev)

    xo = [wcopy(k, own[k], blk(k, 1, 0, 0), dev_x) for k in range(2)]
    yo = [wcopy(2 + k, own[k], blk(k, 0, 0, 1), dev_y) for k in range(2)]
    co = [wcopy(4 + k, own[k], blk(k, 0, 1, 0), dev_c) for k in range(3)]

    def dhalf(h):
        return wd_in.at[pl.ds(h * hf, hf), :]

    xd = [wcopy(7 + h, dhalf(h), blk(2, 1, 0, 0, h), dev_x) for h in range(2)]
    yd = [wcopy(9 + h, dhalf(h), blk(2, 0, 0, 1, h), dev_y) for h in range(2)]
    ra = [wcopy(11 + k, blk(k, 1, 0, 0, 0), blk(k, 1, 0, 1, 0), dev_y) for k in range(3)]
    rb = [wcopy(14 + k, blk(k, 0, 0, 1, 1), blk(k, 1, 0, 1, 1), dev_x) for k in range(3)]
    cx = [wcopy(17 + k, blk(k, 1, 0, 0), blk(k, 1, 1, 0), dev_c) for k in range(2)]
    cy = [wcopy(19 + k, blk(k, 0, 0, 1), blk(k, 0, 1, 1), dev_c) for k in range(2)]
    cxd = [wcopy(21 + h, blk(2, 1, 0, 0, h), blk(2, 1, 1, 0, h), dev_c) for h in range(2)]
    cyd = [wcopy(23 + h, blk(2, 0, 0, 1, h), blk(2, 0, 1, 1, h), dev_c) for h in range(2)]
    cra = [wcopy(25 + k, blk(k, 1, 0, 1, 0), blk(k, 1, 1, 1, 0), dev_c) for k in range(3)]
    crb = [wcopy(28 + k, blk(k, 1, 0, 1, 1), blk(k, 1, 1, 1, 1), dev_c) for k in range(3)]
    nw = 31

    def slot(j, s):
        return (xa, dya)[j].at[pl.ds(s * nr, nr)]

    def acopy(src, dst, j):
        return remote(
            slot(j, src), slot(j, dst), gs.at[nw + 2 * dst + j], gr.at[nw + 2 * dst + j], dev_a
        )

    def bcopy(src, dst, j):
        return remote(
            slot(j, src), slot(j, dst), gs.at[nw + 8 + 2 * dst + j], gr.at[nw + 2 * dst + j], dev_b
        )

    def got(s, j):
        acopy(s, s, j).wait_recv()

    for k in range(2):
        xo[k].start()
        yo[k].start()
    with sc("rows_in"):
        for cp in local[:8]:
            cp.wait()
    for j in range(2):
        acopy(0, 1, j).start()

    @mid
    def _():
        for j in range(2):
            bcopy(0, 2, j).start()

    for k in range(3):
        co[k].start()

    eye[...] = (
        lax.broadcasted_iota(jnp.int32, (hd, hd), 0) == lax.broadcasted_iota(jnp.int32, (hd, hd), 1)
    ).astype(f32).astype(bf)

    with sc("xt0"):
        transpose_x(1, (0,))

    def pass_on(s, j):
        with sc(f"rows{s}_{j}"):
            got(s, j)
        if s == 1:
            bcopy(1, 3, j).start()
        else:
            acopy(s, s, j).start()

    for k in range(2):
        with sc(f"gx{k}"):
            xo[k].wait_recv()
        ra[k].start()
        cx[k].start()
        with sc(f"gy{k}"):
            yo[k].wait_recv()
        rb[k].start()
        cy[k].start()
        if k == 1:
            xd[0].start()
            yd[1].start()
            xd[1].start()
            yd[0].start()

        @mid
        def _():
            pass_on(1, k)
            pass_on(2, k)

    for k in range(2):
        with sc(f"gr{k}"):
            ra[k].wait_recv()
            cra[k].start()
            rb[k].wait_recv()
            crb[k].start()
    for cp in local[8:]:
        cp.wait()
    with sc("gc01"):
        for cp in (*co[:2], *cx, *cy, *cra[:2], *crb[:2]):
            cp.wait_recv()

    def front_h(s):
        @pl.loop(0, f // ft)
        def _(i):
            col = pl.ds(pl.multiple_of(i * ft, ft), ft)
            a = mm(xa[rows(s), :], wg[:, col])
            b = mm(xa[rows(s), :], wu[:, col])
            act[2, rows(s), col] = (a * jax.nn.sigmoid(a) * b).astype(bf)

    def keep_h(s, i, h):
        for q in range(ft // hd):
            col = pl.ds(pl.multiple_of(i * ft + q * hd, hd), hd)
            ht[col, rows(s)] = mmt(eye[...], h[:, q * hd : (q + 1) * hd]).astype(bf)

    def front(s):
        @pl.loop(0, f // ft)
        def _(i):
            col = pl.ds(pl.multiple_of(i * ft, ft), ft)
            a = mm(xa[rows(s), :], wg[:, col])
            b = mm(xa[rows(s), :], wu[:, col])
            g = mmt(dya[rows(s), :], wd[col, :])
            sig = jax.nn.sigmoid(a)
            sa = a * sig
            h = (sa * b).astype(bf)
            act[2, rows(s), col] = h
            act[0, rows(s), col] = (g * b * sig * (1.0 + a * (1.0 - sig))).astype(bf)
            act[1, rows(s), col] = (g * sa).astype(bf)
            keep_h(s, i, h)

    nb = kf // ft

    def front_ab(s):
        @pl.loop(0, f // ft)
        def _(i):
            col = pl.ds(pl.multiple_of(i * ft, ft), ft)
            kcol = pl.ds(pl.multiple_of((i % nb) * ft, ft), ft)
            a = mm(xa[rows(s), :], wg[:, col])
            b = mm(xa[rows(s), :], wu[:, col])
            sig = jax.nn.sigmoid(a)
            sa = a * sig
            h = (sa * b).astype(bf)
            act[2, rows(s), col] = h
            fst[i // nb, pl.ds(0, nr), kcol] = sa
            nst[i // nb, pl.ds(0, nr), kcol] = b * sig * (1.0 + a * (1.0 - sig))
            keep_h(s, i, h)

    def front_g(s):
        @pl.loop(0, f // ft)
        def _(i):
            col = pl.ds(pl.multiple_of(i * ft, ft), ft)
            kcol = pl.ds(pl.multiple_of((i % nb) * ft, ft), ft)
            g = mmt(dya[rows(s), :], wd[col, :])
            act[0, rows(s), col] = (g * nst[i // nb, pl.ds(0, nr), kcol]).astype(bf)
            act[1, rows(s), col] = (g * fst[i // nb, pl.ds(0, nr), kcol]).astype(bf)

    def back(kind, s, r):
        col = pl.ds(pl.multiple_of(r * kd, kd), kd)
        if kind == 0:
            return mm(act[2, rows(s), :], wd[:, col])
        return mmt(act[0, rows(s), :], wg[col, :]) + mmt(act[1, rows(s), :], wu[col, :])

    def zcopy(q, kind, r, half, dev):
        i = 4 * kind + r
        return remote(zs.at[4 * half + r], zl.at[q, i], zsend.at[4 * half + r], zrecv.at[q, i], dev)

    def zload_(q, kind, r, slot):
        return pltpu.make_async_copy(zl.at[q, 4 * kind + r], cst.at[slot, pl.ds(0, nr), pl.ds(0, kd)], zload.at[slot])

    def chunk(kind, s, r, half, q_add, first):
        if q_add is not None:
            with sc("zrecv"):
                zcopy(q_add, kind, r, half, dev_a).wait_recv()
            zload_(q_add, kind, r, r % 2).start()
        v = back(kind, s, r)
        if q_add is not None:
            zload_(q_add, kind, r, r % 2).wait()
            v = v + cst[r % 2, pl.ds(0, nr), pl.ds(0, kd)]
        if not first:
            with sc("zsend"):
                zcopy(0, kind, r, half, dev_a).wait_send()
        zs[4 * half + r] = v

    def job(kind, s, half, q_add, q_dst, dev, first=False):
        with sc(f"job{kind}_{s}"):
            @pl.loop(0, 4)
            def _(r):
                chunk(kind, s, r, half, q_add, first)

                @pl.when(r > 0)
                def _():
                    zcopy(q_dst, kind, r - 1, half, dev).start()

        zcopy(q_dst, kind, 3, half, dev).start()

    def finish(kind, adds):
        res, out = ((xa, y_out), (dya, dx_out))[kind]

        def store(r):
            col = pl.ds(pl.multiple_of(r * kd, kd), kd)
            return pltpu.make_async_copy(res.at[rows(1), col], out.at[:, ncol(r)], osem.at[r])

        with sc(f"fin{kind}"):
            @pl.loop(0, 4)
            def _(r):
                v = back(kind, 0, r)
                v = v + res[rows(0), pl.ds(pl.multiple_of(r * kd, kd), kd)].astype(f32)
                for n, q in enumerate(adds):
                    with sc("finrecv"):
                        zcopy(q, kind, r, 0, dev_a).wait_recv()
                    zload_(q, kind, r, n).start()
                for n, q in enumerate(adds):
                    zload_(q, kind, r, n).wait()
                    v = v + cst[n, pl.ds(0, nr), pl.ds(0, kd)]

                res[rows(1), pl.ds(pl.multiple_of(r * kd, kd), kd)] = v.astype(bf)
                store(r).start()

            for r in range(4):
                store(r).wait()

    def unit(rc, rx, j, put):
        ryi, k, half = j // 6, (j // 2) % 3, j % 2
        f0 = (1 - ryi) * kf

        @pl.when(k < 2)
        def _():
            a = xt[rc, pl.ds(pl.multiple_of(half * hd, hd), hd), :]
            b = act[k, :, pl.ds(pl.multiple_of(f0, kf), kf)]
            put(pl.ds(0, kf), mm(a, b))

        @pl.when(k == 2)
        def _():
            b = dya[:, pl.ds((2 * rc + rx) * kd, kd)]
            for q in range(2):
                a = ht[pl.ds(pl.multiple_of(f0 + half * hf + q * hd, hd), hd), :]
                put(pl.ds(q * kd, kd), mm(a, b))

    def fcopy(u):
        return remote(fst.at[u % 3], far_r.at[u], fsend.at[u % 3], frecv.at[u], dev_c)

    def ncopy(u):
        return pltpu.make_async_copy(nst.at[u % 2], near.at[u], nstore.at[u % 2])

    def ccopy(u):
        return pltpu.make_async_copy(far_r.at[u], cst.at[u % 2], cload.at[u % 2])

    def xcopy1(i, u):
        return remote(near.at[u], xr1.at[i], xs1.at[i], xq1.at[i], dev_x)

    def ycopy1(i, u):
        return remote(near.at[u], yr1.at[i], ys1.at[i], yq1.at[i], dev_y)

    def nsend(rx, j):
        ryi, k, half = j // 6, (j // 2) % 3, j % 2
        u = 12 * (1 - rx) + j
        if rx:
            @pl.when(half == 0)
            def _():
                xcopy1(ryi * 3 + k, u).start()

        @pl.when((half == 1) & (ryi == 0))
        def _():
            ycopy1(3 * (1 - rx) + k, u).start()

    def dw(rx):
        base = 12 * (1 - rx)

        with sc(f"dw{rx}"):
            @pl.loop(0, 12 + LAG)
            def _(j):
                u = base + j
                w = u - LAG

                @pl.when(j < 12)
                def _():
                    @pl.when(u > 2)
                    def _():
                        with sc("fsend"):
                            fcopy(u).wait_send()

                    def put(col, v):
                        fst[u % 3, :, col] = v

                    unit(1, rx, j, put)

                @pl.when((j > 0) & (j < 13))
                def _():
                    fcopy(u - 1).start()

                @pl.when((j >= LAG - 1) & (j < 11 + LAG))
                def _():
                    with sc("frecv"):
                        fcopy(w + 1).wait_recv()
                    ccopy(w + 1).start()

                @pl.when(j >= LAG)
                def _():
                    with sc("cwait"):
                        ccopy(w).wait()

                    def put(col, v):
                        nst[w % 2, :, col] = v + cst[w % 2, :, col]

                    unit(0, rx, j - LAG, put)

                    @pl.when(j > LAG)
                    def _():
                        with sc("nwait"):
                            ncopy(w - 1).wait()
                        nsend(rx, j - LAG - 1)

                    ncopy(w).start()

            ncopy(base + 11).wait()
            nsend(rx, 11)

    def add_pair(units, waits, arrived, dsts, after=(None, None)):
        cn = [pltpu.make_async_copy(near.at[u], fst.at[h], cin.at[h]) for h, u in enumerate(units)]
        cr = [pltpu.make_async_copy(v, cst.at[h], cload.at[h]) for h, v in enumerate(arrived)]
        cd = [pltpu.make_async_copy(nst.at[h], t, nstore.at[h]) for h, t in enumerate(dsts)]
        st = min(64, hd)
        for h in range(2):
            cn[h].start()
        for h in range(2):
            waits[h].wait_recv()
            cr[h].start()
        for h in range(2):
            cn[h].wait()
            cr[h].wait()

            @pl.loop(0, hd // st)
            def _(i):
                row = pl.ds(pl.multiple_of(i * st, st), st)
                nst[h, row, :] = fst[h, row, :] + cst[h, row, :]

            cd[h].start()
        for h in range(2):
            cd[h].wait()
            if after[h] is not None:
                after[h].start()

    def uid(rx, ry, k, half):
        return 12 * (1 - rx) + 6 * (1 - ry) + 2 * k + half

    def ycopy2(k):
        return remote(near.at[uid(0, 1, k, 0)], r2.at[2 * k], s2.at[2 * k], q2.at[2 * k], dev_y)

    def xcopy2(k):
        return remote(near.at[uid(1, 0, k, 1)], r2.at[2 * k + 1], s2.at[2 * k + 1], q2.at[2 * k + 1], dev_x)

    def second(k):
        ua, ub = uid(0, 1, k, 0), uid(1, 0, k, 1)
        with sc(f"second{k}"):
            add_pair(
                (ua, ub), (xcopy1(k, 0), ycopy1(k, 0)), (xr1.at[k], yr1.at[k]), (near.at[ua], near.at[ub]),
                (ycopy2(k), xcopy2(k)),
            )

    def third(k):
        ua, ub = uid(0, 0, k, 0), uid(0, 0, k, 1)
        with sc(f"third{k}"):
            add_pair(
                (ua, ub), (xcopy1(3 + k, 0), ycopy1(3 + k, 0)), (xr1.at[3 + k], yr1.at[3 + k]),
                (n00.at[2 * k], n00.at[2 * k + 1]),
            )

    @end
    def _():
        with sc("e_rows1"):
            got(1, 0)

    with sc("front_ab1"):
        front_ab(1)
    with sc("xt1"):
        transpose_x(1, (1,))

    with sc("gd0"):
        xd[0].wait_recv()
        ra[2].start()
        cxd[0].start()
        yd[1].wait_recv()
        rb[2].start()
        cyd[1].start()

    @end
    def _():
        with sc("e_rows2"):
            got(2, 0)
        with sc("front_h2"):
            front_h(2)
        with sc("xt2"):
            transpose_x(1, (2,))

    with sc("gd1"):
        yd[0].wait_recv()
        cyd[0].start()
        xd[1].wait_recv()
        cxd[1].start()

    @mid
    def _():
        pass_on(3, 0)

    def early(r):
        chunk(0, 1, r, 0, None, True)

    def early_send(r):
        zcopy(0, 0, r, 0, dev_a).start()

    @end
    def _():
        early(0)

    with sc("gc2a"):
        co[2].wait_recv()
        cyd[0].wait_recv()
        cyd[1].wait_recv()

    @end
    def _():
        early(2)
        early_send(0)

    with sc("gr2"):
        ra[2].wait_recv()
        cra[2].start()
        rb[2].wait_recv()
        crb[2].start()

    @mid
    def _():
        pass_on(3, 1)

    @end
    def _():
        early_send(2)
        early(1)

    with sc("gc2b"):
        for cp in (*cxd, cra[2], crb[2]):
            cp.wait_recv()

    @end
    def _():
        early(3)
        early_send(1)
        got(1, 1)
        got(2, 1)
        early_send(3)
        job(0, 2, 1, None, 1, dev_a, True)

    with sc("front_g1"):
        front_g(1)
    with sc("front0"):
        front(0)
    with sc("front2"):
        front(2)

    @end
    def _():
        with sc("e_rows3"):
            got(3, 0)

    @mid
    def _():
        transpose_x(1, (2,))

    with sc("front_ab3"):
        front_ab(3)
    with sc("xt3"):
        transpose_x(1, (3,))

    @end
    def _():
        with sc("e_rows3"):
            got(3, 1)

    with sc("front_g3"):
        front_g(3)

    dw(1)

    @end
    def _():
        job(0, 3, 0, None, 2, dev_a)

    @mid
    def _():
        job(0, 2, 0, 1, 3, dev_b, True)

    with sc("xtb"):
        transpose_x(0, range(4))
    dw(0)
    for u in range(3):
        fcopy(u).wait_send()
    for cp in (*xo, *yo, *co, *xd, *yd, *ra, *rb, *cx, *cy, *cxd, *cyd, *cra, *crb):
        cp.wait_send()
    for j in range(2):
        acopy(0, 1, j).wait_send()

    @mid
    def _():
        for j in range(2):
            bcopy(0, 2, j).wait_send()
            bcopy(1, 3, j).wait_send()
            acopy(2, 2, j).wait_send()
            acopy(3, 3, j).wait_send()


    @end
    def _():
        job(1, 3, 1, None, 2, dev_a)
        second(0)
        second(1)
        second(2)
        job(1, 2, 0, None, 1, dev_a)
        third(0)
        third(1)
        job(1, 1, 1, None, 0, dev_a)
        third(2)
        finish(0, (0,))
        finish(1, (0,))

    @mid
    def _():
        job(0, 3, 1, 2, 4, dev_b, True)
        second(0)
        second(1)
        second(2)
        job(0, 1, 0, 4, 0, dev_a)
        job(1, 3, 1, 2, 4, dev_b)
        third(0)
        third(1)
        job(1, 1, 0, 4, 0, dev_a)
        job(1, 2, 1, 1, 3, dev_b)
        third(2)
        finish(0, (0, 3))
        finish(1, (0, 3))

    with sc("drain"):
        for k in range(3):
            ycopy2(k).wait_recv()
            xcopy2(k).wait_recv()
        for half in range(2):
            for r in range(4):
                zcopy(0, 0, r, half, dev_a).wait_send()
        for i in range(6):
            xcopy1(i, 0).wait_send()
            ycopy1(i, 0).wait_send()
        for k in range(3):
            ycopy2(k).wait_send()
            xcopy2(k).wait_send()


def fused(x, dy, wg, wu, wd):
    nr, d = x.shape
    kd, kf = wg.shape
    f, hd = 2 * kf, kd // 2
    hbm = pl.BlockSpec(memory_space=pl.ANY)
    sds = jax.ShapeDtypeStruct
    out_shape = (
        sds((nr, d), bf), sds((nr, d), bf),
        sds((6, hd, kf), f32), sds((6, hd, kf), f32),
        sds((5, 8, nr, kd), f32), sds((24, hd, kf), f32), sds((24, hd, kf), f32),
        sds((6, hd, kf), f32), sds((6, hd, kf), f32),
    )
    dma = pltpu.SemaphoreType.DMA
    return pl.pallas_call(
        kernel,
        name="fused",
        out_shape=out_shape,
        in_specs=[hbm] * 5,
        out_specs=(hbm,) * len(out_shape),
        scratch_shapes=[
            pltpu.VMEM((d, f), bf), pltpu.VMEM((d, f), bf), pltpu.VMEM((f, d), bf),
            pltpu.VMEM((4 * nr, d), bf), pltpu.VMEM((4 * nr, d), bf), pltpu.VMEM((3, 4 * nr, f), bf),
            pltpu.VMEM((8, nr, kd), f32), pltpu.VMEM((2, kd, 4 * nr), bf), pltpu.VMEM((f, 4 * nr), bf),
            pltpu.VMEM((hd, hd), bf),
            pltpu.VMEM((3, hd, kf), f32), pltpu.VMEM((2, hd, kf), f32), pltpu.VMEM((2, hd, kf), f32),
            dma((47,)), dma((39,)), dma((11,)), dma((8,)), dma((5, 8)), dma((2,)), dma((3,)), dma((24,)), dma((2,)),
            dma((2,)), dma((6,)), dma((6,)), dma((6,)), dma((6,)), dma((6,)), dma((6,)), dma((2,)), dma((4,)),
        ],
        compiler_params=pltpu.CompilerParams(collective_id=0, has_side_effects=True, vmem_limit_bytes=VMEM_LIMIT),
    )(x, dy, wg, wu, wd)


def tail_kernel(y_in, dx_in, a_in, b_in, y, dx, dwg, dwu, dwd, va, vb, vo, vy, sa, sb, so, sy, sz):
    hd, kf = va.shape[1:]
    kd = dwd.shape[1]
    ca = [pltpu.make_async_copy(a_in.at[i], va.at[i], sa.at[i]) for i in range(6)]
    cb = [pltpu.make_async_copy(b_in.at[i], vb.at[i], sb.at[i]) for i in range(6)]
    cy = [pltpu.make_async_copy(r, vy.at[i], sy.at[i]) for i, r in enumerate((y_in, dx_in))]
    cz = [pltpu.make_async_copy(vy.at[i], r, sz.at[i]) for i, r in enumerate((y, dx))]
    for c in cy:
        c.start()
    for i in range(6):
        ca[i].start()
        cb[i].start()
    for i in range(2):
        cy[i].wait()
        cz[i].start()
    co = []
    for i in range(6):
        ca[i].wait()
        cb[i].wait()
        st = min(64, hd)

        @pl.loop(0, hd // st)
        def _(j):
            row = pl.ds(pl.multiple_of(j * st, st), st)
            vo[i, row, :] = va[i, row, :] + vb[i, row, :]

        k, h = i // 2, i % 2
        if k < 2:
            out = [((dwg, dwu)[k].at[pl.ds(h * hd, hd)], vo.at[i])]
        else:
            out = [(dwd.at[pl.ds((2 * h + q) * hd, hd)], vo.at[i, :, pl.ds(q * kd, kd)]) for q in range(2)]
        for n, (t, v) in enumerate(out):
            co.append(pltpu.make_async_copy(v, t, so.at[i, n]))
            co[-1].start()
    for c in cz + co:
        c.wait()


def tail(y, dx, a, b, kd, kf):
    hbm = pl.BlockSpec(memory_space=pl.ANY)
    sds = jax.ShapeDtypeStruct
    dma = pltpu.SemaphoreType.DMA
    return pl.pallas_call(
        tail_kernel,
        name="tail",
        out_shape=(sds(y.shape, bf), sds(y.shape, bf), sds((kd, kf), f32), sds((kd, kf), f32), sds((kf, kd), f32)),
        in_specs=[hbm] * 4,
        out_specs=(hbm,) * 5,
        scratch_shapes=[
            pltpu.VMEM(a.shape, f32), pltpu.VMEM(a.shape, f32), pltpu.VMEM(a.shape, f32), pltpu.VMEM((2, *y.shape), bf),
            dma((6,)), dma((6,)), dma((6, 2)), dma((2,)), dma((2,)),
        ],
        compiler_params=pltpu.CompilerParams(vmem_limit_bytes=VMEM_LIMIT),
    )(y, dx, a, b)


def solution(mesh):
    rows = P(("dp", "tp"), None)
    wsp = P("dp", "tp")
    dsp = P("tp", "dp")

    def local(x, w_gate, w_up, w_down, dy):
        y, dx, a, b = fused(x, dy, w_gate, w_up, w_down)[:4]
        return tail(y, dx, a, b, *w_gate.shape)

    return jax.shard_map(local, mesh=mesh, in_specs=(rows, wsp, wsp, dsp, rows), out_specs=(rows, rows, wsp, wsp, dsp), check_vma=False)
```

```python
import jax
import jax.numpy as jnp
from jax import lax
from jax.experimental import pallas as pl
from jax.experimental.pallas import tpu as pltpu
from jax.sharding import PartitionSpec as P

MESH = pl.DeviceIdType.MESH
f32 = jnp.float32
bf = jnp.bfloat16
VMEM_LIMIT = 67043328
sc = jax.named_scope
LAG = 3


def mm(a, b):
    return lax.dot_general(a, b, (((1,), (0,)), ((), ())), preferred_element_type=f32)


def mmt(a, b):
    return lax.dot_general(a, b, (((1,), (1,)), ((), ())), preferred_element_type=f32)


def kernel(
    x_in, dy_in, wg_in, wu_in, wd_in,
    y_out, dx_out, dwg_out, dwu_out, dwd_out, n00, r2, zl, far_r, near, xr1, yr1, stash,
    wg, wu, wd, xa, dya, act, zs, xt, ht, eye, fst, nst, cst,
    gs, gr, lsem, zsend, zrecv, zload, fsend, frecv, nstore, cload, xs1, xq1, ys1, yq1, s2, q2, cin, osem, dsem, ssem,
):
    tp = lax.axis_index("tp")
    dp = lax.axis_index("dp")
    z, y = tp // 2, tp % 2
    x, c = dp // 2, dp % 2
    is_end = (z == 0) | (z == 3)
    is_mid = (z == 1) | (z == 2)
    dev_x = {"tp": tp, "dp": 2 * (1 - x) + c}
    dev_y = {"tp": 2 * z + 1 - y, "dp": dp}
    dev_c = {"tp": tp, "dp": 2 * x + 1 - c}
    dev_a = {"tp": 2 * (z + 1 - 2 * (z % 2)) + y, "dp": dp}
    dev_b = {"tp": 2 * (3 - z) + y, "dp": dp}

    nr, d = x_in.shape
    kd, kf = wg_in.shape
    f = 2 * kf
    hd = kd // 2
    hf = kf // 2

    def end(fn):
        pl.when(is_end)(fn)

    def mid(fn):
        pl.when(is_mid)(fn)

    def nat(r):
        rc, rx = r // 2, r % 2
        return 2 * (x + rx - 2 * x * rx) + c + rc - 2 * c * rc

    def ncol(r):
        return pl.ds(pl.multiple_of(nat(r) * kd, kd), kd)

    def remote(src, dst, ss, rs, dev):
        return pltpu.make_async_remote_copy(
            src_ref=src, dst_ref=dst, send_sem=ss, recv_sem=rs, device_id=dev, device_id_type=MESH
        )

    own = (wg_in, wu_in, wd_in)

    def blk(k, rx, rc, ry, h=None):
        d0 = (2 * rc + rx) * kd
        if k < 2:
            ref = (wg, wu)[k]
            if h is None:
                return ref.at[pl.ds(d0, kd), pl.ds(ry * kf, kf)]
            return ref.at[pl.ds(d0 + h * hd, hd), pl.ds(ry * kf, kf)]
        if h is None:
            return wd.at[pl.ds(ry * kf, kf), pl.ds(d0, kd)]
        return wd.at[pl.ds(ry * kf + h * hf, hf), pl.ds(d0, kd)]

    local = []
    for r in range(4):
        local.append((x_in.at[:, ncol(r)], xa.at[pl.ds(0, nr), pl.ds(r * kd, kd)]))
    for r in range(4):
        local.append((dy_in.at[:, ncol(r)], dya.at[pl.ds(0, nr), pl.ds(r * kd, kd)]))
    for k in range(3):
        local.append((own[k], blk(k, 0, 0, 0)))
    local = [pltpu.make_async_copy(s, t, lsem.at[i]) for i, (s, t) in enumerate(local)]
    for cp in local:
        cp.start()

    bar = pltpu.get_barrier_semaphore()
    for dev in (dev_x, dev_y, dev_c, dev_a, dev_b):
        pl.semaphore_signal(bar, inc=1, device_id=dev, device_id_type=MESH)

    with sc("barrier"):
        pl.semaphore_wait(bar, 5)

    ft = min(256, f)

    def rows(s):
        return pl.ds(s * nr, nr)

    def transpose_x(rx, lo, hi):
        @pl.loop(lo, hi)
        def _(s):
            row = pl.ds(pl.multiple_of(s * nr, nr), nr)
            for rc in range(2):
                for h in range(2):
                    v = mmt(eye[...], xa[row, pl.ds((2 * rc + rx) * kd + h * hd, hd)])
                    xt[rc, pl.ds(h * hd, hd), row] = v.astype(bf)

    def wcopy(i, src, dst, dev):
        return remote(src, dst, gs.at[i], gr.at[i], dev)

    def dhalf(h):
        return wd_in.at[pl.ds(h * hf, hf), :]

    xo = [wcopy(k, own[k], blk(k, 1, 0, 0), dev_x) for k in range(2)]
    yo = [wcopy(2 + k, own[k], blk(k, 0, 0, 1), dev_y) for k in range(2)]
    co = [wcopy(4 + k, own[k], blk(k, 0, 1, 0), dev_c) for k in range(3)]
    xd = [wcopy(7 + h, dhalf(h), blk(2, 1, 0, 0, h), dev_x) for h in range(2)]
    yd = [wcopy(9 + h, dhalf(h), blk(2, 0, 0, 1, h), dev_y) for h in range(2)]
    rg = wcopy(11, blk(0, 0, 0, 1), blk(0, 1, 0, 1), dev_x)
    rua = wcopy(12, blk(1, 1, 0, 0, 0), blk(1, 1, 0, 1, 0), dev_y)
    rub = wcopy(13, blk(1, 0, 0, 1, 1), blk(1, 1, 0, 1, 1), dev_x)
    rd = [wcopy(14 + h, blk(2, 1, 0, 0, h), blk(2, 1, 0, 1, h), dev_y) for h in range(2)]
    cx = [wcopy(16 + k, blk(k, 1, 0, 0), blk(k, 1, 1, 0), dev_c) for k in range(2)]
    cy = [wcopy(18 + k, blk(k, 0, 0, 1), blk(k, 0, 1, 1), dev_c) for k in range(2)]
    cxd = [wcopy(20 + h, blk(2, 1, 0, 0, h), blk(2, 1, 1, 0, h), dev_c) for h in range(2)]
    cyd = [wcopy(22 + h, blk(2, 0, 0, 1, h), blk(2, 0, 1, 1, h), dev_c) for h in range(2)]
    crg = wcopy(24, blk(0, 1, 0, 1), blk(0, 1, 1, 1), dev_c)
    crua = wcopy(25, blk(1, 1, 0, 1, 0), blk(1, 1, 1, 1, 0), dev_c)
    crub = wcopy(26, blk(1, 1, 0, 1, 1), blk(1, 1, 1, 1, 1), dev_c)
    crd = [wcopy(27 + h, blk(2, 1, 0, 1, h), blk(2, 1, 1, 1, h), dev_c) for h in range(2)]
    wcopies = (*xo, *yo, *co, *xd, *yd, rg, rua, rub, *rd, *cx, *cy, *cxd, *cyd, crg, crua, crub, *crd)
    nw = 31

    def slot(j, s):
        return (xa, dya)[j].at[pl.ds(s * nr, nr)]

    def acopy(src, dst, j):
        return remote(
            slot(j, src), slot(j, dst), gs.at[nw + 2 * dst + j], gr.at[nw + 2 * dst + j], dev_a
        )

    def bcopy(src, dst, j):
        return remote(
            slot(j, src), slot(j, dst), gs.at[nw + 8 + 2 * dst + j], gr.at[nw + 2 * dst + j], dev_b
        )

    def got(s, j):
        acopy(s, s, j).wait_recv()

    def stash_copy(s, p, n):
        return pltpu.make_async_copy((fst, nst)[n].at[p, pl.ds(0, nr)], stash.at[s, p, n], ssem.at[2 * p + n])

    def stash_load(s, p, n):
        return pltpu.make_async_copy(stash.at[s, p, n], (fst, nst)[n].at[p, pl.ds(0, nr)], ssem.at[2 * p + n])

    pending = [None, None]

    def flush(p):
        if pending[p] is not None:
            for n in range(2):
                stash_copy(pending[p], p, n).wait()
        pending[p] = None

    def part_ab(s, p):
        with sc(f"ab{s}_{p}"):
            flush(p)

            @pl.loop(0, kf // ft)
            def _(i):
                col = pl.ds(pl.multiple_of(p * kf + i * ft, ft), ft)
                kcol = pl.ds(pl.multiple_of(i * ft, ft), ft)
                a = mm(xa[rows(s), :], wg[:, col])
                b = mm(xa[rows(s), :], wu[:, col])
                sig = jax.nn.sigmoid(a)
                sa = a * sig
                act[2, rows(s), col] = (sa * b).astype(bf)
                fst[p, pl.ds(0, nr), kcol] = sa
                nst[p, pl.ds(0, nr), kcol] = b * sig * (1.0 + a * (1.0 - sig))

            for n in range(2):
                stash_copy(s, p, n).start()
            pending[p] = s

    gt = min(512, kf)

    def part_g(s, p):
        @pl.loop(0, kf // gt)
        def _(i):
            col = pl.ds(pl.multiple_of(p * kf + i * gt, gt), gt)
            kcol = pl.ds(pl.multiple_of(i * gt, gt), gt)
            g = mmt(dya[rows(s), :], wd[col, :])
            act[0, rows(s), col] = (g * nst[p, pl.ds(0, nr), kcol]).astype(bf)
            act[1, rows(s), col] = (g * fst[p, pl.ds(0, nr), kcol]).astype(bf)

    def gload(s):
        for p in range(2):
            for n in range(2):
                stash_load(s, p, n).start()

    def front_g(s, then):
        with sc(f"g{s}"):
            for p in range(2):
                for n in range(2):
                    stash_load(s, p, n).wait()
                part_g(s, p)
                if then is not None:
                    for n in range(2):
                        stash_load(then, p, n).start()

    def keep_h(s):
        hb = min(4, f // hd)
        with sc(f"ht{s}"):
            @pl.loop(0, f // (hb * hd))
            def _(i):
                for q in range(hb):
                    col = pl.ds(pl.multiple_of((i * hb + q) * hd, hd), hd)
                    ht[col, rows(s)] = mmt(eye[...], act[2, rows(s), col]).astype(bf)

    def back(kind, s, r):
        col = pl.ds(pl.multiple_of(r * kd, kd), kd)
        if kind == 0:
            return mm(act[2, rows(s), :], wd[:, col])
        return mmt(act[0, rows(s), :], wg[col, :]) + mmt(act[1, rows(s), :], wu[col, :])

    def zcopy(q, kind, r, half, dev):
        i = 4 * kind + r
        return remote(zs.at[4 * half + r], zl.at[q, i], zsend.at[4 * half + r], zrecv.at[q, i], dev)

    def zload_(q, kind, r, slot):
        return pltpu.make_async_copy(zl.at[q, 4 * kind + r], cst.at[slot, pl.ds(0, nr), pl.ds(0, kd)], zload.at[slot])

    def chunk(kind, s, r, half, q_add, first):
        i = 4 * half + r
        if q_add is not None:
            with sc("zrecv"):
                zcopy(q_add, kind, r, half, dev_a).wait_recv()
            zload_(q_add, kind, r, r % 2).start()
        if not first:
            with sc("zsend"):
                zcopy(0, kind, r, half, dev_a).wait_send()
        zs[i] = back(kind, s, r)
        if q_add is not None:
            zload_(q_add, kind, r, r % 2).wait()
            zs[i] = zs[i] + cst[r % 2, pl.ds(0, nr), pl.ds(0, kd)]

    def job(kind, s, half, q_add, q_dst, dev, first=False):
        with sc(f"job{kind}_{s}"):
            @pl.loop(0, 4)
            def _(r):
                chunk(kind, s, r, half, q_add, first)

                @pl.when(r > 0)
                def _():
                    zcopy(q_dst, kind, r - 1, half, dev).start()

        zcopy(q_dst, kind, 3, half, dev).start()

    def store(kind, r):
        res, out = ((xa, y_out), (dya, dx_out))[kind]
        col = pl.ds(pl.multiple_of(r * kd, kd), kd)
        return pltpu.make_async_copy(res.at[rows(1), col], out.at[:, ncol(r)], osem.at[4 * kind + r])

    def finish(kind, adds, lo=0, hi=4):
        res = (xa, dya)[kind]
        with sc(f"fin{kind}"):
            @pl.loop(lo, hi)
            def _(r):
                col = pl.ds(pl.multiple_of(r * kd, kd), kd)
                part = (pl.ds(0, nr), pl.ds(0, kd))
                nst[0, *part] = back(kind, 0, r)
                for n, q in enumerate(adds):
                    with sc("finrecv"):
                        zcopy(q, kind, r, 0, dev_a).wait_recv()
                    zload_(q, kind, r, n).start()
                for n, q in enumerate(adds):
                    zload_(q, kind, r, n).wait()
                v = nst[0, *part] + res[rows(0), col].astype(f32)
                for n in range(len(adds)):
                    v = v + cst[n, *part]
                res[rows(1), col] = v.astype(bf)
                store(kind, r).start()

    def unit(rc, rx, j, put):
        ryi, k, half = j // 6, (j // 2) % 3, j % 2
        f0 = (1 - ryi) * kf

        @pl.when(k < 2)
        def _():
            a = xt[rc, pl.ds(pl.multiple_of(half * hd, hd), hd), :]
            for q in range(2):
                b = act[k, :, pl.ds(pl.multiple_of(f0 + q * kd, kd), kd)]
                put(pl.ds(q * kd, kd), mm(a, b))

        @pl.when(k == 2)
        def _():
            b = dya[:, pl.ds((2 * rc + rx) * kd, kd)]
            for q in range(2):
                a = ht[pl.ds(pl.multiple_of(f0 + half * hf + q * hd, hd), hd), :]
                put(pl.ds(q * kd, kd), mm(a, b))

    def fcopy(u):
        return remote(fst.at[u % 3], far_r.at[u], fsend.at[u % 3], frecv.at[u], dev_c)

    def ncopy(u):
        return pltpu.make_async_copy(nst.at[u % 2], near.at[u], nstore.at[u % 2])

    def ccopy(u):
        return pltpu.make_async_copy(far_r.at[u], cst.at[u % 2], cload.at[u % 2])

    def xcopy1(i, u):
        return remote(near.at[u], xr1.at[i], xs1.at[i], xq1.at[i], dev_x)

    def ycopy1(i, u):
        return remote(near.at[u], yr1.at[i], ys1.at[i], yq1.at[i], dev_y)

    def nsend(rx, j):
        ryi, k, half = j // 6, (j // 2) % 3, j % 2
        u = 12 * (1 - rx) + j
        if rx:
            @pl.when(half == 0)
            def _():
                xcopy1(ryi * 3 + k, u).start()

        @pl.when((half == 1) & (ryi == 0))
        def _():
            ycopy1(3 * (1 - rx) + k, u).start()

    def dw(rx):
        base = 12 * (1 - rx)

        with sc(f"dw{rx}"):
            @pl.loop(0, 12 + LAG)
            def _(j):
                u = base + j
                w = u - LAG

                @pl.when(j < 12)
                def _():
                    @pl.when(u > 2)
                    def _():
                        with sc("fsend"):
                            fcopy(u).wait_send()

                    def put(col, v):
                        fst[u % 3, :, col] = v

                    unit(1, rx, j, put)

                @pl.when((j > 0) & (j < 13))
                def _():
                    fcopy(u - 1).start()

                @pl.when((j >= LAG - 1) & (j < 11 + LAG))
                def _():
                    with sc("frecv"):
                        fcopy(w + 1).wait_recv()
                    ccopy(w + 1).start()

                @pl.when(j >= LAG)
                def _():
                    with sc("cwait"):
                        ccopy(w).wait()

                    def put(col, v):
                        nst[w % 2, :, col] = v + cst[w % 2, :, col]

                    unit(0, rx, j - LAG, put)

                    @pl.when(j > LAG)
                    def _():
                        with sc("nwait"):
                            ncopy(w - 1).wait()
                        nsend(rx, j - LAG - 1)

                    ncopy(w).start()

            ncopy(base + 11).wait()
            nsend(rx, 11)

    def add_pair(units, waits, arrived, dsts, after=(None, None)):
        cn = [pltpu.make_async_copy(near.at[u], fst.at[h], cin.at[h]) for h, u in enumerate(units)]
        cr = [pltpu.make_async_copy(v, cst.at[h], cload.at[h]) for h, v in enumerate(arrived)]
        cd = [pltpu.make_async_copy(nst.at[h], t, nstore.at[h]) for h, t in enumerate(dsts)]
        st = min(64, hd)
        for h in range(2):
            cn[h].start()
        for h in range(2):
            waits[h].wait_recv()
            cr[h].start()
        for h in range(2):
            cn[h].wait()
            cr[h].wait()

            @pl.loop(0, hd // st)
            def _(i):
                row = pl.ds(pl.multiple_of(i * st, st), st)
                nst[h, row, :] = fst[h, row, :] + cst[h, row, :]

            cd[h].start()
        for h in range(2):
            cd[h].wait()
            if after[h] is not None:
                after[h].start()

    def uid(rx, ry, k, half):
        return 12 * (1 - rx) + 6 * (1 - ry) + 2 * k + half

    def ycopy2(k):
        return remote(near.at[uid(0, 1, k, 0)], r2.at[2 * k], s2.at[2 * k], q2.at[2 * k], dev_y)

    def xcopy2(k):
        return remote(near.at[uid(1, 0, k, 1)], r2.at[2 * k + 1], s2.at[2 * k + 1], q2.at[2 * k + 1], dev_x)

    def second(k):
        ua, ub = uid(0, 1, k, 0), uid(1, 0, k, 1)
        with sc(f"second{k}"):
            add_pair(
                (ua, ub), (xcopy1(k, 0), ycopy1(k, 0)), (xr1.at[k], yr1.at[k]), (near.at[ua], near.at[ub]),
                (ycopy2(k), xcopy2(k)),
            )

    def third(k):
        ua, ub = uid(0, 0, k, 0), uid(0, 0, k, 1)
        with sc(f"third{k}"):
            add_pair(
                (ua, ub), (xcopy1(3 + k, 0), ycopy1(3 + k, 0)), (xr1.at[3 + k], yr1.at[3 + k]),
                (n00.at[2 * k], n00.at[2 * k + 1]),
            )

    def fourth(k):
        units = (n00.at[2 * k], n00.at[2 * k + 1])
        if k < 2:
            dsts = [[((dwg_out, dwu_out)[k].at[pl.ds(h * hd, hd)], pl.ds(0, kf))] for h in range(2)]
        else:
            dsts = [[(dwd_out.at[pl.ds((2 * h + q) * hd, hd)], pl.ds(q * kd, kd)) for q in range(2)] for h in range(2)]
        cn = [pltpu.make_async_copy(u, fst.at[h], cin.at[h]) for h, u in enumerate(units)]
        cr = [pltpu.make_async_copy(r2.at[2 * k + h], cst.at[h], cload.at[h]) for h in range(2)]
        cd = [
            [pltpu.make_async_copy(nst.at[h, :, col], t, dsem.at[h, n]) for n, (t, col) in enumerate(dsts[h])]
            for h in range(2)
        ]
        st = min(64, hd)
        with sc(f"fourth{k}"):
            for h in range(2):
                cn[h].start()
            for h in range(2):
                (ycopy2, xcopy2)[h](k).wait_recv()
                cr[h].start()
            for h in range(2):
                cn[h].wait()
                cr[h].wait()

                @pl.loop(0, hd // st)
                def _(i):
                    row = pl.ds(pl.multiple_of(i * st, st), st)
                    nst[h, row, :] = fst[h, row, :] + cst[h, row, :]

                for cp in cd[h]:
                    cp.start()
            for h in range(2):
                for cp in cd[h]:
                    cp.wait()

    for k in range(2):
        xo[k].start()
        yo[k].start()
    for h in range(2):
        yd[h].start()
    with sc("rows_in"):
        for cp in local[:8]:
            cp.wait()
    for j in range(2):
        acopy(0, 1, j).start()

    @mid
    def _():
        for j in range(2):
            bcopy(0, 2, j).start()

    for k in range(3):
        co[k].start()

    eye[...] = (
        lax.broadcasted_iota(jnp.int32, (hd, hd), 0) == lax.broadcasted_iota(jnp.int32, (hd, hd), 1)
    ).astype(f32).astype(bf)

    with sc("xt0"):
        transpose_x(1, 0, 1)

    def pass_on(s, j):
        with sc(f"rows{s}_{j}"):
            got(s, j)
        if s == 1:
            bcopy(1, 3, j).start()
        else:
            acopy(s, s, j).start()

    with sc("gx0"):
        xo[0].wait_recv()
        cx[0].start()
        yo[0].wait_recv()
    rg.start()
    cy[0].start()

    @mid
    def _():
        pass_on(1, 0)
        pass_on(2, 0)

    with sc("gx1"):
        xo[1].wait_recv()
        rua.start()
        cx[1].start()
        yo[1].wait_recv()
    rub.start()
    for h in range(2):
        xd[h].start()
    cy[1].start()

    @mid
    def _():
        pass_on(1, 1)
        pass_on(2, 1)

    @end
    def _():
        with sc("e_rows1"):
            got(1, 0)

    for cp in local[8:]:
        cp.wait()
    with sc("gc0"):
        for cp in (*co[:2], *cx):
            cp.wait_recv()
    part_ab(1, 0)
    part_ab(0, 0)
    with sc("gyd"):
        for h in range(2):
            yd[h].wait_recv()
            cyd[h].start()
        rg.wait_recv()
        crg.start()

    @end
    def _():
        with sc("e_rows2"):
            got(2, 0)

    part_ab(2, 0)

    @mid
    def _():
        pass_on(3, 0)

    with sc("gru"):
        rua.wait_recv()
        crua.start()
        rub.wait_recv()
        crub.start()
    with sc("gc1"):
        for cp in (*cy, crg, crua, crub):
            cp.wait_recv()
    part_ab(1, 1)
    with sc("gc2"):
        for cp in (co[2], *cyd):
            cp.wait_recv()

    def early(s, odd):
        with sc(f"early{s}_{odd}"):
            @pl.loop(0, 2)
            def _(i):
                chunk(0, s, 2 * i + odd, s - 1, None, True)

                @pl.when(i > 0)
                def _():
                    early_send(s, odd)

    def early_send(s, r):
        zcopy(s - 1, 0, r, s - 1, dev_a).start()

    @end
    def _():
        early(1, 0)

    part_ab(0, 1)

    @end
    def _():
        early_send(1, 2)

    with sc("gd0"):
        xd[0].wait_recv()
        rd[0].start()
        cxd[0].start()
    part_ab(2, 1)

    @end
    def _():
        early(2, 0)

    @mid
    def _():
        pass_on(3, 1)

    transpose_x(1, 1, 3)
    keep_h(1)

    @end
    def _():
        early_send(2, 2)

    with sc("gd1"):
        xd[1].wait_recv()
        rd[1].start()
        cxd[1].start()
    keep_h(0)
    keep_h(2)
    with sc("gd2"):
        for h in range(2):
            rd[h].wait_recv()
            crd[h].start()

    with sc("gd3"):
        for cp in (*cxd, *crd):
            cp.wait_recv()

    @end
    def _():
        early(1, 1)
        early_send(1, 3)
        early(2, 1)
        got(1, 1)
        got(2, 1)
        with sc("e_rows3"):
            got(3, 0)

    part_ab(3, 0)

    @end
    def _():
        early_send(2, 3)

    part_ab(3, 1)
    transpose_x(1, 3, 4)
    flush(0)
    flush(1)
    gload(1)
    keep_h(3)
    front_g(1, 0)
    front_g(0, 2)
    front_g(2, 3)

    @end
    def _():
        with sc("e_rows3"):
            got(3, 1)

    front_g(3, None)
    dw(1)

    @end
    def _():
        job(0, 3, 0, None, 2, dev_a)

    @mid
    def _():
        job(0, 2, 0, 1, 3, dev_b, True)

    with sc("xtb"):
        transpose_x(0, 0, 4)
    dw(0)
    for u in range(3):
        fcopy(u).wait_send()
    for cp in wcopies:
        cp.wait_send()
    for j in range(2):
        acopy(0, 1, j).wait_send()

    @mid
    def _():
        for j in range(2):
            bcopy(0, 2, j).wait_send()
            bcopy(1, 3, j).wait_send()
            acopy(2, 2, j).wait_send()
            acopy(3, 3, j).wait_send()

    @end
    def _():
        job(1, 3, 1, None, 2, dev_a)
        second(0)
        second(1)
        second(2)
        job(1, 2, 0, None, 1, dev_a)
        third(0)
        third(1)
        job(1, 1, 1, None, 0, dev_a)
        third(2)
        finish(0, (0,))
        fourth(0)
        finish(1, (0,), 0, 2)
        fourth(1)
        finish(1, (0,), 2, 4)
        fourth(2)

    @mid
    def _():
        job(0, 3, 1, 2, 4, dev_b, True)
        second(0)
        second(1)
        second(2)
        job(0, 1, 0, 4, 0, dev_a)
        job(1, 3, 1, 2, 4, dev_b)
        third(0)
        third(1)
        job(1, 1, 0, 4, 0, dev_a)
        job(1, 2, 1, 1, 3, dev_b)
        third(2)
        finish(0, (0, 3))
        fourth(0)
        fourth(1)
        finish(1, (0, 3), 0, 3)
        fourth(2)
        finish(1, (0, 3), 3, 4)

    for kind in range(2):
        for r in range(4):
            store(kind, r).wait()
    with sc("drain"):
        for half in range(2):
            for r in range(4):
                zcopy(0, 0, r, half, dev_a).wait_send()
        for i in range(6):
            xcopy1(i, 0).wait_send()
            ycopy1(i, 0).wait_send()
        for k in range(3):
            ycopy2(k).wait_send()
            xcopy2(k).wait_send()


def fused(x, dy, wg, wu, wd):
    nr, d = x.shape
    kd, kf = wg.shape
    f, hd = 2 * kf, kd // 2
    hbm = pl.BlockSpec(memory_space=pl.ANY)
    sds = jax.ShapeDtypeStruct
    out_shape = (
        sds((nr, d), bf), sds((nr, d), bf), sds((kd, kf), f32), sds((kd, kf), f32), sds((kf, kd), f32),
        sds((6, hd, kf), f32), sds((6, hd, kf), f32),
        sds((5, 8, nr, kd), f32), sds((24, hd, kf), f32), sds((24, hd, kf), f32),
        sds((6, hd, kf), f32), sds((6, hd, kf), f32), sds((4, 2, 2, nr, kf), f32),
    )
    dma = pltpu.SemaphoreType.DMA
    return pl.pallas_call(
        kernel,
        name="fused",
        out_shape=out_shape,
        in_specs=[hbm] * 5,
        out_specs=(hbm,) * len(out_shape),
        scratch_shapes=[
            pltpu.VMEM((d, f), bf), pltpu.VMEM((d, f), bf), pltpu.VMEM((f, d), bf),
            pltpu.VMEM((4 * nr, d), bf), pltpu.VMEM((4 * nr, d), bf), pltpu.VMEM((3, 4 * nr, f), bf),
            pltpu.VMEM((8, nr, kd), f32), pltpu.VMEM((2, kd, 4 * nr), bf), pltpu.VMEM((f, 4 * nr), bf),
            pltpu.VMEM((hd, hd), bf),
            pltpu.VMEM((3, hd, kf), f32), pltpu.VMEM((2, hd, kf), f32), pltpu.VMEM((2, hd, kf), f32),
            dma((47,)), dma((39,)), dma((11,)), dma((8,)), dma((5, 8)), dma((2,)), dma((3,)), dma((24,)), dma((2,)),
            dma((2,)), dma((6,)), dma((6,)), dma((6,)), dma((6,)), dma((6,)), dma((6,)), dma((2,)), dma((8,)), dma((2, 2)), dma((4,)),
        ],
        compiler_params=pltpu.CompilerParams(collective_id=0, has_side_effects=True, vmem_limit_bytes=VMEM_LIMIT),
    )(x, dy, wg, wu, wd)


def tail_kernel(*refs):
    n = 5
    src, dst, buf, (si, so) = refs[:n], refs[n : 2 * n], refs[2 * n : 3 * n], refs[3 * n :]
    pieces = [(i, h) for i in range(n) for h in range(1 if i < 2 else 2)]

    def part(r, h, i):
        m = r.shape[0] // (1 if i < 2 else 2)
        return r.at[pl.ds(h * m, m)]

    ci = [pltpu.make_async_copy(part(src[i], h, i), part(buf[i], h, i), si.at[j]) for j, (i, h) in enumerate(pieces)]
    co = [pltpu.make_async_copy(part(buf[i], h, i), part(dst[i], h, i), so.at[j]) for j, (i, h) in enumerate(pieces)]
    for c in ci:
        c.start()
    for c, o in zip(ci, co):
        c.wait()
        o.start()
    for o in co:
        o.wait()


def tail(*arrays):
    hbm = pl.BlockSpec(memory_space=pl.ANY)
    dma = pltpu.SemaphoreType.DMA
    return pl.pallas_call(
        tail_kernel,
        name="tail",
        out_shape=tuple(jax.ShapeDtypeStruct(v.shape, v.dtype) for v in arrays),
        in_specs=[hbm] * 5,
        out_specs=(hbm,) * 5,
        scratch_shapes=[*(pltpu.VMEM(v.shape, v.dtype) for v in arrays), dma((8,)), dma((8,))],
        compiler_params=pltpu.CompilerParams(vmem_limit_bytes=VMEM_LIMIT),
    )(*arrays)


def solution(mesh):
    rows = P(("dp", "tp"), None)
    wsp = P("dp", "tp")
    dsp = P("tp", "dp")

    def local(x, w_gate, w_up, w_down, dy):
        return tail(*fused(x, dy, w_gate, w_up, w_down)[:5])

    return jax.shard_map(local, mesh=mesh, in_specs=(rows, wsp, wsp, dsp, rows), out_specs=(rows, rows, wsp, wsp, dsp), check_vma=False)
```

```python
import jax
import jax.numpy as jnp
from jax import lax
from jax.experimental import pallas as pl
from jax.experimental.pallas import tpu as pltpu
from jax.sharding import PartitionSpec as P

MESH = pl.DeviceIdType.MESH
f32 = jnp.float32
bf = jnp.bfloat16
VMEM_LIMIT = 67043328
sc = jax.named_scope
LAG = 4


def mm(a, b):
    return lax.dot_general(a, b, (((1,), (0,)), ((), ())), preferred_element_type=f32)


def mmt(a, b):
    return lax.dot_general(a, b, (((1,), (1,)), ((), ())), preferred_element_type=f32)


def kernel(
    x_in, dy_in, wg_in, wu_in, wd_in,
    y_out, dx_out, dwg_out, dwu_out, dwd_out, n00, r2, zl, far_r, near, xr1, yr1, stash,
    wg, wu, wd, xa, dya, act, zs, xt, ht, eye, fst, nst, cst,
    gs, gr, lsem, zsend, zrecv, zload, fsend, frecv, nstore, cload, xs1, xq1, ys1, yq1, s2, q2, cin, osem, dsem, ssem,
):
    tp = lax.axis_index("tp")
    dp = lax.axis_index("dp")
    z, y = tp // 2, tp % 2
    x, c = dp // 2, dp % 2
    is_end = (z == 0) | (z == 3)
    is_mid = (z == 1) | (z == 2)
    dev_x = {"tp": tp, "dp": 2 * (1 - x) + c}
    dev_y = {"tp": 2 * z + 1 - y, "dp": dp}
    dev_c = {"tp": tp, "dp": 2 * x + 1 - c}
    dev_a = {"tp": 2 * (z + 1 - 2 * (z % 2)) + y, "dp": dp}
    dev_b = {"tp": 2 * (3 - z) + y, "dp": dp}

    nr, d = x_in.shape
    kd, kf = wg_in.shape
    f = 2 * kf
    hd = kd // 2
    hf = kf // 2

    def end(fn):
        pl.when(is_end)(fn)

    def mid(fn):
        pl.when(is_mid)(fn)

    def nat(r):
        rc, rx = r // 2, r % 2
        return 2 * (x + rx - 2 * x * rx) + c + rc - 2 * c * rc

    def ncol(r):
        return pl.ds(pl.multiple_of(nat(r) * kd, kd), kd)

    def remote(src, dst, ss, rs, dev):
        return pltpu.make_async_remote_copy(
            src_ref=src, dst_ref=dst, send_sem=ss, recv_sem=rs, device_id=dev, device_id_type=MESH
        )

    own = (wg_in, wu_in, wd_in)

    def blk(k, rx, rc, ry, lo=0, n=None):
        d0 = (2 * rc + rx) * kd + lo
        n = kd if n is None else n
        if k < 2:
            return (wg, wu)[k].at[pl.ds(d0, n), pl.ds(ry * kf, kf)]
        return wd.at[pl.ds(ry * kf, kf), pl.ds(d0, n)]

    local = []
    for r in range(4):
        local.append((x_in.at[:, ncol(r)], xa.at[pl.ds(0, nr), pl.ds(r * kd, kd)]))
    for r in range(4):
        local.append((dy_in.at[:, ncol(r)], dya.at[pl.ds(0, nr), pl.ds(r * kd, kd)]))
    for k in range(3):
        local.append((own[k], blk(k, 0, 0, 0)))
    local = [pltpu.make_async_copy(s, t, lsem.at[i]) for i, (s, t) in enumerate(local)]
    for cp in local:
        cp.start()

    bar = pltpu.get_barrier_semaphore()
    for dev in (dev_x, dev_y, dev_c, dev_a, dev_b):
        pl.semaphore_signal(bar, inc=1, device_id=dev, device_id_type=MESH)

    with sc("barrier"):
        pl.semaphore_wait(bar, 5)

    ft = min(256, f)

    def rows(s):
        return pl.ds(s * nr, nr)

    def transpose_x(rx, lo, hi):
        @pl.loop(lo, hi)
        def _(s):
            row = pl.ds(pl.multiple_of(s * nr, nr), nr)
            for rc in range(2):
                for h in range(2):
                    v = mmt(eye[...], xa[row, pl.ds((2 * rc + rx) * kd + h * hd, hd)])
                    xt[rc, pl.ds(h * hd, hd), row] = v.astype(bf)

    def wcopy(i, src, dst, dev):
        return remote(src, dst, gs.at[i], gr.at[i], dev)

    def half(rx, rc, ry, h):
        return blk(2, rx, rc, ry, h * hd, hd)

    ua = 3 * kd // 4
    xo = [wcopy(k, own[k], blk(k, 1, 0, 0), dev_x) for k in range(2)]
    yo = [wcopy(2 + k, own[k], blk(k, 0, 0, 1), dev_y) for k in range(2)]
    co = [wcopy(4 + k, own[k], blk(k, 0, 1, 0), dev_c) for k in range(3)]
    xd = [wcopy(7 + h, wd_in.at[:, pl.ds(h * hd, hd)], half(1, 0, 0, h), dev_x) for h in range(2)]
    yd = [wcopy(9 + h, wd_in.at[:, pl.ds(h * hd, hd)], half(0, 0, 1, h), dev_y) for h in range(2)]
    rg = wcopy(11, blk(0, 0, 0, 1), blk(0, 1, 0, 1), dev_x)
    rua = wcopy(12, blk(1, 1, 0, 0, 0, ua), blk(1, 1, 0, 1, 0, ua), dev_y)
    rub = wcopy(13, blk(1, 0, 0, 1, ua, kd - ua), blk(1, 1, 0, 1, ua, kd - ua), dev_x)
    rd = [wcopy(14 + h, half(1, 0, 0, h), half(1, 0, 1, h), dev_y) for h in range(2)]
    cx = [wcopy(16 + k, blk(k, 1, 0, 0), blk(k, 1, 1, 0), dev_c) for k in range(2)]
    cy = [wcopy(18 + k, blk(k, 0, 0, 1), blk(k, 0, 1, 1), dev_c) for k in range(2)]
    cxd = [wcopy(20 + h, half(1, 0, 0, h), half(1, 1, 0, h), dev_c) for h in range(2)]
    cyd = [wcopy(22 + h, half(0, 0, 1, h), half(0, 1, 1, h), dev_c) for h in range(2)]
    crg = wcopy(24, blk(0, 1, 0, 1), blk(0, 1, 1, 1), dev_c)
    crua = wcopy(25, blk(1, 1, 0, 1, 0, ua), blk(1, 1, 1, 1, 0, ua), dev_c)
    crub = wcopy(26, blk(1, 1, 0, 1, ua, kd - ua), blk(1, 1, 1, 1, ua, kd - ua), dev_c)
    crd = [wcopy(27 + h, half(1, 0, 1, h), half(1, 1, 1, h), dev_c) for h in range(2)]
    wcopies = (*xo, *yo, *co, *xd, *yd, rg, rua, rub, *rd, *cx, *cy, *cxd, *cyd, crg, crua, crub, *crd)
    nw = 31

    def slot(j, s):
        return (xa, dya)[j].at[pl.ds(s * nr, nr)]

    def acopy(src, dst, j):
        return remote(
            slot(j, src), slot(j, dst), gs.at[nw + 2 * dst + j], gr.at[nw + 2 * dst + j], dev_a
        )

    def bcopy(src, dst, j):
        return remote(
            slot(j, src), slot(j, dst), gs.at[nw + 8 + 2 * dst + j], gr.at[nw + 2 * dst + j], dev_b
        )

    def got(s, j):
        acopy(s, s, j).wait_recv()

    def stash_copy(s, p, n):
        return pltpu.make_async_copy((fst, nst)[n].at[p, pl.ds(0, nr)], stash.at[s, p, n], ssem.at[2 * p + n])

    def factor(s, n):
        return nst if n else cst if s == 3 else fst

    def stash_load(s, p, n):
        return pltpu.make_async_copy(stash.at[s, p, n], factor(s, n).at[p, pl.ds(0, nr)], ssem.at[2 * p + n])

    pending = [None, None]

    def flush(p):
        if pending[p] is not None:
            for n in range(2):
                stash_copy(pending[p], p, n).wait()
        pending[p] = None

    def ab_tiles(s, p, step):
        @pl.loop(0, kf // ft)
        def _(i):
            col = pl.ds(pl.multiple_of(p * kf + i * ft, ft), ft)
            at = (p, pl.ds(0, nr), pl.ds(pl.multiple_of(i * ft, ft), ft))

            def some_b(rx):
                b0, b1 = pl.ds(rx * kd, kd), pl.ds((2 + rx) * kd, kd)
                return mm(xa[rows(s), b0], wu[b0, col]) + mm(xa[rows(s), b1], wu[b1, col])

            if step == 1:
                fst[at] = mm(xa[rows(s), :], wg[:, col])
                nst[at] = some_b(0)
                return
            if step == 2:
                a = fst[at]
                b = nst[at] + some_b(1)
            else:
                a = mm(xa[rows(s), :], wg[:, col])
                b = mm(xa[rows(s), :], wu[:, col])
            sig = jax.nn.sigmoid(a)
            sa = a * sig
            act[2, rows(s), col] = (sa * b).astype(bf)
            fst[at] = sa
            nst[at] = b * sig * (1.0 + a * (1.0 - sig))

    def part_ab(s, p, step=0):
        with sc(f"ab{s}_{p}"):
            flush(p)
            ab_tiles(s, p, step)
            if step != 1:
                for n in range(2):
                    stash_copy(s, p, n).start()
                pending[p] = s

    gt = min(512, kf)

    def part_g(s, p):
        @pl.loop(0, kf // gt)
        def _(i):
            col = pl.ds(pl.multiple_of(p * kf + i * gt, gt), gt)
            kcol = pl.ds(pl.multiple_of(i * gt, gt), gt)
            g = mmt(dya[rows(s), :], wd[col, :])
            act[0, rows(s), col] = (g * factor(s, 1)[p, pl.ds(0, nr), kcol]).astype(bf)
            act[1, rows(s), col] = (g * factor(s, 0)[p, pl.ds(0, nr), kcol]).astype(bf)

    def gload(s):
        for p in range(2):
            for n in range(2):
                stash_load(s, p, n).start()

    def half_g(s, p, then):
        with sc(f"g{s}_{p}"):
            for n in range(2):
                stash_load(s, p, n).wait()
            part_g(s, p)
            if then is not None:
                for n in range(2):
                    stash_load(then, p, n).start()

    def front_g(s, then):
        for p in range(2):
            half_g(s, p, then)

    def keep_h(s):
        hb = min(4, f // hd)
        with sc(f"ht{s}"):
            @pl.loop(0, f // (hb * hd))
            def _(i):
                for q in range(hb):
                    col = pl.ds(pl.multiple_of((i * hb + q) * hd, hd), hd)
                    ht[col, rows(s)] = mmt(eye[...], act[2, rows(s), col]).astype(bf)

    def back(kind, s, r):
        col = pl.ds(pl.multiple_of(r * kd, kd), kd)
        if kind == 0:
            return mm(act[2, rows(s), :], wd[:, col])
        return mmt(act[0, rows(s), :], wg[col, :]) + mmt(act[1, rows(s), :], wu[col, :])

    def zcopy(q, kind, r, half, dev):
        i = 4 * kind + r
        return remote(zs.at[4 * half + r], zl.at[q, i], zsend.at[4 * half + r], zrecv.at[q, i], dev)

    def zload_(q, kind, r, slot):
        return pltpu.make_async_copy(zl.at[q, 4 * kind + r], cst.at[slot, pl.ds(0, nr), pl.ds(0, kd)], zload.at[slot])

    def chunk(kind, s, r, half, q_add, first):
        i = 4 * half + r
        if q_add is not None:
            with sc("zrecv"):
                zcopy(q_add, kind, r, half, dev_a).wait_recv()
            zload_(q_add, kind, r, r % 2).start()
        if not first:
            with sc("zsend"):
                zcopy(0, kind, r, half, dev_a).wait_send()
        zs[i] = back(kind, s, r)
        if q_add is not None:
            zload_(q_add, kind, r, r % 2).wait()
            zs[i] = zs[i] + cst[r % 2, pl.ds(0, nr), pl.ds(0, kd)]

    def jobs(*specs):
        with sc("job" + "_".join(f"{kind}{s}" for kind, s, *_ in specs)):
            @pl.loop(0, 4)
            def _(r):
                for kind, s, h, q_add, q_dst, dev, first in specs:
                    chunk(kind, s, r, h, q_add, first)
                    zcopy(q_dst, kind, r, h, dev).start()

    def store(kind, r):
        res, out = ((xa, y_out), (dya, dx_out))[kind]
        col = pl.ds(pl.multiple_of(r * kd, kd), kd)
        return pltpu.make_async_copy(res.at[rows(1), col], out.at[:, ncol(r)], osem.at[4 * kind + r])

    def finish(kind, adds, lo=0, hi=4):
        res = (xa, dya)[kind]
        with sc(f"fin{kind}"):
            @pl.loop(lo, hi)
            def _(r):
                col = pl.ds(pl.multiple_of(r * kd, kd), kd)
                part = (pl.ds(0, nr), pl.ds(0, kd))
                nst[0, *part] = back(kind, 0, r)
                for n, q in enumerate(adds):
                    with sc("finrecv"):
                        zcopy(q, kind, r, 0, dev_a).wait_recv()
                    zload_(q, kind, r, n).start()
                for n, q in enumerate(adds):
                    zload_(q, kind, r, n).wait()
                v = nst[0, *part] + res[rows(0), col].astype(f32)
                for n in range(len(adds)):
                    v = v + cst[n, *part]
                res[rows(1), col] = v.astype(bf)
                store(kind, r).start()

    def unit(rc, rx, j, put):
        ryi, k, half = j // 6, ((j // 2) % 3 + 2) % 3, j % 2
        f0 = (1 - ryi) * kf

        @pl.when(k < 2)
        def _():
            a = xt[rc, pl.ds(pl.multiple_of(half * hd, hd), hd), :]
            for q in range(2):
                b = act[k, :, pl.ds(pl.multiple_of(f0 + q * kd, kd), kd)]
                put(pl.ds(q * kd, kd), mm(a, b))

        @pl.when(k == 2)
        def _():
            b = dya[:, pl.ds((2 * rc + rx) * kd, kd)]
            for q in range(2):
                a = ht[pl.ds(pl.multiple_of(f0 + half * hf + q * hd, hd), hd), :]
                put(pl.ds(q * kd, kd), mm(a, b))

    def fcopy(u):
        return remote(fst.at[u % 3], far_r.at[u], fsend.at[u % 3], frecv.at[u], dev_c)

    def ncopy(u):
        return pltpu.make_async_copy(nst.at[u % 2], near.at[u], nstore.at[u % 2])

    def ccopy(u):
        return pltpu.make_async_copy(far_r.at[u], cst.at[u % 2], cload.at[u % 2])

    def xcopy1(i, u):
        return remote(near.at[u], xr1.at[i], xs1.at[i], xq1.at[i], dev_x)

    def ycopy1(i, u):
        return remote(near.at[u], yr1.at[i], ys1.at[i], yq1.at[i], dev_y)

    def nsend(rx, j):
        ryi, k, half = j // 6, (j // 2) % 3, j % 2
        u = 12 * (1 - rx) + j
        if rx:
            @pl.when(half == 0)
            def _():
                xcopy1(ryi * 3 + k, u).start()

        @pl.when((half == 1) & (ryi == 0))
        def _():
            ycopy1(3 * (1 - rx) + k, u).start()

    def far_unit(rx, j):
        u = 12 * (1 - rx) + j

        @pl.when(u > 2)
        def _():
            with sc("fsend"):
                fcopy(u).wait_send()

        def put(col, v):
            fst[u % 3, :, col] = v

        unit(1, rx, j, put)
        fcopy(u).start()

    def dw_first(rx, n):
        with sc("dwfirst"):
            @pl.loop(0, n)
            def _(j):
                far_unit(rx, j)

    def dw(rx, first):
        base = 12 * (1 - rx)

        with sc(f"dw{rx}"):
            @pl.loop(first, 12 + LAG)
            def _(j):
                w = base + j - LAG

                @pl.when(j < 12)
                def _():
                    far_unit(rx, j)

                @pl.when((j >= LAG - 1) & (j < 11 + LAG))
                def _():
                    with sc("frecv"):
                        fcopy(w + 1).wait_recv()
                    ccopy(w + 1).start()

                @pl.when(j >= LAG)
                def _():
                    with sc("cwait"):
                        ccopy(w).wait()

                    def put(col, v):
                        nst[w % 2, :, col] = v + cst[w % 2, :, col]

                    unit(0, rx, j - LAG, put)

                    @pl.when(j > LAG)
                    def _():
                        with sc("nwait"):
                            ncopy(w - 1).wait()
                        nsend(rx, j - LAG - 1)

                    ncopy(w).start()

            ncopy(base + 11).wait()
            nsend(rx, 11)

    def add_pair(units, waits, arrived, dsts, after=(None, None)):
        cn = [pltpu.make_async_copy(near.at[u], fst.at[h], cin.at[h]) for h, u in enumerate(units)]
        cr = [pltpu.make_async_copy(v, cst.at[h], cload.at[h]) for h, v in enumerate(arrived)]
        cd = [pltpu.make_async_copy(nst.at[h], t, nstore.at[h]) for h, t in enumerate(dsts)]
        st = min(64, hd)
        for h in range(2):
            cn[h].start()
        for h in range(2):
            waits[h].wait_recv()
            cr[h].start()
        for h in range(2):
            cn[h].wait()
            cr[h].wait()

            @pl.loop(0, hd // st)
            def _(i):
                row = pl.ds(pl.multiple_of(i * st, st), st)
                nst[h, row, :] = fst[h, row, :] + cst[h, row, :]

            cd[h].start()
        for h in range(2):
            cd[h].wait()
            if after[h] is not None:
                after[h].start()

    def uid(rx, ry, k, half):
        return 12 * (1 - rx) + 6 * (1 - ry) + 2 * k + half

    def ycopy2(k):
        return remote(near.at[uid(0, 1, k, 0)], r2.at[2 * k], s2.at[2 * k], q2.at[2 * k], dev_y)

    def xcopy2(k):
        return remote(near.at[uid(1, 0, k, 1)], r2.at[2 * k + 1], s2.at[2 * k + 1], q2.at[2 * k + 1], dev_x)

    def second(k):
        ua, ub = uid(0, 1, k, 0), uid(1, 0, k, 1)
        with sc(f"second{k}"):
            add_pair(
                (ua, ub), (xcopy1(k, 0), ycopy1(k, 0)), (xr1.at[k], yr1.at[k]), (near.at[ua], near.at[ub]),
                (ycopy2(k), xcopy2(k)),
            )

    def third(k):
        ua, ub = uid(0, 0, k, 0), uid(0, 0, k, 1)
        with sc(f"third{k}"):
            add_pair(
                (ua, ub), (xcopy1(3 + k, 0), ycopy1(3 + k, 0)), (xr1.at[3 + k], yr1.at[3 + k]),
                (n00.at[2 * k], n00.at[2 * k + 1]),
            )

    def fourth(k):
        units = (n00.at[2 * k], n00.at[2 * k + 1])
        if k > 0:
            dsts = [[((dwg_out, dwu_out)[k - 1].at[pl.ds(h * hd, hd)], pl.ds(0, kf))] for h in range(2)]
        else:
            dsts = [[(dwd_out.at[pl.ds((2 * h + q) * hd, hd)], pl.ds(q * kd, kd)) for q in range(2)] for h in range(2)]
        cn = [pltpu.make_async_copy(u, fst.at[h], cin.at[h]) for h, u in enumerate(units)]
        cr = [pltpu.make_async_copy(r2.at[2 * k + h], cst.at[h], cload.at[h]) for h in range(2)]
        cd = [
            [pltpu.make_async_copy(nst.at[h, :, col], t, dsem.at[h, n]) for n, (t, col) in enumerate(dsts[h])]
            for h in range(2)
        ]
        st = min(64, hd)
        with sc(f"fourth{k}"):
            for h in range(2):
                cn[h].start()
            for h in range(2):
                (ycopy2, xcopy2)[h](k).wait_recv()
                cr[h].start()
            for h in range(2):
                cn[h].wait()
                cr[h].wait()

                @pl.loop(0, hd // st)
                def _(i):
                    row = pl.ds(pl.multiple_of(i * st, st), st)
                    nst[h, row, :] = fst[h, row, :] + cst[h, row, :]

                for cp in cd[h]:
                    cp.start()
            for h in range(2):
                for cp in cd[h]:
                    cp.wait()

    for k in range(2):
        xo[k].start()
        yo[k].start()
    yd[0].start()
    with sc("rows_in"):
        for cp in local[:8]:
            cp.wait()
    for j in range(2):
        acopy(0, 1, j).start()

    @mid
    def _():
        for j in range(2):
            bcopy(0, 2, j).start()

    for k in range(3):
        co[k].start()

    eye[...] = (
        lax.broadcasted_iota(jnp.int32, (hd, hd), 0) == lax.broadcasted_iota(jnp.int32, (hd, hd), 1)
    ).astype(f32).astype(bf)

    with sc("xt0"):
        transpose_x(1, 0, 1)

    def pass_on(s, j):
        with sc(f"rows{s}_{j}"):
            got(s, j)
        if s == 1:
            bcopy(1, 3, j).start()
        else:
            acopy(s, s, j).start()

    with sc("gx0"):
        xo[0].wait_recv()
        cx[0].start()
        yo[0].wait_recv()
    rg.start()
    cy[0].start()

    @mid
    def _():
        pass_on(1, 0)
        pass_on(2, 0)

    with sc("gx1"):
        xo[1].wait_recv()
        rua.start()
        yd[1].start()
        cx[1].start()
        yo[1].wait_recv()
    rub.start()
    for h in range(2):
        xd[h].start()
    cy[1].start()

    @mid
    def _():
        pass_on(1, 1)
        pass_on(2, 1)

    @end
    def _():
        with sc("e_rows1"):
            got(1, 0)

    for cp in local[8:]:
        cp.wait()
    with sc("gc0"):
        for cp in (*co[:2], *cx):
            cp.wait_recv()
    part_ab(1, 0)
    part_ab(0, 0)
    with sc("gyd"):
        yd[0].wait_recv()
        cyd[0].start()
        rg.wait_recv()
        crg.start()
    with sc("gc1"):
        for cp in (*cy, crg):
            cp.wait_recv()
    part_ab(1, 1, 1)

    @mid
    def _():
        pass_on(3, 0)

    with sc("gru"):
        rua.wait_recv()
        crua.start()
        rub.wait_recv()
        crub.start()
    with sc("gc2"):
        for cp in (crua, crub):
            cp.wait_recv()
    part_ab(1, 1, 2)
    with sc("gc3"):
        for cp in (co[2], cyd[0]):
            cp.wait_recv()

    def early_half(h):
        with sc(f"early1_{h}"):
            @pl.loop(0, 2)
            def _(i):
                r = 2 * i
                col = pl.ds(h * hd, hd)
                v = mm(act[2, rows(1), :], wd[:, pl.ds(pl.multiple_of(r * kd + h * hd, hd), hd)])
                zs[r, :, col] = v
                remote(zs.at[r, :, col], zl.at[0, r, :, col], zsend.at[r], zrecv.at[0, r], dev_a).start()

    def early(s, odd):
        with sc(f"early{s}_{odd}"):
            @pl.loop(0, 2)
            def _(i):
                r = 2 * i + odd
                chunk(0, s, r, s - 1, None, True)
                zcopy(s - 1, 0, r, s - 1, dev_a).start()

    @end
    def _():
        early_half(0)
        with sc("e_rows2"):
            got(2, 0)

    part_ab(2, 0)
    with sc("gd0"):
        yd[1].wait_recv()
        cyd[1].start()
        xd[0].wait_recv()
        rd[0].start()
        cxd[0].start()
        cyd[1].wait_recv()

    @end
    def _():
        early_half(1)

    part_ab(2, 1)

    @end
    def _():
        early(2, 0)

    @mid
    def _():
        pass_on(3, 1)

    with sc("gd1"):
        xd[1].wait_recv()
        rd[1].start()
        cxd[1].start()
    part_ab(0, 1)
    with sc("gd2"):
        rd[0].wait_recv()
        crd[0].start()
    transpose_x(1, 1, 3)
    keep_h(1)
    keep_h(0)
    keep_h(2)
    with sc("gd3"):
        rd[1].wait_recv()
        crd[1].start()
        for cp in (*cxd, *crd):
            cp.wait_recv()

    @end
    def _():
        early(1, 1)
        early(2, 1)
        got(1, 1)
        got(2, 1)
        with sc("e_rows3"):
            got(3, 0)

    part_ab(3, 0)
    part_ab(3, 1)
    flush(0)
    flush(1)
    gload(1)
    transpose_x(1, 3, 4)
    keep_h(3)
    front_g(1, 0)
    front_g(0, 2)
    front_g(2, 3)

    @end
    def _():
        with sc("e_rows3"):
            got(3, 1)

    dw_first(1, 2)
    half_g(3, 1, None)
    half_g(3, 0, None)
    dw(1, 2)

    @end
    def _():
        jobs((0, 3, 0, None, 2, dev_a, False))

    @mid
    def _():
        jobs((0, 2, 0, 1, 3, dev_b, True))

    with sc("xtb"):
        transpose_x(0, 0, 4)
    dw(0, 0)
    for u in range(3):
        fcopy(u).wait_send()
    for cp in wcopies:
        cp.wait_send()
    for j in range(2):
        acopy(0, 1, j).wait_send()

    @mid
    def _():
        for j in range(2):
            bcopy(0, 2, j).wait_send()
            bcopy(1, 3, j).wait_send()
            acopy(2, 2, j).wait_send()
            acopy(3, 3, j).wait_send()

    @end
    def _():
        jobs((1, 3, 1, None, 2, dev_a, False))
        second(0)
        second(1)
        second(2)
        jobs((1, 2, 0, None, 1, dev_a, False))
        third(0)
        third(1)
        jobs((1, 1, 1, None, 0, dev_a, False))
        third(2)
        finish(0, (0,))
        fourth(0)
        finish(1, (0,), 0, 2)
        fourth(1)
        finish(1, (0,), 2, 4)
        fourth(2)

    @mid
    def _():
        jobs((0, 3, 1, 2, 4, dev_b, True))
        second(0)
        second(1)
        second(2)
        jobs((0, 1, 0, 4, 0, dev_a, False), (1, 3, 1, 2, 4, dev_b, False))
        third(0)
        third(1)
        jobs((1, 1, 0, 4, 0, dev_a, False), (1, 2, 1, 1, 3, dev_b, False))
        third(2)
        finish(0, (0, 3))
        fourth(0)
        fourth(1)
        finish(1, (0, 3), 0, 3)
        fourth(2)
        finish(1, (0, 3), 3, 4)

    for kind in range(2):
        for r in range(4):
            store(kind, r).wait()
    with sc("drain"):
        for half in range(2):
            for r in range(4):
                zcopy(0, 0, r, half, dev_a).wait_send()
        for i in range(6):
            xcopy1(i, 0).wait_send()
            ycopy1(i, 0).wait_send()
        for k in range(3):
            ycopy2(k).wait_send()
            xcopy2(k).wait_send()


def fused(x, dy, wg, wu, wd):
    nr, d = x.shape
    kd, kf = wg.shape
    f, hd = 2 * kf, kd // 2
    hbm = pl.BlockSpec(memory_space=pl.ANY)
    sds = jax.ShapeDtypeStruct
    out_shape = (
        sds((nr, d), bf), sds((nr, d), bf), sds((kd, kf), f32), sds((kd, kf), f32), sds((kf, kd), f32),
        sds((6, hd, kf), f32), sds((6, hd, kf), f32),
        sds((5, 8, nr, kd), f32), sds((24, hd, kf), f32), sds((24, hd, kf), f32),
        sds((6, hd, kf), f32), sds((6, hd, kf), f32), sds((4, 2, 2, nr, kf), f32),
    )
    dma = pltpu.SemaphoreType.DMA
    return pl.pallas_call(
        kernel,
        name="fused",
        out_shape=out_shape,
        in_specs=[hbm] * 5,
        out_specs=(hbm,) * len(out_shape),
        scratch_shapes=[
            pltpu.VMEM((d, f), bf), pltpu.VMEM((d, f), bf), pltpu.VMEM((f, d), bf),
            pltpu.VMEM((4 * nr, d), bf), pltpu.VMEM((4 * nr, d), bf), pltpu.VMEM((3, 4 * nr, f), bf),
            pltpu.VMEM((8, nr, kd), f32), pltpu.VMEM((2, kd, 4 * nr), bf), pltpu.VMEM((f, 4 * nr), bf),
            pltpu.VMEM((hd, hd), bf),
            pltpu.VMEM((3, hd, kf), f32), pltpu.VMEM((2, hd, kf), f32), pltpu.VMEM((2, hd, kf), f32),
            dma((47,)), dma((39,)), dma((11,)), dma((8,)), dma((5, 8)), dma((2,)), dma((3,)), dma((24,)), dma((2,)),
            dma((2,)), dma((6,)), dma((6,)), dma((6,)), dma((6,)), dma((6,)), dma((6,)), dma((2,)), dma((8,)), dma((2, 2)), dma((4,)),
        ],
        compiler_params=pltpu.CompilerParams(collective_id=0, has_side_effects=True, vmem_limit_bytes=VMEM_LIMIT),
    )(x, dy, wg, wu, wd)


def tail_kernel(*refs):
    n = 5
    src, dst, buf, (si, so) = refs[:n], refs[n : 2 * n], refs[2 * n : 3 * n], refs[3 * n :]
    pieces = [(i, h) for i in range(n) for h in range(1 if i < 2 else 2)]

    def part(r, h, i):
        m = r.shape[0] // (1 if i < 2 else 2)
        return r.at[pl.ds(h * m, m)]

    ci = [pltpu.make_async_copy(part(src[i], h, i), part(buf[i], h, i), si.at[j]) for j, (i, h) in enumerate(pieces)]
    co = [pltpu.make_async_copy(part(buf[i], h, i), part(dst[i], h, i), so.at[j]) for j, (i, h) in enumerate(pieces)]
    for c in ci:
        c.start()
    for c, o in zip(ci, co):
        c.wait()
        o.start()
    for o in co:
        o.wait()


def tail(*arrays):
    hbm = pl.BlockSpec(memory_space=pl.ANY)
    dma = pltpu.SemaphoreType.DMA
    return pl.pallas_call(
        tail_kernel,
        name="tail",
        out_shape=tuple(jax.ShapeDtypeStruct(v.shape, v.dtype) for v in arrays),
        in_specs=[hbm] * 5,
        out_specs=(hbm,) * 5,
        scratch_shapes=[*(pltpu.VMEM(v.shape, v.dtype) for v in arrays), dma((8,)), dma((8,))],
        compiler_params=pltpu.CompilerParams(vmem_limit_bytes=VMEM_LIMIT),
    )(*arrays)


def solution(mesh):
    rows = P(("dp", "tp"), None)
    wsp = P("dp", "tp")
    dsp = P("tp", "dp")

    def local(x, w_gate, w_up, w_down, dy):
        return tail(*fused(x, dy, w_gate, w_up, w_down)[:5])

    return jax.shard_map(local, mesh=mesh, in_specs=(rows, wsp, wsp, dsp, rows), out_specs=(rows, rows, wsp, wsp, dsp), check_vma=False)
```

```python
import jax
import jax.numpy as jnp
from jax import lax
from jax.experimental import pallas as pl
from jax.experimental.pallas import tpu as pltpu
from jax.sharding import PartitionSpec as P

MESH = pl.DeviceIdType.MESH
f32 = jnp.float32
bf = jnp.bfloat16
VMEM_LIMIT = 67043328
sc = jax.named_scope
LAG = 4


def mm(a, b):
    return lax.dot_general(a, b, (((1,), (0,)), ((), ())), preferred_element_type=f32)


def mmt(a, b):
    return lax.dot_general(a, b, (((1,), (1,)), ((), ())), preferred_element_type=f32)


def natural(dp, r, kd):
    x, c, rc, rx = dp // 2, dp % 2, r // 2, r % 2
    n = 2 * (x + rx - 2 * x * rx) + c + rc - 2 * c * rc
    return pl.ds(pl.multiple_of(n * kd, kd), kd)


def kernel(
    x_in, dy_in, wg_in, wu_in, wd_in,
    xa, dya, dwv, n00, r2, zl, far_r, near, xr1, yr1, stash,
    wg, wu, wd, act, zs, xt, ht, eye, cst,
    gs, gr, lsem, zsend, zrecv, zload, fsend, frecv, nstore, cload, xs1, xq1, ys1, yq1, s2, q2, cin, ssem,
):
    tp = lax.axis_index("tp")
    dp = lax.axis_index("dp")
    z, y = tp // 2, tp % 2
    x, c = dp // 2, dp % 2
    is_end = (z == 0) | (z == 3)
    is_mid = (z == 1) | (z == 2)
    dev_x = {"tp": tp, "dp": 2 * (1 - x) + c}
    dev_y = {"tp": 2 * z + 1 - y, "dp": dp}
    dev_c = {"tp": tp, "dp": 2 * x + 1 - c}
    dev_a = {"tp": 2 * (z + 1 - 2 * (z % 2)) + y, "dp": dp}
    dev_b = {"tp": 2 * (3 - z) + y, "dp": dp}

    fst, nst = dwv.at[pl.ds(0, 3)], dwv.at[pl.ds(3, 2)]
    nr, d = x_in.shape
    kd, kf = wg_in.shape
    f = 2 * kf
    hd = kd // 2
    hf = kf // 2

    def end(fn):
        pl.when(is_end)(fn)

    def mid(fn):
        pl.when(is_mid)(fn)

    def ncol(r):
        return natural(dp, r, kd)

    def remote(src, dst, ss, rs, dev):
        return pltpu.make_async_remote_copy(
            src_ref=src, dst_ref=dst, send_sem=ss, recv_sem=rs, device_id=dev, device_id_type=MESH
        )

    own = (wg_in, wu_in, wd_in)

    def blk(k, rx, rc, ry, lo=0, n=None):
        d0 = (2 * rc + rx) * kd + lo
        n = kd if n is None else n
        if k < 2:
            return (wg, wu)[k].at[pl.ds(d0, n), pl.ds(ry * kf, kf)]
        return wd.at[pl.ds(ry * kf, kf), pl.ds(d0, n)]

    local = [(own[k], blk(k, 0, 0, 0)) for k in range(3)]
    for src, ref in ((x_in, xa), (dy_in, dya)):
        for r in range(4):
            local.append((src.at[:, ncol(r)], ref.at[pl.ds(0, nr), pl.ds(r * kd, kd)]))
    local = [pltpu.make_async_copy(s, t, lsem.at[i]) for i, (s, t) in enumerate(local)]
    for cp in local:
        cp.start()

    bar = pltpu.get_barrier_semaphore()
    for dev in (dev_x, dev_y, dev_c, dev_a, dev_b):
        pl.semaphore_signal(bar, inc=1, device_id=dev, device_id_type=MESH)

    with sc("barrier"):
        pl.semaphore_wait(bar, 5)

    ft = min(256, f)

    def rows(s):
        return pl.ds(s * nr, nr)

    def transpose_x(rx, lo, hi):
        @pl.loop(lo, hi)
        def _(s):
            row = pl.ds(pl.multiple_of(s * nr, nr), nr)
            for rc in range(2):
                for h in range(2):
                    v = mmt(eye[...], xa[row, pl.ds((2 * rc + rx) * kd + h * hd, hd)])
                    xt[rc, pl.ds(h * hd, hd), row] = v.astype(bf)

    def wcopy(i, src, dst, dev):
        return remote(src, dst, gs.at[i], gr.at[i], dev)

    def half(rx, rc, ry, h):
        return blk(2, rx, rc, ry, h * hd, hd)

    ua = 3 * kd // 4
    mine = [blk(k, 0, 0, 0) for k in range(3)]
    xo = [wcopy(k, mine[k], blk(k, 1, 0, 0), dev_x) for k in range(2)]
    yo = [wcopy(2 + k, mine[k], blk(k, 0, 0, 1), dev_y) for k in range(2)]
    co = [wcopy(4 + k, mine[k], blk(k, 0, 1, 0), dev_c) for k in range(3)]
    xd = [wcopy(7 + h, half(0, 0, 0, h), half(1, 0, 0, h), dev_x) for h in range(2)]
    yd = [wcopy(9 + h, half(0, 0, 0, h), half(0, 0, 1, h), dev_y) for h in range(2)]
    rg = wcopy(11, blk(0, 0, 0, 1), blk(0, 1, 0, 1), dev_x)
    cuts = ((0, 2 * kd // 4), (2 * kd // 4, ua))
    rua = [wcopy(i, blk(1, 1, 0, 0, lo, hi - lo), blk(1, 1, 0, 1, lo, hi - lo), dev_y) for i, (lo, hi) in zip((12, 29), cuts)]
    rub = wcopy(13, blk(1, 0, 0, 1, ua, kd - ua), blk(1, 1, 0, 1, ua, kd - ua), dev_x)
    rd = [wcopy(14 + h, half(1, 0, 0, h), half(1, 0, 1, h), dev_y) for h in range(2)]
    cx = [wcopy(16 + k, blk(k, 1, 0, 0), blk(k, 1, 1, 0), dev_c) for k in range(2)]
    cy = [wcopy(18 + k, blk(k, 0, 0, 1), blk(k, 0, 1, 1), dev_c) for k in range(2)]
    cxd = [wcopy(20 + h, half(1, 0, 0, h), half(1, 1, 0, h), dev_c) for h in range(2)]
    cyd = [wcopy(22 + h, half(0, 0, 1, h), half(0, 1, 1, h), dev_c) for h in range(2)]
    crg = wcopy(24, blk(0, 1, 0, 1), blk(0, 1, 1, 1), dev_c)
    crua = [wcopy(i, blk(1, 1, 0, 1, lo, hi - lo), blk(1, 1, 1, 1, lo, hi - lo), dev_c) for i, (lo, hi) in zip((25, 30), cuts)]
    crub = wcopy(26, blk(1, 1, 0, 1, ua, kd - ua), blk(1, 1, 1, 1, ua, kd - ua), dev_c)
    crd = [wcopy(27 + h, half(1, 0, 1, h), half(1, 1, 1, h), dev_c) for h in range(2)]
    wcopies = (*xo, *yo, *co, *xd, *yd, rg, *rua, rub, *rd, *cx, *cy, *cxd, *cyd, crg, *crua, crub, *crd)
    nw = 31

    def slot(j, s):
        return (xa, dya)[j].at[pl.ds(s * nr, nr)]

    def acopy(src, dst, j):
        return remote(
            slot(j, src), slot(j, dst), gs.at[nw + 2 * dst + j], gr.at[nw + 2 * dst + j], dev_a
        )

    def bcopy(src, dst, j):
        return remote(
            slot(j, src), slot(j, dst), gs.at[nw + 8 + 2 * dst + j], gr.at[nw + 2 * dst + j], dev_b
        )

    def got(s, j):
        acopy(s, s, j).wait_recv()

    def stash_copy(s, p, n):
        return pltpu.make_async_copy((fst, nst)[n].at[p, pl.ds(0, nr)], stash.at[s, p, n], ssem.at[2 * p + n])

    def factor(s, n):
        return nst if n else cst if s == 3 else fst

    def stash_load(s, p, n):
        return pltpu.make_async_copy(stash.at[s, p, n], factor(s, n).at[p, pl.ds(0, nr)], ssem.at[2 * p + n])

    pending = [None, None]

    def flush(p):
        if pending[p] is not None:
            for n in range(2):
                stash_copy(pending[p], p, n).wait()
        pending[p] = None

    def ab_tiles(s, p, step):
        @pl.loop(0, kf // ft)
        def _(i):
            col = pl.ds(pl.multiple_of(p * kf + i * ft, ft), ft)
            at = (p, pl.ds(0, nr), pl.ds(pl.multiple_of(i * ft, ft), ft))

            def some_b(rx):
                b0, b1 = pl.ds(rx * kd, kd), pl.ds((2 + rx) * kd, kd)
                return mm(xa[rows(s), b0], wu[b0, col]) + mm(xa[rows(s), b1], wu[b1, col])

            if step == 1:
                fst[at] = mm(xa[rows(s), :], wg[:, col])
                nst[at] = some_b(0)
                return
            if step == 2:
                a = fst[at]
                b = nst[at] + some_b(1)
            else:
                a = mm(xa[rows(s), :], wg[:, col])
                b = mm(xa[rows(s), :], wu[:, col])
            sig = jax.nn.sigmoid(a)
            sa = a * sig
            act[2, rows(s), col] = (sa * b).astype(bf)
            fst[at] = sa
            nst[at] = b * sig * (1.0 + a * (1.0 - sig))

    def part_ab(s, p, step=0):
        with sc(f"ab{s}_{p}"):
            flush(p)
            ab_tiles(s, p, step)
            if step != 1:
                for n in range(2):
                    stash_copy(s, p, n).start()
                pending[p] = s

    gt = min(512, kf)

    def part_g(s, p):
        @pl.loop(0, kf // gt)
        def _(i):
            col = pl.ds(pl.multiple_of(p * kf + i * gt, gt), gt)
            kcol = pl.ds(pl.multiple_of(i * gt, gt), gt)
            g = mmt(dya[rows(s), :], wd[col, :])
            act[0, rows(s), col] = (g * factor(s, 1)[p, pl.ds(0, nr), kcol]).astype(bf)
            act[1, rows(s), col] = (g * factor(s, 0)[p, pl.ds(0, nr), kcol]).astype(bf)

    def gload(s):
        for p in range(2):
            for n in range(2):
                stash_load(s, p, n).start()

    def half_g(s, p, then):
        with sc(f"g{s}_{p}"):
            for n in range(2):
                stash_load(s, p, n).wait()
            part_g(s, p)
            if then is not None:
                for n in range(2):
                    stash_load(then, p, n).start()

    def front_g(s, then):
        for p in range(2):
            half_g(s, p, then)

    def keep_h(s):
        hb = min(4, f // hd)
        with sc(f"ht{s}"):
            @pl.loop(0, f // (hb * hd))
            def _(i):
                for q in range(hb):
                    col = pl.ds(pl.multiple_of((i * hb + q) * hd, hd), hd)
                    ht[col, rows(s)] = mmt(eye[...], act[2, rows(s), col]).astype(bf)

    def back(ref, at, kind, s, r):
        *lead, col = at
        for h in range(2):
            n = pl.ds(pl.multiple_of(r * kd + h * hd, hd), hd)
            if kind == 0:
                v = mm(act[2, rows(s), :], wd[:, n])
            else:
                v = mmt(act[0, rows(s), :], wg[n, :]) + mmt(act[1, rows(s), :], wu[n, :])
            ref[(*lead, pl.ds(0, nr), pl.ds(col + h * hd, hd))] = v

    def zcopy(q, kind, r, half, dev):
        i = 4 * kind + r
        return remote(zs.at[4 * half + r], zl.at[q, i], zsend.at[4 * half + r], zrecv.at[q, i], dev)

    def zload_(q, kind, r, slot):
        return pltpu.make_async_copy(zl.at[q, 4 * kind + r], cst.at[slot, pl.ds(0, nr), pl.ds(0, kd)], zload.at[slot])

    def chunk(kind, s, r, half, q_add, first):
        i = 4 * half + r
        if q_add is not None:
            with sc("zrecv"):
                zcopy(q_add, kind, r, half, dev_a).wait_recv()
            zload_(q_add, kind, r, r % 2).start()
        if not first:
            with sc("zsend"):
                zcopy(0, kind, r, half, dev_a).wait_send()
        back(zs, (i, 0), kind, s, r)
        if q_add is not None:
            zload_(q_add, kind, r, r % 2).wait()
            zs[i] = zs[i] + cst[r % 2, pl.ds(0, nr), pl.ds(0, kd)]

    def jobs(*specs):
        with sc("job" + "_".join(f"{kind}{s}" for kind, s, *_ in specs)):
            @pl.loop(0, 4)
            def _(r):
                for kind, s, h, q_add, q_dst, dev, first in specs:
                    chunk(kind, s, r, h, q_add, first)
                    zcopy(q_dst, kind, r, h, dev).start()

    def finish(kind, adds, lo=0, hi=4):
        res = (xa, dya)[kind]
        with sc(f"fin{kind}"):
            @pl.loop(lo, hi)
            def _(r):
                col = pl.ds(pl.multiple_of(r * kd, kd), kd)
                part = (pl.ds(0, nr), pl.ds(0, kd))
                temp = (0, pl.ds(0, nr), pl.ds(kd, kd))
                back(cst, (0, kd), kind, 0, r)
                for n, q in enumerate(adds):
                    with sc("finrecv"):
                        zcopy(q, kind, r, 0, dev_a).wait_recv()
                    zload_(q, kind, r, n).start()
                for n, q in enumerate(adds):
                    zload_(q, kind, r, n).wait()
                v = cst[temp] + res[rows(0), col].astype(f32)
                for n in range(len(adds)):
                    v = v + cst[n, *part]
                res[rows(1), col] = v.astype(bf)

    def unit(rc, rx, j, put):
        ryi, k, half = j // 6, ((j // 2) % 3 + 2) % 3, j % 2
        f0 = (1 - ryi) * kf

        @pl.when(k < 2)
        def _():
            a = xt[rc, pl.ds(pl.multiple_of(half * hd, hd), hd), :]
            for q in range(4):
                b = act[k, :, pl.ds(pl.multiple_of(f0 + q * hd, hd), hd)]
                put(pl.ds(q * hd, hd), mm(a, b))

        @pl.when(k == 2)
        def _():
            for q in range(4):
                b = dya[:, pl.ds((2 * rc + rx) * kd + q % 2 * hd, hd)]
                a = ht[pl.ds(pl.multiple_of(f0 + half * hf + q // 2 * hd, hd), hd), :]
                put(pl.ds(q * hd, hd), mm(a, b))

    def fcopy(u):
        return remote(fst.at[u % 3], far_r.at[u], fsend.at[u % 3], frecv.at[u], dev_c)

    def ncopy(u):
        return pltpu.make_async_copy(nst.at[(u + 1) % 2], near.at[u], nstore.at[(u + 1) % 2])

    def ccopy(u):
        return pltpu.make_async_copy(far_r.at[u], cst.at[(u + 1) % 2], cload.at[(u + 1) % 2])

    def xcopy1(i, u):
        return remote(near.at[u], xr1.at[i], xs1.at[i], xq1.at[i], dev_x)

    def ycopy1(i, u):
        return remote(near.at[u], yr1.at[i], ys1.at[i], yq1.at[i], dev_y)

    def nsend(rx, j):
        ryi, k, half = j // 6, (j // 2) % 3, j % 2
        u = 12 * (1 - rx) + j
        if rx:
            @pl.when(half == 0)
            def _():
                xcopy1(ryi * 3 + k, u).start()

        @pl.when((half == 1) & (ryi == 0))
        def _():
            ycopy1(3 * (1 - rx) + k, u).start()

    def far_unit(rx, j):
        u = 12 * (1 - rx) + j

        @pl.when(u > 2)
        def _():
            with sc("fsend"):
                fcopy(u).wait_send()

        def put(col, v):
            fst[u % 3, :, col] = v

        unit(1, rx, j, put)
        fcopy(u).start()

    def dw_first(rx, n):
        with sc("dwfirst"):
            @pl.loop(0, n)
            def _(j):
                far_unit(rx, j)

    def near_load(rx, j):
        u = 12 * (1 - rx) + j
        with sc("frecv"):
            fcopy(u).wait_recv()
        ccopy(u).start()

    def near_unit(rx, j):
        u = 12 * (1 - rx) + j
        with sc("cwait"):
            ccopy(u).wait()

        def put(col, v):
            i = (u + 1) % 2
            nst[i, :, col] = v + cst[i, :, col]

        unit(0, rx, j, put)

    def near_done(rx, j):
        with sc("nwait"):
            ncopy(12 * (1 - rx) + j).wait()
        nsend(rx, j)

    def dw(rx, f0, n0):
        base = 12 * (1 - rx)

        with sc(f"dw{rx}"):
            @pl.loop(f0, 12 + LAG)
            def _(j):
                n = j - LAG

                @pl.when(j < 12)
                def _():
                    far_unit(rx, j)

                if n0:
                    @pl.when(j == f0)
                    def _():
                        near_done(rx, n0 - 1)

                @pl.when((n + 1 >= n0) & (n < 11))
                def _():
                    near_load(rx, n + 1)

                @pl.when(n >= n0)
                def _():
                    near_unit(rx, n)

                    @pl.when(n > n0)
                    def _():
                        near_done(rx, n - 1)

                    ncopy(base + n).start()

            near_done(rx, 11)

    def add_pair(units, waits, arrived, dsts, after=(None, None)):
        cn = [pltpu.make_async_copy(near.at[u], fst.at[h], cin.at[h]) for h, u in enumerate(units)]
        cr = [pltpu.make_async_copy(v, cst.at[h], cload.at[h]) for h, v in enumerate(arrived)]
        cd = [pltpu.make_async_copy(nst.at[h], t, nstore.at[h]) for h, t in enumerate(dsts)]
        st = min(64, hd)
        for h in range(2):
            cn[h].start()
        for h in range(2):
            waits[h].wait_recv()
            cr[h].start()
        for h in range(2):
            cn[h].wait()
            cr[h].wait()

            @pl.loop(0, hd // st)
            def _(i):
                row = pl.ds(pl.multiple_of(i * st, st), st)
                nst[h, row, :] = fst[h, row, :] + cst[h, row, :]

            cd[h].start()
        for h in range(2):
            cd[h].wait()
            if after[h] is not None:
                after[h].start()

    def uid(rx, ry, k, half):
        return 12 * (1 - rx) + 6 * (1 - ry) + 2 * k + half

    def ycopy2(k):
        return remote(near.at[uid(0, 1, k, 0)], r2.at[2 * k], s2.at[2 * k], q2.at[2 * k], dev_y)

    def xcopy2(k):
        return remote(near.at[uid(1, 0, k, 1)], r2.at[2 * k + 1], s2.at[2 * k + 1], q2.at[2 * k + 1], dev_x)

    def second(k):
        ua, ub = uid(0, 1, k, 0), uid(1, 0, k, 1)
        with sc(f"second{k}"):
            add_pair(
                (ua, ub), (xcopy1(k, 0), ycopy1(k, 0)), (xr1.at[k], yr1.at[k]), (near.at[ua], near.at[ub]),
                (ycopy2(k), xcopy2(k)),
            )

    def third(k):
        ua, ub = uid(0, 0, k, 0), uid(0, 0, k, 1)
        with sc(f"third{k}"):
            add_pair(
                (ua, ub), (xcopy1(3 + k, 0), ycopy1(3 + k, 0)), (xr1.at[3 + k], yr1.at[3 + k]),
                (n00.at[2 * k], n00.at[2 * k + 1]),
            )

    def fourth(k):
        cn = [pltpu.make_async_copy(n00.at[2 * k + h], dwv.at[2 * k + h], cin.at[h]) for h in range(2)]
        cr = [pltpu.make_async_copy(r2.at[2 * k + h], cst.at[h], cload.at[h]) for h in range(2)]
        st = min(64, hd)
        with sc(f"fourth{k}"):
            for h in range(2):
                cn[h].start()
            for h in range(2):
                (ycopy2, xcopy2)[h](k).wait_recv()
                cr[h].start()
            for h in range(2):
                cn[h].wait()
                cr[h].wait()

                @pl.loop(0, hd // st)
                def _(i):
                    row = pl.ds(pl.multiple_of(i * st, st), st)
                    dwv[2 * k + h, row, :] = dwv[2 * k + h, row, :] + cst[h, row, :]

    with sc("own_in"):
        for k in range(3):
            local[k].wait()
            if k < 2:
                xo[k].start()
                yo[k].start()
        yd[0].start()
        for cp in local[3:]:
            cp.wait()
    for j in range(2):
        acopy(0, 1, j).start()

    @mid
    def _():
        for j in range(2):
            bcopy(0, 2, j).start()

    for k in range(3):
        co[k].start()

    eye[...] = (
        lax.broadcasted_iota(jnp.int32, (hd, hd), 0) == lax.broadcasted_iota(jnp.int32, (hd, hd), 1)
    ).astype(f32).astype(bf)

    with sc("xt0"):
        transpose_x(1, 0, 1)

    def pass_on(s, j):
        with sc(f"rows{s}_{j}"):
            got(s, j)
        if s == 1:
            bcopy(1, 3, j).start()
        else:
            acopy(s, s, j).start()

    with sc("gx0"):
        xo[0].wait_recv()
        cx[0].start()
        yo[0].wait_recv()
    rg.start()
    cy[0].start()

    @mid
    def _():
        pass_on(1, 0)
        pass_on(2, 0)

    with sc("gx1"):
        xo[1].wait_recv()
        for cp in rua:
            cp.start()
        yd[1].start()
        cx[1].start()
        yo[1].wait_recv()
    rub.start()
    for h in range(2):
        xd[h].start()
    cy[1].start()

    @mid
    def _():
        pass_on(1, 1)
        pass_on(2, 1)

    @end
    def _():
        with sc("e_rows1"):
            got(1, 0)

    with sc("gc0"):
        for cp in (*co[:2], *cx):
            cp.wait_recv()
    part_ab(1, 0)
    part_ab(0, 0)
    with sc("gyd"):
        yd[0].wait_recv()
        cyd[0].start()
        rg.wait_recv()
        crg.start()
    with sc("gc1"):
        for cp in (*cy, crg):
            cp.wait_recv()
    part_ab(1, 1, 1)

    @mid
    def _():
        pass_on(3, 0)

    with sc("gru"):
        for cp, fwd in zip((rua[0], rub, rua[1]), (crua[0], crub, crua[1])):
            cp.wait_recv()
            fwd.start()
    with sc("gc2"):
        for cp in (*crua, crub):
            cp.wait_recv()
    part_ab(1, 1, 2)
    with sc("gc3"):
        for cp in (co[2], cyd[0]):
            cp.wait_recv()

    def early_half(h):
        with sc(f"early1_{h}"):
            @pl.loop(0, 2)
            def _(i):
                r = 2 * i
                col = pl.ds(h * hd, hd)
                v = mm(act[2, rows(1), :], wd[:, pl.ds(pl.multiple_of(r * kd + h * hd, hd), hd)])
                zs[r, :, col] = v
                remote(zs.at[r, :, col], zl.at[0, r, :, col], zsend.at[r], zrecv.at[0, r], dev_a).start()

    def early(s, odd):
        with sc(f"early{s}_{odd}"):
            @pl.loop(0, 2)
            def _(i):
                r = 2 * i + odd
                chunk(0, s, r, s - 1, None, True)
                zcopy(s - 1, 0, r, s - 1, dev_a).start()

    @end
    def _():
        early_half(0)
        with sc("e_rows2"):
            got(2, 0)

    part_ab(2, 0)
    with sc("gd0"):
        yd[1].wait_recv()
        cyd[1].start()
        xd[0].wait_recv()
        rd[0].start()
        cxd[0].start()
        cyd[1].wait_recv()

    @end
    def _():
        early_half(1)

    part_ab(2, 1)

    @end
    def _():
        early(2, 0)

    @mid
    def _():
        pass_on(3, 1)

    with sc("gd1"):
        xd[1].wait_recv()
        rd[1].start()
        cxd[1].start()
    part_ab(0, 1)
    with sc("gd2"):
        rd[0].wait_recv()
        crd[0].start()
    transpose_x(1, 1, 3)
    keep_h(1)
    keep_h(0)
    keep_h(2)
    with sc("gd3"):
        rd[1].wait_recv()
        crd[1].start()
        for cp in (*cxd, *crd):
            cp.wait_recv()

    @end
    def _():
        early(1, 1)
        early(2, 1)
        got(1, 1)
        got(2, 1)
        with sc("e_rows3"):
            got(3, 0)

    part_ab(3, 0)
    part_ab(3, 1)
    flush(0)
    flush(1)
    gload(1)
    transpose_x(1, 3, 4)
    keep_h(3)
    front_g(1, 0)
    front_g(0, 2)
    front_g(2, 3)

    @end
    def _():
        with sc("e_rows3"):
            got(3, 1)

    dw_first(1, 2)
    half_g(3, 1, None)
    near_load(1, 0)
    half_g(3, 0, None)
    near_unit(1, 0)
    ncopy(0).start()
    dw(1, 2, 1)

    @end
    def _():
        jobs((0, 3, 0, None, 2, dev_a, False))

    @mid
    def _():
        jobs((0, 2, 0, 1, 3, dev_b, True))

    with sc("xtb"):
        transpose_x(0, 0, 4)
    dw(0, 0, 0)
    for u in range(3):
        fcopy(u).wait_send()
    for cp in wcopies:
        cp.wait_send()
    for j in range(2):
        acopy(0, 1, j).wait_send()

    @mid
    def _():
        for j in range(2):
            bcopy(0, 2, j).wait_send()
            bcopy(1, 3, j).wait_send()
            acopy(2, 2, j).wait_send()
            acopy(3, 3, j).wait_send()

    @end
    def _():
        jobs((1, 3, 1, None, 2, dev_a, False))
        second(0)
        second(1)
        second(2)
        jobs((1, 2, 0, None, 1, dev_a, False))
        third(0)
        third(1)
        jobs((1, 1, 1, None, 0, dev_a, False))
        third(2)
        finish(0, (0,))
        fourth(0)
        finish(1, (0,), 0, 2)
        fourth(1)
        finish(1, (0,), 2, 4)
        fourth(2)

    @mid
    def _():
        jobs((0, 3, 1, 2, 4, dev_b, True))
        second(0)
        second(1)
        second(2)
        jobs((0, 1, 0, 4, 0, dev_a, False), (1, 3, 1, 2, 4, dev_b, False))
        third(0)
        third(1)
        jobs((1, 1, 0, 4, 0, dev_a, False), (1, 2, 1, 1, 3, dev_b, False))
        third(2)
        finish(0, (0, 3))
        fourth(0)
        fourth(1)
        finish(1, (0, 3), 0, 3)
        fourth(2)
        finish(1, (0, 3), 3, 4)

    with sc("drain"):
        for half in range(2):
            for r in range(4):
                zcopy(0, 0, r, half, dev_a).wait_send()
        for i in range(6):
            xcopy1(i, 0).wait_send()
            ycopy1(i, 0).wait_send()
        for k in range(3):
            ycopy2(k).wait_send()
            xcopy2(k).wait_send()


def fused(x, dy, wg, wu, wd):
    nr, d = x.shape
    kd, kf = wg.shape
    f, hd = 2 * kf, kd // 2
    hbm = pl.BlockSpec(memory_space=pl.ANY)
    sds = jax.ShapeDtypeStruct
    out_shape = (
        pltpu.VMEM((4 * nr, d), bf), pltpu.VMEM((4 * nr, d), bf), pltpu.VMEM((6, hd, kf), f32),
        sds((6, hd, kf), f32), sds((6, hd, kf), f32),
        sds((5, 8, nr, kd), f32), sds((24, hd, kf), f32), sds((24, hd, kf), f32),
        sds((6, hd, kf), f32), sds((6, hd, kf), f32), sds((4, 2, 2, nr, kf), f32),
    )
    dma = pltpu.SemaphoreType.DMA
    return pl.pallas_call(
        kernel,
        name="fused",
        out_shape=out_shape,
        in_specs=[hbm] * 5,
        out_specs=(pl.BlockSpec(memory_space=pltpu.VMEM),) * 3 + (hbm,) * (len(out_shape) - 3),
        scratch_shapes=[
            pltpu.VMEM((d, f), bf), pltpu.VMEM((d, f), bf), pltpu.VMEM((f, d), bf),
            pltpu.VMEM((3, 4 * nr, f), bf),
            pltpu.VMEM((8, nr, kd), f32), pltpu.VMEM((2, kd, 4 * nr), bf), pltpu.VMEM((f, 4 * nr), bf),
            pltpu.VMEM((hd, hd), bf),
            pltpu.VMEM((2, hd, kf), f32),
            dma((47,)), dma((39,)), dma((11,)), dma((8,)), dma((5, 8)), dma((2,)), dma((3,)), dma((24,)), dma((2,)),
            dma((2,)), dma((6,)), dma((6,)), dma((6,)), dma((6,)), dma((6,)), dma((6,)), dma((2,)), dma((4,)),
        ],
        compiler_params=pltpu.CompilerParams(collective_id=0, has_side_effects=True, vmem_limit_bytes=VMEM_LIMIT - 14 * 2**20),
    )(x, dy, wg, wu, wd)


def tail_kernel(xa, dya, dwv, y, dx, dwg, dwu, dwd, sem):
    dp = lax.axis_index("dp")
    nr, kd = y.shape[0], dwd.shape[1]
    hd = kd // 2
    copies = []
    for k in range(3):
        for h in range(2):
            v = dwv.at[2 * k + h]
            if k > 0:
                copies.append((v, (dwg, dwu)[k - 1].at[pl.ds(h * hd, hd)]))
            else:
                for q in range(2):
                    copies.append((v.at[:, pl.ds(q * kd, kd)], dwd.at[pl.ds((2 * h + q) * hd, hd)]))
    for src, dst in ((xa, y), (dya, dx)):
        for r in range(4):
            copies.append((src.at[pl.ds(nr, nr), pl.ds(r * kd, kd)], dst.at[:, natural(dp, r, kd)]))
    copies = [pltpu.make_async_copy(s, t, sem.at[i]) for i, (s, t) in enumerate(copies)]
    for c in copies:
        c.start()
    for c in copies:
        c.wait()


def tail(xa, dya, dwv, nr, kd, kf):
    hbm = pl.BlockSpec(memory_space=pl.ANY)
    sds = jax.ShapeDtypeStruct
    d = xa.shape[1]
    return pl.pallas_call(
        tail_kernel,
        name="tail",
        out_shape=(sds((nr, d), bf), sds((nr, d), bf), sds((kd, kf), f32), sds((kd, kf), f32), sds((kf, kd), f32)),
        in_specs=[hbm] * 3,
        out_specs=(hbm,) * 5,
        scratch_shapes=[pltpu.SemaphoreType.DMA((16,))],
        compiler_params=pltpu.CompilerParams(vmem_limit_bytes=2**20),
    )(xa, dya, dwv)


def solution(mesh):
    rows = P(("dp", "tp"), None)
    wsp = P("dp", "tp")
    dsp = P("tp", "dp")

    def local(x, w_gate, w_up, w_down, dy):
        return tail(*fused(x, dy, w_gate, w_up, w_down)[:3], x.shape[0], *w_gate.shape)

    return jax.shard_map(local, mesh=mesh, in_specs=(rows, wsp, wsp, dsp, rows), out_specs=(rows, rows, wsp, wsp, dsp), check_vma=False)
```

```python
import jax
import jax.numpy as jnp
from jax import lax
from jax.experimental import pallas as pl
from jax.experimental.pallas import tpu as pltpu
from jax.sharding import PartitionSpec as P

MESH = pl.DeviceIdType.MESH
f32 = jnp.float32
bf = jnp.bfloat16
VMEM_LIMIT = 67043328
sc = jax.named_scope
LAG = 4


def mm(a, b):
    return lax.dot_general(a, b, (((1,), (0,)), ((), ())), preferred_element_type=f32)


def mmt(a, b):
    return lax.dot_general(a, b, (((1,), (1,)), ((), ())), preferred_element_type=f32)


def natural(dp, r, kd):
    x, c, rc, rx = dp // 2, dp % 2, r // 2, r % 2
    n = 2 * (x + rx - 2 * x * rx) + c + rc - 2 * c * rc
    return pl.ds(pl.multiple_of(n * kd, kd), kd)


def kernel(
    x_in, dy_in, wg_in, wu_in, wd_in,
    xa, dya, dwv, n00, r2, zl, far_r, near, xr1, yr1, stash,
    wg, wu, wd, act, zs, xt, ht, eye, cst,
    gs, gr, lsem, zsend, zrecv, zload, fsend, frecv, nstore, cload, xs1, xq1, ys1, yq1, s2, q2, cin, ssem,
):
    tp = lax.axis_index("tp")
    dp = lax.axis_index("dp")
    z, y = tp // 2, tp % 2
    x, c = dp // 2, dp % 2
    is_end = (z == 0) | (z == 3)
    is_mid = (z == 1) | (z == 2)
    dev_x = {"tp": tp, "dp": 2 * (1 - x) + c}
    dev_y = {"tp": 2 * z + 1 - y, "dp": dp}
    dev_c = {"tp": tp, "dp": 2 * x + 1 - c}
    dev_a = {"tp": 2 * (z + 1 - 2 * (z % 2)) + y, "dp": dp}
    dev_b = {"tp": 2 * (3 - z) + y, "dp": dp}

    fst, nst = dwv.at[pl.ds(0, 3)], dwv.at[pl.ds(3, 2)]
    nr, d = x_in.shape
    kd, kf = wg_in.shape
    f = 2 * kf
    hd = kd // 2
    hf = kf // 2

    def end(fn):
        pl.when(is_end)(fn)

    def mid(fn):
        pl.when(is_mid)(fn)

    def ncol(r):
        return natural(dp, r, kd)

    def remote(src, dst, ss, rs, dev):
        return pltpu.make_async_remote_copy(
            src_ref=src, dst_ref=dst, send_sem=ss, recv_sem=rs, device_id=dev, device_id_type=MESH
        )

    own = (wg_in, wu_in, wd_in)

    def blk(k, rx, rc, ry, lo=0, n=None):
        d0 = (2 * rc + rx) * kd + lo
        n = kd if n is None else n
        if k < 2:
            return (wg, wu)[k].at[pl.ds(d0, n), pl.ds(ry * kf, kf)]
        return wd.at[pl.ds(ry * kf, kf), pl.ds(d0, n)]

    local = [(own[k], blk(k, 0, 0, 0)) for k in range(3)]
    for src, ref in ((x_in, xa), (dy_in, dya)):
        for r in range(4):
            local.append((src.at[:, ncol(r)], ref.at[pl.ds(0, nr), pl.ds(r * kd, kd)]))
    local = [pltpu.make_async_copy(s, t, lsem.at[i]) for i, (s, t) in enumerate(local)]
    for cp in local:
        cp.start()

    bar = pltpu.get_barrier_semaphore()
    for dev in (dev_x, dev_y, dev_c, dev_a, dev_b):
        pl.semaphore_signal(bar, inc=1, device_id=dev, device_id_type=MESH)

    with sc("barrier"):
        pl.semaphore_wait(bar, 5)

    ft = min(256, f)

    def rows(s):
        return pl.ds(s * nr, nr)

    def transpose_x(rx, lo, hi):
        @pl.loop(lo, hi)
        def _(s):
            row = pl.ds(pl.multiple_of(s * nr, nr), nr)
            for rc in range(2):
                for h in range(2):
                    v = mmt(eye[...], xa[row, pl.ds((2 * rc + rx) * kd + h * hd, hd)])
                    xt[rc, pl.ds(h * hd, hd), row] = v.astype(bf)

    def wcopy(i, src, dst, dev):
        return remote(src, dst, gs.at[i], gr.at[i], dev)

    def half(rx, rc, ry, h):
        return blk(2, rx, rc, ry, h * hd, hd)

    qd = kd // 4

    def quarter(rx, rc, ry, h):
        return blk(2, rx, rc, ry, h * qd, qd)

    ua = 15 * kd // 16
    mine = [blk(k, 0, 0, 0) for k in range(3)]
    xo = [wcopy(k, mine[k], blk(k, 1, 0, 0), dev_x) for k in range(2)]
    yo = [wcopy(2 + k, mine[k], blk(k, 0, 0, 1), dev_y) for k in range(2)]
    co = [wcopy(4 + k, mine[k], blk(k, 0, 1, 0), dev_c) for k in range(3)]
    xd = [wcopy(7 + h, half(0, 0, 0, h), half(1, 0, 0, h), dev_x) for h in range(2)]
    yd = [wcopy(9 + h, quarter(0, 0, 0, h), quarter(0, 0, 1, h), dev_y) for h in range(4)]
    rg = [wcopy(13 + h, blk(0, 0, 0, 1, h * hd, hd), blk(0, 1, 0, 1, h * hd, hd), dev_x) for h in range(2)]
    rua = wcopy(15, blk(1, 1, 0, 0, 0, ua), blk(1, 1, 0, 1, 0, ua), dev_y)
    rub = wcopy(16, blk(1, 0, 0, 1, ua, kd - ua), blk(1, 1, 0, 1, ua, kd - ua), dev_x)
    rd = [wcopy(17 + h, half(1, 0, 0, h), half(1, 0, 1, h), dev_y) for h in range(2)]
    cx = [wcopy(19 + k, blk(k, 1, 0, 0), blk(k, 1, 1, 0), dev_c) for k in range(2)]
    cy = [wcopy(21 + k, blk(k, 0, 0, 1), blk(k, 0, 1, 1), dev_c) for k in range(2)]
    cxd = [wcopy(23 + h, half(1, 0, 0, h), half(1, 1, 0, h), dev_c) for h in range(2)]
    cyd = [wcopy(25 + h, quarter(0, 0, 1, h), quarter(0, 1, 1, h), dev_c) for h in range(4)]
    crg = [wcopy(29 + h, blk(0, 1, 0, 1, h * hd, hd), blk(0, 1, 1, 1, h * hd, hd), dev_c) for h in range(2)]
    crua = wcopy(31, blk(1, 1, 0, 1, 0, ua), blk(1, 1, 1, 1, 0, ua), dev_c)
    crub = wcopy(32, blk(1, 1, 0, 1, ua, kd - ua), blk(1, 1, 1, 1, ua, kd - ua), dev_c)
    crd = [wcopy(33 + h, half(1, 0, 1, h), half(1, 1, 1, h), dev_c) for h in range(2)]
    wcopies = (*xo, *yo, *co, *xd, *yd, *rg, rua, rub, *rd, *cx, *cy, *cxd, *cyd, *crg, crua, crub, *crd)
    nw = 35

    def slot(j, s):
        return (xa, dya)[j].at[pl.ds(s * nr, nr)]

    def acopy(src, dst, j):
        return remote(
            slot(j, src), slot(j, dst), gs.at[nw + 2 * dst + j], gr.at[nw + 2 * dst + j], dev_a
        )

    def bcopy(src, dst, j):
        return remote(
            slot(j, src), slot(j, dst), gs.at[nw + 8 + 2 * dst + j], gr.at[nw + 2 * dst + j], dev_b
        )

    def got(s, j):
        acopy(s, s, j).wait_recv()

    def stash_copy(s, p, n):
        return pltpu.make_async_copy((fst, nst)[n].at[p, pl.ds(0, nr)], stash.at[s, p, n], ssem.at[2 * p + n])

    def factor(s, n):
        return nst if n else cst if s == 3 else fst

    def stash_load(s, p, n):
        return pltpu.make_async_copy(stash.at[s, p, n], factor(s, n).at[p, pl.ds(0, nr)], ssem.at[2 * p + n])

    pending = [None, None]

    def flush(p):
        if pending[p] is not None:
            for n in range(2):
                stash_copy(pending[p], p, n).wait()
        pending[p] = None

    def ab_tiles(s, p, step):
        @pl.loop(0, kf // ft)
        def _(i):
            col = pl.ds(pl.multiple_of(p * kf + i * ft, ft), ft)
            at = (p, pl.ds(0, nr), pl.ds(pl.multiple_of(i * ft, ft), ft))

            def some(w, rx):
                b0, b1 = pl.ds(rx * kd, kd), pl.ds((2 + rx) * kd, kd)
                return mm(xa[rows(s), b0], w[b0, col]) + mm(xa[rows(s), b1], w[b1, col])

            if step == 1:
                fst[at], nst[at] = some(wg, 0), some(wu, 0)
                return
            if step == 2:
                a, b = fst[at] + some(wg, 1), nst[at] + some(wu, 1)
            else:
                a = mm(xa[rows(s), :], wg[:, col])
                b = mm(xa[rows(s), :], wu[:, col])
            sig = jax.nn.sigmoid(a)
            sa = a * sig
            act[2, rows(s), col] = (sa * b).astype(bf)
            fst[at] = sa
            nst[at] = b * sig * (1.0 + a * (1.0 - sig))

    def part_ab(s, p, step=0):
        with sc(f"ab{s}_{p}"):
            flush(p)
            ab_tiles(s, p, step)
            if step != 1:
                for n in range(2):
                    stash_copy(s, p, n).start()
                pending[p] = s

    gt = min(512, kf)

    def part_g(s, p):
        @pl.loop(0, kf // gt)
        def _(i):
            col = pl.ds(pl.multiple_of(p * kf + i * gt, gt), gt)
            kcol = pl.ds(pl.multiple_of(i * gt, gt), gt)
            g = mmt(dya[rows(s), :], wd[col, :])
            act[0, rows(s), col] = (g * factor(s, 1)[p, pl.ds(0, nr), kcol]).astype(bf)
            act[1, rows(s), col] = (g * factor(s, 0)[p, pl.ds(0, nr), kcol]).astype(bf)

    def gload(s):
        for p in range(2):
            for n in range(2):
                stash_load(s, p, n).start()

    def half_g(s, p, then):
        with sc(f"g{s}"):
            for n in range(2):
                stash_load(s, p, n).wait()
            part_g(s, p)
            if then is not None:
                for n in range(2):
                    stash_load(then, p, n).start()

    def front_g(s, then):
        @pl.loop(0, 2)
        def _(p):
            half_g(s, p, then)

    def keep_h(lo, hi):
        hb = min(4, f // hd)
        nh = f // (hb * hd)
        with sc("ht"):
            @pl.loop(lo * nh, hi * nh)
            def _(i):
                row = pl.ds(pl.multiple_of(i // nh * nr, nr), nr)
                for q in range(hb):
                    col = pl.ds(pl.multiple_of((i % nh * hb + q) * hd, hd), hd)
                    ht[col, row] = mmt(eye[...], act[2, row, col]).astype(bf)

    def back(ref, at, kind, s, r):
        *lead, c0 = at

        @pl.loop(0, 2)
        def _(h):
            n = pl.ds(pl.multiple_of(r * kd + h * hd, hd), hd)
            if kind == 0:
                v = mm(act[2, rows(s), :], wd[:, n])
            else:
                v = mmt(act[0, rows(s), :], wg[n, :]) + mmt(act[1, rows(s), :], wu[n, :])
            ref[(*lead, pl.ds(0, nr), pl.ds(pl.multiple_of(c0 + h * hd, hd), hd))] = v

    def zcopy(q, kind, r, half, dev):
        i = 4 * kind + r
        return remote(zs.at[4 * half + r], zl.at[q, i], zsend.at[4 * half + r], zrecv.at[q, i], dev)

    def zload_(q, kind, r, slot):
        return pltpu.make_async_copy(zl.at[q, 4 * kind + r], cst.at[slot, pl.ds(0, nr), pl.ds(0, kd)], zload.at[slot])

    def chunk(kind, s, r, half, q_add, first):
        i = 4 * half + r
        if q_add is not None:
            with sc("zrecv"):
                zcopy(q_add, kind, r, half, dev_a).wait_recv()
            zload_(q_add, kind, r, r % 2).start()
        if not first:
            with sc("zsend"):
                zcopy(0, kind, r, half, dev_a).wait_send()
        back(zs, (i, 0), kind, s, r)
        if q_add is not None:
            zload_(q_add, kind, r, r % 2).wait()
            zs[i] = zs[i] + cst[r % 2, pl.ds(0, nr), pl.ds(0, kd)]

    def jobs(*specs):
        with sc("job" + "_".join(f"{kind}{s}" for kind, s, *_ in specs)):
            @pl.loop(0, 4)
            def _(r):
                for kind, s, h, q_add, q_dst, dev, first in specs:
                    chunk(kind, s, r, h, q_add, first)
                    zcopy(q_dst, kind, r, h, dev).start()

    def finish(kind, adds, lo=0, hi=4):
        res = (xa, dya)[kind]
        with sc(f"fin{kind}"):
            @pl.loop(lo, hi)
            def _(r):
                col = pl.ds(pl.multiple_of(r * kd, kd), kd)
                part = (pl.ds(0, nr), pl.ds(0, kd))
                temp = (0, pl.ds(0, nr), pl.ds(kd, kd))
                back(cst, (0, kd), kind, 0, r)
                for n, q in enumerate(adds):
                    with sc("finrecv"):
                        zcopy(q, kind, r, 0, dev_a).wait_recv()
                    zload_(q, kind, r, n).start()
                for n, q in enumerate(adds):
                    zload_(q, kind, r, n).wait()
                v = cst[temp] + res[rows(0), col].astype(f32)
                for n in range(len(adds)):
                    v = v + cst[n, *part]
                res[rows(1), col] = v.astype(bf)

    def unit(rc, rx, j, put):
        ryi, k, half = j // 6, ((j // 2) % 3 + 2) % 3, j % 2
        f0 = (1 - ryi) * kf

        @pl.when(k < 2)
        def _():
            a = xt[rc, pl.ds(pl.multiple_of(half * hd, hd), hd), :]
            for q in range(4):
                b = act[k, :, pl.ds(pl.multiple_of(f0 + q * hd, hd), hd)]
                put(pl.ds(q * hd, hd), mm(a, b))

        @pl.when(k == 2)
        def _():
            for q in range(4):
                b = dya[:, pl.ds((2 * rc + rx) * kd + q % 2 * hd, hd)]
                a = ht[pl.ds(pl.multiple_of(f0 + half * hf + q // 2 * hd, hd), hd), :]
                put(pl.ds(q * hd, hd), mm(a, b))

    def fcopy(u):
        return remote(fst.at[u % 3], far_r.at[u], fsend.at[u % 3], frecv.at[u], dev_c)

    def ncopy(u):
        return pltpu.make_async_copy(nst.at[(u + 1) % 2], near.at[u], nstore.at[(u + 1) % 2])

    def ccopy(u):
        return pltpu.make_async_copy(far_r.at[u], cst.at[(u + 1) % 2], cload.at[(u + 1) % 2])

    def xcopy1(i, u):
        return remote(near.at[u], xr1.at[i], xs1.at[i], xq1.at[i], dev_x)

    def ycopy1(i, u):
        return remote(near.at[u], yr1.at[i], ys1.at[i], yq1.at[i], dev_y)

    def nsend(rx, j):
        ryi, k, half = j // 6, (j // 2) % 3, j % 2
        u = 12 * (1 - rx) + j
        if rx:
            @pl.when(half == 0)
            def _():
                xcopy1(ryi * 3 + k, u).start()

        @pl.when((half == 1) & (ryi == 0))
        def _():
            ycopy1(3 * (1 - rx) + k, u).start()

    def far_unit(rx, j):
        u = 12 * (1 - rx) + j

        @pl.when(u > 2)
        def _():
            with sc("fsend"):
                fcopy(u).wait_send()

        def put(col, v):
            fst[u % 3, :, col] = v

        unit(1, rx, j, put)
        fcopy(u).start()

    def dw_first(rx, n):
        with sc("dwfirst"):
            @pl.loop(0, n)
            def _(j):
                far_unit(rx, j)

    def near_load(rx, j):
        u = 12 * (1 - rx) + j
        with sc("frecv"):
            fcopy(u).wait_recv()
        ccopy(u).start()

    def near_unit(rx, j):
        u = 12 * (1 - rx) + j
        with sc("cwait"):
            ccopy(u).wait()

        def put(col, v):
            i = (u + 1) % 2
            nst[i, :, col] = v + cst[i, :, col]

        unit(0, rx, j, put)

    def near_done(rx, j):
        with sc("nwait"):
            ncopy(12 * (1 - rx) + j).wait()
        nsend(rx, j)

    def dw(rx, f0, n0):
        base = 12 * (1 - rx)

        with sc(f"dw{rx}"):
            @pl.loop(f0, 12 + LAG)
            def _(j):
                n = j - LAG

                @pl.when(j < 12)
                def _():
                    far_unit(rx, j)

                if n0:
                    @pl.when(j == f0)
                    def _():
                        for i in range(n0):
                            near_done(rx, i)

                @pl.when((n + 1 >= n0) & (n < 11))
                def _():
                    near_load(rx, n + 1)

                @pl.when(n >= n0)
                def _():
                    near_unit(rx, n)

                    @pl.when(n > n0)
                    def _():
                        near_done(rx, n - 1)

                    ncopy(base + n).start()

            near_done(rx, 11)

    def add_pair(units, waits, arrived, dsts, after=(None, None)):
        cn = [pltpu.make_async_copy(near.at[u], fst.at[h], cin.at[h]) for h, u in enumerate(units)]
        cr = [pltpu.make_async_copy(v, cst.at[h], cload.at[h]) for h, v in enumerate(arrived)]
        cd = [pltpu.make_async_copy(nst.at[h], t, nstore.at[h]) for h, t in enumerate(dsts)]
        st = min(64, hd)
        for h in range(2):
            cn[h].start()
        for h in range(2):
            waits[h].wait_recv()
            cr[h].start()
        for h in range(2):
            cn[h].wait()
            cr[h].wait()

            @pl.loop(0, hd // st)
            def _(i):
                row = pl.ds(pl.multiple_of(i * st, st), st)
                nst[h, row, :] = fst[h, row, :] + cst[h, row, :]

            cd[h].start()
        for h in range(2):
            cd[h].wait()
            if after[h] is not None:
                after[h].start()

    def uid(rx, ry, k, half):
        return 12 * (1 - rx) + 6 * (1 - ry) + 2 * k + half

    def ycopy2(k):
        return remote(near.at[uid(0, 1, k, 0)], r2.at[2 * k], s2.at[2 * k], q2.at[2 * k], dev_y)

    def xcopy2(k):
        return remote(near.at[uid(1, 0, k, 1)], r2.at[2 * k + 1], s2.at[2 * k + 1], q2.at[2 * k + 1], dev_x)

    def second(k):
        ua, ub = uid(0, 1, k, 0), uid(1, 0, k, 1)
        with sc(f"second{k}"):
            add_pair(
                (ua, ub), (xcopy1(k, 0), ycopy1(k, 0)), (xr1.at[k], yr1.at[k]), (near.at[ua], near.at[ub]),
                (ycopy2(k), xcopy2(k)),
            )

    def third(k):
        ua, ub = uid(0, 0, k, 0), uid(0, 0, k, 1)
        with sc(f"third{k}"):
            add_pair(
                (ua, ub), (xcopy1(3 + k, 0), ycopy1(3 + k, 0)), (xr1.at[3 + k], yr1.at[3 + k]),
                (n00.at[2 * k], n00.at[2 * k + 1]),
            )

    def fourth(k):
        cn = [pltpu.make_async_copy(n00.at[2 * k + h], dwv.at[2 * k + h], cin.at[h]) for h in range(2)]
        cr = [pltpu.make_async_copy(r2.at[2 * k + h], cst.at[h], cload.at[h]) for h in range(2)]
        st = min(64, hd)
        with sc(f"fourth{k}"):
            for h in range(2):
                cn[h].start()
            for h in range(2):
                (ycopy2, xcopy2)[h](k).wait_recv()
                cr[h].start()
            for h in range(2):
                cn[h].wait()
                cr[h].wait()

                @pl.loop(0, hd // st)
                def _(i):
                    row = pl.ds(pl.multiple_of(i * st, st), st)
                    dwv[2 * k + h, row, :] = dwv[2 * k + h, row, :] + cst[h, row, :]

    with sc("own_in"):
        for k in range(3):
            local[k].wait()
            if k < 2:
                xo[k].start()
                yo[k].start()
        for cp in local[3:]:
            cp.wait()
    for j in range(2):
        acopy(0, 1, j).start()

    @mid
    def _():
        for j in range(2):
            bcopy(0, 2, j).start()

    for k in range(3):
        co[k].start()

    eye[...] = (
        lax.broadcasted_iota(jnp.int32, (hd, hd), 0) == lax.broadcasted_iota(jnp.int32, (hd, hd), 1)
    ).astype(f32).astype(bf)

    with sc("xt0"):
        transpose_x(1, 0, 1)

    def pass_on(s, j):
        with sc(f"rows{s}_{j}"):
            got(s, j)
        if s == 1:
            bcopy(1, 3, j).start()
        else:
            acopy(s, s, j).start()

    with sc("gx0"):
        xo[0].wait_recv()
        cx[0].start()
        yo[0].wait_recv()
    for cp in rg:
        cp.start()
    cy[0].start()

    @mid
    def _():
        pass_on(1, 0)
        pass_on(2, 0)

    with sc("gx1"):
        xo[1].wait_recv()
        rua.start()
        for cp in yd:
            cp.start()
        cx[1].start()
        yo[1].wait_recv()
    rub.start()
    for cp in xd:
        cp.start()
    cy[1].start()

    @mid
    def _():
        pass_on(1, 1)
        pass_on(2, 1)

    @end
    def _():
        with sc("e_rows1"):
            got(1, 0)

    with sc("gc0"):
        for cp in (*co[:2], *cx):
            cp.wait_recv()
    part_ab(1, 0)
    with sc("gc1"):
        for cp in cy:
            cp.wait_recv()
    part_ab(1, 1, 1)
    part_ab(0, 0)
    with sc("grg0"):
        rg[0].wait_recv()
        crg[0].start()
    with sc("gru"):
        for cp, fwd in ((rua, crua), (rg[1], crg[1]), (rub, crub)):
            cp.wait_recv()
            fwd.start()
    with sc("gc2"):
        for cp in (*crg, crua, crub):
            cp.wait_recv()
    part_ab(1, 1, 2)

    def early_part(h):
        with sc(f"early1_{h}"):
            @pl.loop(0, 2)
            def _(i):
                r = 2 * i
                col = pl.ds(h * qd, qd)
                v = mm(act[2, rows(1), :], wd[:, pl.ds(pl.multiple_of(r * kd + h * qd, qd), qd)])
                zs[r, :, col] = v
                remote(zs.at[r, :, col], zl.at[0, r, :, col], zsend.at[r], zrecv.at[0, r], dev_a).start()

    def early(s, odd):
        with sc(f"early{s}_{odd}"):
            @pl.loop(0, 2)
            def _(i):
                r = 2 * i + odd
                chunk(0, s, r, s - 1, None, True)
                zcopy(s - 1, 0, r, s - 1, dev_a).start()

    def down_part(h):
        with sc("gyd"):
            yd[h].wait_recv()
            cyd[h].start()
            cyd[h].wait_recv()

        @end
        def _():
            early_part(h)

    co[2].wait_recv()
    down_part(0)
    down_part(1)

    @end
    def _():
        with sc("e_rows2"):
            got(2, 0)

    @mid
    def _():
        pass_on(3, 0)

    part_ab(2, 0)
    down_part(2)
    down_part(3)
    with sc("gd0"):
        xd[0].wait_recv()
        rd[0].start()
        cxd[0].start()
    part_ab(2, 1)

    @end
    def _():
        early(2, 0)

    @mid
    def _():
        pass_on(3, 1)

    with sc("gd1"):
        xd[1].wait_recv()
        rd[1].start()
        cxd[1].start()
    part_ab(0, 1)
    with sc("gd2"):
        rd[0].wait_recv()
        crd[0].start()
    transpose_x(1, 1, 3)
    keep_h(0, 3)
    with sc("gd3"):
        rd[1].wait_recv()
        crd[1].start()
        for cp in (*cxd, *crd):
            cp.wait_recv()

    @end
    def _():
        early(1, 1)
        early(2, 1)
        got(1, 1)
        got(2, 1)
        with sc("e_rows3"):
            got(3, 0)

    part_ab(3, 0)
    part_ab(3, 1)
    flush(0)
    flush(1)
    gload(1)
    transpose_x(1, 3, 4)
    keep_h(3, 4)
    front_g(1, 0)
    front_g(0, 2)
    front_g(2, 3)

    @end
    def _():
        with sc("e_rows3"):
            got(3, 1)

    dw_first(1, 2)
    half_g(3, 1, None)
    near_load(1, 0)
    half_g(3, 0, None)
    near_load(1, 1)

    @pl.loop(0, 2)
    def _(j):
        near_unit(1, j)
        ncopy(j).start()

    dw(1, 2, 2)

    @end
    def _():
        jobs((0, 3, 0, None, 2, dev_a, False))

    @mid
    def _():
        jobs((0, 2, 0, 1, 3, dev_b, True))

    with sc("xtb"):
        transpose_x(0, 0, 4)
    dw(0, 0, 0)
    for u in range(3):
        fcopy(u).wait_send()
    for cp in wcopies:
        cp.wait_send()
    for j in range(2):
        acopy(0, 1, j).wait_send()

    @mid
    def _():
        for j in range(2):
            bcopy(0, 2, j).wait_send()
            bcopy(1, 3, j).wait_send()
            acopy(2, 2, j).wait_send()
            acopy(3, 3, j).wait_send()

    @end
    def _():
        jobs((1, 3, 1, None, 2, dev_a, False))
        second(0)
        second(1)
        second(2)
        jobs((1, 2, 0, None, 1, dev_a, False))
        third(0)
        third(1)
        jobs((1, 1, 1, None, 0, dev_a, False))
        third(2)
        finish(0, (0,))
        fourth(0)
        finish(1, (0,), 0, 2)
        fourth(1)
        finish(1, (0,), 2, 4)
        fourth(2)

    @mid
    def _():
        jobs((0, 3, 1, 2, 4, dev_b, True))
        second(0)
        second(1)
        second(2)
        jobs((0, 1, 0, 4, 0, dev_a, False), (1, 3, 1, 2, 4, dev_b, False))
        third(0)
        third(1)
        jobs((1, 1, 0, 4, 0, dev_a, False), (1, 2, 1, 1, 3, dev_b, False))
        third(2)
        finish(0, (0, 3))
        fourth(0)
        fourth(1)
        finish(1, (0, 3), 0, 3)
        fourth(2)
        finish(1, (0, 3), 3, 4)

    with sc("drain"):
        for half in range(2):
            for r in range(4):
                zcopy(0, 0, r, half, dev_a).wait_send()
        for i in range(6):
            xcopy1(i, 0).wait_send()
            ycopy1(i, 0).wait_send()
        for k in range(3):
            ycopy2(k).wait_send()
            xcopy2(k).wait_send()


def fused(x, dy, wg, wu, wd):
    nr, d = x.shape
    kd, kf = wg.shape
    f, hd = 2 * kf, kd // 2
    hbm = pl.BlockSpec(memory_space=pl.ANY)
    sds = jax.ShapeDtypeStruct
    out_shape = (
        pltpu.VMEM((4 * nr, d), bf), pltpu.VMEM((4 * nr, d), bf), pltpu.VMEM((6, hd, kf), f32),
        sds((6, hd, kf), f32), sds((6, hd, kf), f32),
        sds((5, 8, nr, kd), f32), sds((24, hd, kf), f32), sds((24, hd, kf), f32),
        sds((6, hd, kf), f32), sds((6, hd, kf), f32), sds((4, 2, 2, nr, kf), f32),
    )
    dma = pltpu.SemaphoreType.DMA
    return pl.pallas_call(
        kernel,
        name="fused",
        out_shape=out_shape,
        in_specs=[hbm] * 5,
        out_specs=(pl.BlockSpec(memory_space=pltpu.VMEM),) * 3 + (hbm,) * (len(out_shape) - 3),
        scratch_shapes=[
            pltpu.VMEM((d, f), bf), pltpu.VMEM((d, f), bf), pltpu.VMEM((f, d), bf),
            pltpu.VMEM((3, 4 * nr, f), bf),
            pltpu.VMEM((8, nr, kd), f32), pltpu.VMEM((2, kd, 4 * nr), bf), pltpu.VMEM((f, 4 * nr), bf),
            pltpu.VMEM((hd, hd), bf),
            pltpu.VMEM((2, hd, kf), f32),
            dma((51,)), dma((43,)), dma((11,)), dma((8,)), dma((5, 8)), dma((2,)), dma((3,)), dma((24,)), dma((2,)),
            dma((2,)), dma((6,)), dma((6,)), dma((6,)), dma((6,)), dma((6,)), dma((6,)), dma((2,)), dma((4,)),
        ],
        compiler_params=pltpu.CompilerParams(collective_id=0, has_side_effects=True, vmem_limit_bytes=VMEM_LIMIT - 14 * 2**20),
    )(x, dy, wg, wu, wd)


def tail_kernel(xa, dya, dwv, y, dx, dwg, dwu, dwd, sem):
    dp = lax.axis_index("dp")
    nr, kd = y.shape[0], dwd.shape[1]
    hd = kd // 2
    copies = []
    for k in range(3):
        for h in range(2):
            v = dwv.at[2 * k + h]
            if k > 0:
                copies.append((v, (dwg, dwu)[k - 1].at[pl.ds(h * hd, hd)]))
            else:
                for q in range(2):
                    copies.append((v.at[:, pl.ds(q * kd, kd)], dwd.at[pl.ds((2 * h + q) * hd, hd)]))
    for src, dst in ((xa, y), (dya, dx)):
        for r in range(4):
            copies.append((src.at[pl.ds(nr, nr), pl.ds(r * kd, kd)], dst.at[:, natural(dp, r, kd)]))
    copies = [pltpu.make_async_copy(s, t, sem.at[i]) for i, (s, t) in enumerate(copies)]
    for c in copies:
        c.start()
    for c in copies:
        c.wait()


def tail(xa, dya, dwv, nr, kd, kf):
    hbm = pl.BlockSpec(memory_space=pl.ANY)
    sds = jax.ShapeDtypeStruct
    d = xa.shape[1]
    return pl.pallas_call(
        tail_kernel,
        name="tail",
        out_shape=(sds((nr, d), bf), sds((nr, d), bf), sds((kd, kf), f32), sds((kd, kf), f32), sds((kf, kd), f32)),
        in_specs=[hbm] * 3,
        out_specs=(hbm,) * 5,
        scratch_shapes=[pltpu.SemaphoreType.DMA((16,))],
        compiler_params=pltpu.CompilerParams(vmem_limit_bytes=2**20),
    )(xa, dya, dwv)


def solution(mesh):
    rows = P(("dp", "tp"), None)
    wsp = P("dp", "tp")
    dsp = P("tp", "dp")

    def local(x, w_gate, w_up, w_down, dy):
        return tail(*fused(x, dy, w_gate, w_up, w_down)[:3], x.shape[0], *w_gate.shape)

    return jax.shard_map(local, mesh=mesh, in_specs=(rows, wsp, wsp, dsp, rows), out_specs=(rows, rows, wsp, wsp, dsp), check_vma=False)
```

```python
import jax
import jax.numpy as jnp
from jax import lax
from jax.experimental import pallas as pl
from jax.experimental.pallas import tpu as pltpu
from jax.sharding import PartitionSpec as P

MESH = pl.DeviceIdType.MESH
f32 = jnp.float32
bf = jnp.bfloat16
VMEM_LIMIT = 67043328
sc = jax.named_scope
LAG = 4


def mm(a, b):
    return lax.dot_general(a, b, (((1,), (0,)), ((), ())), preferred_element_type=f32)


def mmt(a, b):
    return lax.dot_general(a, b, (((1,), (1,)), ((), ())), preferred_element_type=f32)


def natural(dp, r, kd):
    x, c, rc, rx = dp // 2, dp % 2, r // 2, r % 2
    n = 2 * (x + rx - 2 * x * rx) + c + rc - 2 * c * rc
    return pl.ds(pl.multiple_of(n * kd, kd), kd)


def kernel(
    x_in, dy_in, wg_in, wu_in, wd_in,
    xa, dya, dwv, n00, r2, zl, far_r, near, xr1, yr1, stash,
    wg, wu, wd, act, zs, xt, ht, eye, cst,
    gs, gr, lsem, zsend, zrecv, zload, fsend, frecv, nstore, cload, xs1, xq1, ys1, yq1, s2, q2, cin, ssem,
):
    tp = lax.axis_index("tp")
    dp = lax.axis_index("dp")
    z, y = tp // 2, tp % 2
    x, c = dp // 2, dp % 2
    is_end = (z == 0) | (z == 3)
    is_mid = (z == 1) | (z == 2)
    dev_x = {"tp": tp, "dp": 2 * (1 - x) + c}
    dev_y = {"tp": 2 * z + 1 - y, "dp": dp}
    dev_c = {"tp": tp, "dp": 2 * x + 1 - c}
    dev_a = {"tp": 2 * (z + 1 - 2 * (z % 2)) + y, "dp": dp}
    dev_b = {"tp": 2 * (3 - z) + y, "dp": dp}

    fst, nst = dwv.at[pl.ds(0, 3)], dwv.at[pl.ds(3, 2)]
    nr, d = x_in.shape
    kd, kf = wg_in.shape
    f = 2 * kf
    hd = kd // 2
    hf = kf // 2

    def end(fn):
        pl.when(is_end)(fn)

    def mid(fn):
        pl.when(is_mid)(fn)

    def ncol(r):
        return natural(dp, r, kd)

    def remote(src, dst, ss, rs, dev):
        return pltpu.make_async_remote_copy(
            src_ref=src, dst_ref=dst, send_sem=ss, recv_sem=rs, device_id=dev, device_id_type=MESH
        )

    own = (wg_in, wu_in, wd_in)

    def blk(k, rx, rc, ry, lo=0, n=None):
        d0 = (2 * rc + rx) * kd + lo
        n = kd if n is None else n
        if k < 2:
            return (wg, wu)[k].at[pl.ds(d0, n), pl.ds(ry * kf, kf)]
        return wd.at[pl.ds(ry * kf, kf), pl.ds(d0, n)]

    local = [(own[k], blk(k, 0, 0, 0)) for k in range(3)]
    for src, ref in ((x_in, xa), (dy_in, dya)):
        for r in range(4):
            local.append((src.at[:, ncol(r)], ref.at[pl.ds(0, nr), pl.ds(r * kd, kd)]))
    local = [pltpu.make_async_copy(s, t, lsem.at[i]) for i, (s, t) in enumerate(local)]
    for cp in local:
        cp.start()

    bar = pltpu.get_barrier_semaphore()
    for dev in (dev_x, dev_y, dev_c, dev_a, dev_b):
        pl.semaphore_signal(bar, inc=1, device_id=dev, device_id_type=MESH)

    with sc("barrier"):
        pl.semaphore_wait(bar, 5)

    ft = min(256, f)

    def rows(s):
        return pl.ds(s * nr, nr)

    def transpose_x(rx, lo, hi):
        @pl.loop(lo, hi)
        def _(s):
            row = pl.ds(pl.multiple_of(s * nr, nr), nr)
            for rc in range(2):
                for h in range(2):
                    v = mmt(eye[...], xa[row, pl.ds((2 * rc + rx) * kd + h * hd, hd)])
                    xt[rc, pl.ds(h * hd, hd), row] = v.astype(bf)

    def wcopy(i, src, dst, dev):
        return remote(src, dst, gs.at[i], gr.at[i], dev)

    def half(rx, rc, ry, h):
        return blk(2, rx, rc, ry, h * hd, hd)

    ua = 3 * kd // 4
    mine = [blk(k, 0, 0, 0) for k in range(3)]
    xo = [wcopy(k, mine[k], blk(k, 1, 0, 0), dev_x) for k in range(2)]
    yo = [wcopy(2 + k, mine[k], blk(k, 0, 0, 1), dev_y) for k in range(2)]
    co = [wcopy(4 + k, mine[k], blk(k, 0, 1, 0), dev_c) for k in range(3)]
    xd = [wcopy(7 + h, half(0, 0, 0, h), half(1, 0, 0, h), dev_x) for h in range(2)]
    yd = [wcopy(9 + h, half(0, 0, 0, h), half(0, 0, 1, h), dev_y) for h in range(2)]
    rg = wcopy(11, blk(0, 0, 0, 1), blk(0, 1, 0, 1), dev_x)
    cuts = ((0, 2 * kd // 4), (2 * kd // 4, ua))
    rua = [wcopy(i, blk(1, 1, 0, 0, lo, hi - lo), blk(1, 1, 0, 1, lo, hi - lo), dev_y) for i, (lo, hi) in zip((12, 29), cuts)]
    rub = wcopy(13, blk(1, 0, 0, 1, ua, kd - ua), blk(1, 1, 0, 1, ua, kd - ua), dev_x)
    rd = [wcopy(14 + h, half(1, 0, 0, h), half(1, 0, 1, h), dev_y) for h in range(2)]
    cx = [wcopy(16 + k, blk(k, 1, 0, 0), blk(k, 1, 1, 0), dev_c) for k in range(2)]
    cy = [wcopy(18 + k, blk(k, 0, 0, 1), blk(k, 0, 1, 1), dev_c) for k in range(2)]
    cxd = [wcopy(20 + h, half(1, 0, 0, h), half(1, 1, 0, h), dev_c) for h in range(2)]
    cyd = [wcopy(22 + h, half(0, 0, 1, h), half(0, 1, 1, h), dev_c) for h in range(2)]
    crg = wcopy(24, blk(0, 1, 0, 1), blk(0, 1, 1, 1), dev_c)
    crua = [wcopy(i, blk(1, 1, 0, 1, lo, hi - lo), blk(1, 1, 1, 1, lo, hi - lo), dev_c) for i, (lo, hi) in zip((25, 30), cuts)]
    crub = wcopy(26, blk(1, 1, 0, 1, ua, kd - ua), blk(1, 1, 1, 1, ua, kd - ua), dev_c)
    crd = [wcopy(27 + h, half(1, 0, 1, h), half(1, 1, 1, h), dev_c) for h in range(2)]
    wcopies = (*xo, *yo, *co, *xd, *yd, rg, *rua, rub, *rd, *cx, *cy, *cxd, *cyd, crg, *crua, crub, *crd)
    nw = 31

    def slot(j, s):
        return (xa, dya)[j].at[pl.ds(s * nr, nr)]

    def acopy(src, dst, j):
        return remote(
            slot(j, src), slot(j, dst), gs.at[nw + 2 * dst + j], gr.at[nw + 2 * dst + j], dev_a
        )

    def bcopy(src, dst, j):
        return remote(
            slot(j, src), slot(j, dst), gs.at[nw + 8 + 2 * dst + j], gr.at[nw + 2 * dst + j], dev_b
        )

    def got(s, j):
        acopy(s, s, j).wait_recv()

    def stash_copy(s, p, n):
        return pltpu.make_async_copy((fst, nst)[n].at[p, pl.ds(0, nr)], stash.at[s, p, n], ssem.at[2 * p + n])

    def factor(s, n):
        return nst if n else cst if s == 3 else fst

    def stash_load(s, p, n):
        return pltpu.make_async_copy(stash.at[s, p, n], factor(s, n).at[p, pl.ds(0, nr)], ssem.at[2 * p + n])

    pending = [None, None]

    def flush(p):
        if pending[p] is not None:
            for n in range(2):
                stash_copy(pending[p], p, n).wait()
        pending[p] = None

    def ab_tiles(s, p, step):
        @pl.loop(0, kf // ft)
        def _(i):
            col = pl.ds(pl.multiple_of(p * kf + i * ft, ft), ft)
            at = (p, pl.ds(0, nr), pl.ds(pl.multiple_of(i * ft, ft), ft))

            def some_b(rx):
                b0, b1 = pl.ds(rx * kd, kd), pl.ds((2 + rx) * kd, kd)
                return mm(xa[rows(s), b0], wu[b0, col]) + mm(xa[rows(s), b1], wu[b1, col])

            if step == 1:
                fst[at] = mm(xa[rows(s), :], wg[:, col])
                nst[at] = some_b(0)
                return
            if step == 2:
                a = fst[at]
                b = nst[at] + some_b(1)
            else:
                a = mm(xa[rows(s), :], wg[:, col])
                b = mm(xa[rows(s), :], wu[:, col])
            sig = jax.nn.sigmoid(a)
            sa = a * sig
            act[2, rows(s), col] = (sa * b).astype(bf)
            fst[at] = sa
            nst[at] = b * sig * (1.0 + a * (1.0 - sig))

    def part_ab(s, p, step=0):
        with sc(f"ab{s}_{p}"):
            flush(p)
            ab_tiles(s, p, step)
            if step != 1:
                for n in range(2):
                    stash_copy(s, p, n).start()
                pending[p] = s

    gt = min(512, kf)

    def part_g(s, p):
        @pl.loop(0, kf // gt)
        def _(i):
            col = pl.ds(pl.multiple_of(p * kf + i * gt, gt), gt)
            kcol = pl.ds(pl.multiple_of(i * gt, gt), gt)
            g = mmt(dya[rows(s), :], wd[col, :])
            act[0, rows(s), col] = (g * factor(s, 1)[p, pl.ds(0, nr), kcol]).astype(bf)
            act[1, rows(s), col] = (g * factor(s, 0)[p, pl.ds(0, nr), kcol]).astype(bf)

    def gload(s):
        for p in range(2):
            for n in range(2):
                stash_load(s, p, n).start()

    def half_g(s, p, then):
        with sc(f"g{s}"):
            for n in range(2):
                stash_load(s, p, n).wait()
            part_g(s, p)
            if then is not None:
                for n in range(2):
                    stash_load(then, p, n).start()

    def front_g(s, then):
        @pl.loop(0, 2)
        def _(p):
            half_g(s, p, then)

    def keep_h(lo, hi):
        hb = min(4, f // hd)
        nh = f // (hb * hd)
        with sc("ht"):
            @pl.loop(lo * nh, hi * nh)
            def _(i):
                row = pl.ds(pl.multiple_of(i // nh * nr, nr), nr)
                for q in range(hb):
                    col = pl.ds(pl.multiple_of((i % nh * hb + q) * hd, hd), hd)
                    ht[col, row] = mmt(eye[...], act[2, row, col]).astype(bf)

    def back(ref, at, kind, s, r):
        *lead, c0 = at

        @pl.loop(0, 2)
        def _(h):
            n = pl.ds(pl.multiple_of(r * kd + h * hd, hd), hd)
            if kind == 0:
                v = mm(act[2, rows(s), :], wd[:, n])
            else:
                v = mmt(act[0, rows(s), :], wg[n, :]) + mmt(act[1, rows(s), :], wu[n, :])
            ref[(*lead, pl.ds(0, nr), pl.ds(pl.multiple_of(c0 + h * hd, hd), hd))] = v

    def zcopy(q, kind, r, half, dev):
        i = 4 * kind + r
        return remote(zs.at[4 * half + r], zl.at[q, i], zsend.at[4 * half + r], zrecv.at[q, i], dev)

    def zload_(q, kind, r, slot):
        return pltpu.make_async_copy(zl.at[q, 4 * kind + r], cst.at[slot, pl.ds(0, nr), pl.ds(0, kd)], zload.at[slot])

    def chunk(kind, s, r, half, q_add, first):
        i = 4 * half + r
        if q_add is not None:
            with sc("zrecv"):
                zcopy(q_add, kind, r, half, dev_a).wait_recv()
            zload_(q_add, kind, r, r % 2).start()
        if not first:
            with sc("zsend"):
                zcopy(0, kind, r, half, dev_a).wait_send()
        back(zs, (i, 0), kind, s, r)
        if q_add is not None:
            zload_(q_add, kind, r, r % 2).wait()
            zs[i] = zs[i] + cst[r % 2, pl.ds(0, nr), pl.ds(0, kd)]

    def jobs(*specs):
        with sc("job" + "_".join(f"{kind}{s}" for kind, s, *_ in specs)):
            @pl.loop(0, 4)
            def _(r):
                for kind, s, h, q_add, q_dst, dev, first in specs:
                    chunk(kind, s, r, h, q_add, first)
                    zcopy(q_dst, kind, r, h, dev).start()

    def finish(kind, adds, lo=0, hi=4):
        res = (xa, dya)[kind]
        with sc(f"fin{kind}"):
            @pl.loop(lo, hi)
            def _(r):
                col = pl.ds(pl.multiple_of(r * kd, kd), kd)
                part = (pl.ds(0, nr), pl.ds(0, kd))
                temp = (0, pl.ds(0, nr), pl.ds(kd, kd))
                back(cst, (0, kd), kind, 0, r)
                for n, q in enumerate(adds):
                    with sc("finrecv"):
                        zcopy(q, kind, r, 0, dev_a).wait_recv()
                    zload_(q, kind, r, n).start()
                for n, q in enumerate(adds):
                    zload_(q, kind, r, n).wait()
                v = cst[temp] + res[rows(0), col].astype(f32)
                for n in range(len(adds)):
                    v = v + cst[n, *part]
                res[rows(1), col] = v.astype(bf)

    def unit(rc, rx, j, put):
        ryi, k, half = j // 6, ((j // 2) % 3 + 2) % 3, j % 2
        f0 = (1 - ryi) * kf

        @pl.when(k < 2)
        def _():
            a = xt[rc, pl.ds(pl.multiple_of(half * hd, hd), hd), :]
            for q in range(4):
                b = act[k, :, pl.ds(pl.multiple_of(f0 + q * hd, hd), hd)]
                put(pl.ds(q * hd, hd), mm(a, b))

        @pl.when(k == 2)
        def _():
            for q in range(4):
                b = dya[:, pl.ds((2 * rc + rx) * kd + q % 2 * hd, hd)]
                a = ht[pl.ds(pl.multiple_of(f0 + half * hf + q // 2 * hd, hd), hd), :]
                put(pl.ds(q * hd, hd), mm(a, b))

    def fcopy(u):
        return remote(fst.at[u % 3], far_r.at[u], fsend.at[u % 3], frecv.at[u], dev_c)

    def ncopy(u):
        return pltpu.make_async_copy(nst.at[(u + 1) % 2], near.at[u], nstore.at[(u + 1) % 2])

    def ccopy(u):
        return pltpu.make_async_copy(far_r.at[u], cst.at[(u + 1) % 2], cload.at[(u + 1) % 2])

    def xcopy1(i, u):
        return remote(near.at[u], xr1.at[i], xs1.at[i], xq1.at[i], dev_x)

    def ycopy1(i, u):
        return remote(near.at[u], yr1.at[i], ys1.at[i], yq1.at[i], dev_y)

    def nsend(rx, j):
        ryi, k, half = j // 6, (j // 2) % 3, j % 2
        u = 12 * (1 - rx) + j
        if rx:
            @pl.when(half == 0)
            def _():
                xcopy1(ryi * 3 + k, u).start()

        @pl.when((half == 1) & (ryi == 0))
        def _():
            ycopy1(3 * (1 - rx) + k, u).start()

    def far_unit(rx, j):
        u = 12 * (1 - rx) + j

        @pl.when(u > 2)
        def _():
            with sc("fsend"):
                fcopy(u).wait_send()

        def put(col, v):
            fst[u % 3, :, col] = v

        unit(1, rx, j, put)
        fcopy(u).start()

    def dw_first(rx, n):
        with sc("dwfirst"):
            @pl.loop(0, n)
            def _(j):
                far_unit(rx, j)

    def near_load(rx, j):
        u = 12 * (1 - rx) + j
        with sc("frecv"):
            fcopy(u).wait_recv()
        ccopy(u).start()

    def near_unit(rx, j):
        u = 12 * (1 - rx) + j
        with sc("cwait"):
            ccopy(u).wait()

        def put(col, v):
            i = (u + 1) % 2
            nst[i, :, col] = v + cst[i, :, col]

        unit(0, rx, j, put)

    def near_done(rx, j):
        with sc("nwait"):
            ncopy(12 * (1 - rx) + j).wait()
        nsend(rx, j)

    def dw(rx, f0, n0):
        base = 12 * (1 - rx)

        with sc(f"dw{rx}"):
            @pl.loop(f0, 12 + LAG)
            def _(j):
                n = j - LAG

                @pl.when(j < 12)
                def _():
                    far_unit(rx, j)

                @pl.when((n + 1 >= n0) & (n < 11))
                def _():
                    near_load(rx, n + 1)

                @pl.when(n >= n0)
                def _():
                    near_unit(rx, n)

                    @pl.when(n > n0)
                    def _():
                        near_done(rx, n - 1)

                    ncopy(base + n).start()

            near_done(rx, 11)

    def add_pair(units, waits, arrived, dsts, after=(None, None)):
        cn = [pltpu.make_async_copy(near.at[u], fst.at[h], cin.at[h]) for h, u in enumerate(units)]
        cr = [pltpu.make_async_copy(v, cst.at[h], cload.at[h]) for h, v in enumerate(arrived)]
        cd = [pltpu.make_async_copy(nst.at[h], t, nstore.at[h]) for h, t in enumerate(dsts)]
        st = min(64, hd)
        for h in range(2):
            cn[h].start()
        for h in range(2):
            waits[h].wait_recv()
            cr[h].start()
        for h in range(2):
            cn[h].wait()
            cr[h].wait()

            @pl.loop(0, hd // st)
            def _(i):
                row = pl.ds(pl.multiple_of(i * st, st), st)
                nst[h, row, :] = fst[h, row, :] + cst[h, row, :]

            cd[h].start()
        for h in range(2):
            cd[h].wait()
            if after[h] is not None:
                after[h].start()

    def uid(rx, ry, k, half):
        return 12 * (1 - rx) + 6 * (1 - ry) + 2 * k + half

    def ycopy2(k):
        return remote(near.at[uid(0, 1, k, 0)], r2.at[2 * k], s2.at[2 * k], q2.at[2 * k], dev_y)

    def xcopy2(k):
        return remote(near.at[uid(1, 0, k, 1)], r2.at[2 * k + 1], s2.at[2 * k + 1], q2.at[2 * k + 1], dev_x)

    def second(k):
        ua, ub = uid(0, 1, k, 0), uid(1, 0, k, 1)
        with sc(f"second{k}"):
            add_pair(
                (ua, ub), (xcopy1(k, 0), ycopy1(k, 0)), (xr1.at[k], yr1.at[k]), (near.at[ua], near.at[ub]),
                (ycopy2(k), xcopy2(k)),
            )

    def third(k):
        ua, ub = uid(0, 0, k, 0), uid(0, 0, k, 1)
        with sc(f"third{k}"):
            add_pair(
                (ua, ub), (xcopy1(3 + k, 0), ycopy1(3 + k, 0)), (xr1.at[3 + k], yr1.at[3 + k]),
                (n00.at[2 * k], n00.at[2 * k + 1]),
            )

    def fourth(k):
        cn = [pltpu.make_async_copy(n00.at[2 * k + h], dwv.at[2 * k + h], cin.at[h]) for h in range(2)]
        cr = [pltpu.make_async_copy(r2.at[2 * k + h], cst.at[h], cload.at[h]) for h in range(2)]
        st = min(64, hd)
        with sc(f"fourth{k}"):
            for h in range(2):
                cn[h].start()
            for h in range(2):
                (ycopy2, xcopy2)[h](k).wait_recv()
                cr[h].start()
            for h in range(2):
                cn[h].wait()
                cr[h].wait()

                @pl.loop(0, hd // st)
                def _(i):
                    row = pl.ds(pl.multiple_of(i * st, st), st)
                    dwv[2 * k + h, row, :] = dwv[2 * k + h, row, :] + cst[h, row, :]

    with sc("own_in"):
        for k in range(3):
            local[k].wait()
            if k < 2:
                xo[k].start()
                yo[k].start()
        yd[0].start()
        for cp in local[3:]:
            cp.wait()
    for j in range(2):
        acopy(0, 1, j).start()

    @mid
    def _():
        for j in range(2):
            bcopy(0, 2, j).start()

    for k in range(3):
        co[k].start()

    eye[...] = (
        lax.broadcasted_iota(jnp.int32, (hd, hd), 0) == lax.broadcasted_iota(jnp.int32, (hd, hd), 1)
    ).astype(f32).astype(bf)

    with sc("xt0"):
        transpose_x(1, 0, 1)

    def pass_on(s, j):
        with sc(f"rows{s}_{j}"):
            got(s, j)
        if s == 1:
            bcopy(1, 3, j).start()
        else:
            acopy(s, s, j).start()

    with sc("gx0"):
        xo[0].wait_recv()
        cx[0].start()
        yo[0].wait_recv()
    rg.start()
    cy[0].start()

    @mid
    def _():
        pass_on(1, 0)
        pass_on(2, 0)

    with sc("gx1"):
        xo[1].wait_recv()
        for cp in rua:
            cp.start()
        yd[1].start()
        cx[1].start()
        yo[1].wait_recv()
    rub.start()
    for h in range(2):
        xd[h].start()
    cy[1].start()

    @mid
    def _():
        pass_on(1, 1)
        pass_on(2, 1)

    @end
    def _():
        with sc("e_rows1"):
            got(1, 0)

    with sc("gc0"):
        for cp in (*co[:2], *cx):
            cp.wait_recv()
    part_ab(1, 0)
    part_ab(0, 0)
    with sc("gyd"):
        yd[0].wait_recv()
        cyd[0].start()
        rg.wait_recv()
        crg.start()
    with sc("gc1"):
        for cp in (*cy, crg):
            cp.wait_recv()
    part_ab(1, 1, 1)

    @mid
    def _():
        pass_on(3, 0)

    with sc("gru"):
        for cp, fwd in zip((rua[0], rub, rua[1]), (crua[0], crub, crua[1])):
            cp.wait_recv()
            fwd.start()
    with sc("gc2"):
        for cp in (*crua, crub):
            cp.wait_recv()
    part_ab(1, 1, 2)
    with sc("gc3"):
        for cp in (co[2], cyd[0]):
            cp.wait_recv()

    def early_half(h):
        with sc(f"early1_{h}"):
            @pl.loop(0, 2)
            def _(i):
                r = 2 * i
                col = pl.ds(h * hd, hd)
                v = mm(act[2, rows(1), :], wd[:, pl.ds(pl.multiple_of(r * kd + h * hd, hd), hd)])
                zs[r, :, col] = v
                remote(zs.at[r, :, col], zl.at[0, r, :, col], zsend.at[r], zrecv.at[0, r], dev_a).start()

    def early(s, odd):
        with sc(f"early{s}_{odd}"):
            @pl.loop(0, 2)
            def _(i):
                r = 2 * i + odd
                chunk(0, s, r, s - 1, None, True)
                zcopy(s - 1, 0, r, s - 1, dev_a).start()

    @end
    def _():
        early_half(0)
        with sc("e_rows2"):
            got(2, 0)

    part_ab(2, 0)
    with sc("gd0"):
        yd[1].wait_recv()
        cyd[1].start()
        xd[0].wait_recv()
        rd[0].start()
        cxd[0].start()
        cyd[1].wait_recv()

    @end
    def _():
        early_half(1)

    part_ab(2, 1)

    @end
    def _():
        early(2, 0)

    @mid
    def _():
        pass_on(3, 1)

    with sc("gd1"):
        xd[1].wait_recv()
        rd[1].start()
        cxd[1].start()
    part_ab(0, 1)
    with sc("gd2"):
        rd[0].wait_recv()
        crd[0].start()
    transpose_x(1, 1, 3)
    keep_h(0, 3)
    with sc("gd3"):
        rd[1].wait_recv()
        crd[1].start()
        for cp in (*cxd, *crd):
            cp.wait_recv()

    @end
    def _():
        early(1, 1)
        early(2, 1)
        got(1, 1)
        got(2, 1)
        with sc("e_rows3"):
            got(3, 0)

    part_ab(3, 0)
    part_ab(3, 1)
    flush(0)
    flush(1)
    gload(1)
    transpose_x(1, 3, 4)
    keep_h(3, 4)
    front_g(1, 0)
    front_g(0, 2)
    front_g(2, 3)

    @end
    def _():
        with sc("e_rows3"):
            got(3, 1)

    dw_first(1, 2)
    half_g(3, 1, None)
    near_load(1, 0)
    half_g(3, 0, None)
    near_load(1, 1)

    @pl.loop(0, 2)
    def _(j):
        near_unit(1, j)
        ncopy(j).start()

    for j in range(2):
        near_done(1, j)
    dw(1, 2, 2)

    @end
    def _():
        jobs((0, 3, 0, None, 2, dev_a, False))

    @mid
    def _():
        jobs((0, 2, 0, 1, 3, dev_b, True))

    with sc("xtb"):
        transpose_x(0, 0, 4)
    dw(0, 0, 0)
    for u in range(3):
        fcopy(u).wait_send()
    for cp in wcopies:
        cp.wait_send()
    for j in range(2):
        acopy(0, 1, j).wait_send()

    @mid
    def _():
        for j in range(2):
            bcopy(0, 2, j).wait_send()
            bcopy(1, 3, j).wait_send()
            acopy(2, 2, j).wait_send()
            acopy(3, 3, j).wait_send()

    @end
    def _():
        jobs((1, 3, 1, None, 2, dev_a, False))
        second(0)
        second(1)
        second(2)
        jobs((1, 2, 0, None, 1, dev_a, False))
        third(0)
        third(1)
        jobs((1, 1, 1, None, 0, dev_a, False))
        third(2)
        finish(0, (0,))
        fourth(0)
        finish(1, (0,), 0, 2)
        fourth(1)
        finish(1, (0,), 2, 4)
        fourth(2)

    @mid
    def _():
        jobs((0, 3, 1, 2, 4, dev_b, True))
        second(0)
        second(1)
        second(2)
        jobs((0, 1, 0, 4, 0, dev_a, False), (1, 3, 1, 2, 4, dev_b, False))
        third(0)
        third(1)
        jobs((1, 1, 0, 4, 0, dev_a, False), (1, 2, 1, 1, 3, dev_b, False))
        third(2)
        finish(0, (0, 3))
        fourth(0)
        fourth(1)
        finish(1, (0, 3), 0, 3)
        fourth(2)
        finish(1, (0, 3), 3, 4)

    with sc("drain"):
        for half in range(2):
            for r in range(4):
                zcopy(0, 0, r, half, dev_a).wait_send()
        for i in range(6):
            xcopy1(i, 0).wait_send()
            ycopy1(i, 0).wait_send()
        for k in range(3):
            ycopy2(k).wait_send()
            xcopy2(k).wait_send()


def fused(x, dy, wg, wu, wd):
    nr, d = x.shape
    kd, kf = wg.shape
    f, hd = 2 * kf, kd // 2
    hbm = pl.BlockSpec(memory_space=pl.ANY)
    sds = jax.ShapeDtypeStruct
    out_shape = (
        pltpu.VMEM((4 * nr, d), bf), pltpu.VMEM((4 * nr, d), bf), pltpu.VMEM((6, hd, kf), f32),
        sds((6, hd, kf), f32), sds((6, hd, kf), f32),
        sds((5, 8, nr, kd), f32), sds((24, hd, kf), f32), sds((24, hd, kf), f32),
        sds((6, hd, kf), f32), sds((6, hd, kf), f32), sds((4, 2, 2, nr, kf), f32),
    )
    dma = pltpu.SemaphoreType.DMA
    return pl.pallas_call(
        kernel,
        name="fused",
        out_shape=out_shape,
        in_specs=[hbm] * 5,
        out_specs=(pl.BlockSpec(memory_space=pltpu.VMEM),) * 3 + (hbm,) * (len(out_shape) - 3),
        scratch_shapes=[
            pltpu.VMEM((d, f), bf), pltpu.VMEM((d, f), bf), pltpu.VMEM((f, d), bf),
            pltpu.VMEM((3, 4 * nr, f), bf),
            pltpu.VMEM((8, nr, kd), f32), pltpu.VMEM((2, kd, 4 * nr), bf), pltpu.VMEM((f, 4 * nr), bf),
            pltpu.VMEM((hd, hd), bf),
            pltpu.VMEM((2, hd, kf), f32),
            dma((47,)), dma((39,)), dma((11,)), dma((8,)), dma((5, 8)), dma((2,)), dma((3,)), dma((24,)), dma((2,)),
            dma((2,)), dma((6,)), dma((6,)), dma((6,)), dma((6,)), dma((6,)), dma((6,)), dma((2,)), dma((4,)),
        ],
        compiler_params=pltpu.CompilerParams(collective_id=0, has_side_effects=True, vmem_limit_bytes=VMEM_LIMIT - 14 * 2**20),
    )(x, dy, wg, wu, wd)


def tail_kernel(xa, dya, dwv, y, dx, dwg, dwu, dwd, sem):
    dp = lax.axis_index("dp")
    nr, kd = y.shape[0], dwd.shape[1]
    hd = kd // 2
    copies = []
    for k in range(3):
        for h in range(2):
            v = dwv.at[2 * k + h]
            if k > 0:
                copies.append((v, (dwg, dwu)[k - 1].at[pl.ds(h * hd, hd)]))
            else:
                for q in range(2):
                    copies.append((v.at[:, pl.ds(q * kd, kd)], dwd.at[pl.ds((2 * h + q) * hd, hd)]))
    for src, dst in ((xa, y), (dya, dx)):
        for r in range(4):
            copies.append((src.at[pl.ds(nr, nr), pl.ds(r * kd, kd)], dst.at[:, natural(dp, r, kd)]))
    copies = [pltpu.make_async_copy(s, t, sem.at[i]) for i, (s, t) in enumerate(copies)]
    for c in copies:
        c.start()
    for c in copies:
        c.wait()


def tail(xa, dya, dwv, nr, kd, kf):
    hbm = pl.BlockSpec(memory_space=pl.ANY)
    sds = jax.ShapeDtypeStruct
    d = xa.shape[1]
    return pl.pallas_call(
        tail_kernel,
        name="tail",
        out_shape=(sds((nr, d), bf), sds((nr, d), bf), sds((kd, kf), f32), sds((kd, kf), f32), sds((kf, kd), f32)),
        in_specs=[hbm] * 3,
        out_specs=(hbm,) * 5,
        scratch_shapes=[pltpu.SemaphoreType.DMA((16,))],
        compiler_params=pltpu.CompilerParams(vmem_limit_bytes=2**20),
    )(xa, dya, dwv)


def solution(mesh):
    rows = P(("dp", "tp"), None)
    wsp = P("dp", "tp")
    dsp = P("tp", "dp")

    def local(x, w_gate, w_up, w_down, dy):
        return tail(*fused(x, dy, w_gate, w_up, w_down)[:3], x.shape[0], *w_gate.shape)

    return jax.shard_map(local, mesh=mesh, in_specs=(rows, wsp, wsp, dsp, rows), out_specs=(rows, rows, wsp, wsp, dsp), check_vma=False)
```

```python
import jax
import jax.numpy as jnp
from jax import lax
from jax.experimental import pallas as pl
from jax.experimental.pallas import tpu as pltpu
from jax.sharding import PartitionSpec as P

MESH = pl.DeviceIdType.MESH
f32 = jnp.float32
bf = jnp.bfloat16
VMEM_LIMIT = 67043328
sc = jax.named_scope
LAG = 4


def mm(a, b):
    return lax.dot_general(a, b, (((1,), (0,)), ((), ())), preferred_element_type=f32)


def mmt(a, b):
    return lax.dot_general(a, b, (((1,), (1,)), ((), ())), preferred_element_type=f32)


def natural(dp, r, kd):
    x, c, rc, rx = dp // 2, dp % 2, r // 2, r % 2
    n = 2 * (x + rx - 2 * x * rx) + c + rc - 2 * c * rc
    return pl.ds(pl.multiple_of(n * kd, kd), kd)


def kernel(
    x_in, dy_in, wg_in, wu_in, wd_in,
    xa, dya, dwv, zl, n00, r2, far_r, near, xr1, yr1, stash,
    wg, wu, wd, act, zs, xt, ht, eye, cst,
    gs, gr, lsem, zsend, zrecv, zload, fsend, frecv, nstore, cload, xs1, xq1, ys1, yq1, s2, q2, cin, ssem,
):
    tp = lax.axis_index("tp")
    dp = lax.axis_index("dp")
    z, y = tp // 2, tp % 2
    x, c = dp // 2, dp % 2
    is_end = (z == 0) | (z == 3)
    is_mid = (z == 1) | (z == 2)
    dev_x = {"tp": tp, "dp": 2 * (1 - x) + c}
    dev_y = {"tp": 2 * z + 1 - y, "dp": dp}
    dev_c = {"tp": tp, "dp": 2 * x + 1 - c}
    dev_a = {"tp": 2 * (z + 1 - 2 * (z % 2)) + y, "dp": dp}
    dev_b = {"tp": 2 * (3 - z) + y, "dp": dp}

    fst, nst = dwv.at[pl.ds(0, 3)], dwv.at[pl.ds(3, 2)]
    nr, d = x_in.shape
    kd, kf = wg_in.shape
    f = 2 * kf
    hd = kd // 2
    hf = kf // 2

    def end(fn):
        pl.when(is_end)(fn)

    def mid(fn):
        pl.when(is_mid)(fn)

    def ncol(r):
        return natural(dp, r, kd)

    def remote(src, dst, ss, rs, dev):
        return pltpu.make_async_remote_copy(
            src_ref=src, dst_ref=dst, send_sem=ss, recv_sem=rs, device_id=dev, device_id_type=MESH
        )

    own = (wg_in, wu_in, wd_in)

    def blk(k, rx, rc, ry, lo=0, n=None):
        d0 = (2 * rc + rx) * kd + lo
        n = kd if n is None else n
        if k < 2:
            return (wg, wu)[k].at[pl.ds(d0, n), pl.ds(ry * kf, kf)]
        return wd.at[pl.ds(ry * kf, kf), pl.ds(d0, n)]

    local = [(own[k], blk(k, 0, 0, 0)) for k in range(3)]
    for src, ref in ((x_in, xa), (dy_in, dya)):
        for r in range(4):
            local.append((src.at[:, ncol(r)], ref.at[pl.ds(0, nr), pl.ds(r * kd, kd)]))
    local = [pltpu.make_async_copy(s, t, lsem.at[i]) for i, (s, t) in enumerate(local)]
    for cp in local:
        cp.start()

    bar = pltpu.get_barrier_semaphore()
    for dev in (dev_x, dev_y, dev_c, dev_a, dev_b):
        pl.semaphore_signal(bar, inc=1, device_id=dev, device_id_type=MESH)

    with sc("barrier"):
        pl.semaphore_wait(bar, 5)

    ft = min(256, f)

    def rows(s):
        return pl.ds(s * nr, nr)

    def transpose_x(rx, lo, hi):
        @pl.loop(lo, hi)
        def _(s):
            row = pl.ds(pl.multiple_of(s * nr, nr), nr)
            for rc in range(2):
                for h in range(2):
                    v = mmt(eye[...], xa[row, pl.ds((2 * rc + rx) * kd + h * hd, hd)])
                    xt[rc, pl.ds(h * hd, hd), row] = v.astype(bf)

    def wcopy(i, src, dst, dev):
        return remote(src, dst, gs.at[i], gr.at[i], dev)

    def half(rx, rc, ry, h):
        return blk(2, rx, rc, ry, h * hd, hd)

    ua = 3 * kd // 4
    mine = [blk(k, 0, 0, 0) for k in range(3)]
    xo = [wcopy(k, mine[k], blk(k, 1, 0, 0), dev_x) for k in range(2)]
    yo = [wcopy(2 + k, mine[k], blk(k, 0, 0, 1), dev_y) for k in range(2)]
    co = [wcopy(4 + k, mine[k], blk(k, 0, 1, 0), dev_c) for k in range(3)]
    xd = [wcopy(7 + h, half(0, 0, 0, h), half(1, 0, 0, h), dev_x) for h in range(2)]
    yd = [wcopy(9 + h, half(0, 0, 0, h), half(0, 0, 1, h), dev_y) for h in range(2)]
    rg = wcopy(11, blk(0, 0, 0, 1), blk(0, 1, 0, 1), dev_x)
    ay, ax = ((0, 5 * kd // 8), (5 * kd // 8, ua)), ((ua, 7 * kd // 8), (7 * kd // 8, kd))
    rua = [wcopy(i, blk(1, 1, 0, 0, lo, hi - lo), blk(1, 1, 0, 1, lo, hi - lo), dev_y) for i, (lo, hi) in zip((12, 29), ay)]
    rub = [wcopy(i, blk(1, 0, 0, 1, lo, hi - lo), blk(1, 1, 0, 1, lo, hi - lo), dev_x) for i, (lo, hi) in zip((13, 31), ax)]
    rd = [wcopy(14 + h, half(1, 0, 0, h), half(1, 0, 1, h), dev_y) for h in range(2)]
    cx = [wcopy(16 + k, blk(k, 1, 0, 0), blk(k, 1, 1, 0), dev_c) for k in range(2)]
    cy = [wcopy(18 + k, blk(k, 0, 0, 1), blk(k, 0, 1, 1), dev_c) for k in range(2)]
    cxd = [wcopy(20 + h, half(1, 0, 0, h), half(1, 1, 0, h), dev_c) for h in range(2)]
    cyd = [wcopy(22 + h, half(0, 0, 1, h), half(0, 1, 1, h), dev_c) for h in range(2)]
    crg = wcopy(24, blk(0, 1, 0, 1), blk(0, 1, 1, 1), dev_c)
    crua = [wcopy(i, blk(1, 1, 0, 1, lo, hi - lo), blk(1, 1, 1, 1, lo, hi - lo), dev_c) for i, (lo, hi) in zip((25, 30), ay)]
    crub = [wcopy(i, blk(1, 1, 0, 1, lo, hi - lo), blk(1, 1, 1, 1, lo, hi - lo), dev_c) for i, (lo, hi) in zip((26, 32), ax)]
    crd = [wcopy(27 + h, half(1, 0, 1, h), half(1, 1, 1, h), dev_c) for h in range(2)]
    wcopies = (*xo, *yo, *co, *xd, *yd, rg, *rua, *rub, *rd, *cx, *cy, *cxd, *cyd, crg, *crua, *crub, *crd)
    nw = 33

    def slot(j, s):
        return (xa, dya)[j].at[pl.ds(s * nr, nr)]

    def acopy(src, dst, j):
        return remote(
            slot(j, src), slot(j, dst), gs.at[nw + 2 * dst + j], gr.at[nw + 2 * dst + j], dev_a
        )

    def bcopy(src, dst, j):
        return remote(
            slot(j, src), slot(j, dst), gs.at[nw + 8 + 2 * dst + j], gr.at[nw + 2 * dst + j], dev_b
        )

    def got(s, j):
        acopy(s, s, j).wait_recv()

    def stash_copy(s, p, n):
        return pltpu.make_async_copy((fst, nst)[n].at[p, pl.ds(0, nr)], stash.at[s, p, n], ssem.at[2 * p + n])

    def factor(s, n):
        return nst if n else cst if s == 3 else fst

    def stash_load(s, p, n):
        return pltpu.make_async_copy(stash.at[s, p, n], factor(s, n).at[p, pl.ds(0, nr)], ssem.at[2 * p + n])

    pending = [None, None]

    def flush(p):
        if pending[p] is not None:
            for n in range(2):
                stash_copy(pending[p], p, n).wait()
        pending[p] = None

    def ab_tiles(s, p, step):
        def tile(i):
            col = pl.ds(pl.multiple_of(p * kf + i * ft, ft), ft)
            at = (p, pl.ds(0, nr), pl.ds(pl.multiple_of(i * ft, ft), ft))

            def some_b(rx):
                b0, b1 = pl.ds(rx * kd, kd), pl.ds((2 + rx) * kd, kd)
                return mm(xa[rows(s), b0], wu[b0, col]) + mm(xa[rows(s), b1], wu[b1, col])

            if step == 1:
                fst[at] = mm(xa[rows(s), :], wg[:, col])
                nst[at] = some_b(0)
                return
            if step == 2:
                a = fst[at]
                b = nst[at] + some_b(1)
            else:
                a = mm(xa[rows(s), :], wg[:, col])
                b = mm(xa[rows(s), :], wu[:, col])
            sig = jax.nn.sigmoid(a)
            sa = a * sig
            act[2, rows(s), col] = (sa * b).astype(bf)
            fst[at] = sa
            nst[at] = b * sig * (1.0 + a * (1.0 - sig))

        m = 2 if step == 2 and kf // ft > 1 else 1

        @pl.loop(0, kf // ft // m)
        def _(i):
            for q in range(m):
                tile(i * m + q)

    def part_ab(s, p, step=0):
        with sc(f"ab{s}_{p}"):
            flush(p)
            ab_tiles(s, p, step)
            if step != 1:
                for n in range(2):
                    stash_copy(s, p, n).start()
                pending[p] = s

    gt = min(512, kf)

    def part_g(s, p):
        @pl.loop(0, kf // gt)
        def _(i):
            col = pl.ds(pl.multiple_of(p * kf + i * gt, gt), gt)
            kcol = pl.ds(pl.multiple_of(i * gt, gt), gt)
            g = mmt(dya[rows(s), :], wd[col, :])
            act[0, rows(s), col] = (g * factor(s, 1)[p, pl.ds(0, nr), kcol]).astype(bf)
            act[1, rows(s), col] = (g * factor(s, 0)[p, pl.ds(0, nr), kcol]).astype(bf)

    def gload(s):
        for p in range(2):
            for n in range(2):
                stash_load(s, p, n).start()

    def half_g(s, p, then):
        with sc(f"g{s}"):
            for n in range(2):
                stash_load(s, p, n).wait()
            part_g(s, p)
            if then is not None:
                for n in range(2):
                    stash_load(then, p, n).start()

    def front_g(s, then):
        @pl.loop(0, 2)
        def _(p):
            half_g(s, p, then)

    def keep_h(lo, hi):
        hb = min(4, f // hd)
        nh = f // (hb * hd)
        with sc("ht"):
            @pl.loop(lo * nh, hi * nh)
            def _(i):
                row = pl.ds(pl.multiple_of(i // nh * nr, nr), nr)
                for q in range(hb):
                    col = pl.ds(pl.multiple_of((i % nh * hb + q) * hd, hd), hd)
                    ht[col, row] = mmt(eye[...], act[2, row, col]).astype(bf)

    def back(ref, at, kind, s, r):
        *lead, c0 = at

        @pl.loop(0, 2)
        def _(h):
            n = pl.ds(pl.multiple_of(r * kd + h * hd, hd), hd)
            if kind == 0:
                v = mm(act[2, rows(s), :], wd[:, n])
            else:
                v = mmt(act[0, rows(s), :], wg[n, :]) + mmt(act[1, rows(s), :], wu[n, :])
            ref[(*lead, pl.ds(0, nr), pl.ds(pl.multiple_of(c0 + h * hd, hd), hd))] = v

    def zcopy(q, kind, r, half, dev):
        i = 4 * kind + r
        return remote(zs.at[4 * half + r], zl.at[q, i], zsend.at[4 * half + r], zrecv.at[q, i], dev)

    def zload_(q, kind, r, slot):
        return pltpu.make_async_copy(zl.at[q, 4 * kind + r], cst.at[slot, pl.ds(0, nr), pl.ds(0, kd)], zload.at[slot])

    def chunk(kind, s, r, half, q_add, first):
        i = 4 * half + r
        if q_add is not None:
            with sc("zrecv"):
                zcopy(q_add, kind, r, half, dev_a).wait_recv()
            zload_(q_add, kind, r, r % 2).start()
        if not first:
            with sc("zsend"):
                zcopy(0, kind, r, half, dev_a).wait_send()
        back(zs, (i, 0), kind, s, r)
        if q_add is not None:
            zload_(q_add, kind, r, r % 2).wait()
            zs[i] = zs[i] + cst[r % 2, pl.ds(0, nr), pl.ds(0, kd)]

    def jobs(*specs):
        with sc("job" + "_".join(f"{kind}{s}" for kind, s, *_ in specs)):
            @pl.loop(0, 4)
            def _(r):
                for kind, s, h, q_add, q_dst, dev, first in specs:
                    chunk(kind, s, r, h, q_add, first)
                    zcopy(q_dst, kind, r, h, dev).start()

    def last_part():
        back(cst, (0, kd), 1, 0, 3)
        at = (0, pl.ds(0, nr), pl.ds(kd, kd))
        cst[at] = cst[at] + dya[rows(0), pl.ds(3 * kd, kd)].astype(f32)
        cp = pltpu.make_async_copy(cst.at[at], zl.at[1, 7], zload.at[0])
        cp.start()
        cp.wait()

    def finish(kind, adds, lo=0, hi=4):
        res = (xa, dya)[kind]
        with sc(f"fin{kind}"):
            @pl.loop(lo, hi)
            def _(r):
                col = pl.ds(pl.multiple_of(r * kd, kd), kd)
                part = (pl.ds(0, nr), pl.ds(0, kd))
                temp = (0, pl.ds(0, nr), pl.ds(kd, kd))
                back(cst, (0, kd), kind, 0, r)
                for n, q in enumerate(adds):
                    with sc("finrecv"):
                        zcopy(q, kind, r, 0, dev_a).wait_recv()
                    zload_(q, kind, r, n).start()
                for n, q in enumerate(adds):
                    zload_(q, kind, r, n).wait()
                v = cst[temp] + res[rows(0), col].astype(f32)
                for n in range(len(adds)):
                    v = v + cst[n, *part]
                res[rows(1), col] = v.astype(bf)

    def unit(rc, rx, j, put):
        ryi, k, half = j // 6, ((j // 2) % 3 + 2) % 3, j % 2
        f0 = (1 - ryi) * kf

        @pl.when(k < 2)
        def _():
            a = xt[rc, pl.ds(pl.multiple_of(half * hd, hd), hd), :]
            for q in range(4):
                b = act[k, :, pl.ds(pl.multiple_of(f0 + q * hd, hd), hd)]
                put(pl.ds(q * hd, hd), mm(a, b))

        @pl.when(k == 2)
        def _():
            for q in range(4):
                b = dya[:, pl.ds((2 * rc + rx) * kd + q % 2 * hd, hd)]
                a = ht[pl.ds(pl.multiple_of(f0 + half * hf + q // 2 * hd, hd), hd), :]
                put(pl.ds(q * hd, hd), mm(a, b))

    def fcopy(u):
        return remote(fst.at[u % 3], far_r.at[u], fsend.at[u % 3], frecv.at[u], dev_c)

    def ncopy(u):
        return pltpu.make_async_copy(nst.at[(u + 1) % 2], near.at[u], nstore.at[(u + 1) % 2])

    def ccopy(u):
        return pltpu.make_async_copy(far_r.at[u], cst.at[(u + 1) % 2], cload.at[(u + 1) % 2])

    def xcopy1(i, u):
        return remote(near.at[u], xr1.at[i], xs1.at[i], xq1.at[i], dev_x)

    def ycopy1(i, u):
        return remote(near.at[u], yr1.at[i], ys1.at[i], yq1.at[i], dev_y)

    def nsend(rx, j):
        ryi, k, half = j // 6, (j // 2) % 3, j % 2
        u = 12 * (1 - rx) + j
        if rx:
            @pl.when(half == 0)
            def _():
                xcopy1(ryi * 3 + k, u).start()

        @pl.when((half == 1) & (ryi == 0))
        def _():
            ycopy1(3 * (1 - rx) + k, u).start()

    def far_unit(rx, j):
        u = 12 * (1 - rx) + j

        @pl.when(u > 2)
        def _():
            with sc("fsend"):
                fcopy(u).wait_send()

        def put(col, v):
            fst[u % 3, :, col] = v

        unit(1, rx, j, put)
        fcopy(u).start()

    def dw_first(rx, n):
        with sc("dwfirst"):
            @pl.loop(0, n)
            def _(j):
                far_unit(rx, j)

    def near_load(rx, j):
        u = 12 * (1 - rx) + j
        with sc("frecv"):
            fcopy(u).wait_recv()
        ccopy(u).start()

    def near_unit(rx, j):
        u = 12 * (1 - rx) + j
        with sc("cwait"):
            ccopy(u).wait()

        def put(col, v):
            i = (u + 1) % 2
            nst[i, :, col] = v + cst[i, :, col]

        unit(0, rx, j, put)

    def near_done(rx, j):
        with sc("nwait"):
            ncopy(12 * (1 - rx) + j).wait()
        nsend(rx, j)

    def dw(rx, f0, n0):
        base = 12 * (1 - rx)

        with sc(f"dw{rx}"):
            @pl.loop(f0, 12 + LAG)
            def _(j):
                n = j - LAG

                @pl.when(j < 12)
                def _():
                    far_unit(rx, j)

                @pl.when((n + 1 >= n0) & (n < 11))
                def _():
                    near_load(rx, n + 1)

                @pl.when(n >= n0)
                def _():
                    near_unit(rx, n)

                    @pl.when(n > n0)
                    def _():
                        near_done(rx, n - 1)

                    ncopy(base + n).start()

            near_done(rx, 11)

    def add_pair(units, waits, arrived, dsts, after=(None, None)):
        cn = [pltpu.make_async_copy(near.at[u], fst.at[h], cin.at[h]) for h, u in enumerate(units)]
        cr = [pltpu.make_async_copy(v, cst.at[h], cload.at[h]) for h, v in enumerate(arrived)]
        cd = [pltpu.make_async_copy(nst.at[h], t, nstore.at[h]) for h, t in enumerate(dsts)]
        st = min(64, hd)
        for h in range(2):
            cn[h].start()
        for h in range(2):
            waits[h].wait_recv()
            cr[h].start()
        for h in range(2):
            cn[h].wait()
            cr[h].wait()

            @pl.loop(0, hd // st)
            def _(i):
                row = pl.ds(pl.multiple_of(i * st, st), st)
                nst[h, row, :] = fst[h, row, :] + cst[h, row, :]

            cd[h].start()
        for h in range(2):
            cd[h].wait()
            if after[h] is not None:
                after[h].start()

    def uid(rx, ry, k, half):
        return 12 * (1 - rx) + 6 * (1 - ry) + 2 * k + half

    def ycopy2(k):
        return remote(near.at[uid(0, 1, k, 0)], r2.at[2 * k], s2.at[2 * k], q2.at[2 * k], dev_y)

    def xcopy2(k):
        return remote(near.at[uid(1, 0, k, 1)], r2.at[2 * k + 1], s2.at[2 * k + 1], q2.at[2 * k + 1], dev_x)

    def second(k):
        ua, ub = uid(0, 1, k, 0), uid(1, 0, k, 1)
        with sc(f"second{k}"):
            add_pair(
                (ua, ub), (xcopy1(k, 0), ycopy1(k, 0)), (xr1.at[k], yr1.at[k]), (near.at[ua], near.at[ub]),
                (ycopy2(k), xcopy2(k)),
            )

    def third(k):
        ua, ub = uid(0, 0, k, 0), uid(0, 0, k, 1)
        with sc(f"third{k}"):
            add_pair(
                (ua, ub), (xcopy1(3 + k, 0), ycopy1(3 + k, 0)), (xr1.at[3 + k], yr1.at[3 + k]),
                (n00.at[2 * k], n00.at[2 * k + 1]),
            )

    def fourth(k):
        cn = [pltpu.make_async_copy(n00.at[2 * k + h], dwv.at[2 * k + h], cin.at[h]) for h in range(2)]
        cr = [pltpu.make_async_copy(r2.at[2 * k + h], cst.at[h], cload.at[h]) for h in range(2)]
        st = min(64, hd)
        with sc(f"fourth{k}"):
            for h in range(2):
                cn[h].start()
            for h in range(2):
                (ycopy2, xcopy2)[h](k).wait_recv()
                cr[h].start()
            for h in range(2):
                cn[h].wait()
                cr[h].wait()

                @pl.loop(0, hd // st)
                def _(i):
                    row = pl.ds(pl.multiple_of(i * st, st), st)
                    dwv[2 * k + h, row, :] = dwv[2 * k + h, row, :] + cst[h, row, :]

    with sc("own_in"):
        for k in range(3):
            local[k].wait()
            if k < 2:
                xo[k].start()
                yo[k].start()
        yd[0].start()
        for cp in local[3:]:
            cp.wait()
    for j in range(2):
        acopy(0, 1, j).start()

    @mid
    def _():
        for j in range(2):
            bcopy(0, 2, j).start()

    for k in range(3):
        co[k].start()

    eye[...] = (
        lax.broadcasted_iota(jnp.int32, (hd, hd), 0) == lax.broadcasted_iota(jnp.int32, (hd, hd), 1)
    ).astype(f32).astype(bf)

    with sc("xt0"):
        transpose_x(1, 0, 1)

    def pass_on(s, j):
        with sc(f"rows{s}_{j}"):
            got(s, j)
        if s == 1:
            bcopy(1, 3, j).start()
        else:
            acopy(s, s, j).start()

    with sc("gx0"):
        xo[0].wait_recv()
        cx[0].start()
        yo[0].wait_recv()
    rg.start()
    cy[0].start()

    @mid
    def _():
        pass_on(1, 0)
        pass_on(2, 0)

    with sc("gx1"):
        xo[1].wait_recv()
        for cp in rua:
            cp.start()
        yd[1].start()
        cx[1].start()
        yo[1].wait_recv()
    for cp in rub:
        cp.start()
    for h in range(2):
        xd[h].start()
    cy[1].start()

    @mid
    def _():
        pass_on(1, 1)
        pass_on(2, 1)

    @end
    def _():
        with sc("e_rows1"):
            got(1, 0)

    with sc("gc0"):
        for cp in (*co[:2], *cx):
            cp.wait_recv()
    part_ab(1, 0)
    part_ab(0, 0)
    with sc("gyd"):
        yd[0].wait_recv()
        cyd[0].start()
        rg.wait_recv()
        crg.start()
    with sc("gc1"):
        for cp in (*cy, crg):
            cp.wait_recv()
    part_ab(1, 1, 1)

    @mid
    def _():
        pass_on(3, 0)

    with sc("gru"):
        for cp, fwd in zip((*rua[:1], *rub[:1], *rua[1:], *rub[1:]), (*crua[:1], *crub[:1], *crua[1:], *crub[1:])):
            cp.wait_recv()
            fwd.start()
    with sc("gc2"):
        for cp in (*crua, *crub):
            cp.wait_recv()
    part_ab(1, 1, 2)
    with sc("gc3"):
        for cp in (co[2], cyd[0]):
            cp.wait_recv()

    def early_half(h):
        with sc(f"early1_{h}"):
            @pl.loop(0, 2)
            def _(i):
                r = 2 * i
                col = pl.ds(h * hd, hd)
                v = mm(act[2, rows(1), :], wd[:, pl.ds(pl.multiple_of(r * kd + h * hd, hd), hd)])
                zs[r, :, col] = v
                remote(zs.at[r, :, col], zl.at[0, r, :, col], zsend.at[r], zrecv.at[0, r], dev_a).start()

    def early(s, odd):
        with sc(f"early{s}_{odd}"):
            @pl.loop(0, 2)
            def _(i):
                r = 2 * i + odd
                chunk(0, s, r, s - 1, None, True)
                zcopy(s - 1, 0, r, s - 1, dev_a).start()

    @end
    def _():
        early_half(0)
        with sc("e_rows2"):
            got(2, 0)

    part_ab(2, 0)
    with sc("gd0"):
        yd[1].wait_recv()
        cyd[1].start()
        xd[0].wait_recv()
        rd[0].start()
        cxd[0].start()
        cyd[1].wait_recv()

    @end
    def _():
        early_half(1)

    part_ab(2, 1)

    @end
    def _():
        early(2, 0)

    @mid
    def _():
        pass_on(3, 1)

    with sc("gd1"):
        xd[1].wait_recv()
        rd[1].start()
        cxd[1].start()
    part_ab(0, 1)
    with sc("gd2"):
        rd[0].wait_recv()
        crd[0].start()
    transpose_x(1, 1, 3)
    keep_h(0, 3)
    with sc("gd3"):
        rd[1].wait_recv()
        crd[1].start()
        for cp in (*cxd, *crd):
            cp.wait_recv()

    @end
    def _():
        early(1, 1)
        early(2, 1)
        got(1, 1)
        got(2, 1)
        with sc("e_rows3"):
            got(3, 0)

    part_ab(3, 0)
    part_ab(3, 1)
    flush(0)
    flush(1)
    gload(1)
    transpose_x(1, 3, 4)
    keep_h(3, 4)
    front_g(1, 0)
    front_g(0, 2)
    front_g(2, 3)

    @end
    def _():
        with sc("e_rows3"):
            got(3, 1)

    dw_first(1, 2)
    half_g(3, 1, None)
    near_load(1, 0)
    half_g(3, 0, None)
    near_load(1, 1)

    @pl.loop(0, 2)
    def _(j):
        near_unit(1, j)
        ncopy(j).start()

    for j in range(2):
        near_done(1, j)
    dw(1, 2, 2)

    @end
    def _():
        jobs((0, 3, 0, None, 2, dev_a, False))

    @mid
    def _():
        jobs((0, 2, 0, 1, 3, dev_b, True))

    with sc("xtb"):
        transpose_x(0, 0, 4)
    dw(0, 0, 0)
    for u in range(3):
        fcopy(u).wait_send()
    for cp in wcopies:
        cp.wait_send()
    for j in range(2):
        acopy(0, 1, j).wait_send()

    @mid
    def _():
        for j in range(2):
            bcopy(0, 2, j).wait_send()
            bcopy(1, 3, j).wait_send()
            acopy(2, 2, j).wait_send()
            acopy(3, 3, j).wait_send()

    @end
    def _():
        jobs((1, 3, 1, None, 2, dev_a, False))
        second(0)
        second(1)
        second(2)
        jobs((1, 2, 0, None, 1, dev_a, False))
        third(0)
        third(1)
        jobs((1, 1, 1, None, 0, dev_a, False))
        third(2)
        finish(0, (0,))
        last_part()
        fourth(0)
        finish(1, (0,), 0, 2)
        fourth(1)
        finish(1, (0,), 2, 3)
        fourth(2)

    @mid
    def _():
        jobs((0, 3, 1, 2, 4, dev_b, True))
        second(0)
        second(1)
        second(2)
        jobs((0, 1, 0, 4, 0, dev_a, False), (1, 3, 1, 2, 4, dev_b, False))
        third(0)
        third(1)
        jobs((1, 1, 0, 4, 0, dev_a, False), (1, 2, 1, 1, 3, dev_b, False))
        third(2)
        finish(0, (0, 3))
        fourth(0)
        fourth(1)
        last_part()
        finish(1, (0, 3), 0, 3)
        fourth(2)
        zcopy(3, 1, 3, 0, dev_a).wait_recv()

    zcopy(0, 1, 3, 0, dev_a).wait_recv()

    with sc("drain"):
        for half in range(2):
            for r in range(4):
                zcopy(0, 0, r, half, dev_a).wait_send()
        for i in range(6):
            xcopy1(i, 0).wait_send()
            ycopy1(i, 0).wait_send()
        for k in range(3):
            ycopy2(k).wait_send()
            xcopy2(k).wait_send()


def fused(x, dy, wg, wu, wd):
    nr, d = x.shape
    kd, kf = wg.shape
    f, hd = 2 * kf, kd // 2
    hbm = pl.BlockSpec(memory_space=pl.ANY)
    sds = jax.ShapeDtypeStruct
    out_shape = (
        pltpu.VMEM((4 * nr, d), bf), pltpu.VMEM((4 * nr, d), bf), pltpu.VMEM((6, hd, kf), f32),
        sds((5, 8, nr, kd), f32), sds((6, hd, kf), f32), sds((6, hd, kf), f32),
        sds((24, hd, kf), f32), sds((24, hd, kf), f32),
        sds((6, hd, kf), f32), sds((6, hd, kf), f32), sds((4, 2, 2, nr, kf), f32),
    )
    dma = pltpu.SemaphoreType.DMA
    return pl.pallas_call(
        kernel,
        name="fused",
        out_shape=out_shape,
        in_specs=[hbm] * 5,
        out_specs=(pl.BlockSpec(memory_space=pltpu.VMEM),) * 3 + (hbm,) * (len(out_shape) - 3),
        scratch_shapes=[
            pltpu.VMEM((d, f), bf), pltpu.VMEM((d, f), bf), pltpu.VMEM((f, d), bf),
            pltpu.VMEM((3, 4 * nr, f), bf),
            pltpu.VMEM((8, nr, kd), f32), pltpu.VMEM((2, kd, 4 * nr), bf), pltpu.VMEM((f, 4 * nr), bf),
            pltpu.VMEM((hd, hd), bf),
            pltpu.VMEM((2, hd, kf), f32),
            dma((49,)), dma((41,)), dma((11,)), dma((8,)), dma((5, 8)), dma((2,)), dma((3,)), dma((24,)), dma((2,)),
            dma((2,)), dma((6,)), dma((6,)), dma((6,)), dma((6,)), dma((6,)), dma((6,)), dma((2,)), dma((4,)),
        ],
        compiler_params=pltpu.CompilerParams(collective_id=0, has_side_effects=True, vmem_limit_bytes=VMEM_LIMIT - 14 * 2**20),
    )(x, dy, wg, wu, wd)


def tail_kernel(xa, dya, dwv, zl, y, dx, dwg, dwu, dwd, buf, out, sem, lsem):
    dp = lax.axis_index("dp")
    z = lax.axis_index("tp") // 2
    is_mid = (z == 1) | (z == 2)
    nr, kd = y.shape[0], dwd.shape[1]
    hd = kd // 2
    srcs = (zl.at[1, 7], zl.at[0, 7], zl.at[3, 7])
    loads = [pltpu.make_async_copy(v, buf.at[i], lsem.at[i]) for i, v in enumerate(srcs)]
    loads[0].start()
    loads[1].start()

    @pl.when(is_mid)
    def _():
        loads[2].start()

    copies = []
    for k in range(3):
        for h in range(2):
            v = dwv.at[2 * k + h]
            if k > 0:
                copies.append((v, (dwg, dwu)[k - 1].at[pl.ds(h * hd, hd)]))
            else:
                for q in range(2):
                    copies.append((v.at[:, pl.ds(q * kd, kd)], dwd.at[pl.ds((2 * h + q) * hd, hd)]))
    for src, dst, n in ((xa, y, 4), (dya, dx, 3)):
        for r in range(n):
            copies.append((src.at[pl.ds(nr, nr), pl.ds(r * kd, kd)], dst.at[:, natural(dp, r, kd)]))
    copies.append((out, dx.at[:, natural(dp, 3, kd)]))
    copies = [pltpu.make_async_copy(s, t, sem.at[i]) for i, (s, t) in enumerate(copies)]
    for c in copies[:-1]:
        c.start()
    loads[0].wait()
    loads[1].wait()
    buf[0] = buf[0] + buf[1]

    @pl.when(is_mid)
    def _():
        loads[2].wait()
        buf[0] = buf[0] + buf[2]

    out[...] = buf[0].astype(bf)
    copies[-1].start()
    for c in copies:
        c.wait()


def tail(xa, dya, dwv, zl, nr, kd, kf):
    hbm = pl.BlockSpec(memory_space=pl.ANY)
    sds = jax.ShapeDtypeStruct
    d = xa.shape[1]
    dma = pltpu.SemaphoreType.DMA
    return pl.pallas_call(
        tail_kernel,
        name="tail",
        out_shape=(sds((nr, d), bf), sds((nr, d), bf), sds((kd, kf), f32), sds((kd, kf), f32), sds((kf, kd), f32)),
        in_specs=[hbm] * 4,
        out_specs=(hbm,) * 5,
        scratch_shapes=[pltpu.VMEM((3, nr, kd), f32), pltpu.VMEM((nr, kd), bf), dma((16,)), dma((3,))],
        compiler_params=pltpu.CompilerParams(vmem_limit_bytes=VMEM_LIMIT - 27 * 2**20),
    )(xa, dya, dwv, zl)


def solution(mesh):
    rows = P(("dp", "tp"), None)
    wsp = P("dp", "tp")
    dsp = P("tp", "dp")

    def local(x, w_gate, w_up, w_down, dy):
        return tail(*fused(x, dy, w_gate, w_up, w_down)[:4], x.shape[0], *w_gate.shape)

    return jax.shard_map(local, mesh=mesh, in_specs=(rows, wsp, wsp, dsp, rows), out_specs=(rows, rows, wsp, wsp, dsp), check_vma=False)
```

```python
import jax
import jax.numpy as jnp
from jax import lax
from jax.experimental import pallas as pl
from jax.experimental.pallas import tpu as pltpu
from jax.sharding import PartitionSpec as P

MESH = pl.DeviceIdType.MESH
f32 = jnp.float32
bf = jnp.bfloat16
VMEM_LIMIT = 67043328
sc = jax.named_scope
LAG = 4


def mm(a, b):
    return lax.dot_general(a, b, (((1,), (0,)), ((), ())), preferred_element_type=f32)


def mmt(a, b):
    return lax.dot_general(a, b, (((1,), (1,)), ((), ())), preferred_element_type=f32)


def natural(dp, r, kd):
    x, c, rc, rx = dp // 2, dp % 2, r // 2, r % 2
    n = 2 * (x + rx - 2 * x * rx) + c + rc - 2 * c * rc
    return pl.ds(pl.multiple_of(n * kd, kd), kd)


def kernel(
    x_in, dy_in, wg_in, wu_in, wd_in,
    xa, dya, dwv, zl, near, n00, far_r, xr1, yr1, stash,
    wg, wu, wd, act, zs, xt, ht, eye, cst,
    gs, gr, lsem, zsend, zrecv, zload, fsend, frecv, nstore, cload, xs1, xq1, ys1, yq1, s2, q2, cin, ssem,
):
    tp = lax.axis_index("tp")
    dp = lax.axis_index("dp")
    z, y = tp // 2, tp % 2
    x, c = dp // 2, dp % 2
    is_end = (z == 0) | (z == 3)
    is_mid = (z == 1) | (z == 2)
    dev_x = {"tp": tp, "dp": 2 * (1 - x) + c}
    dev_y = {"tp": 2 * z + 1 - y, "dp": dp}
    dev_c = {"tp": tp, "dp": 2 * x + 1 - c}
    dev_a = {"tp": 2 * (z + 1 - 2 * (z % 2)) + y, "dp": dp}
    dev_b = {"tp": 2 * (3 - z) + y, "dp": dp}

    r2 = near.at[pl.ds(24, 6)]
    fst, nst = dwv.at[pl.ds(0, 3)], dwv.at[pl.ds(3, 2)]
    nr, d = x_in.shape
    kd, kf = wg_in.shape
    f = 2 * kf
    hd = kd // 2
    hf = kf // 2

    def end(fn):
        pl.when(is_end)(fn)

    def mid(fn):
        pl.when(is_mid)(fn)

    def ncol(r):
        return natural(dp, r, kd)

    def remote(src, dst, ss, rs, dev):
        return pltpu.make_async_remote_copy(
            src_ref=src, dst_ref=dst, send_sem=ss, recv_sem=rs, device_id=dev, device_id_type=MESH
        )

    own = (wg_in, wu_in, wd_in)

    def blk(k, rx, rc, ry, lo=0, n=None):
        d0 = (2 * rc + rx) * kd + lo
        n = kd if n is None else n
        if k < 2:
            return (wg, wu)[k].at[pl.ds(d0, n), pl.ds(ry * kf, kf)]
        return wd.at[pl.ds(ry * kf, kf), pl.ds(d0, n)]

    local = [(own[k], blk(k, 0, 0, 0)) for k in range(3)]
    for src, ref in ((x_in, xa), (dy_in, dya)):
        for r in range(4):
            local.append((src.at[:, ncol(r)], ref.at[pl.ds(0, nr), pl.ds(r * kd, kd)]))
    local = [pltpu.make_async_copy(s, t, lsem.at[i]) for i, (s, t) in enumerate(local)]
    for cp in local:
        cp.start()

    bar = pltpu.get_barrier_semaphore()
    for dev in (dev_x, dev_y, dev_c, dev_a, dev_b):
        pl.semaphore_signal(bar, inc=1, device_id=dev, device_id_type=MESH)

    with sc("barrier"):
        pl.semaphore_wait(bar, 5)

    ft = min(256, f)

    def rows(s):
        return pl.ds(s * nr, nr)

    def transpose_x(rx, lo, hi):
        @pl.loop(lo, hi)
        def _(s):
            row = pl.ds(pl.multiple_of(s * nr, nr), nr)
            for rc in range(2):
                for h in range(2):
                    v = mmt(eye[...], xa[row, pl.ds((2 * rc + rx) * kd + h * hd, hd)])
                    xt[rc, pl.ds(h * hd, hd), row] = v.astype(bf)

    def wcopy(i, src, dst, dev):
        return remote(src, dst, gs.at[i], gr.at[i], dev)

    def half(rx, rc, ry, h):
        return blk(2, rx, rc, ry, h * hd, hd)

    ua = 3 * kd // 4
    mine = [blk(k, 0, 0, 0) for k in range(3)]
    xo = [wcopy(k, mine[k], blk(k, 1, 0, 0), dev_x) for k in range(2)]
    yo = [wcopy(2 + k, mine[k], blk(k, 0, 0, 1), dev_y) for k in range(2)]
    co = [wcopy(4 + k, mine[k], blk(k, 0, 1, 0), dev_c) for k in range(3)]
    xd = [wcopy(7 + h, half(0, 0, 0, h), half(1, 0, 0, h), dev_x) for h in range(2)]
    yd = [wcopy(9 + h, half(0, 0, 0, h), half(0, 0, 1, h), dev_y) for h in range(2)]
    rg = wcopy(11, blk(0, 0, 0, 1), blk(0, 1, 0, 1), dev_x)
    ay, ax = ((0, 5 * kd // 8), (5 * kd // 8, ua)), ((ua, 7 * kd // 8), (7 * kd // 8, kd))
    rua = [wcopy(i, blk(1, 1, 0, 0, lo, hi - lo), blk(1, 1, 0, 1, lo, hi - lo), dev_y) for i, (lo, hi) in zip((12, 29), ay)]
    rub = [wcopy(i, blk(1, 0, 0, 1, lo, hi - lo), blk(1, 1, 0, 1, lo, hi - lo), dev_x) for i, (lo, hi) in zip((13, 31), ax)]
    rd = [wcopy(14 + h, half(1, 0, 0, h), half(1, 0, 1, h), dev_y) for h in range(2)]
    cx = [wcopy(16 + k, blk(k, 1, 0, 0), blk(k, 1, 1, 0), dev_c) for k in range(2)]
    cy = [wcopy(18 + k, blk(k, 0, 0, 1), blk(k, 0, 1, 1), dev_c) for k in range(2)]
    cxd = [wcopy(20 + h, half(1, 0, 0, h), half(1, 1, 0, h), dev_c) for h in range(2)]
    cyd = [wcopy(22 + h, half(0, 0, 1, h), half(0, 1, 1, h), dev_c) for h in range(2)]
    crg = wcopy(24, blk(0, 1, 0, 1), blk(0, 1, 1, 1), dev_c)
    crua = [wcopy(i, blk(1, 1, 0, 1, lo, hi - lo), blk(1, 1, 1, 1, lo, hi - lo), dev_c) for i, (lo, hi) in zip((25, 30), ay)]
    crub = [wcopy(i, blk(1, 1, 0, 1, lo, hi - lo), blk(1, 1, 1, 1, lo, hi - lo), dev_c) for i, (lo, hi) in zip((26, 32), ax)]
    crd = [wcopy(27 + h, half(1, 0, 1, h), half(1, 1, 1, h), dev_c) for h in range(2)]
    wcopies = (*xo, *yo, *co, *xd, *yd, rg, *rua, *rub, *rd, *cx, *cy, *cxd, *cyd, crg, *crua, *crub, *crd)
    nw = 33

    def slot(j, s):
        return (xa, dya)[j].at[pl.ds(s * nr, nr)]

    def acopy(src, dst, j):
        return remote(
            slot(j, src), slot(j, dst), gs.at[nw + 2 * dst + j], gr.at[nw + 2 * dst + j], dev_a
        )

    def bcopy(src, dst, j):
        return remote(
            slot(j, src), slot(j, dst), gs.at[nw + 8 + 2 * dst + j], gr.at[nw + 2 * dst + j], dev_b
        )

    def got(s, j):
        acopy(s, s, j).wait_recv()

    def stash_copy(s, p, n):
        return pltpu.make_async_copy((fst, nst)[n].at[p, pl.ds(0, nr)], stash.at[s, p, n], ssem.at[2 * p + n])

    def factor(s, n):
        return nst if n else cst if s == 3 else fst

    def stash_load(s, p, n):
        return pltpu.make_async_copy(stash.at[s, p, n], factor(s, n).at[p, pl.ds(0, nr)], ssem.at[2 * p + n])

    pending = [None, None]

    def flush(p):
        if pending[p] is not None:
            for n in range(2):
                stash_copy(pending[p], p, n).wait()
        pending[p] = None

    def ab_tiles(s, p, step):
        def tile(i):
            col = pl.ds(pl.multiple_of(p * kf + i * ft, ft), ft)
            at = (p, pl.ds(0, nr), pl.ds(pl.multiple_of(i * ft, ft), ft))

            def some_b(rx):
                b0, b1 = pl.ds(rx * kd, kd), pl.ds((2 + rx) * kd, kd)
                return mm(xa[rows(s), b0], wu[b0, col]) + mm(xa[rows(s), b1], wu[b1, col])

            if step == 1:
                fst[at] = mm(xa[rows(s), :], wg[:, col])
                nst[at] = some_b(0)
                return
            if step == 2:
                a = fst[at]
                b = nst[at] + some_b(1)
            else:
                a = mm(xa[rows(s), :], wg[:, col])
                b = mm(xa[rows(s), :], wu[:, col])
            sig = jax.nn.sigmoid(a)
            sa = a * sig
            act[2, rows(s), col] = (sa * b).astype(bf)
            fst[at] = sa
            nst[at] = b * sig * (1.0 + a * (1.0 - sig))

        m = 2 if step == 2 and kf // ft > 1 else 1

        @pl.loop(0, kf // ft // m)
        def _(i):
            for q in range(m):
                tile(i * m + q)

    def part_ab(s, p, step=0):
        with sc(f"ab{s}_{p}"):
            flush(p)
            ab_tiles(s, p, step)
            if step != 1:
                for n in range(2):
                    stash_copy(s, p, n).start()
                pending[p] = s

    gt = min(512, kf)

    def part_g(s, p):
        @pl.loop(0, kf // gt)
        def _(i):
            col = pl.ds(pl.multiple_of(p * kf + i * gt, gt), gt)
            kcol = pl.ds(pl.multiple_of(i * gt, gt), gt)
            g = mmt(dya[rows(s), :], wd[col, :])
            act[0, rows(s), col] = (g * factor(s, 1)[p, pl.ds(0, nr), kcol]).astype(bf)
            act[1, rows(s), col] = (g * factor(s, 0)[p, pl.ds(0, nr), kcol]).astype(bf)

    def gload(s):
        for p in range(2):
            for n in range(2):
                stash_load(s, p, n).start()

    def half_g(s, p, then):
        with sc(f"g{s}"):
            for n in range(2):
                stash_load(s, p, n).wait()
            part_g(s, p)
            if then is not None:
                for n in range(2):
                    stash_load(then, p, n).start()

    def front_g(s, then):
        @pl.loop(0, 2)
        def _(p):
            half_g(s, p, then)

    def keep_h(lo, hi):
        hb = min(4, f // hd)
        nh = f // (hb * hd)
        with sc("ht"):
            @pl.loop(lo * nh, hi * nh)
            def _(i):
                row = pl.ds(pl.multiple_of(i // nh * nr, nr), nr)
                for q in range(hb):
                    col = pl.ds(pl.multiple_of((i % nh * hb + q) * hd, hd), hd)
                    ht[col, row] = mmt(eye[...], act[2, row, col]).astype(bf)

    def back(ref, at, kind, s, r):
        *lead, c0 = at

        @pl.loop(0, 2)
        def _(h):
            n = pl.ds(pl.multiple_of(r * kd + h * hd, hd), hd)
            if kind == 0:
                v = mm(act[2, rows(s), :], wd[:, n])
            else:
                v = mmt(act[0, rows(s), :], wg[n, :]) + mmt(act[1, rows(s), :], wu[n, :])
            ref[(*lead, pl.ds(0, nr), pl.ds(pl.multiple_of(c0 + h * hd, hd), hd))] = v

    def zcopy(q, kind, r, half, dev):
        i = 4 * kind + r
        return remote(zs.at[4 * half + r], zl.at[q, i], zsend.at[4 * half + r], zrecv.at[q, i], dev)

    def zload_(q, kind, r, slot):
        return pltpu.make_async_copy(zl.at[q, 4 * kind + r], cst.at[slot, pl.ds(0, nr), pl.ds(0, kd)], zload.at[slot])

    def chunk(kind, s, r, half, q_add, first):
        i = 4 * half + r
        if q_add is not None:
            with sc("zrecv"):
                zcopy(q_add, kind, r, half, dev_a).wait_recv()
            zload_(q_add, kind, r, r % 2).start()
        if not first:
            with sc("zsend"):
                zcopy(0, kind, r, half, dev_a).wait_send()
        back(zs, (i, 0), kind, s, r)
        if q_add is not None:
            zload_(q_add, kind, r, r % 2).wait()
            zs[i] = zs[i] + cst[r % 2, pl.ds(0, nr), pl.ds(0, kd)]

    def jobs(*specs):
        with sc("job" + "_".join(f"{kind}{s}" for kind, s, *_ in specs)):
            @pl.loop(0, 4)
            def _(r):
                for kind, s, h, q_add, q_dst, dev, first in specs:
                    chunk(kind, s, r, h, q_add, first)
                    zcopy(q_dst, kind, r, h, dev).start()

    def last_part():
        back(cst, (0, kd), 1, 0, 3)
        at = (0, pl.ds(0, nr), pl.ds(kd, kd))
        cst[at] = cst[at] + dya[rows(0), pl.ds(3 * kd, kd)].astype(f32)
        cp = pltpu.make_async_copy(cst.at[at], zl.at[1, 7], zload.at[0])
        cp.start()
        cp.wait()

    def finish(kind, adds, lo=0, hi=4):
        res = (xa, dya)[kind]
        with sc(f"fin{kind}"):
            @pl.loop(lo, hi)
            def _(r):
                col = pl.ds(pl.multiple_of(r * kd, kd), kd)
                part = (pl.ds(0, nr), pl.ds(0, kd))
                temp = (0, pl.ds(0, nr), pl.ds(kd, kd))
                back(cst, (0, kd), kind, 0, r)
                for n, q in enumerate(adds):
                    with sc("finrecv"):
                        zcopy(q, kind, r, 0, dev_a).wait_recv()
                    zload_(q, kind, r, n).start()
                for n, q in enumerate(adds):
                    zload_(q, kind, r, n).wait()
                v = cst[temp] + res[rows(0), col].astype(f32)
                for n in range(len(adds)):
                    v = v + cst[n, *part]
                res[rows(1), col] = v.astype(bf)

    def unit(rc, rx, j, put):
        ryi, k, half = j // 6, ((j // 2) % 3 + 2) % 3, j % 2
        f0 = (1 - ryi) * kf

        @pl.when(k < 2)
        def _():
            a = xt[rc, pl.ds(pl.multiple_of(half * hd, hd), hd), :]
            for q in range(4):
                b = act[k, :, pl.ds(pl.multiple_of(f0 + q * hd, hd), hd)]
                put(pl.ds(q * hd, hd), mm(a, b))

        @pl.when(k == 2)
        def _():
            for q in range(4):
                b = dya[:, pl.ds((2 * rc + rx) * kd + q % 2 * hd, hd)]
                a = ht[pl.ds(pl.multiple_of(f0 + half * hf + q // 2 * hd, hd), hd), :]
                put(pl.ds(q * hd, hd), mm(a, b))

    def fcopy(u):
        return remote(fst.at[u % 3], far_r.at[u], fsend.at[u % 3], frecv.at[u], dev_c)

    def ncopy(u):
        return pltpu.make_async_copy(nst.at[(u + 1) % 2], near.at[u], nstore.at[(u + 1) % 2])

    def ccopy(u):
        return pltpu.make_async_copy(far_r.at[u], cst.at[(u + 1) % 2], cload.at[(u + 1) % 2])

    def xcopy1(i, u):
        return remote(near.at[u], xr1.at[i], xs1.at[i], xq1.at[i], dev_x)

    def ycopy1(i, u):
        return remote(near.at[u], yr1.at[i], ys1.at[i], yq1.at[i], dev_y)

    def nsend(rx, j):
        ryi, k, half = j // 6, (j // 2) % 3, j % 2
        u = 12 * (1 - rx) + j
        if rx:
            @pl.when(half == 0)
            def _():
                xcopy1(ryi * 3 + k, u).start()

        @pl.when((half == 1) & (ryi == 0))
        def _():
            ycopy1(3 * (1 - rx) + k, u).start()

    def far_unit(rx, j):
        u = 12 * (1 - rx) + j

        @pl.when(u > 2)
        def _():
            with sc("fsend"):
                fcopy(u).wait_send()

        def put(col, v):
            fst[u % 3, :, col] = v

        unit(1, rx, j, put)
        fcopy(u).start()

    def dw_first(rx, n):
        with sc("dwfirst"):
            @pl.loop(0, n)
            def _(j):
                far_unit(rx, j)

    def near_load(rx, j):
        u = 12 * (1 - rx) + j
        with sc("frecv"):
            fcopy(u).wait_recv()
        ccopy(u).start()

    def near_unit(rx, j):
        u = 12 * (1 - rx) + j
        with sc("cwait"):
            ccopy(u).wait()

        def put(col, v):
            i = (u + 1) % 2
            nst[i, :, col] = v + cst[i, :, col]

        unit(0, rx, j, put)

    def near_done(rx, j):
        with sc("nwait"):
            ncopy(12 * (1 - rx) + j).wait()
        nsend(rx, j)

    def dw(rx, f0, n0):
        base = 12 * (1 - rx)

        with sc(f"dw{rx}"):
            @pl.loop(f0, 12 + LAG)
            def _(j):
                n = j - LAG

                @pl.when(j < 12)
                def _():
                    far_unit(rx, j)

                @pl.when((n + 1 >= n0) & (n < 11))
                def _():
                    near_load(rx, n + 1)

                @pl.when(n >= n0)
                def _():
                    near_unit(rx, n)

                    @pl.when(n > n0)
                    def _():
                        near_done(rx, n - 1)

                    ncopy(base + n).start()

            near_done(rx, 11)

    def add_pair(units, waits, arrived, dsts, after=(None, None)):
        cn = [pltpu.make_async_copy(near.at[u], fst.at[h], cin.at[h]) for h, u in enumerate(units)]
        cr = [pltpu.make_async_copy(v, cst.at[h], cload.at[h]) for h, v in enumerate(arrived)]
        cd = [pltpu.make_async_copy(nst.at[h], t, nstore.at[h]) for h, t in enumerate(dsts)]
        st = min(64, hd)
        for h in range(2):
            cn[h].start()
        for h in range(2):
            waits[h].wait_recv()
            cr[h].start()
        for h in range(2):
            cn[h].wait()
            cr[h].wait()

            @pl.loop(0, hd // st)
            def _(i):
                row = pl.ds(pl.multiple_of(i * st, st), st)
                nst[h, row, :] = fst[h, row, :] + cst[h, row, :]

            cd[h].start()
        for h in range(2):
            cd[h].wait()
            if after[h] is not None:
                after[h].start()

    def uid(rx, ry, k, half):
        return 12 * (1 - rx) + 6 * (1 - ry) + 2 * k + half

    def ycopy2(k):
        return remote(near.at[uid(0, 1, k, 0)], r2.at[2 * k], s2.at[2 * k], q2.at[2 * k], dev_y)

    def xcopy2(k):
        return remote(near.at[uid(1, 0, k, 1)], r2.at[2 * k + 1], s2.at[2 * k + 1], q2.at[2 * k + 1], dev_x)

    def second(k):
        ua, ub = uid(0, 1, k, 0), uid(1, 0, k, 1)
        with sc(f"second{k}"):
            add_pair(
                (ua, ub), (xcopy1(k, 0), ycopy1(k, 0)), (xr1.at[k], yr1.at[k]), (near.at[ua], near.at[ub]),
                (ycopy2(k), xcopy2(k)),
            )

    def third(k):
        ua, ub = uid(0, 0, k, 0), uid(0, 0, k, 1)
        with sc(f"third{k}"):
            add_pair(
                (ua, ub), (xcopy1(3 + k, 0), ycopy1(3 + k, 0)), (xr1.at[3 + k], yr1.at[3 + k]),
                (n00.at[2 * k], n00.at[2 * k + 1]),
            )

    def fourth(k):
        cn = [pltpu.make_async_copy(n00.at[2 * k + h], dwv.at[2 * k + h], cin.at[h]) for h in range(2)]
        cr = [pltpu.make_async_copy(r2.at[2 * k + h], cst.at[h], cload.at[h]) for h in range(2)]
        st = min(64, hd)
        with sc(f"fourth{k}"):
            for h in range(2):
                cn[h].start()
            for h in range(2):
                (ycopy2, xcopy2)[h](k).wait_recv()
                cr[h].start()
            for h in range(2):
                cn[h].wait()
                cr[h].wait()

                @pl.loop(0, hd // st)
                def _(i):
                    row = pl.ds(pl.multiple_of(i * st, st), st)
                    dwv[2 * k + h, row, :] = dwv[2 * k + h, row, :] + cst[h, row, :]

    with sc("own_in"):
        for k in range(3):
            local[k].wait()
            if k < 2:
                xo[k].start()
                yo[k].start()
        yd[0].start()
        for cp in local[3:]:
            cp.wait()
    for j in range(2):
        acopy(0, 1, j).start()

    @mid
    def _():
        for j in range(2):
            bcopy(0, 2, j).start()

    for k in range(3):
        co[k].start()

    eye[...] = (
        lax.broadcasted_iota(jnp.int32, (hd, hd), 0) == lax.broadcasted_iota(jnp.int32, (hd, hd), 1)
    ).astype(f32).astype(bf)

    with sc("xt0"):
        transpose_x(1, 0, 1)

    def pass_on(s, j):
        with sc(f"rows{s}_{j}"):
            got(s, j)
        if s == 1:
            bcopy(1, 3, j).start()
        else:
            acopy(s, s, j).start()

    with sc("gx0"):
        xo[0].wait_recv()
        cx[0].start()
        yo[0].wait_recv()
    rg.start()
    cy[0].start()

    @mid
    def _():
        pass_on(1, 0)
        pass_on(2, 0)

    with sc("gx1"):
        xo[1].wait_recv()
        for cp in rua:
            cp.start()
        yd[1].start()
        cx[1].start()
        yo[1].wait_recv()
    for cp in rub:
        cp.start()
    for h in range(2):
        xd[h].start()
    cy[1].start()

    @mid
    def _():
        pass_on(1, 1)
        pass_on(2, 1)

    @end
    def _():
        with sc("e_rows1"):
            got(1, 0)

    with sc("gc0"):
        for cp in (*co[:2], *cx):
            cp.wait_recv()
    part_ab(1, 0)
    part_ab(0, 0)
    with sc("gyd"):
        yd[0].wait_recv()
        cyd[0].start()
        rg.wait_recv()
        crg.start()
    with sc("gc1"):
        for cp in (*cy, crg):
            cp.wait_recv()
    part_ab(1, 1, 1)

    @mid
    def _():
        pass_on(3, 0)

    with sc("gru"):
        for cp, fwd in zip((*rua[:1], *rub[:1], *rua[1:], *rub[1:]), (*crua[:1], *crub[:1], *crua[1:], *crub[1:])):
            cp.wait_recv()
            fwd.start()
    with sc("gc2"):
        for cp in (*crua, *crub):
            cp.wait_recv()
    part_ab(1, 1, 2)
    with sc("gc3"):
        for cp in (co[2], cyd[0]):
            cp.wait_recv()

    def early_half(h):
        with sc(f"early1_{h}"):
            @pl.loop(0, 2)
            def _(i):
                r = 2 * i
                col = pl.ds(h * hd, hd)
                v = mm(act[2, rows(1), :], wd[:, pl.ds(pl.multiple_of(r * kd + h * hd, hd), hd)])
                zs[r, :, col] = v
                remote(zs.at[r, :, col], zl.at[0, r, :, col], zsend.at[r], zrecv.at[0, r], dev_a).start()

    def early(s, odd):
        with sc(f"early{s}_{odd}"):
            @pl.loop(0, 2)
            def _(i):
                r = 2 * i + odd
                chunk(0, s, r, s - 1, None, True)
                zcopy(s - 1, 0, r, s - 1, dev_a).start()

    @end
    def _():
        early_half(0)
        with sc("e_rows2"):
            got(2, 0)

    part_ab(2, 0)
    with sc("gd0"):
        yd[1].wait_recv()
        cyd[1].start()
        xd[0].wait_recv()
        rd[0].start()
        cxd[0].start()
        cyd[1].wait_recv()

    @end
    def _():
        early_half(1)

    part_ab(2, 1)

    @end
    def _():
        early(2, 0)

    @mid
    def _():
        pass_on(3, 1)

    with sc("gd1"):
        xd[1].wait_recv()
        rd[1].start()
        cxd[1].start()
    part_ab(0, 1)
    with sc("gd2"):
        rd[0].wait_recv()
        crd[0].start()
    transpose_x(1, 1, 3)
    keep_h(0, 3)
    with sc("gd3"):
        rd[1].wait_recv()
        crd[1].start()
        for cp in (*cxd, *crd):
            cp.wait_recv()

    @end
    def _():
        early(1, 1)
        early(2, 1)
        got(1, 1)
        got(2, 1)
        with sc("e_rows3"):
            got(3, 0)

    part_ab(3, 0)
    part_ab(3, 1)
    flush(0)
    flush(1)
    gload(1)
    transpose_x(1, 3, 4)
    keep_h(3, 4)
    front_g(1, 0)
    front_g(0, 2)
    front_g(2, 3)

    @end
    def _():
        with sc("e_rows3"):
            got(3, 1)

    dw_first(1, 2)
    half_g(3, 1, None)
    near_load(1, 0)
    half_g(3, 0, None)
    near_load(1, 1)

    @pl.loop(0, 2)
    def _(j):
        near_unit(1, j)
        ncopy(j).start()

    for j in range(2):
        near_done(1, j)
    dw(1, 2, 2)

    @end
    def _():
        jobs((0, 3, 0, None, 2, dev_a, False))

    @mid
    def _():
        jobs((0, 2, 0, 1, 3, dev_b, True))

    with sc("xtb"):
        transpose_x(0, 0, 4)
    dw(0, 0, 0)
    for u in range(3):
        fcopy(u).wait_send()
    for cp in wcopies:
        cp.wait_send()
    for j in range(2):
        acopy(0, 1, j).wait_send()

    @mid
    def _():
        for j in range(2):
            bcopy(0, 2, j).wait_send()
            bcopy(1, 3, j).wait_send()
            acopy(2, 2, j).wait_send()
            acopy(3, 3, j).wait_send()

    @end
    def _():
        jobs((1, 3, 1, None, 2, dev_a, False))
        second(0)
        second(1)
        second(2)
        jobs((1, 2, 0, None, 1, dev_a, False))
        third(0)
        third(1)
        jobs((1, 1, 1, None, 0, dev_a, False))
        third(2)
        finish(0, (0,))
        last_part()
        fourth(0)
        finish(1, (0,), 0, 2)
        fourth(1)
        finish(1, (0,), 2, 3)
        for h in range(2):
            pltpu.make_async_copy(n00.at[4 + h], dwv.at[4 + h], cin.at[h]).start()
        for h in range(2):
            pltpu.make_async_copy(n00.at[4 + h], dwv.at[4 + h], cin.at[h]).wait()
        with sc("fourth2"):
            ycopy2(2).wait_recv()
            xcopy2(2).wait_recv()

    @mid
    def _():
        jobs((0, 3, 1, 2, 4, dev_b, True))
        second(0)
        second(1)
        second(2)
        jobs((0, 1, 0, 4, 0, dev_a, False), (1, 3, 1, 2, 4, dev_b, False))
        third(0)
        third(1)
        jobs((1, 1, 0, 4, 0, dev_a, False), (1, 2, 1, 1, 3, dev_b, False))
        third(2)
        finish(0, (0, 3))
        fourth(0)
        fourth(1)
        last_part()
        finish(1, (0, 3), 0, 3)
        fourth(2)
        zcopy(3, 1, 3, 0, dev_a).wait_recv()

    zcopy(0, 1, 3, 0, dev_a).wait_recv()

    with sc("drain"):
        for half in range(2):
            for r in range(4):
                zcopy(0, 0, r, half, dev_a).wait_send()
        for i in range(6):
            xcopy1(i, 0).wait_send()
            ycopy1(i, 0).wait_send()
        for k in range(3):
            ycopy2(k).wait_send()
            xcopy2(k).wait_send()


def fused(x, dy, wg, wu, wd):
    nr, d = x.shape
    kd, kf = wg.shape
    f, hd = 2 * kf, kd // 2
    hbm = pl.BlockSpec(memory_space=pl.ANY)
    sds = jax.ShapeDtypeStruct
    out_shape = (
        pltpu.VMEM((4 * nr, d), bf), pltpu.VMEM((4 * nr, d), bf), pltpu.VMEM((6, hd, kf), f32),
        sds((5, 8, nr, kd), f32), sds((30, hd, kf), f32), sds((6, hd, kf), f32), sds((24, hd, kf), f32),
        sds((6, hd, kf), f32), sds((6, hd, kf), f32), sds((4, 2, 2, nr, kf), f32),
    )
    dma = pltpu.SemaphoreType.DMA
    return pl.pallas_call(
        kernel,
        name="fused",
        out_shape=out_shape,
        in_specs=[hbm] * 5,
        out_specs=(pl.BlockSpec(memory_space=pltpu.VMEM),) * 3 + (hbm,) * (len(out_shape) - 3),
        scratch_shapes=[
            pltpu.VMEM((d, f), bf), pltpu.VMEM((d, f), bf), pltpu.VMEM((f, d), bf),
            pltpu.VMEM((3, 4 * nr, f), bf),
            pltpu.VMEM((8, nr, kd), f32), pltpu.VMEM((2, kd, 4 * nr), bf), pltpu.VMEM((f, 4 * nr), bf),
            pltpu.VMEM((hd, hd), bf),
            pltpu.VMEM((2, hd, kf), f32),
            dma((49,)), dma((41,)), dma((11,)), dma((8,)), dma((5, 8)), dma((2,)), dma((3,)), dma((24,)), dma((2,)),
            dma((2,)), dma((6,)), dma((6,)), dma((6,)), dma((6,)), dma((6,)), dma((6,)), dma((2,)), dma((4,)),
        ],
        compiler_params=pltpu.CompilerParams(collective_id=0, has_side_effects=True, vmem_limit_bytes=VMEM_LIMIT - 14 * 2**20),
    )(x, dy, wg, wu, wd)


def tail_kernel(xa, dya, dwv, zl, near, y, dx, dwg, dwu, dwd, buf, ubuf, out, sem, lsem, usem):
    dp = lax.axis_index("dp")
    z = lax.axis_index("tp") // 2
    is_mid = (z == 1) | (z == 2)
    is_end = (z == 0) | (z == 3)
    nr, kd = y.shape[0], dwd.shape[1]
    hd = kd // 2
    units = [pltpu.make_async_copy(near.at[28 + h], ubuf.at[h], usem.at[h]) for h in range(2)]

    @pl.when(is_end)
    def _():
        for c in units:
            c.start()

    srcs = (zl.at[1, 7], zl.at[0, 7], zl.at[3, 7])
    loads = [pltpu.make_async_copy(v, buf.at[i], lsem.at[i]) for i, v in enumerate(srcs)]
    loads[0].start()
    loads[1].start()

    @pl.when(is_mid)
    def _():
        loads[2].start()

    copies = [(dwv.at[4 + h], dwu.at[pl.ds(h * hd, hd)]) for h in range(2)]
    for h in range(2):
        copies.append((dwv.at[2 + h], dwg.at[pl.ds(h * hd, hd)]))
        for q in range(2):
            copies.append((dwv.at[h, :, pl.ds(q * kd, kd)], dwd.at[pl.ds((2 * h + q) * hd, hd)]))
    for src, dst, n in ((xa, y, 4), (dya, dx, 3)):
        for r in range(n):
            copies.append((src.at[pl.ds(nr, nr), pl.ds(r * kd, kd)], dst.at[:, natural(dp, r, kd)]))
    copies.append((out, dx.at[:, natural(dp, 3, kd)]))
    copies = [pltpu.make_async_copy(s, t, sem.at[i]) for i, (s, t) in enumerate(copies)]
    for c in copies[2:-1]:
        c.start()

    @pl.when(is_mid)
    def _():
        for c in copies[:2]:
            c.start()

    loads[0].wait()
    loads[1].wait()
    buf[0] = buf[0] + buf[1]

    @pl.when(is_mid)
    def _():
        loads[2].wait()
        buf[0] = buf[0] + buf[2]

    out[...] = buf[0].astype(bf)
    copies[-1].start()

    @pl.when(is_end)
    def _():
        st = min(64, hd)
        for h in range(2):
            units[h].wait()

            @pl.loop(0, hd // st)
            def _(i):
                row = pl.ds(pl.multiple_of(i * st, st), st)
                ubuf[h, row, :] = dwv[4 + h, row, :] + ubuf[h, row, :]

            pltpu.make_async_copy(ubuf.at[h], dwu.at[pl.ds(h * hd, hd)], sem.at[h]).start()

    for c in copies:
        c.wait()


def tail(xa, dya, dwv, zl, near, nr, kd, kf):
    hbm = pl.BlockSpec(memory_space=pl.ANY)
    sds = jax.ShapeDtypeStruct
    d = xa.shape[1]
    dma = pltpu.SemaphoreType.DMA
    return pl.pallas_call(
        tail_kernel,
        name="tail",
        out_shape=(sds((nr, d), bf), sds((nr, d), bf), sds((kd, kf), f32), sds((kd, kf), f32), sds((kf, kd), f32)),
        in_specs=[hbm] * 2 + [pl.BlockSpec(memory_space=pltpu.VMEM)] + [hbm] * 2,
        out_specs=(hbm,) * 5,
        scratch_shapes=[
            pltpu.VMEM((3, nr, kd), f32), pltpu.VMEM((2, kd // 2, kf), f32), pltpu.VMEM((nr, kd), bf),
            dma((16,)), dma((3,)), dma((2,)),
        ],
        compiler_params=pltpu.CompilerParams(vmem_limit_bytes=VMEM_LIMIT - 27 * 2**20),
    )(xa, dya, dwv, zl, near)


def solution(mesh):
    rows = P(("dp", "tp"), None)
    wsp = P("dp", "tp")
    dsp = P("tp", "dp")

    def local(x, w_gate, w_up, w_down, dy):
        return tail(*fused(x, dy, w_gate, w_up, w_down)[:5], x.shape[0], *w_gate.shape)

    return jax.shard_map(local, mesh=mesh, in_specs=(rows, wsp, wsp, dsp, rows), out_specs=(rows, rows, wsp, wsp, dsp), check_vma=False)
```

```python
import jax
import jax.numpy as jnp
from jax import lax
from jax.experimental import pallas as pl
from jax.experimental.pallas import tpu as pltpu
from jax.sharding import PartitionSpec as P

MESH = pl.DeviceIdType.MESH
f32 = jnp.float32
bf = jnp.bfloat16
VMEM_LIMIT = 67043328
sc = jax.named_scope
LAG = 4


def mm(a, b):
    return lax.dot_general(a, b, (((1,), (0,)), ((), ())), preferred_element_type=f32)


def mmt(a, b):
    return lax.dot_general(a, b, (((1,), (1,)), ((), ())), preferred_element_type=f32)


def natural(dp, r, kd):
    x, c, rc, rx = dp // 2, dp % 2, r // 2, r % 2
    n = 2 * (x + rx - 2 * x * rx) + c + rc - 2 * c * rc
    return pl.ds(pl.multiple_of(n * kd, kd), kd)


def kernel(
    x_in, dy_in, wg_in, wu_in, wd_in,
    xa, dya, dwv, zl, n00, r2, far_r, near, xr1, yr1, stash,
    wg, wu, wd, act, zs, xt, ht, eye, cst,
    gs, gr, lsem, zsend, zrecv, zload, fsend, frecv, nstore, cload, xs1, xq1, ys1, yq1, s2, q2, cin, ssem,
):
    tp = lax.axis_index("tp")
    dp = lax.axis_index("dp")
    z, y = tp // 2, tp % 2
    x, c = dp // 2, dp % 2
    is_end = (z == 0) | (z == 3)
    is_mid = (z == 1) | (z == 2)
    dev_x = {"tp": tp, "dp": 2 * (1 - x) + c}
    dev_y = {"tp": 2 * z + 1 - y, "dp": dp}
    dev_c = {"tp": tp, "dp": 2 * x + 1 - c}
    dev_a = {"tp": 2 * (z + 1 - 2 * (z % 2)) + y, "dp": dp}
    dev_b = {"tp": 2 * (3 - z) + y, "dp": dp}

    fst, nst = dwv.at[pl.ds(0, 3)], dwv.at[pl.ds(3, 2)]
    nr, d = x_in.shape
    kd, kf = wg_in.shape
    f = 2 * kf
    hd = kd // 2
    hf = kf // 2

    def end(fn):
        pl.when(is_end)(fn)

    def mid(fn):
        pl.when(is_mid)(fn)

    def ncol(r):
        return natural(dp, r, kd)

    def remote(src, dst, ss, rs, dev):
        return pltpu.make_async_remote_copy(
            src_ref=src, dst_ref=dst, send_sem=ss, recv_sem=rs, device_id=dev, device_id_type=MESH
        )

    own = (wg_in, wu_in, wd_in)

    def blk(k, rx, rc, ry, lo=0, n=None):
        d0 = (2 * rc + rx) * kd + lo
        n = kd if n is None else n
        if k < 2:
            return (wg, wu)[k].at[pl.ds(d0, n), pl.ds(ry * kf, kf)]
        return wd.at[pl.ds(ry * kf, kf), pl.ds(d0, n)]

    local = [(own[k], blk(k, 0, 0, 0)) for k in range(3)]
    for src, ref in ((x_in, xa), (dy_in, dya)):
        for r in range(4):
            local.append((src.at[:, ncol(r)], ref.at[pl.ds(0, nr), pl.ds(r * kd, kd)]))
    local = [pltpu.make_async_copy(s, t, lsem.at[i]) for i, (s, t) in enumerate(local)]
    for cp in local:
        cp.start()

    bar = pltpu.get_barrier_semaphore()
    for dev in (dev_x, dev_y, dev_c, dev_a, dev_b):
        pl.semaphore_signal(bar, inc=1, device_id=dev, device_id_type=MESH)

    with sc("barrier"):
        pl.semaphore_wait(bar, 5)

    ft = min(256, f)

    def rows(s):
        return pl.ds(s * nr, nr)

    def transpose_x(rx, lo, hi):
        @pl.loop(lo, hi)
        def _(s):
            row = pl.ds(pl.multiple_of(s * nr, nr), nr)
            for rc in range(2):
                for h in range(2):
                    v = mmt(eye[...], xa[row, pl.ds((2 * rc + rx) * kd + h * hd, hd)])
                    xt[rc, pl.ds(h * hd, hd), row] = v.astype(bf)

    def wcopy(i, src, dst, dev):
        return remote(src, dst, gs.at[i], gr.at[i], dev)

    def half(rx, rc, ry, h):
        return blk(2, rx, rc, ry, h * hd, hd)

    ua = 3 * kd // 4
    mine = [blk(k, 0, 0, 0) for k in range(3)]
    xo = [wcopy(k, mine[k], blk(k, 1, 0, 0), dev_x) for k in range(2)]
    yo = [wcopy(2 + k, mine[k], blk(k, 0, 0, 1), dev_y) for k in range(2)]
    co = [wcopy(4 + k, mine[k], blk(k, 0, 1, 0), dev_c) for k in range(3)]
    xd = [wcopy(7 + h, half(0, 0, 0, h), half(1, 0, 0, h), dev_x) for h in range(2)]
    yd = [wcopy(9 + h, half(0, 0, 0, h), half(0, 0, 1, h), dev_y) for h in range(2)]
    rg = wcopy(11, blk(0, 0, 0, 1), blk(0, 1, 0, 1), dev_x)
    ay, ax = ((0, kd // 2), (kd // 2, ua)), ((ua, 7 * kd // 8), (7 * kd // 8, kd))
    rua = [wcopy(i, blk(1, 1, 0, 0, lo, hi - lo), blk(1, 1, 0, 1, lo, hi - lo), dev_y) for i, (lo, hi) in zip((12, 29), ay)]
    rub = [wcopy(i, blk(1, 0, 0, 1, lo, hi - lo), blk(1, 1, 0, 1, lo, hi - lo), dev_x) for i, (lo, hi) in zip((13, 31), ax)]
    rd = [wcopy(14 + h, half(1, 0, 0, h), half(1, 0, 1, h), dev_y) for h in range(2)]
    cx = [wcopy(16 + k, blk(k, 1, 0, 0), blk(k, 1, 1, 0), dev_c) for k in range(2)]
    cy = [wcopy(18 + k, blk(k, 0, 0, 1), blk(k, 0, 1, 1), dev_c) for k in range(2)]
    cxd = [wcopy(20 + h, half(1, 0, 0, h), half(1, 1, 0, h), dev_c) for h in range(2)]
    cyd = [wcopy(22 + h, half(0, 0, 1, h), half(0, 1, 1, h), dev_c) for h in range(2)]
    crg = wcopy(24, blk(0, 1, 0, 1), blk(0, 1, 1, 1), dev_c)
    crua = [wcopy(i, blk(1, 1, 0, 1, lo, hi - lo), blk(1, 1, 1, 1, lo, hi - lo), dev_c) for i, (lo, hi) in zip((25, 30), ay)]
    crub = [wcopy(i, blk(1, 1, 0, 1, lo, hi - lo), blk(1, 1, 1, 1, lo, hi - lo), dev_c) for i, (lo, hi) in zip((26, 32), ax)]
    crd = [wcopy(27 + h, half(1, 0, 1, h), half(1, 1, 1, h), dev_c) for h in range(2)]
    wcopies = (*xo, *yo, *co, *xd, *yd, rg, *rua, *rub, *rd, *cx, *cy, *cxd, *cyd, crg, *crua, *crub, *crd)
    nw = 33

    def slot(j, s):
        return (xa, dya)[j].at[pl.ds(s * nr, nr)]

    def acopy(src, dst, j):
        return remote(
            slot(j, src), slot(j, dst), gs.at[nw + 2 * dst + j], gr.at[nw + 2 * dst + j], dev_a
        )

    def bcopy(src, dst, j):
        return remote(
            slot(j, src), slot(j, dst), gs.at[nw + 8 + 2 * dst + j], gr.at[nw + 2 * dst + j], dev_b
        )

    def got(s, j):
        acopy(s, s, j).wait_recv()

    def stash_copy(s, p, n):
        return pltpu.make_async_copy((fst, nst)[n].at[p, pl.ds(0, nr)], stash.at[s, p, n], ssem.at[2 * p + n])

    def factor(s, n):
        return nst if n else cst if s == 3 else fst

    def stash_load(s, p, n):
        return pltpu.make_async_copy(stash.at[s, p, n], factor(s, n).at[p, pl.ds(0, nr)], ssem.at[2 * p + n])

    pending = [None, None]

    def flush(p):
        if pending[p] is not None:
            for n in range(2):
                stash_copy(pending[p], p, n).wait()
        pending[p] = None

    late = kd + ay[1][0]

    def ab_tiles(s, p, step):
        def tile(i):
            col = pl.ds(pl.multiple_of(p * kf + i * ft, ft), ft)
            at = (p, pl.ds(0, nr), pl.ds(pl.multiple_of(i * ft, ft), ft))

            def b_rows(lo, hi):
                b0, b1 = pl.ds(lo, hi - lo), pl.ds(2 * kd + lo, hi - lo)
                return mm(xa[rows(s), b0], wu[b0, col]) + mm(xa[rows(s), b1], wu[b1, col])

            if step == 1:
                fst[at] = mm(xa[rows(s), :], wg[:, col])
                nst[at] = b_rows(0, kd)
                return
            if step == 3:
                nst[at] = nst[at] + b_rows(kd, late)
                return
            if step == 2:
                a = fst[at]
                b = nst[at] + b_rows(late, 2 * kd)
            else:
                a = mm(xa[rows(s), :], wg[:, col])
                b = mm(xa[rows(s), :], wu[:, col])
            sig = jax.nn.sigmoid(a)
            sa = a * sig
            act[2, rows(s), col] = (sa * b).astype(bf)
            fst[at] = sa
            nst[at] = b * sig * (1.0 + a * (1.0 - sig))

        m = 2 if step > 1 and kf // ft > 1 else 1

        @pl.loop(0, kf // ft // m)
        def _(i):
            for q in range(m):
                tile(i * m + q)

    def part_ab(s, p, step=0):
        with sc(f"ab{s}_{p}"):
            flush(p)
            ab_tiles(s, p, step)
            if step in (0, 2):
                for n in range(2):
                    stash_copy(s, p, n).start()
                pending[p] = s

    gt = min(512, kf)

    def part_g(s, p):
        @pl.loop(0, kf // gt)
        def _(i):
            col = pl.ds(pl.multiple_of(p * kf + i * gt, gt), gt)
            kcol = pl.ds(pl.multiple_of(i * gt, gt), gt)
            g = mmt(dya[rows(s), :], wd[col, :])
            act[0, rows(s), col] = (g * factor(s, 1)[p, pl.ds(0, nr), kcol]).astype(bf)
            act[1, rows(s), col] = (g * factor(s, 0)[p, pl.ds(0, nr), kcol]).astype(bf)

    def gload(s):
        for p in range(2):
            for n in range(2):
                stash_load(s, p, n).start()

    def half_g(s, p, then):
        with sc(f"g{s}"):
            for n in range(2):
                stash_load(s, p, n).wait()
            part_g(s, p)
            if then is not None:
                for n in range(2):
                    stash_load(then, p, n).start()

    def front_g(s, then):
        @pl.loop(0, 2)
        def _(p):
            half_g(s, p, then)

    def keep_h(lo, hi):
        hb = min(4, f // hd)
        nh = f // (hb * hd)
        with sc("ht"):
            @pl.loop(lo * nh, hi * nh)
            def _(i):
                row = pl.ds(pl.multiple_of(i // nh * nr, nr), nr)
                for q in range(hb):
                    col = pl.ds(pl.multiple_of((i % nh * hb + q) * hd, hd), hd)
                    ht[col, row] = mmt(eye[...], act[2, row, col]).astype(bf)

    def back(ref, at, kind, s, r):
        *lead, c0 = at

        @pl.loop(0, 2)
        def _(h):
            n = pl.ds(pl.multiple_of(r * kd + h * hd, hd), hd)
            if kind == 0:
                v = mm(act[2, rows(s), :], wd[:, n])
            else:
                v = mmt(act[0, rows(s), :], wg[n, :]) + mmt(act[1, rows(s), :], wu[n, :])
            ref[(*lead, pl.ds(0, nr), pl.ds(pl.multiple_of(c0 + h * hd, hd), hd))] = v

    def zcopy(q, kind, r, half, dev):
        i = 4 * kind + r
        return remote(zs.at[4 * half + r], zl.at[q, i], zsend.at[4 * half + r], zrecv.at[q, i], dev)

    def zload_(q, kind, r, slot):
        return pltpu.make_async_copy(zl.at[q, 4 * kind + r], cst.at[slot, pl.ds(0, nr), pl.ds(0, kd)], zload.at[slot])

    def chunk(kind, s, r, half, q_add, first):
        i = 4 * half + r
        if q_add is not None:
            with sc("zrecv"):
                zcopy(q_add, kind, r, half, dev_a).wait_recv()
            zload_(q_add, kind, r, r % 2).start()
        if not first:
            with sc("zsend"):
                zcopy(0, kind, r, half, dev_a).wait_send()
        back(zs, (i, 0), kind, s, r)
        if q_add is not None:
            zload_(q_add, kind, r, r % 2).wait()
            zs[i] = zs[i] + cst[r % 2, pl.ds(0, nr), pl.ds(0, kd)]

    def jobs(*specs):
        with sc("job" + "_".join(f"{kind}{s}" for kind, s, *_ in specs)):
            @pl.loop(0, 4)
            def _(r):
                for kind, s, h, q_add, q_dst, dev, first in specs:
                    chunk(kind, s, r, h, q_add, first)
                    zcopy(q_dst, kind, r, h, dev).start()

    def last_part():
        back(cst, (0, kd), 1, 0, 3)
        at = (0, pl.ds(0, nr), pl.ds(kd, kd))
        cst[at] = cst[at] + dya[rows(0), pl.ds(3 * kd, kd)].astype(f32)
        cp = pltpu.make_async_copy(cst.at[at], zl.at[1, 7], zload.at[0])
        cp.start()
        cp.wait()

    def finish(kind, adds, lo=0, hi=4):
        res = (xa, dya)[kind]
        with sc(f"fin{kind}"):
            @pl.loop(lo, hi)
            def _(r):
                col = pl.ds(pl.multiple_of(r * kd, kd), kd)
                part = (pl.ds(0, nr), pl.ds(0, kd))
                temp = (0, pl.ds(0, nr), pl.ds(kd, kd))
                back(cst, (0, kd), kind, 0, r)
                for n, q in enumerate(adds):
                    with sc("finrecv"):
                        zcopy(q, kind, r, 0, dev_a).wait_recv()
                    zload_(q, kind, r, n).start()
                for n, q in enumerate(adds):
                    zload_(q, kind, r, n).wait()
                v = cst[temp] + res[rows(0), col].astype(f32)
                for n in range(len(adds)):
                    v = v + cst[n, *part]
                res[rows(1), col] = v.astype(bf)

    def unit(rc, rx, j, put):
        ryi, k, half = j // 6, ((j // 2) % 3 + 2) % 3, j % 2
        f0 = (1 - ryi) * kf

        @pl.when(k < 2)
        def _():
            a = xt[rc, pl.ds(pl.multiple_of(half * hd, hd), hd), :]
            for q in range(4):
                b = act[k, :, pl.ds(pl.multiple_of(f0 + q * hd, hd), hd)]
                put(pl.ds(q * hd, hd), mm(a, b))

        @pl.when(k == 2)
        def _():
            for q in range(4):
                b = dya[:, pl.ds((2 * rc + rx) * kd + q % 2 * hd, hd)]
                a = ht[pl.ds(pl.multiple_of(f0 + half * hf + q // 2 * hd, hd), hd), :]
                put(pl.ds(q * hd, hd), mm(a, b))

    def fcopy(u):
        return remote(fst.at[u % 3], far_r.at[u], fsend.at[u % 3], frecv.at[u], dev_c)

    def ncopy(u):
        return pltpu.make_async_copy(nst.at[(u + 1) % 2], near.at[u], nstore.at[(u + 1) % 2])

    def ccopy(u):
        return pltpu.make_async_copy(far_r.at[u], cst.at[(u + 1) % 2], cload.at[(u + 1) % 2])

    def xcopy1(i, u):
        return remote(near.at[u], xr1.at[i], xs1.at[i], xq1.at[i], dev_x)

    def ycopy1(i, u):
        return remote(near.at[u], yr1.at[i], ys1.at[i], yq1.at[i], dev_y)

    def nsend(rx, j):
        ryi, k, half = j // 6, (j // 2) % 3, j % 2
        u = 12 * (1 - rx) + j
        if rx:
            @pl.when(half == 0)
            def _():
                xcopy1(ryi * 3 + k, u).start()

        @pl.when((half == 1) & (ryi == 0))
        def _():
            ycopy1(3 * (1 - rx) + k, u).start()

    def far_unit(rx, j):
        u = 12 * (1 - rx) + j

        @pl.when(u > 2)
        def _():
            with sc("fsend"):
                fcopy(u).wait_send()

        def put(col, v):
            fst[u % 3, :, col] = v

        unit(1, rx, j, put)
        fcopy(u).start()

    def dw_first(rx, n):
        with sc("dwfirst"):
            @pl.loop(0, n)
            def _(j):
                far_unit(rx, j)

    def near_load(rx, j):
        u = 12 * (1 - rx) + j
        with sc("frecv"):
            fcopy(u).wait_recv()
        ccopy(u).start()

    def near_unit(rx, j):
        u = 12 * (1 - rx) + j
        with sc("cwait"):
            ccopy(u).wait()

        def put(col, v):
            i = (u + 1) % 2
            nst[i, :, col] = v + cst[i, :, col]

        unit(0, rx, j, put)

    def near_done(rx, j):
        with sc("nwait"):
            ncopy(12 * (1 - rx) + j).wait()
        nsend(rx, j)

    def dw(rx, f0, n0):
        base = 12 * (1 - rx)

        with sc(f"dw{rx}"):
            @pl.loop(f0, 12 + LAG)
            def _(j):
                n = j - LAG

                @pl.when(j < 12)
                def _():
                    far_unit(rx, j)

                @pl.when((n + 1 >= n0) & (n < 11))
                def _():
                    near_load(rx, n + 1)

                @pl.when(n >= n0)
                def _():
                    near_unit(rx, n)

                    @pl.when(n > n0)
                    def _():
                        near_done(rx, n - 1)

                    ncopy(base + n).start()

            near_done(rx, 11)

    def add_pair(units, waits, arrived, dsts, after=(None, None)):
        cn = [pltpu.make_async_copy(near.at[u], fst.at[h], cin.at[h]) for h, u in enumerate(units)]
        cr = [pltpu.make_async_copy(v, cst.at[h], cload.at[h]) for h, v in enumerate(arrived)]
        cd = [pltpu.make_async_copy(nst.at[h], t, nstore.at[h]) for h, t in enumerate(dsts)]
        st = min(64, hd)
        for h in range(2):
            cn[h].start()
        for h in range(2):
            waits[h].wait_recv()
            cr[h].start()
        for h in range(2):
            cn[h].wait()
            cr[h].wait()

            @pl.loop(0, hd // st)
            def _(i):
                row = pl.ds(pl.multiple_of(i * st, st), st)
                nst[h, row, :] = fst[h, row, :] + cst[h, row, :]

            cd[h].start()
        for h in range(2):
            cd[h].wait()
            if after[h] is not None:
                after[h].start()

    def uid(rx, ry, k, half):
        return 12 * (1 - rx) + 6 * (1 - ry) + 2 * k + half

    def ycopy2(k):
        return remote(near.at[uid(0, 1, k, 0)], r2.at[2 * k], s2.at[2 * k], q2.at[2 * k], dev_y)

    def xcopy2(k):
        return remote(near.at[uid(1, 0, k, 1)], r2.at[2 * k + 1], s2.at[2 * k + 1], q2.at[2 * k + 1], dev_x)

    def second(k):
        ua, ub = uid(0, 1, k, 0), uid(1, 0, k, 1)
        with sc(f"second{k}"):
            add_pair(
                (ua, ub), (xcopy1(k, 0), ycopy1(k, 0)), (xr1.at[k], yr1.at[k]), (near.at[ua], near.at[ub]),
                (ycopy2(k), xcopy2(k)),
            )

    def third(k):
        ua, ub = uid(0, 0, k, 0), uid(0, 0, k, 1)
        with sc(f"third{k}"):
            add_pair(
                (ua, ub), (xcopy1(3 + k, 0), ycopy1(3 + k, 0)), (xr1.at[3 + k], yr1.at[3 + k]),
                (n00.at[2 * k], n00.at[2 * k + 1]),
            )

    def fourth(k):
        cn = [pltpu.make_async_copy(n00.at[2 * k + h], dwv.at[2 * k + h], cin.at[h]) for h in range(2)]
        cr = [pltpu.make_async_copy(r2.at[2 * k + h], cst.at[h], cload.at[h]) for h in range(2)]
        st = min(64, hd)
        with sc(f"fourth{k}"):
            for h in range(2):
                cn[h].start()
            for h in range(2):
                (ycopy2, xcopy2)[h](k).wait_recv()
                cr[h].start()
            for h in range(2):
                cn[h].wait()
                cr[h].wait()

                @pl.loop(0, hd // st)
                def _(i):
                    row = pl.ds(pl.multiple_of(i * st, st), st)
                    dwv[2 * k + h, row, :] = dwv[2 * k + h, row, :] + cst[h, row, :]

    with sc("own_in"):
        for k in range(3):
            local[k].wait()
            if k < 2:
                xo[k].start()
                yo[k].start()
        yd[0].start()
        for cp in local[3:]:
            cp.wait()
    for j in range(2):
        acopy(0, 1, j).start()

    @mid
    def _():
        for j in range(2):
            bcopy(0, 2, j).start()

    for k in range(3):
        co[k].start()

    eye[...] = (
        lax.broadcasted_iota(jnp.int32, (hd, hd), 0) == lax.broadcasted_iota(jnp.int32, (hd, hd), 1)
    ).astype(f32).astype(bf)

    with sc("xt0"):
        transpose_x(1, 0, 1)

    def pass_on(s, j):
        with sc(f"rows{s}_{j}"):
            got(s, j)
        if s == 1:
            bcopy(1, 3, j).start()
        else:
            acopy(s, s, j).start()

    with sc("gx0"):
        xo[0].wait_recv()
        cx[0].start()
        yo[0].wait_recv()
    rg.start()
    cy[0].start()

    @mid
    def _():
        pass_on(1, 0)
        pass_on(2, 0)

    with sc("gx1"):
        xo[1].wait_recv()
        for cp in rua:
            cp.start()
        yd[1].start()
        cx[1].start()
        yo[1].wait_recv()
    for cp in rub:
        cp.start()
    for h in range(2):
        xd[h].start()
    cy[1].start()

    @mid
    def _():
        pass_on(1, 1)
        pass_on(2, 1)

    @end
    def _():
        with sc("e_rows1"):
            got(1, 0)

    with sc("gc0"):
        for cp in (*co[:2], *cx):
            cp.wait_recv()
    part_ab(1, 0)
    part_ab(0, 0)
    with sc("gyd"):
        yd[0].wait_recv()
        cyd[0].start()
        rg.wait_recv()
        crg.start()
    with sc("gc1"):
        for cp in (*cy, crg):
            cp.wait_recv()
    part_ab(1, 1, 1)

    @mid
    def _():
        pass_on(3, 0)

    with sc("gru0"):
        for cp, fwd in ((rua[0], crua[0]), (rub[0], crub[0])):
            cp.wait_recv()
            fwd.start()
        crua[0].wait_recv()
    part_ab(1, 1, 3)
    with sc("gru1"):
        for cp, fwd in ((rua[1], crua[1]), (rub[1], crub[1])):
            cp.wait_recv()
            fwd.start()
    with sc("gc2"):
        for cp in (crua[1], *crub):
            cp.wait_recv()
    part_ab(1, 1, 2)
    with sc("gc3"):
        for cp in (co[2], cyd[0]):
            cp.wait_recv()

    def early_half(h):
        with sc(f"early1_{h}"):
            @pl.loop(0, 2)
            def _(i):
                r = 2 * i
                col = pl.ds(h * hd, hd)
                v = mm(act[2, rows(1), :], wd[:, pl.ds(pl.multiple_of(r * kd + h * hd, hd), hd)])
                zs[r, :, col] = v
                remote(zs.at[r, :, col], zl.at[0, r, :, col], zsend.at[r], zrecv.at[0, r], dev_a).start()

    def early(s, odd):
        with sc(f"early{s}_{odd}"):
            @pl.loop(0, 2)
            def _(i):
                r = 2 * i + odd
                chunk(0, s, r, s - 1, None, True)
                zcopy(s - 1, 0, r, s - 1, dev_a).start()

    @end
    def _():
        early_half(0)
        with sc("e_rows2"):
            got(2, 0)

    part_ab(2, 0)
    with sc("gd0"):
        yd[1].wait_recv()
        cyd[1].start()
        xd[0].wait_recv()
        rd[0].start()
        cxd[0].start()
        cyd[1].wait_recv()

    @end
    def _():
        early_half(1)

    part_ab(2, 1)

    @end
    def _():
        early(2, 0)

    @mid
    def _():
        pass_on(3, 1)

    with sc("gd1"):
        xd[1].wait_recv()
        rd[1].start()
        cxd[1].start()
    part_ab(0, 1)
    with sc("gd2"):
        rd[0].wait_recv()
        crd[0].start()
    transpose_x(1, 1, 3)
    keep_h(0, 3)
    with sc("gd3"):
        rd[1].wait_recv()
        crd[1].start()
        for cp in (*cxd, *crd):
            cp.wait_recv()

    @end
    def _():
        early(1, 1)
        early(2, 1)
        got(1, 1)
        got(2, 1)
        with sc("e_rows3"):
            got(3, 0)

    part_ab(3, 0)
    part_ab(3, 1)
    flush(0)
    flush(1)
    gload(1)
    transpose_x(1, 3, 4)
    keep_h(3, 4)
    front_g(1, 0)
    front_g(0, 2)
    front_g(2, 3)

    @end
    def _():
        with sc("e_rows3"):
            got(3, 1)

    dw_first(1, 2)
    half_g(3, 1, None)
    near_load(1, 0)
    half_g(3, 0, None)
    near_load(1, 1)

    @pl.loop(0, 2)
    def _(j):
        near_unit(1, j)
        ncopy(j).start()

    for j in range(2):
        near_done(1, j)
    dw(1, 2, 2)

    @end
    def _():
        jobs((0, 3, 0, None, 2, dev_a, False))

    @mid
    def _():
        jobs((0, 2, 0, 1, 3, dev_b, True))

    with sc("xtb"):
        transpose_x(0, 0, 4)
    dw(0, 0, 0)
    for u in range(3):
        fcopy(u).wait_send()
    for cp in wcopies:
        cp.wait_send()
    for j in range(2):
        acopy(0, 1, j).wait_send()

    @mid
    def _():
        for j in range(2):
            bcopy(0, 2, j).wait_send()
            bcopy(1, 3, j).wait_send()
            acopy(2, 2, j).wait_send()
            acopy(3, 3, j).wait_send()

    @end
    def _():
        jobs((1, 3, 1, None, 2, dev_a, False))
        second(0)
        second(1)
        second(2)
        jobs((1, 2, 0, None, 1, dev_a, False))
        third(0)
        third(1)
        jobs((1, 1, 1, None, 0, dev_a, False))
        third(2)
        finish(0, (0,))
        last_part()
        fourth(0)
        finish(1, (0,), 0, 2)
        fourth(1)
        finish(1, (0,), 2, 3)
        fourth(2)

    @mid
    def _():
        jobs((0, 3, 1, 2, 4, dev_b, True))
        second(0)
        second(1)
        second(2)
        jobs((0, 1, 0, 4, 0, dev_a, False), (1, 3, 1, 2, 4, dev_b, False))
        third(0)
        third(1)
        jobs((1, 1, 0, 4, 0, dev_a, False), (1, 2, 1, 1, 3, dev_b, False))
        third(2)
        finish(0, (0, 3))
        fourth(0)
        fourth(1)
        last_part()
        finish(1, (0, 3), 0, 3)
        fourth(2)
        zcopy(3, 1, 3, 0, dev_a).wait_recv()

    zcopy(0, 1, 3, 0, dev_a).wait_recv()

    with sc("drain"):
        for half in range(2):
            for r in range(4):
                zcopy(0, 0, r, half, dev_a).wait_send()
        for i in range(6):
            xcopy1(i, 0).wait_send()
            ycopy1(i, 0).wait_send()
        for k in range(3):
            ycopy2(k).wait_send()
            xcopy2(k).wait_send()


def fused(x, dy, wg, wu, wd):
    nr, d = x.shape
    kd, kf = wg.shape
    f, hd = 2 * kf, kd // 2
    hbm = pl.BlockSpec(memory_space=pl.ANY)
    sds = jax.ShapeDtypeStruct
    out_shape = (
        pltpu.VMEM((4 * nr, d), bf), pltpu.VMEM((4 * nr, d), bf), pltpu.VMEM((6, hd, kf), f32),
        sds((5, 8, nr, kd), f32), sds((6, hd, kf), f32), sds((6, hd, kf), f32),
        sds((24, hd, kf), f32), sds((24, hd, kf), f32),
        sds((6, hd, kf), f32), sds((6, hd, kf), f32), sds((4, 2, 2, nr, kf), f32),
    )
    dma = pltpu.SemaphoreType.DMA
    return pl.pallas_call(
        kernel,
        name="fused",
        out_shape=out_shape,
        in_specs=[hbm] * 5,
        out_specs=(pl.BlockSpec(memory_space=pltpu.VMEM),) * 3 + (hbm,) * (len(out_shape) - 3),
        scratch_shapes=[
            pltpu.VMEM((d, f), bf), pltpu.VMEM((d, f), bf), pltpu.VMEM((f, d), bf),
            pltpu.VMEM((3, 4 * nr, f), bf),
            pltpu.VMEM((8, nr, kd), f32), pltpu.VMEM((2, kd, 4 * nr), bf), pltpu.VMEM((f, 4 * nr), bf),
            pltpu.VMEM((hd, hd), bf),
            pltpu.VMEM((2, hd, kf), f32),
            dma((49,)), dma((41,)), dma((11,)), dma((8,)), dma((5, 8)), dma((2,)), dma((3,)), dma((24,)), dma((2,)),
            dma((2,)), dma((6,)), dma((6,)), dma((6,)), dma((6,)), dma((6,)), dma((6,)), dma((2,)), dma((4,)),
        ],
        compiler_params=pltpu.CompilerParams(collective_id=0, has_side_effects=True, vmem_limit_bytes=VMEM_LIMIT - 14 * 2**20),
    )(x, dy, wg, wu, wd)


def tail_kernel(xa, dya, dwv, zl, y, dx, dwg, dwu, dwd, buf, out, sem, lsem):
    dp = lax.axis_index("dp")
    z = lax.axis_index("tp") // 2
    is_mid = (z == 1) | (z == 2)
    nr, kd = y.shape[0], dwd.shape[1]
    hd = kd // 2
    srcs = (zl.at[1, 7], zl.at[0, 7], zl.at[3, 7])
    loads = [pltpu.make_async_copy(v, buf.at[i], lsem.at[i]) for i, v in enumerate(srcs)]
    loads[0].start()
    loads[1].start()

    @pl.when(is_mid)
    def _():
        loads[2].start()

    copies = []
    for k in range(3):
        for h in range(2):
            v = dwv.at[2 * k + h]
            if k > 0:
                copies.append((v, (dwg, dwu)[k - 1].at[pl.ds(h * hd, hd)]))
            else:
                for q in range(2):
                    copies.append((v.at[:, pl.ds(q * kd, kd)], dwd.at[pl.ds((2 * h + q) * hd, hd)]))
    for src, dst, n in ((xa, y, 4), (dya, dx, 3)):
        for r in range(n):
            copies.append((src.at[pl.ds(nr, nr), pl.ds(r * kd, kd)], dst.at[:, natural(dp, r, kd)]))
    copies.append((out, dx.at[:, natural(dp, 3, kd)]))
    copies = [pltpu.make_async_copy(s, t, sem.at[i]) for i, (s, t) in enumerate(copies)]
    for c in copies[:-1]:
        c.start()
    loads[0].wait()
    loads[1].wait()
    buf[0] = buf[0] + buf[1]

    @pl.when(is_mid)
    def _():
        loads[2].wait()
        buf[0] = buf[0] + buf[2]

    out[...] = buf[0].astype(bf)
    copies[-1].start()
    for c in copies:
        c.wait()


def tail(xa, dya, dwv, zl, nr, kd, kf):
    hbm = pl.BlockSpec(memory_space=pl.ANY)
    sds = jax.ShapeDtypeStruct
    d = xa.shape[1]
    dma = pltpu.SemaphoreType.DMA
    return pl.pallas_call(
        tail_kernel,
        name="tail",
        out_shape=(sds((nr, d), bf), sds((nr, d), bf), sds((kd, kf), f32), sds((kd, kf), f32), sds((kf, kd), f32)),
        in_specs=[hbm] * 4,
        out_specs=(hbm,) * 5,
        scratch_shapes=[pltpu.VMEM((3, nr, kd), f32), pltpu.VMEM((nr, kd), bf), dma((16,)), dma((3,))],
        compiler_params=pltpu.CompilerParams(vmem_limit_bytes=VMEM_LIMIT - 27 * 2**20),
    )(xa, dya, dwv, zl)


def solution(mesh):
    rows = P(("dp", "tp"), None)
    wsp = P("dp", "tp")
    dsp = P("tp", "dp")

    def local(x, w_gate, w_up, w_down, dy):
        return tail(*fused(x, dy, w_gate, w_up, w_down)[:4], x.shape[0], *w_gate.shape)

    return jax.shard_map(local, mesh=mesh, in_specs=(rows, wsp, wsp, dsp, rows), out_specs=(rows, rows, wsp, wsp, dsp), check_vma=False)
```

```python
import jax
import jax.numpy as jnp
from jax import lax
from jax.experimental import pallas as pl
from jax.experimental.pallas import tpu as pltpu
from jax.sharding import PartitionSpec as P

MESH = pl.DeviceIdType.MESH
f32 = jnp.float32
bf = jnp.bfloat16
VMEM_LIMIT = 67043328
sc = jax.named_scope
LAG = 4


def mm(a, b):
    return lax.dot_general(a, b, (((1,), (0,)), ((), ())), preferred_element_type=f32)


def mmt(a, b):
    return lax.dot_general(a, b, (((1,), (1,)), ((), ())), preferred_element_type=f32)


def natural(dp, r, kd):
    x, c, rc, rx = dp // 2, dp % 2, r // 2, r % 2
    n = 2 * (x + rx - 2 * x * rx) + c + rc - 2 * c * rc
    return pl.ds(pl.multiple_of(n * kd, kd), kd)


def kernel(
    x_in, dy_in, wg_in, wu_in, wd_in,
    xa, dya, dwv, zl, n00, r2, far_r, near, xr1, yr1, stash,
    wg, wu, wd, act, zs, xt, ht, eye, cst,
    gs, gr, lsem, zsend, zrecv, zload, fsend, frecv, nstore, cload, xs1, xq1, ys1, yq1, s2, q2, cin, ssem,
):
    tp = lax.axis_index("tp")
    dp = lax.axis_index("dp")
    z, y = tp // 2, tp % 2
    x, c = dp // 2, dp % 2
    is_end = (z == 0) | (z == 3)
    is_mid = (z == 1) | (z == 2)
    dev_x = {"tp": tp, "dp": 2 * (1 - x) + c}
    dev_y = {"tp": 2 * z + 1 - y, "dp": dp}
    dev_c = {"tp": tp, "dp": 2 * x + 1 - c}
    dev_a = {"tp": 2 * (z + 1 - 2 * (z % 2)) + y, "dp": dp}
    dev_b = {"tp": 2 * (3 - z) + y, "dp": dp}

    fst, nst = dwv.at[pl.ds(0, 3)], dwv.at[pl.ds(3, 2)]
    nr, d = x_in.shape
    kd, kf = wg_in.shape
    f = 2 * kf
    hd = kd // 2
    hf = kf // 2

    def end(fn):
        pl.when(is_end)(fn)

    def mid(fn):
        pl.when(is_mid)(fn)

    def ncol(r):
        return natural(dp, r, kd)

    def remote(src, dst, ss, rs, dev):
        return pltpu.make_async_remote_copy(
            src_ref=src, dst_ref=dst, send_sem=ss, recv_sem=rs, device_id=dev, device_id_type=MESH
        )

    own = (wg_in, wu_in, wd_in)

    def blk(k, rx, rc, ry, lo=0, n=None):
        d0 = (2 * rc + rx) * kd + lo
        n = kd if n is None else n
        if k < 2:
            return (wg, wu)[k].at[pl.ds(d0, n), pl.ds(ry * kf, kf)]
        return wd.at[pl.ds(ry * kf, kf), pl.ds(d0, n)]

    local = [(own[k], blk(k, 0, 0, 0)) for k in range(3)]
    for src, ref in ((x_in, xa), (dy_in, dya)):
        for r in range(4):
            local.append((src.at[:, ncol(r)], ref.at[pl.ds(0, nr), pl.ds(r * kd, kd)]))
    local = [pltpu.make_async_copy(s, t, lsem.at[i]) for i, (s, t) in enumerate(local)]
    for cp in local:
        cp.start()

    bar = pltpu.get_barrier_semaphore()
    for dev in (dev_x, dev_y, dev_c, dev_a, dev_b):
        pl.semaphore_signal(bar, inc=1, device_id=dev, device_id_type=MESH)

    with sc("barrier"):
        pl.semaphore_wait(bar, 5)

    ft = min(256, f)

    def rows(s):
        return pl.ds(s * nr, nr)

    def transpose_x(rx, lo, hi):
        @pl.loop(lo, hi)
        def _(s):
            row = pl.ds(pl.multiple_of(s * nr, nr), nr)
            for rc in range(2):
                for h in range(2):
                    v = mmt(eye[...], xa[row, pl.ds((2 * rc + rx) * kd + h * hd, hd)])
                    xt[rc, pl.ds(h * hd, hd), row] = v.astype(bf)

    def wcopy(i, src, dst, dev):
        return remote(src, dst, gs.at[i], gr.at[i], dev)

    def half(rx, rc, ry, h):
        return blk(2, rx, rc, ry, h * hd, hd)

    ua = 3 * kd // 4
    mine = [blk(k, 0, 0, 0) for k in range(3)]
    xo = [wcopy(k, mine[k], blk(k, 1, 0, 0), dev_x) for k in range(2)]
    yo = [wcopy(2 + k, mine[k], blk(k, 0, 0, 1), dev_y) for k in range(2)]
    co = [wcopy(4 + k, mine[k], blk(k, 0, 1, 0), dev_c) for k in range(3)]
    xd = [wcopy(7 + h, half(0, 0, 0, h), half(1, 0, 0, h), dev_x) for h in range(2)]
    yd = [wcopy(9 + h, half(0, 0, 0, h), half(0, 0, 1, h), dev_y) for h in range(2)]
    rg = wcopy(11, blk(0, 0, 0, 1), blk(0, 1, 0, 1), dev_x)
    ay, ax = ((0, 5 * kd // 8), (5 * kd // 8, ua)), ((ua, 7 * kd // 8), (7 * kd // 8, kd))
    rua = [wcopy(i, blk(1, 1, 0, 0, lo, hi - lo), blk(1, 1, 0, 1, lo, hi - lo), dev_y) for i, (lo, hi) in zip((12, 29), ay)]
    rub = [wcopy(i, blk(1, 0, 0, 1, lo, hi - lo), blk(1, 1, 0, 1, lo, hi - lo), dev_x) for i, (lo, hi) in zip((13, 31), ax)]
    rd = [wcopy(14 + h, half(1, 0, 0, h), half(1, 0, 1, h), dev_y) for h in range(2)]
    cx = [wcopy(16 + k, blk(k, 1, 0, 0), blk(k, 1, 1, 0), dev_c) for k in range(2)]
    cy = [wcopy(18 + k, blk(k, 0, 0, 1), blk(k, 0, 1, 1), dev_c) for k in range(2)]
    cxd = [wcopy(20 + h, half(1, 0, 0, h), half(1, 1, 0, h), dev_c) for h in range(2)]
    cyd = [wcopy(22 + h, half(0, 0, 1, h), half(0, 1, 1, h), dev_c) for h in range(2)]
    crg = wcopy(24, blk(0, 1, 0, 1), blk(0, 1, 1, 1), dev_c)
    crua = [wcopy(i, blk(1, 1, 0, 1, lo, hi - lo), blk(1, 1, 1, 1, lo, hi - lo), dev_c) for i, (lo, hi) in zip((25, 30), ay)]
    crub = [wcopy(i, blk(1, 1, 0, 1, lo, hi - lo), blk(1, 1, 1, 1, lo, hi - lo), dev_c) for i, (lo, hi) in zip((26, 32), ax)]
    crd = [wcopy(27 + h, half(1, 0, 1, h), half(1, 1, 1, h), dev_c) for h in range(2)]
    wcopies = (*xo, *yo, *co, *xd, *yd, rg, *rua, *rub, *rd, *cx, *cy, *cxd, *cyd, crg, *crua, *crub, *crd)
    nw = 33

    def slot(j, s):
        return (xa, dya)[j].at[pl.ds(s * nr, nr)]

    def acopy(src, dst, j):
        return remote(
            slot(j, src), slot(j, dst), gs.at[nw + 2 * dst + j], gr.at[nw + 2 * dst + j], dev_a
        )

    def bcopy(src, dst, j):
        return remote(
            slot(j, src), slot(j, dst), gs.at[nw + 8 + 2 * dst + j], gr.at[nw + 2 * dst + j], dev_b
        )

    def got(s, j):
        acopy(s, s, j).wait_recv()

    def stash_copy(s, p, n):
        return pltpu.make_async_copy((fst, nst)[n].at[p, pl.ds(0, nr)], stash.at[s, p, n], ssem.at[2 * p + n])

    def factor(s, n):
        return nst if n else cst if s == 3 else fst

    def stash_load(s, p, n):
        return pltpu.make_async_copy(stash.at[s, p, n], factor(s, n).at[p, pl.ds(0, nr)], ssem.at[2 * p + n])

    pending = [None, None]

    def flush(p):
        if pending[p] is not None:
            for n in range(2):
                stash_copy(pending[p], p, n).wait()
        pending[p] = None

    def ab_tiles(s, p, step):
        def tile(i):
            col = pl.ds(pl.multiple_of(p * kf + i * ft, ft), ft)
            at = (p, pl.ds(0, nr), pl.ds(pl.multiple_of(i * ft, ft), ft))

            def some_b(rx):
                b0, b1 = pl.ds(rx * kd, kd), pl.ds((2 + rx) * kd, kd)
                return mm(xa[rows(s), b0], wu[b0, col]) + mm(xa[rows(s), b1], wu[b1, col])

            if step == 1:
                fst[at] = mm(xa[rows(s), :], wg[:, col])
                nst[at] = some_b(0)
                return
            if step == 2:
                a = fst[at]
                b = nst[at] + some_b(1)
            else:
                a = mm(xa[rows(s), :], wg[:, col])
                b = mm(xa[rows(s), :], wu[:, col])
            sig = jax.nn.sigmoid(a)
            sa = a * sig
            act[2, rows(s), col] = (sa * b).astype(bf)
            fst[at] = sa
            nst[at] = b * sig * (1.0 + a * (1.0 - sig))

        m = 2 if step == 2 and kf // ft > 1 else 1

        @pl.loop(0, kf // ft // m)
        def _(i):
            for q in range(m):
                tile(i * m + q)

    def part_ab(s, p, step=0):
        with sc(f"ab{s}_{p}"):
            flush(p)
            ab_tiles(s, p, step)
            if step != 1:
                for n in range(2):
                    stash_copy(s, p, n).start()
                pending[p] = s

    gt = min(512, kf)

    def part_g(s, p):
        @pl.loop(0, kf // gt)
        def _(i):
            col = pl.ds(pl.multiple_of(p * kf + i * gt, gt), gt)
            kcol = pl.ds(pl.multiple_of(i * gt, gt), gt)
            g = mmt(dya[rows(s), :], wd[col, :])
            act[0, rows(s), col] = (g * factor(s, 1)[p, pl.ds(0, nr), kcol]).astype(bf)
            act[1, rows(s), col] = (g * factor(s, 0)[p, pl.ds(0, nr), kcol]).astype(bf)

    def gload(s):
        for p in range(2):
            for n in range(2):
                stash_load(s, p, n).start()

    def half_g(s, p, then):
        with sc(f"g{s}"):
            for n in range(2):
                stash_load(s, p, n).wait()
            part_g(s, p)
            if then is not None:
                for n in range(2):
                    stash_load(then, p, n).start()

    def front_g(s, then):
        @pl.loop(0, 2)
        def _(p):
            half_g(s, p, then)

    def keep_h(lo, hi):
        hb = min(4, f // hd)
        nh = f // (hb * hd)
        with sc("ht"):
            @pl.loop(lo * nh, hi * nh)
            def _(i):
                row = pl.ds(pl.multiple_of(i // nh * nr, nr), nr)
                for q in range(hb):
                    col = pl.ds(pl.multiple_of((i % nh * hb + q) * hd, hd), hd)
                    ht[col, row] = mmt(eye[...], act[2, row, col]).astype(bf)

    def back(ref, at, kind, s, r):
        *lead, c0 = at

        @pl.loop(0, 2)
        def _(h):
            n = pl.ds(pl.multiple_of(r * kd + h * hd, hd), hd)
            if kind == 0:
                v = mm(act[2, rows(s), :], wd[:, n])
            else:
                v = mmt(act[0, rows(s), :], wg[n, :]) + mmt(act[1, rows(s), :], wu[n, :])
            ref[(*lead, pl.ds(0, nr), pl.ds(pl.multiple_of(c0 + h * hd, hd), hd))] = v

    def zcopy(q, kind, r, half, dev):
        i = 4 * kind + r
        return remote(zs.at[4 * half + r], zl.at[q, i], zsend.at[4 * half + r], zrecv.at[q, i], dev)

    def zload_(q, kind, r, slot):
        return pltpu.make_async_copy(zl.at[q, 4 * kind + r], cst.at[slot, pl.ds(0, nr), pl.ds(0, kd)], zload.at[slot])

    def chunk(kind, s, r, half, q_add, first):
        i = 4 * half + r
        if q_add is not None:
            with sc("zrecv"):
                zcopy(q_add, kind, r, half, dev_a).wait_recv()
            zload_(q_add, kind, r, r % 2).start()
        if not first:
            with sc("zsend"):
                zcopy(0, kind, r, half, dev_a).wait_send()
        back(zs, (i, 0), kind, s, r)
        if q_add is not None:
            zload_(q_add, kind, r, r % 2).wait()
            zs[i] = zs[i] + cst[r % 2, pl.ds(0, nr), pl.ds(0, kd)]

    def jobs(*specs):
        with sc("job" + "_".join(f"{kind}{s}" for kind, s, *_ in specs)):
            @pl.loop(0, 4)
            def _(r):
                for kind, s, h, q_add, q_dst, dev, first in specs:
                    chunk(kind, s, r, h, q_add, first)
                    zcopy(q_dst, kind, r, h, dev).start()

    def last_part():
        back(cst, (0, kd), 1, 0, 3)
        at = (0, pl.ds(0, nr), pl.ds(kd, kd))
        cst[at] = cst[at] + dya[rows(0), pl.ds(3 * kd, kd)].astype(f32)
        cp = pltpu.make_async_copy(cst.at[at], zl.at[1, 7], zload.at[0])
        cp.start()
        cp.wait()

    def finish(kind, adds, lo=0, hi=4):
        res = (xa, dya)[kind]
        with sc(f"fin{kind}"):
            @pl.loop(lo, hi)
            def _(r):
                col = pl.ds(pl.multiple_of(r * kd, kd), kd)
                part = (pl.ds(0, nr), pl.ds(0, kd))
                temp = (0, pl.ds(0, nr), pl.ds(kd, kd))
                back(cst, (0, kd), kind, 0, r)
                for n, q in enumerate(adds):
                    with sc("finrecv"):
                        zcopy(q, kind, r, 0, dev_a).wait_recv()
                    zload_(q, kind, r, n).start()
                for n, q in enumerate(adds):
                    zload_(q, kind, r, n).wait()
                v = cst[temp] + res[rows(0), col].astype(f32)
                for n in range(len(adds)):
                    v = v + cst[n, *part]
                res[rows(1), col] = v.astype(bf)

    def unit(rc, rx, j, put):
        ryi, k, half = j // 6, ((j // 2) % 3 + 2) % 3, j % 2
        f0 = (1 - ryi) * kf

        @pl.when(k < 2)
        def _():
            a = xt[rc, pl.ds(pl.multiple_of(half * hd, hd), hd), :]
            for q in range(4):
                b = act[k, :, pl.ds(pl.multiple_of(f0 + q * hd, hd), hd)]
                put(pl.ds(q * hd, hd), mm(a, b))

        @pl.when(k == 2)
        def _():
            for q in range(4):
                b = dya[:, pl.ds((2 * rc + rx) * kd + q % 2 * hd, hd)]
                a = ht[pl.ds(pl.multiple_of(f0 + half * hf + q // 2 * hd, hd), hd), :]
                put(pl.ds(q * hd, hd), mm(a, b))

    def fcopy(u):
        return remote(fst.at[u % 3], far_r.at[u], fsend.at[u % 3], frecv.at[u], dev_c)

    def ncopy(u):
        return pltpu.make_async_copy(nst.at[(u + 1) % 2], near.at[u], nstore.at[(u + 1) % 2])

    def ccopy(u):
        return pltpu.make_async_copy(far_r.at[u], cst.at[(u + 1) % 2], cload.at[(u + 1) % 2])

    def xcopy1(i, u):
        return remote(near.at[u], xr1.at[i], xs1.at[i], xq1.at[i], dev_x)

    def ycopy1(i, u):
        return remote(near.at[u], yr1.at[i], ys1.at[i], yq1.at[i], dev_y)

    def nsend(rx, j):
        ryi, k, half = j // 6, (j // 2) % 3, j % 2
        u = 12 * (1 - rx) + j
        if rx:
            @pl.when(half == 0)
            def _():
                xcopy1(ryi * 3 + k, u).start()

        @pl.when((half == 1) & (ryi == 0))
        def _():
            ycopy1(3 * (1 - rx) + k, u).start()

    def far_unit(rx, j):
        u = 12 * (1 - rx) + j

        @pl.when(u > 2)
        def _():
            with sc("fsend"):
                fcopy(u).wait_send()

        def put(col, v):
            fst[u % 3, :, col] = v

        unit(1, rx, j, put)
        fcopy(u).start()

    def far_start(lo, hi):
        t = pl.ds(lo * nr, (hi - lo) * nr)
        with sc("farstart"):
            @pl.loop(0, 2)
            def _(j):
                for q in range(4):
                    a = ht[pl.ds(pl.multiple_of(kf + j * hf + q // 2 * hd, hd), hd), t]
                    v = mm(a, dya[t, pl.ds(3 * kd + q % 2 * hd, hd)])
                    at = (j, slice(None), pl.ds(q * hd, hd))
                    fst[at] = fst[at] + v if lo else v

                if lo:
                    fcopy(j).start()

    def near_load(rx, j):
        u = 12 * (1 - rx) + j
        with sc("frecv"):
            fcopy(u).wait_recv()
        ccopy(u).start()

    def near_unit(rx, j):
        u = 12 * (1 - rx) + j
        with sc("cwait"):
            ccopy(u).wait()

        def put(col, v):
            i = (u + 1) % 2
            nst[i, :, col] = v + cst[i, :, col]

        unit(0, rx, j, put)

    def near_done(rx, j):
        with sc("nwait"):
            ncopy(12 * (1 - rx) + j).wait()
        nsend(rx, j)

    def dw(rx, f0, n0):
        base = 12 * (1 - rx)

        with sc(f"dw{rx}"):
            @pl.loop(f0, 12 + LAG)
            def _(j):
                n = j - LAG

                @pl.when(j < 12)
                def _():
                    far_unit(rx, j)

                @pl.when((n + 1 >= n0) & (n < 11))
                def _():
                    near_load(rx, n + 1)

                @pl.when(n >= n0)
                def _():
                    near_unit(rx, n)

                    @pl.when(n > n0)
                    def _():
                        near_done(rx, n - 1)

                    ncopy(base + n).start()

            near_done(rx, 11)

    def add_pair(units, waits, arrived, dsts, after=(None, None)):
        cn = [pltpu.make_async_copy(near.at[u], fst.at[h], cin.at[h]) for h, u in enumerate(units)]
        cr = [pltpu.make_async_copy(v, cst.at[h], cload.at[h]) for h, v in enumerate(arrived)]
        cd = [pltpu.make_async_copy(nst.at[h], t, nstore.at[h]) for h, t in enumerate(dsts)]
        st = min(64, hd)
        for h in range(2):
            cn[h].start()
        for h in range(2):
            waits[h].wait_recv()
            cr[h].start()
        for h in range(2):
            cn[h].wait()
            cr[h].wait()

            @pl.loop(0, hd // st)
            def _(i):
                row = pl.ds(pl.multiple_of(i * st, st), st)
                nst[h, row, :] = fst[h, row, :] + cst[h, row, :]

            cd[h].start()
        for h in range(2):
            cd[h].wait()
            if after[h] is not None:
                after[h].start()

    def uid(rx, ry, k, half):
        return 12 * (1 - rx) + 6 * (1 - ry) + 2 * k + half

    def ycopy2(k):
        return remote(near.at[uid(0, 1, k, 0)], r2.at[2 * k], s2.at[2 * k], q2.at[2 * k], dev_y)

    def xcopy2(k):
        return remote(near.at[uid(1, 0, k, 1)], r2.at[2 * k + 1], s2.at[2 * k + 1], q2.at[2 * k + 1], dev_x)

    def second(k):
        ua, ub = uid(0, 1, k, 0), uid(1, 0, k, 1)
        with sc(f"second{k}"):
            add_pair(
                (ua, ub), (xcopy1(k, 0), ycopy1(k, 0)), (xr1.at[k], yr1.at[k]), (near.at[ua], near.at[ub]),
                (ycopy2(k), xcopy2(k)),
            )

    def third(k):
        ua, ub = uid(0, 0, k, 0), uid(0, 0, k, 1)
        with sc(f"third{k}"):
            add_pair(
                (ua, ub), (xcopy1(3 + k, 0), ycopy1(3 + k, 0)), (xr1.at[3 + k], yr1.at[3 + k]),
                (n00.at[2 * k], n00.at[2 * k + 1]),
            )

    def fourth(k):
        cn = [pltpu.make_async_copy(n00.at[2 * k + h], dwv.at[2 * k + h], cin.at[h]) for h in range(2)]
        cr = [pltpu.make_async_copy(r2.at[2 * k + h], cst.at[h], cload.at[h]) for h in range(2)]
        st = min(64, hd)
        with sc(f"fourth{k}"):
            for h in range(2):
                cn[h].start()
            for h in range(2):
                (ycopy2, xcopy2)[h](k).wait_recv()
                cr[h].start()
            for h in range(2):
                cn[h].wait()
                cr[h].wait()

                @pl.loop(0, hd // st)
                def _(i):
                    row = pl.ds(pl.multiple_of(i * st, st), st)
                    dwv[2 * k + h, row, :] = dwv[2 * k + h, row, :] + cst[h, row, :]

    with sc("own_in"):
        for k in range(3):
            local[k].wait()
            if k < 2:
                xo[k].start()
                yo[k].start()
        yd[0].start()
        for cp in local[3:]:
            cp.wait()
    for j in range(2):
        acopy(0, 1, j).start()

    @mid
    def _():
        for j in range(2):
            bcopy(0, 2, j).start()

    for k in range(3):
        co[k].start()

    eye[...] = (
        lax.broadcasted_iota(jnp.int32, (hd, hd), 0) == lax.broadcasted_iota(jnp.int32, (hd, hd), 1)
    ).astype(f32).astype(bf)

    with sc("xt0"):
        transpose_x(1, 0, 1)

    def pass_on(s, j):
        with sc(f"rows{s}_{j}"):
            got(s, j)
        if s == 1:
            bcopy(1, 3, j).start()
        else:
            acopy(s, s, j).start()

    with sc("gx0"):
        xo[0].wait_recv()
        cx[0].start()
        yo[0].wait_recv()
    rg.start()
    cy[0].start()

    @mid
    def _():
        pass_on(1, 0)
        pass_on(2, 0)

    with sc("gx1"):
        xo[1].wait_recv()
        for cp in rua:
            cp.start()
        yd[1].start()
        cx[1].start()
        yo[1].wait_recv()
    for cp in rub:
        cp.start()
    for h in range(2):
        xd[h].start()
    cy[1].start()

    @mid
    def _():
        pass_on(1, 1)
        pass_on(2, 1)

    @end
    def _():
        with sc("e_rows1"):
            got(1, 0)

    with sc("gc0"):
        for cp in (*co[:2], *cx):
            cp.wait_recv()
    part_ab(1, 0)
    part_ab(0, 0)
    with sc("gyd"):
        yd[0].wait_recv()
        cyd[0].start()
        rg.wait_recv()
        crg.start()
    with sc("gc1"):
        for cp in (*cy, crg):
            cp.wait_recv()
    part_ab(1, 1, 1)
    co[2].wait_recv()

    @end
    def _():
        @pl.loop(0, 2)
        def _(i):
            n = pl.ds(pl.multiple_of(2 * i * kd, kd), hd)
            zs[2 * i, :, pl.ds(0, hd)] = mm(act[2, rows(1), pl.ds(0, kf)], wd[pl.ds(0, kf), n])

    @mid
    def _():
        pass_on(3, 0)

    with sc("gru"):
        for cp, fwd in zip((*rua[:1], *rub[:1], *rua[1:], *rub[1:]), (*crua[:1], *crub[:1], *crua[1:], *crub[1:])):
            cp.wait_recv()
            fwd.start()
    with sc("gc2"):
        for cp in (*crua, *crub):
            cp.wait_recv()
    part_ab(1, 1, 2)
    with sc("gc3"):
        cyd[0].wait_recv()

    def early_half(h):
        with sc(f"early1_{h}"):
            @pl.loop(0, 2)
            def _(i):
                r = 2 * i
                col = pl.ds(h * hd, hd)
                n = pl.ds(pl.multiple_of(r * kd + h * hd, hd), hd)
                if h == 0:
                    v = zs[r, :, col] + mm(act[2, rows(1), pl.ds(kf, kf)], wd[pl.ds(kf, kf), n])
                else:
                    v = mm(act[2, rows(1), :], wd[:, n])
                zs[r, :, col] = v
                remote(zs.at[r, :, col], zl.at[0, r, :, col], zsend.at[r], zrecv.at[0, r], dev_a).start()

    def early(s, odd):
        with sc(f"early{s}_{odd}"):
            @pl.loop(0, 2)
            def _(i):
                r = 2 * i + odd
                chunk(0, s, r, s - 1, None, True)
                zcopy(s - 1, 0, r, s - 1, dev_a).start()

    @end
    def _():
        early_half(0)
        with sc("e_rows2"):
            got(2, 0)

    part_ab(2, 0)
    with sc("gd0"):
        yd[1].wait_recv()
        cyd[1].start()
        xd[0].wait_recv()
        rd[0].start()
        cxd[0].start()
        cyd[1].wait_recv()

    @end
    def _():
        early_half(1)

    part_ab(2, 1)

    @end
    def _():
        early(2, 0)

    @mid
    def _():
        pass_on(3, 1)

    with sc("gd1"):
        xd[1].wait_recv()
        rd[1].start()
        cxd[1].start()
    part_ab(0, 1)
    with sc("gd2"):
        rd[0].wait_recv()
        crd[0].start()
    transpose_x(1, 1, 3)
    keep_h(0, 3)
    with sc("gd3"):
        rd[1].wait_recv()
        crd[1].start()
        for cp in (*cxd, *crd):
            cp.wait_recv()

    @end
    def _():
        early(1, 1)
        early(2, 1)
        got(1, 1)
        got(2, 1)
        with sc("e_rows3"):
            got(3, 0)

    part_ab(3, 0)
    part_ab(3, 1)
    flush(0)
    flush(1)
    gload(1)
    transpose_x(1, 3, 4)
    keep_h(3, 4)
    front_g(1, 0)
    front_g(0, 2)
    front_g(2, 3)
    far_start(0, 3)

    @end
    def _():
        with sc("e_rows3"):
            got(3, 1)

    far_start(3, 4)
    half_g(3, 1, None)
    near_load(1, 0)
    half_g(3, 0, None)
    near_load(1, 1)

    @pl.loop(0, 2)
    def _(j):
        near_unit(1, j)
        ncopy(j).start()

    for j in range(2):
        near_done(1, j)
    dw(1, 2, 2)

    @end
    def _():
        jobs((0, 3, 0, None, 2, dev_a, False))

    @mid
    def _():
        jobs((0, 2, 0, 1, 3, dev_b, True))

    with sc("xtb"):
        transpose_x(0, 0, 4)
    dw(0, 0, 0)
    for u in range(3):
        fcopy(u).wait_send()
    for cp in wcopies:
        cp.wait_send()
    for j in range(2):
        acopy(0, 1, j).wait_send()

    @mid
    def _():
        for j in range(2):
            bcopy(0, 2, j).wait_send()
            bcopy(1, 3, j).wait_send()
            acopy(2, 2, j).wait_send()
            acopy(3, 3, j).wait_send()

    @end
    def _():
        jobs((1, 3, 1, None, 2, dev_a, False))
        second(0)
        second(1)
        second(2)
        jobs((1, 2, 0, None, 1, dev_a, False))
        third(0)
        third(1)
        jobs((1, 1, 1, None, 0, dev_a, False))
        third(2)
        finish(0, (0,))
        last_part()
        fourth(0)
        finish(1, (0,), 0, 2)
        fourth(1)
        finish(1, (0,), 2, 3)
        fourth(2)

    @mid
    def _():
        jobs((0, 3, 1, 2, 4, dev_b, True))
        second(0)
        second(1)
        second(2)
        jobs((0, 1, 0, 4, 0, dev_a, False), (1, 3, 1, 2, 4, dev_b, False))
        third(0)
        third(1)
        jobs((1, 1, 0, 4, 0, dev_a, False), (1, 2, 1, 1, 3, dev_b, False))
        third(2)
        finish(0, (0, 3))
        fourth(0)
        fourth(1)
        last_part()
        finish(1, (0, 3), 0, 3)
        fourth(2)
        zcopy(3, 1, 3, 0, dev_a).wait_recv()

    zcopy(0, 1, 3, 0, dev_a).wait_recv()

    with sc("drain"):
        for half in range(2):
            for r in range(4):
                zcopy(0, 0, r, half, dev_a).wait_send()
        for i in range(6):
            xcopy1(i, 0).wait_send()
            ycopy1(i, 0).wait_send()
        for k in range(3):
            ycopy2(k).wait_send()
            xcopy2(k).wait_send()


def fused(x, dy, wg, wu, wd):
    nr, d = x.shape
    kd, kf = wg.shape
    f, hd = 2 * kf, kd // 2
    hbm = pl.BlockSpec(memory_space=pl.ANY)
    sds = jax.ShapeDtypeStruct
    out_shape = (
        pltpu.VMEM((4 * nr, d), bf), pltpu.VMEM((4 * nr, d), bf), pltpu.VMEM((6, hd, kf), f32),
        sds((5, 8, nr, kd), f32), sds((6, hd, kf), f32), sds((6, hd, kf), f32),
        sds((24, hd, kf), f32), sds((24, hd, kf), f32),
        sds((6, hd, kf), f32), sds((6, hd, kf), f32), sds((4, 2, 2, nr, kf), f32),
    )
    dma = pltpu.SemaphoreType.DMA
    return pl.pallas_call(
        kernel,
        name="fused",
        out_shape=out_shape,
        in_specs=[hbm] * 5,
        out_specs=(pl.BlockSpec(memory_space=pltpu.VMEM),) * 3 + (hbm,) * (len(out_shape) - 3),
        scratch_shapes=[
            pltpu.VMEM((d, f), bf), pltpu.VMEM((d, f), bf), pltpu.VMEM((f, d), bf),
            pltpu.VMEM((3, 4 * nr, f), bf),
            pltpu.VMEM((8, nr, kd), f32), pltpu.VMEM((2, kd, 4 * nr), bf), pltpu.VMEM((f, 4 * nr), bf),
            pltpu.VMEM((hd, hd), bf),
            pltpu.VMEM((2, hd, kf), f32),
            dma((49,)), dma((41,)), dma((11,)), dma((8,)), dma((5, 8)), dma((2,)), dma((3,)), dma((24,)), dma((2,)),
            dma((2,)), dma((6,)), dma((6,)), dma((6,)), dma((6,)), dma((6,)), dma((6,)), dma((2,)), dma((4,)),
        ],
        compiler_params=pltpu.CompilerParams(collective_id=0, has_side_effects=True, vmem_limit_bytes=VMEM_LIMIT - 14 * 2**20),
    )(x, dy, wg, wu, wd)


def tail_kernel(xa, dya, dwv, zl, y, dx, dwg, dwu, dwd, buf, out, sem, lsem):
    dp = lax.axis_index("dp")
    z = lax.axis_index("tp") // 2
    is_mid = (z == 1) | (z == 2)
    nr, kd = y.shape[0], dwd.shape[1]
    hd = kd // 2
    srcs = (zl.at[1, 7], zl.at[0, 7], zl.at[3, 7])
    loads = [pltpu.make_async_copy(v, buf.at[i], lsem.at[i]) for i, v in enumerate(srcs)]
    loads[0].start()
    loads[1].start()

    @pl.when(is_mid)
    def _():
        loads[2].start()

    copies = []
    for k in range(3):
        for h in range(2):
            v = dwv.at[2 * k + h]
            if k > 0:
                copies.append((v, (dwg, dwu)[k - 1].at[pl.ds(h * hd, hd)]))
            else:
                for q in range(2):
                    copies.append((v.at[:, pl.ds(q * kd, kd)], dwd.at[pl.ds((2 * h + q) * hd, hd)]))
    for src, dst, n in ((xa, y, 4), (dya, dx, 3)):
        for r in range(n):
            copies.append((src.at[pl.ds(nr, nr), pl.ds(r * kd, kd)], dst.at[:, natural(dp, r, kd)]))
    copies.append((out, dx.at[:, natural(dp, 3, kd)]))
    copies = [pltpu.make_async_copy(s, t, sem.at[i]) for i, (s, t) in enumerate(copies)]
    for c in copies[:-1]:
        c.start()
    loads[0].wait()
    loads[1].wait()
    buf[0] = buf[0] + buf[1]

    @pl.when(is_mid)
    def _():
        loads[2].wait()
        buf[0] = buf[0] + buf[2]

    out[...] = buf[0].astype(bf)
    copies[-1].start()
    for c in copies:
        c.wait()


def tail(xa, dya, dwv, zl, nr, kd, kf):
    hbm = pl.BlockSpec(memory_space=pl.ANY)
    sds = jax.ShapeDtypeStruct
    d = xa.shape[1]
    dma = pltpu.SemaphoreType.DMA
    return pl.pallas_call(
        tail_kernel,
        name="tail",
        out_shape=(sds((nr, d), bf), sds((nr, d), bf), sds((kd, kf), f32), sds((kd, kf), f32), sds((kf, kd), f32)),
        in_specs=[hbm] * 4,
        out_specs=(hbm,) * 5,
        scratch_shapes=[pltpu.VMEM((3, nr, kd), f32), pltpu.VMEM((nr, kd), bf), dma((16,)), dma((3,))],
        compiler_params=pltpu.CompilerParams(vmem_limit_bytes=VMEM_LIMIT - 27 * 2**20),
    )(xa, dya, dwv, zl)


def solution(mesh):
    rows = P(("dp", "tp"), None)
    wsp = P("dp", "tp")
    dsp = P("tp", "dp")

    def local(x, w_gate, w_up, w_down, dy):
        return tail(*fused(x, dy, w_gate, w_up, w_down)[:4], x.shape[0], *w_gate.shape)

    return jax.shard_map(local, mesh=mesh, in_specs=(rows, wsp, wsp, dsp, rows), out_specs=(rows, rows, wsp, wsp, dsp), check_vma=False)
```

```python
import jax
import jax.numpy as jnp
from jax import lax
from jax.experimental import pallas as pl
from jax.experimental.pallas import tpu as pltpu
from jax.sharding import PartitionSpec as P

MESH = pl.DeviceIdType.MESH
f32 = jnp.float32
bf = jnp.bfloat16
VMEM_LIMIT = 67043328
sc = jax.named_scope
LAG = 4


def mm(a, b):
    return lax.dot_general(a, b, (((1,), (0,)), ((), ())), preferred_element_type=f32)


def mmt(a, b):
    return lax.dot_general(a, b, (((1,), (1,)), ((), ())), preferred_element_type=f32)


def natural(dp, r, kd):
    x, c, rc, rx = dp // 2, dp % 2, r // 2, r % 2
    n = 2 * (x + rx - 2 * x * rx) + c + rc - 2 * c * rc
    return pl.ds(pl.multiple_of(n * kd, kd), kd)


def kernel(
    x_in, dy_in, wg_in, wu_in, wd_in,
    xa, dya, dwv, zl, n00, r2, far_r, near, xr1, yr1, stash,
    wg, wu, wd, act, zs, xt, ht, eye, cst,
    gs, gr, lsem, zsend, zrecv, zload, fsend, frecv, nstore, cload, xs1, xq1, ys1, yq1, s2, q2, cin, ssem,
):
    tp = lax.axis_index("tp")
    dp = lax.axis_index("dp")
    z, y = tp // 2, tp % 2
    x, c = dp // 2, dp % 2
    is_end = (z == 0) | (z == 3)
    is_mid = (z == 1) | (z == 2)
    dev_x = {"tp": tp, "dp": 2 * (1 - x) + c}
    dev_y = {"tp": 2 * z + 1 - y, "dp": dp}
    dev_c = {"tp": tp, "dp": 2 * x + 1 - c}
    dev_a = {"tp": 2 * (z + 1 - 2 * (z % 2)) + y, "dp": dp}
    dev_b = {"tp": 2 * (3 - z) + y, "dp": dp}

    fst, nst = dwv.at[pl.ds(0, 3)], dwv.at[pl.ds(3, 2)]
    nr, d = x_in.shape
    kd, kf = wg_in.shape
    f = 2 * kf
    hd = kd // 2
    hf = kf // 2

    def end(fn):
        pl.when(is_end)(fn)

    def mid(fn):
        pl.when(is_mid)(fn)

    def ncol(r):
        return natural(dp, r, kd)

    def remote(src, dst, ss, rs, dev):
        return pltpu.make_async_remote_copy(
            src_ref=src, dst_ref=dst, send_sem=ss, recv_sem=rs, device_id=dev, device_id_type=MESH
        )

    own = (wg_in, wu_in, wd_in)

    def blk(k, rx, rc, ry, lo=0, n=None):
        d0 = (2 * rc + rx) * kd + lo
        n = kd if n is None else n
        if k < 2:
            return (wg, wu)[k].at[pl.ds(d0, n), pl.ds(ry * kf, kf)]
        return wd.at[pl.ds(ry * kf, kf), pl.ds(d0, n)]

    local = [(own[k], blk(k, 0, 0, 0)) for k in range(3)]
    for src, ref in ((x_in, xa), (dy_in, dya)):
        for r in range(4):
            local.append((src.at[:, ncol(r)], ref.at[pl.ds(0, nr), pl.ds(r * kd, kd)]))
    local = [pltpu.make_async_copy(s, t, lsem.at[i]) for i, (s, t) in enumerate(local)]
    for cp in local:
        cp.start()

    bar = pltpu.get_barrier_semaphore()
    for dev in (dev_x, dev_y, dev_c, dev_a, dev_b):
        pl.semaphore_signal(bar, inc=1, device_id=dev, device_id_type=MESH)

    with sc("barrier"):
        pl.semaphore_wait(bar, 5)

    ft = min(256, f)

    def rows(s):
        return pl.ds(s * nr, nr)

    def transpose_x(rx, lo, hi):
        @pl.loop(lo, hi)
        def _(s):
            row = pl.ds(pl.multiple_of(s * nr, nr), nr)
            for rc in range(2):
                for h in range(2):
                    v = mmt(eye[...], xa[row, pl.ds((2 * rc + rx) * kd + h * hd, hd)])
                    xt[rc, pl.ds(h * hd, hd), row] = v.astype(bf)

    def wcopy(i, src, dst, dev):
        return remote(src, dst, gs.at[i], gr.at[i], dev)

    def half(rx, rc, ry, h):
        return blk(2, rx, rc, ry, h * hd, hd)

    ua = 3 * kd // 4
    mine = [blk(k, 0, 0, 0) for k in range(3)]
    xo = [wcopy(k, mine[k], blk(k, 1, 0, 0), dev_x) for k in range(2)]
    yo = [wcopy(2 + k, mine[k], blk(k, 0, 0, 1), dev_y) for k in range(2)]
    co = [wcopy(4 + k, mine[k], blk(k, 0, 1, 0), dev_c) for k in range(3)]
    xd = [wcopy(7 + h, half(0, 0, 0, h), half(1, 0, 0, h), dev_x) for h in range(2)]
    yd = [wcopy(9 + h, half(0, 0, 0, h), half(0, 0, 1, h), dev_y) for h in range(2)]
    rg = wcopy(11, blk(0, 0, 0, 1), blk(0, 1, 0, 1), dev_x)
    ay, ax = ((0, 5 * kd // 8), (5 * kd // 8, ua)), ((ua, 7 * kd // 8), (7 * kd // 8, kd))
    rua = [wcopy(i, blk(1, 1, 0, 0, lo, hi - lo), blk(1, 1, 0, 1, lo, hi - lo), dev_y) for i, (lo, hi) in zip((12, 29), ay)]
    rub = [wcopy(i, blk(1, 0, 0, 1, lo, hi - lo), blk(1, 1, 0, 1, lo, hi - lo), dev_x) for i, (lo, hi) in zip((13, 31), ax)]
    rd = [wcopy(14 + h, half(1, 0, 0, h), half(1, 0, 1, h), dev_y) for h in range(2)]
    cx = [wcopy(16 + k, blk(k, 1, 0, 0), blk(k, 1, 1, 0), dev_c) for k in range(2)]
    cy = [wcopy(18 + k, blk(k, 0, 0, 1), blk(k, 0, 1, 1), dev_c) for k in range(2)]
    cxd = [wcopy(20 + h, half(1, 0, 0, h), half(1, 1, 0, h), dev_c) for h in range(2)]
    cyd = [wcopy(22 + h, half(0, 0, 1, h), half(0, 1, 1, h), dev_c) for h in range(2)]
    crg = wcopy(24, blk(0, 1, 0, 1), blk(0, 1, 1, 1), dev_c)
    crua = [wcopy(i, blk(1, 1, 0, 1, lo, hi - lo), blk(1, 1, 1, 1, lo, hi - lo), dev_c) for i, (lo, hi) in zip((25, 30), ay)]
    crub = [wcopy(i, blk(1, 1, 0, 1, lo, hi - lo), blk(1, 1, 1, 1, lo, hi - lo), dev_c) for i, (lo, hi) in zip((26, 32), ax)]
    crd = [wcopy(27 + h, half(1, 0, 1, h), half(1, 1, 1, h), dev_c) for h in range(2)]
    wcopies = (*xo, *yo, *co, *xd, *yd, rg, *rua, *rub, *rd, *cx, *cy, *cxd, *cyd, crg, *crua, *crub, *crd)
    nw = 33

    def slot(j, s):
        return (xa, dya)[j].at[pl.ds(s * nr, nr)]

    def acopy(src, dst, j):
        return remote(
            slot(j, src), slot(j, dst), gs.at[nw + 2 * dst + j], gr.at[nw + 2 * dst + j], dev_a
        )

    def bcopy(src, dst, j):
        return remote(
            slot(j, src), slot(j, dst), gs.at[nw + 8 + 2 * dst + j], gr.at[nw + 2 * dst + j], dev_b
        )

    def got(s, j):
        acopy(s, s, j).wait_recv()

    def stash_copy(s, p, n):
        return pltpu.make_async_copy((fst, nst)[n].at[p, pl.ds(0, nr)], stash.at[s, p, n], ssem.at[2 * p + n])

    def factor(s, n):
        return nst if n else cst if s == 3 else fst

    def stash_load(s, p, n):
        return pltpu.make_async_copy(stash.at[s, p, n], factor(s, n).at[p, pl.ds(0, nr)], ssem.at[2 * p + n])

    pending = [None, None]

    def flush(p):
        if pending[p] is not None:
            for n in range(2):
                stash_copy(pending[p], p, n).wait()
        pending[p] = None

    def ab_tiles(s, p, step):
        def tile(i):
            col = pl.ds(pl.multiple_of(p * kf + i * ft, ft), ft)
            at = (p, pl.ds(0, nr), pl.ds(pl.multiple_of(i * ft, ft), ft))

            def some_b(rx):
                b0, b1 = pl.ds(rx * kd, kd), pl.ds((2 + rx) * kd, kd)
                return mm(xa[rows(s), b0], wu[b0, col]) + mm(xa[rows(s), b1], wu[b1, col])

            if step == 1:
                fst[at] = mm(xa[rows(s), :], wg[:, col])
                nst[at] = some_b(0)
                return
            if step == 2:
                a = fst[at]
                b = nst[at] + some_b(1)
            else:
                a = mm(xa[rows(s), :], wg[:, col])
                b = mm(xa[rows(s), :], wu[:, col])
            sig = jax.nn.sigmoid(a)
            sa = a * sig
            act[2, rows(s), col] = (sa * b).astype(bf)
            fst[at] = sa
            nst[at] = b * sig * (1.0 + a * (1.0 - sig))

        m = 2 if step == 2 and kf // ft > 1 else 1

        @pl.loop(0, kf // ft // m)
        def _(i):
            for q in range(m):
                tile(i * m + q)

    def part_ab(s, p, step=0):
        with sc(f"ab{s}_{p}"):
            flush(p)
            ab_tiles(s, p, step)
            if step != 1:
                for n in range(2):
                    stash_copy(s, p, n).start()
                pending[p] = s

    gt = min(512, kf)

    def part_g(s, p):
        @pl.loop(0, kf // gt)
        def _(i):
            col = pl.ds(pl.multiple_of(p * kf + i * gt, gt), gt)
            kcol = pl.ds(pl.multiple_of(i * gt, gt), gt)
            g = mmt(dya[rows(s), :], wd[col, :])
            act[0, rows(s), col] = (g * factor(s, 1)[p, pl.ds(0, nr), kcol]).astype(bf)
            act[1, rows(s), col] = (g * factor(s, 0)[p, pl.ds(0, nr), kcol]).astype(bf)

    def gload(s):
        for p in range(2):
            for n in range(2):
                stash_load(s, p, n).start()

    def half_g(s, p, then):
        with sc(f"g{s}"):
            for n in range(2):
                stash_load(s, p, n).wait()
            part_g(s, p)
            if then is not None:
                for n in range(2):
                    stash_load(then, p, n).start()

    def front_g(s, then):
        @pl.loop(0, 2)
        def _(p):
            half_g(s, p, then)

    def keep_h(lo, hi):
        hb = min(4, f // hd)
        nh = f // (hb * hd)
        with sc("ht"):
            @pl.loop(lo * nh, hi * nh)
            def _(i):
                row = pl.ds(pl.multiple_of(i // nh * nr, nr), nr)
                for q in range(hb):
                    col = pl.ds(pl.multiple_of((i % nh * hb + q) * hd, hd), hd)
                    ht[col, row] = mmt(eye[...], act[2, row, col]).astype(bf)

    def back(ref, at, kind, s, r):
        *lead, c0 = at

        @pl.loop(0, 2)
        def _(h):
            n = pl.ds(pl.multiple_of(r * kd + h * hd, hd), hd)
            if kind == 0:
                v = mm(act[2, rows(s), :], wd[:, n])
            else:
                v = mmt(act[0, rows(s), :], wg[n, :]) + mmt(act[1, rows(s), :], wu[n, :])
            ref[(*lead, pl.ds(0, nr), pl.ds(pl.multiple_of(c0 + h * hd, hd), hd))] = v

    def zcopy(q, kind, r, half, dev):
        i = 4 * kind + r
        return remote(zs.at[4 * half + r], zl.at[q, i], zsend.at[4 * half + r], zrecv.at[q, i], dev)

    def zload_(q, kind, r, slot):
        return pltpu.make_async_copy(zl.at[q, 4 * kind + r], cst.at[slot, pl.ds(0, nr), pl.ds(0, kd)], zload.at[slot])

    def chunk(kind, s, r, half, q_add, first):
        i = 4 * half + r
        if q_add is not None:
            with sc("zrecv"):
                zcopy(q_add, kind, r, half, dev_a).wait_recv()
            zload_(q_add, kind, r, r % 2).start()
        if not first:
            with sc("zsend"):
                zcopy(0, kind, r, half, dev_a).wait_send()
        back(zs, (i, 0), kind, s, r)
        if q_add is not None:
            zload_(q_add, kind, r, r % 2).wait()
            zs[i] = zs[i] + cst[r % 2, pl.ds(0, nr), pl.ds(0, kd)]

    def jobs(*specs):
        with sc("job" + "_".join(f"{kind}{s}" for kind, s, *_ in specs)):
            @pl.loop(0, 4)
            def _(r):
                for kind, s, h, q_add, q_dst, dev, first in specs:
                    chunk(kind, s, r, h, q_add, first)
                    zcopy(q_dst, kind, r, h, dev).start()

    def last_part():
        back(cst, (0, kd), 1, 0, 3)
        at = (0, pl.ds(0, nr), pl.ds(kd, kd))
        cst[at] = cst[at] + dya[rows(0), pl.ds(3 * kd, kd)].astype(f32)
        cp = pltpu.make_async_copy(cst.at[at], zl.at[1, 7], zload.at[0])
        cp.start()
        cp.wait()

    def finish(kind, adds, lo=0, hi=4):
        res = (xa, dya)[kind]
        with sc(f"fin{kind}"):
            @pl.loop(lo, hi)
            def _(r):
                col = pl.ds(pl.multiple_of(r * kd, kd), kd)
                part = (pl.ds(0, nr), pl.ds(0, kd))
                temp = (0, pl.ds(0, nr), pl.ds(kd, kd))
                back(cst, (0, kd), kind, 0, r)
                for n, q in enumerate(adds):
                    with sc("finrecv"):
                        zcopy(q, kind, r, 0, dev_a).wait_recv()
                    zload_(q, kind, r, n).start()
                for n, q in enumerate(adds):
                    zload_(q, kind, r, n).wait()
                v = cst[temp] + res[rows(0), col].astype(f32)
                for n in range(len(adds)):
                    v = v + cst[n, *part]
                res[rows(1), col] = v.astype(bf)

    def unit(rc, rx, j, put):
        ryi, k, half = j // 6, ((j // 2) % 3 + 2) % 3, j % 2
        f0 = (1 - ryi) * kf

        @pl.when(k < 2)
        def _():
            a = xt[rc, pl.ds(pl.multiple_of(half * hd, hd), hd), :]
            for q in range(4):
                b = act[k, :, pl.ds(pl.multiple_of(f0 + q * hd, hd), hd)]
                put(pl.ds(q * hd, hd), mm(a, b))

        @pl.when(k == 2)
        def _():
            for q in range(4):
                b = dya[:, pl.ds((2 * rc + rx) * kd + q % 2 * hd, hd)]
                a = ht[pl.ds(pl.multiple_of(f0 + half * hf + q // 2 * hd, hd), hd), :]
                put(pl.ds(q * hd, hd), mm(a, b))

    def fcopy(u):
        return remote(fst.at[u % 3], far_r.at[u], fsend.at[u % 3], frecv.at[u], dev_c)

    def ncopy(u):
        return pltpu.make_async_copy(nst.at[(u + 1) % 2], near.at[u], nstore.at[(u + 1) % 2])

    def ccopy(u):
        return pltpu.make_async_copy(far_r.at[u], cst.at[(u + 1) % 2], cload.at[(u + 1) % 2])

    def xcopy1(i, u):
        return remote(near.at[u], xr1.at[i], xs1.at[i], xq1.at[i], dev_x)

    def ycopy1(i, u):
        return remote(near.at[u], yr1.at[i], ys1.at[i], yq1.at[i], dev_y)

    def nsend(rx, j):
        ryi, k, half = j // 6, (j // 2) % 3, j % 2
        u = 12 * (1 - rx) + j
        if rx:
            @pl.when(half == 0)
            def _():
                xcopy1(ryi * 3 + k, u).start()

        @pl.when((half == 1) & (ryi == 0))
        def _():
            ycopy1(3 * (1 - rx) + k, u).start()

    def far_unit(rx, j):
        u = 12 * (1 - rx) + j

        @pl.when(u > 2)
        def _():
            with sc("fsend"):
                fcopy(u).wait_send()

        def put(col, v):
            fst[u % 3, :, col] = v

        unit(1, rx, j, put)
        fcopy(u).start()

    def far_start(lo, hi):
        t = pl.ds(lo * nr, (hi - lo) * nr)
        with sc("farstart"):
            @pl.loop(0, 2)
            def _(j):
                for q in range(4):
                    a = ht[pl.ds(pl.multiple_of(kf + j * hf + q // 2 * hd, hd), hd), t]
                    v = mm(a, dya[t, pl.ds(3 * kd + q % 2 * hd, hd)])
                    at = (j, slice(None), pl.ds(q * hd, hd))
                    fst[at] = fst[at] + v if lo else v

                if lo:
                    fcopy(j).start()

    def near_load(rx, j):
        u = 12 * (1 - rx) + j
        with sc("frecv"):
            fcopy(u).wait_recv()
        ccopy(u).start()

    def near_unit(rx, j):
        u = 12 * (1 - rx) + j
        with sc("cwait"):
            ccopy(u).wait()

        def put(col, v):
            i = (u + 1) % 2
            nst[i, :, col] = v + cst[i, :, col]

        unit(0, rx, j, put)

    def near_done(rx, j):
        with sc("nwait"):
            ncopy(12 * (1 - rx) + j).wait()
        nsend(rx, j)

    def dw(rx, f0, n0):
        base = 12 * (1 - rx)

        with sc(f"dw{rx}"):
            @pl.loop(f0, 12 + LAG)
            def _(j):
                n = j - LAG

                @pl.when(j < 12)
                def _():
                    far_unit(rx, j)

                @pl.when((n + 1 >= n0) & (n < 11))
                def _():
                    near_load(rx, n + 1)

                @pl.when(n >= n0)
                def _():
                    near_unit(rx, n)

                    @pl.when(n > n0)
                    def _():
                        near_done(rx, n - 1)

                    ncopy(base + n).start()

            near_done(rx, 11)

    def add_pair(units, waits, arrived, dsts, after=(None, None)):
        cn = [pltpu.make_async_copy(near.at[u], fst.at[h], cin.at[h]) for h, u in enumerate(units)]
        cr = [pltpu.make_async_copy(v, cst.at[h], cload.at[h]) for h, v in enumerate(arrived)]
        cd = [pltpu.make_async_copy(nst.at[h], t, nstore.at[h]) for h, t in enumerate(dsts)]
        st = min(64, hd)
        for h in range(2):
            cn[h].start()
        for h in range(2):
            waits[h].wait_recv()
            cr[h].start()
        for h in range(2):
            cn[h].wait()
            cr[h].wait()

            @pl.loop(0, hd // st)
            def _(i):
                row = pl.ds(pl.multiple_of(i * st, st), st)
                nst[h, row, :] = fst[h, row, :] + cst[h, row, :]

            cd[h].start()
        for h in range(2):
            cd[h].wait()
            if after[h] is not None:
                after[h].start()

    def uid(rx, ry, k, half):
        return 12 * (1 - rx) + 6 * (1 - ry) + 2 * k + half

    def ycopy2(k):
        return remote(near.at[uid(0, 1, k, 0)], r2.at[2 * k], s2.at[2 * k], q2.at[2 * k], dev_y)

    def xcopy2(k):
        return remote(near.at[uid(1, 0, k, 1)], r2.at[2 * k + 1], s2.at[2 * k + 1], q2.at[2 * k + 1], dev_x)

    def second(k):
        ua, ub = uid(0, 1, k, 0), uid(1, 0, k, 1)
        with sc(f"second{k}"):
            add_pair(
                (ua, ub), (xcopy1(k, 0), ycopy1(k, 0)), (xr1.at[k], yr1.at[k]), (near.at[ua], near.at[ub]),
                (ycopy2(k), xcopy2(k)),
            )

    def third(k):
        ua, ub = uid(0, 0, k, 0), uid(0, 0, k, 1)
        with sc(f"third{k}"):
            add_pair(
                (ua, ub), (xcopy1(3 + k, 0), ycopy1(3 + k, 0)), (xr1.at[3 + k], yr1.at[3 + k]),
                (n00.at[2 * k], n00.at[2 * k + 1]),
            )

    def fourth(k):
        cn = [pltpu.make_async_copy(n00.at[2 * k + h], dwv.at[2 * k + h], cin.at[h]) for h in range(2)]
        cr = [pltpu.make_async_copy(r2.at[2 * k + h], cst.at[h], cload.at[h]) for h in range(2)]
        st = min(64, hd)
        with sc(f"fourth{k}"):
            for h in range(2):
                cn[h].start()
            for h in range(2):
                (ycopy2, xcopy2)[h](k).wait_recv()
                cr[h].start()
            for h in range(2):
                cn[h].wait()
                cr[h].wait()

                @pl.loop(0, hd // st)
                def _(i):
                    row = pl.ds(pl.multiple_of(i * st, st), st)
                    dwv[2 * k + h, row, :] = dwv[2 * k + h, row, :] + cst[h, row, :]

    with sc("own_in"):
        for k in range(3):
            local[k].wait()
            if k < 2:
                xo[k].start()
                yo[k].start()
        yd[0].start()
        for cp in local[3:]:
            cp.wait()
    for j in range(2):
        acopy(0, 1, j).start()

    @mid
    def _():
        for j in range(2):
            bcopy(0, 2, j).start()

    for k in range(3):
        co[k].start()

    eye[...] = (
        lax.broadcasted_iota(jnp.int32, (hd, hd), 0) == lax.broadcasted_iota(jnp.int32, (hd, hd), 1)
    ).astype(f32).astype(bf)

    with sc("xt0"):
        transpose_x(1, 0, 1)

    def pass_on(s, j):
        with sc(f"rows{s}_{j}"):
            got(s, j)
        if s == 1:
            bcopy(1, 3, j).start()
        else:
            acopy(s, s, j).start()

    with sc("gx0"):
        xo[0].wait_recv()
        cx[0].start()
        yo[0].wait_recv()
    rg.start()
    cy[0].start()

    @mid
    def _():
        pass_on(1, 0)
        pass_on(2, 0)

    with sc("gx1"):
        xo[1].wait_recv()
        for cp in rua:
            cp.start()
        yd[1].start()
        cx[1].start()
        yo[1].wait_recv()
    for cp in rub:
        cp.start()
    for h in range(2):
        xd[h].start()
    cy[1].start()

    @mid
    def _():
        pass_on(1, 1)
        pass_on(2, 1)

    @end
    def _():
        with sc("e_rows1"):
            got(1, 0)

    with sc("gc0"):
        for cp in (*co[:2], *cx):
            cp.wait_recv()
    part_ab(1, 0)
    part_ab(0, 0)
    with sc("gyd"):
        yd[0].wait_recv()
        cyd[0].start()
        rg.wait_recv()
        crg.start()
    with sc("gc1"):
        for cp in (*cy, crg):
            cp.wait_recv()
    part_ab(1, 1, 1)
    co[2].wait_recv()

    @end
    def _():
        @pl.loop(0, 2)
        def _(i):
            n = pl.ds(pl.multiple_of(2 * i * kd, kd), hd)
            zs[2 * i, :, pl.ds(0, hd)] = mm(act[2, rows(1), pl.ds(0, kf)], wd[pl.ds(0, kf), n])

    @mid
    def _():
        pass_on(3, 0)

    with sc("gru"):
        for cp, fwd in zip((*rua[:1], *rub[:1], *rua[1:], *rub[1:]), (*crua[:1], *crub[:1], *crua[1:], *crub[1:])):
            cp.wait_recv()
            fwd.start()
    with sc("gc2"):
        for cp in (*crua, *crub):
            cp.wait_recv()
    part_ab(1, 1, 2)
    with sc("gc3"):
        cyd[0].wait_recv()

    def early_half(h):
        with sc(f"early1_{h}"):
            @pl.loop(0, 2)
            def _(i):
                r = 2 * i
                col = pl.ds(h * hd, hd)
                n = pl.ds(pl.multiple_of(r * kd + h * hd, hd), hd)
                if h == 0:
                    v = zs[r, :, col] + mm(act[2, rows(1), pl.ds(kf, kf)], wd[pl.ds(kf, kf), n])
                else:
                    v = mm(act[2, rows(1), :], wd[:, n])
                zs[r, :, col] = v
                remote(zs.at[r, :, col], zl.at[0, r, :, col], zsend.at[r], zrecv.at[0, r], dev_a).start()

    def early(s, odd):
        with sc(f"early{s}_{odd}"):
            @pl.loop(0, 2)
            def _(i):
                r = 2 * i + odd
                chunk(0, s, r, s - 1, None, True)
                zcopy(s - 1, 0, r, s - 1, dev_a).start()

    @end
    def _():
        early_half(0)
        with sc("e_rows2"):
            got(2, 0)

    part_ab(2, 0)
    with sc("gd0"):
        yd[1].wait_recv()
        cyd[1].start()
        xd[0].wait_recv()
        rd[0].start()
        cxd[0].start()
        cyd[1].wait_recv()

    @end
    def _():
        early_half(1)

    part_ab(2, 1)

    @end
    def _():
        early(2, 0)

    @mid
    def _():
        pass_on(3, 1)

    with sc("gd1"):
        xd[1].wait_recv()
        rd[1].start()
        cxd[1].start()
    part_ab(0, 1)
    with sc("gd2"):
        rd[0].wait_recv()
        crd[0].start()
    transpose_x(1, 1, 3)
    keep_h(0, 3)
    with sc("gd3"):
        rd[1].wait_recv()
        crd[1].start()
        for cp in (*cxd, *crd):
            cp.wait_recv()

    @end
    def _():
        early(1, 1)
        early(2, 1)
        got(1, 1)
        got(2, 1)
        with sc("e_rows3"):
            got(3, 0)

    part_ab(3, 0)
    part_ab(3, 1)
    flush(0)
    flush(1)
    gload(1)
    transpose_x(1, 3, 4)
    keep_h(3, 4)
    front_g(1, 0)
    front_g(0, 2)
    front_g(2, 3)
    far_start(0, 3)

    @end
    def _():
        with sc("e_rows3"):
            got(3, 1)

    far_start(3, 4)
    half_g(3, 1, None)
    near_load(1, 0)
    half_g(3, 0, None)
    near_load(1, 1)

    @pl.loop(0, 2)
    def _(j):
        near_unit(1, j)
        ncopy(j).start()

    for j in range(2):
        near_done(1, j)
    dw(1, 2, 2)

    @end
    def _():
        jobs((0, 3, 0, None, 2, dev_a, False))

    @mid
    def _():
        jobs((0, 2, 0, 1, 3, dev_b, True))

    with sc("xtb"):
        transpose_x(0, 0, 4)
    dw(0, 0, 0)
    for u in range(3):
        fcopy(u).wait_send()
    for cp in wcopies:
        cp.wait_send()
    for j in range(2):
        acopy(0, 1, j).wait_send()

    @mid
    def _():
        for j in range(2):
            bcopy(0, 2, j).wait_send()
            bcopy(1, 3, j).wait_send()
            acopy(2, 2, j).wait_send()
            acopy(3, 3, j).wait_send()

    @end
    def _():
        jobs((1, 3, 1, None, 2, dev_a, False))
        second(0)
        second(1)
        second(2)
        jobs((1, 2, 0, None, 1, dev_a, False))
        third(0)
        third(1)
        jobs((1, 1, 1, None, 0, dev_a, False))
        third(2)
        finish(0, (0,))
        last_part()
        fourth(0)
        finish(1, (0,), 0, 2)
        fourth(1)
        finish(1, (0,), 2, 3)
        fourth(2)

    @mid
    def _():
        jobs((0, 3, 1, 2, 4, dev_b, True))
        second(0)
        second(1)
        second(2)
        jobs((0, 1, 0, 4, 0, dev_a, False), (1, 3, 1, 2, 4, dev_b, False))
        third(0)
        third(1)
        jobs((1, 1, 0, 4, 0, dev_a, False), (1, 2, 1, 1, 3, dev_b, False))
        third(2)
        finish(0, (0, 3))
        fourth(0)
        fourth(1)
        last_part()
        finish(1, (0, 3), 0, 3)
        fourth(2)

    with sc("drain"):
        for i in range(6):
            xcopy1(i, 0).wait_send()
            ycopy1(i, 0).wait_send()
        for k in range(3):
            ycopy2(k).wait_send()
            xcopy2(k).wait_send()
        for half in range(2):
            for r in range(4):
                zcopy(0, 0, r, half, dev_a).wait_send()

        @mid
        def _():
            zcopy(3, 1, 3, 0, dev_a).wait_recv()

        zcopy(0, 1, 3, 0, dev_a).wait_recv()


def fused(x, dy, wg, wu, wd):
    nr, d = x.shape
    kd, kf = wg.shape
    f, hd = 2 * kf, kd // 2
    hbm = pl.BlockSpec(memory_space=pl.ANY)
    sds = jax.ShapeDtypeStruct
    out_shape = (
        pltpu.VMEM((4 * nr, d), bf), pltpu.VMEM((4 * nr, d), bf), pltpu.VMEM((6, hd, kf), f32),
        sds((5, 8, nr, kd), f32), sds((6, hd, kf), f32), sds((6, hd, kf), f32),
        sds((24, hd, kf), f32), sds((24, hd, kf), f32),
        sds((6, hd, kf), f32), sds((6, hd, kf), f32), sds((4, 2, 2, nr, kf), f32),
    )
    dma = pltpu.SemaphoreType.DMA
    return pl.pallas_call(
        kernel,
        name="fused",
        out_shape=out_shape,
        in_specs=[hbm] * 5,
        out_specs=(pl.BlockSpec(memory_space=pltpu.VMEM),) * 3 + (hbm,) * (len(out_shape) - 3),
        scratch_shapes=[
            pltpu.VMEM((d, f), bf), pltpu.VMEM((d, f), bf), pltpu.VMEM((f, d), bf),
            pltpu.VMEM((3, 4 * nr, f), bf),
            pltpu.VMEM((8, nr, kd), f32), pltpu.VMEM((2, kd, 4 * nr), bf), pltpu.VMEM((f, 4 * nr), bf),
            pltpu.VMEM((hd, hd), bf),
            pltpu.VMEM((2, hd, kf), f32),
            dma((49,)), dma((41,)), dma((11,)), dma((8,)), dma((5, 8)), dma((2,)), dma((3,)), dma((24,)), dma((2,)),
            dma((2,)), dma((6,)), dma((6,)), dma((6,)), dma((6,)), dma((6,)), dma((6,)), dma((2,)), dma((4,)),
        ],
        compiler_params=pltpu.CompilerParams(collective_id=0, has_side_effects=True, vmem_limit_bytes=VMEM_LIMIT - 14 * 2**20),
    )(x, dy, wg, wu, wd)


def tail_kernel(xa, dya, dwv, zl, y, dx, dwg, dwu, dwd, buf, out, sem, lsem):
    dp = lax.axis_index("dp")
    z = lax.axis_index("tp") // 2
    is_mid = (z == 1) | (z == 2)
    nr, kd = y.shape[0], dwd.shape[1]
    hd = kd // 2
    srcs = (zl.at[1, 7], zl.at[0, 7], zl.at[3, 7])
    loads = [pltpu.make_async_copy(v, buf.at[i], lsem.at[i]) for i, v in enumerate(srcs)]
    loads[0].start()
    loads[1].start()

    @pl.when(is_mid)
    def _():
        loads[2].start()

    copies = []
    for k in range(3):
        for h in range(2):
            v = dwv.at[2 * k + h]
            if k > 0:
                copies.append((v, (dwg, dwu)[k - 1].at[pl.ds(h * hd, hd)]))
            else:
                for q in range(2):
                    copies.append((v.at[:, pl.ds(q * kd, kd)], dwd.at[pl.ds((2 * h + q) * hd, hd)]))
    for src, dst, n in ((xa, y, 4), (dya, dx, 3)):
        for r in range(n):
            copies.append((src.at[pl.ds(nr, nr), pl.ds(r * kd, kd)], dst.at[:, natural(dp, r, kd)]))
    copies.append((out, dx.at[:, natural(dp, 3, kd)]))
    copies = [pltpu.make_async_copy(s, t, sem.at[i]) for i, (s, t) in enumerate(copies)]
    for c in copies[:-1]:
        c.start()
    loads[0].wait()
    loads[1].wait()
    buf[0] = buf[0] + buf[1]

    @pl.when(is_mid)
    def _():
        loads[2].wait()
        buf[0] = buf[0] + buf[2]

    out[...] = buf[0].astype(bf)
    copies[-1].start()
    for c in copies:
        c.wait()


def tail(xa, dya, dwv, zl, nr, kd, kf):
    hbm = pl.BlockSpec(memory_space=pl.ANY)
    sds = jax.ShapeDtypeStruct
    d = xa.shape[1]
    dma = pltpu.SemaphoreType.DMA
    return pl.pallas_call(
        tail_kernel,
        name="tail",
        out_shape=(sds((nr, d), bf), sds((nr, d), bf), sds((kd, kf), f32), sds((kd, kf), f32), sds((kf, kd), f32)),
        in_specs=[hbm] * 4,
        out_specs=(hbm,) * 5,
        scratch_shapes=[pltpu.VMEM((3, nr, kd), f32), pltpu.VMEM((nr, kd), bf), dma((16,)), dma((3,))],
        compiler_params=pltpu.CompilerParams(vmem_limit_bytes=VMEM_LIMIT - 27 * 2**20),
    )(xa, dya, dwv, zl)


def solution(mesh):
    rows = P(("dp", "tp"), None)
    wsp = P("dp", "tp")
    dsp = P("tp", "dp")

    def local(x, w_gate, w_up, w_down, dy):
        return tail(*fused(x, dy, w_gate, w_up, w_down)[:4], x.shape[0], *w_gate.shape)

    return jax.shard_map(local, mesh=mesh, in_specs=(rows, wsp, wsp, dsp, rows), out_specs=(rows, rows, wsp, wsp, dsp), check_vma=False)
```

```python
import jax
import jax.numpy as jnp
from jax import lax
from jax.experimental import pallas as pl
from jax.experimental.pallas import tpu as pltpu
from jax.sharding import PartitionSpec as P

MESH = pl.DeviceIdType.MESH
f32 = jnp.float32
bf = jnp.bfloat16
VMEM_LIMIT = 67043328
sc = jax.named_scope
LAG = 4


def mm(a, b):
    return lax.dot_general(a, b, (((1,), (0,)), ((), ())), preferred_element_type=f32)


def mmt(a, b):
    return lax.dot_general(a, b, (((1,), (1,)), ((), ())), preferred_element_type=f32)


def natural(dp, r, kd):
    x, c, rc, rx = dp // 2, dp % 2, r // 2, r % 2
    n = 2 * (x + rx - 2 * x * rx) + c + rc - 2 * c * rc
    return pl.ds(pl.multiple_of(n * kd, kd), kd)


def kernel(
    x_in, dy_in, wg_in, wu_in, wd_in,
    xa, dya, dwv, zl, n00, r2, far_r, near, xr1, yr1, stash,
    wg, wu, wd, act, zs, xt, ht, eye, cst,
    gs, gr, lsem, zsend, zrecv, zload, fsend, frecv, nstore, cload, xs1, xq1, ys1, yq1, s2, q2, cin, ssem,
):
    tp = lax.axis_index("tp")
    dp = lax.axis_index("dp")
    z, y = tp // 2, tp % 2
    x, c = dp // 2, dp % 2
    is_end = (z == 0) | (z == 3)
    is_mid = (z == 1) | (z == 2)
    dev_x = {"tp": tp, "dp": 2 * (1 - x) + c}
    dev_y = {"tp": 2 * z + 1 - y, "dp": dp}
    dev_c = {"tp": tp, "dp": 2 * x + 1 - c}
    dev_a = {"tp": 2 * (z + 1 - 2 * (z % 2)) + y, "dp": dp}
    dev_b = {"tp": 2 * (3 - z) + y, "dp": dp}

    fst, nst = dwv.at[pl.ds(0, 3)], dwv.at[pl.ds(3, 2)]
    nr, d = x_in.shape
    kd, kf = wg_in.shape
    f = 2 * kf
    hd = kd // 2
    hf = kf // 2

    def end(fn):
        pl.when(is_end)(fn)

    def mid(fn):
        pl.when(is_mid)(fn)

    def ncol(r):
        return natural(dp, r, kd)

    def remote(src, dst, ss, rs, dev):
        return pltpu.make_async_remote_copy(
            src_ref=src, dst_ref=dst, send_sem=ss, recv_sem=rs, device_id=dev, device_id_type=MESH
        )

    own = (wg_in, wu_in, wd_in)

    def blk(k, rx, rc, ry, lo=0, n=None):
        d0 = (2 * rc + rx) * kd + lo
        n = kd if n is None else n
        if k < 2:
            return (wg, wu)[k].at[pl.ds(d0, n), pl.ds(ry * kf, kf)]
        return wd.at[pl.ds(ry * kf, kf), pl.ds(d0, n)]

    local = [(own[k], blk(k, 0, 0, 0)) for k in range(3)]
    for src, ref in ((x_in, xa), (dy_in, dya)):
        for r in range(4):
            local.append((src.at[:, ncol(r)], ref.at[pl.ds(0, nr), pl.ds(r * kd, kd)]))
    local = [pltpu.make_async_copy(s, t, lsem.at[i]) for i, (s, t) in enumerate(local)]
    for cp in local:
        cp.start()

    bar = pltpu.get_barrier_semaphore()
    for dev in (dev_x, dev_y, dev_c, dev_a, dev_b):
        pl.semaphore_signal(bar, inc=1, device_id=dev, device_id_type=MESH)

    with sc("barrier"):
        pl.semaphore_wait(bar, 5)

    ft = min(256, f)

    def rows(s):
        return pl.ds(s * nr, nr)

    def transpose_x(rx, lo, hi):
        @pl.loop(lo, hi)
        def _(s):
            row = pl.ds(pl.multiple_of(s * nr, nr), nr)
            for rc in range(2):
                for h in range(2):
                    v = mmt(eye[...], xa[row, pl.ds((2 * rc + rx) * kd + h * hd, hd)])
                    xt[rc, pl.ds(h * hd, hd), row] = v.astype(bf)

    def wcopy(i, src, dst, dev):
        return remote(src, dst, gs.at[i], gr.at[i], dev)

    def half(rx, rc, ry, h):
        return blk(2, rx, rc, ry, h * hd, hd)

    ua = 3 * kd // 4
    mine = [blk(k, 0, 0, 0) for k in range(3)]
    xo = [wcopy(k, mine[k], blk(k, 1, 0, 0), dev_x) for k in range(2)]
    yo = [wcopy(2 + k, mine[k], blk(k, 0, 0, 1), dev_y) for k in range(2)]
    co = [wcopy(4 + k, mine[k], blk(k, 0, 1, 0), dev_c) for k in range(3)]
    xd = [wcopy(7 + h, half(0, 0, 0, h), half(1, 0, 0, h), dev_x) for h in range(2)]
    yd = [wcopy(9 + h, half(0, 0, 0, h), half(0, 0, 1, h), dev_y) for h in range(2)]
    rg = wcopy(11, blk(0, 0, 0, 1), blk(0, 1, 0, 1), dev_x)
    ay, ax = ((0, 5 * kd // 8), (5 * kd // 8, ua)), ((ua, 7 * kd // 8), (7 * kd // 8, kd))
    rua = [wcopy(i, blk(1, 1, 0, 0, lo, hi - lo), blk(1, 1, 0, 1, lo, hi - lo), dev_y) for i, (lo, hi) in zip((12, 29), ay)]
    rub = [wcopy(i, blk(1, 0, 0, 1, lo, hi - lo), blk(1, 1, 0, 1, lo, hi - lo), dev_x) for i, (lo, hi) in zip((13, 31), ax)]
    rd = [wcopy(14 + h, half(1, 0, 0, h), half(1, 0, 1, h), dev_y) for h in range(2)]
    cx = [wcopy(16 + k, blk(k, 1, 0, 0), blk(k, 1, 1, 0), dev_c) for k in range(2)]
    cy = [wcopy(18 + k, blk(k, 0, 0, 1), blk(k, 0, 1, 1), dev_c) for k in range(2)]
    cxd = [wcopy(20 + h, half(1, 0, 0, h), half(1, 1, 0, h), dev_c) for h in range(2)]
    cyd = [wcopy(22 + h, half(0, 0, 1, h), half(0, 1, 1, h), dev_c) for h in range(2)]
    crg = wcopy(24, blk(0, 1, 0, 1), blk(0, 1, 1, 1), dev_c)
    crua = [wcopy(i, blk(1, 1, 0, 1, lo, hi - lo), blk(1, 1, 1, 1, lo, hi - lo), dev_c) for i, (lo, hi) in zip((25, 30), ay)]
    crub = [wcopy(i, blk(1, 1, 0, 1, lo, hi - lo), blk(1, 1, 1, 1, lo, hi - lo), dev_c) for i, (lo, hi) in zip((26, 32), ax)]
    crd = [wcopy(27 + h, half(1, 0, 1, h), half(1, 1, 1, h), dev_c) for h in range(2)]
    wcopies = (*xo, *yo, *co, *xd, *yd, rg, *rua, *rub, *rd, *cx, *cy, *cxd, *cyd, crg, *crua, *crub, *crd)
    nw = 33

    def slot(j, s):
        return (xa, dya)[j].at[pl.ds(s * nr, nr)]

    def acopy(src, dst, j):
        return remote(
            slot(j, src), slot(j, dst), gs.at[nw + 2 * dst + j], gr.at[nw + 2 * dst + j], dev_a
        )

    def bcopy(src, dst, j):
        return remote(
            slot(j, src), slot(j, dst), gs.at[nw + 8 + 2 * dst + j], gr.at[nw + 2 * dst + j], dev_b
        )

    def got(s, j):
        acopy(s, s, j).wait_recv()

    def stash_copy(s, p, n):
        return pltpu.make_async_copy((fst, nst)[n].at[p, pl.ds(0, nr)], stash.at[s, p, n], ssem.at[2 * p + n])

    def factor(s, n):
        return nst if n else cst if s == 3 else fst

    def stash_load(s, p, n):
        return pltpu.make_async_copy(stash.at[s, p, n], factor(s, n).at[p, pl.ds(0, nr)], ssem.at[2 * p + n])

    pending = [None, None]

    def flush(p):
        if pending[p] is not None:
            for n in range(2):
                stash_copy(pending[p], p, n).wait()
        pending[p] = None

    def ab_tiles(s, p, step):
        def tile(i):
            col = pl.ds(pl.multiple_of(p * kf + i * ft, ft), ft)
            at = (p, pl.ds(0, nr), pl.ds(pl.multiple_of(i * ft, ft), ft))

            def some_b(rx):
                b0, b1 = pl.ds(rx * kd, kd), pl.ds((2 + rx) * kd, kd)
                return mm(xa[rows(s), b0], wu[b0, col]) + mm(xa[rows(s), b1], wu[b1, col])

            if step == 1:
                fst[at] = mm(xa[rows(s), :], wg[:, col])
                nst[at] = some_b(0)
                return
            if step == 2:
                a = fst[at]
                b = nst[at] + some_b(1)
            else:
                a = mm(xa[rows(s), :], wg[:, col])
                b = mm(xa[rows(s), :], wu[:, col])
            sig = jax.nn.sigmoid(a)
            sa = a * sig
            act[2, rows(s), col] = (sa * b).astype(bf)
            fst[at] = sa
            nst[at] = b * sig * (1.0 + a * (1.0 - sig))

        m = min(4, kf // ft) if step == 2 else 1

        @pl.loop(0, kf // ft // m)
        def _(i):
            for q in range(m):
                tile(i * m + q)

    def part_ab(s, p, step=0):
        with sc(f"ab{s}_{p}"):
            flush(p)
            ab_tiles(s, p, step)
            if step != 1:
                for n in range(2):
                    stash_copy(s, p, n).start()
                pending[p] = s

    gt = min(512, kf)

    def part_g(s, p):
        @pl.loop(0, kf // gt)
        def _(i):
            col = pl.ds(pl.multiple_of(p * kf + i * gt, gt), gt)
            kcol = pl.ds(pl.multiple_of(i * gt, gt), gt)
            g = mmt(dya[rows(s), :], wd[col, :])
            act[0, rows(s), col] = (g * factor(s, 1)[p, pl.ds(0, nr), kcol]).astype(bf)
            act[1, rows(s), col] = (g * factor(s, 0)[p, pl.ds(0, nr), kcol]).astype(bf)

    def gload(s):
        for p in range(2):
            for n in range(2):
                stash_load(s, p, n).start()

    def half_g(s, p, then):
        with sc(f"g{s}"):
            for n in range(2):
                stash_load(s, p, n).wait()
            part_g(s, p)
            if then is not None:
                for n in range(2):
                    stash_load(then, p, n).start()

    def front_g(s, then):
        @pl.loop(0, 2)
        def _(p):
            half_g(s, p, then)

    def keep_h(lo, hi):
        hb = min(4, f // hd)
        nh = f // (hb * hd)
        with sc("ht"):
            @pl.loop(lo * nh, hi * nh)
            def _(i):
                row = pl.ds(pl.multiple_of(i // nh * nr, nr), nr)
                for q in range(hb):
                    col = pl.ds(pl.multiple_of((i % nh * hb + q) * hd, hd), hd)
                    ht[col, row] = mmt(eye[...], act[2, row, col]).astype(bf)

    def back(ref, at, kind, s, r):
        *lead, c0 = at

        @pl.loop(0, 2)
        def _(h):
            n = pl.ds(pl.multiple_of(r * kd + h * hd, hd), hd)
            if kind == 0:
                v = mm(act[2, rows(s), :], wd[:, n])
            else:
                v = mmt(act[0, rows(s), :], wg[n, :]) + mmt(act[1, rows(s), :], wu[n, :])
            ref[(*lead, pl.ds(0, nr), pl.ds(pl.multiple_of(c0 + h * hd, hd), hd))] = v

    def zcopy(q, kind, r, half, dev):
        i = 4 * kind + r
        return remote(zs.at[4 * half + r], zl.at[q, i], zsend.at[4 * half + r], zrecv.at[q, i], dev)

    def zload_(q, kind, r, slot):
        return pltpu.make_async_copy(zl.at[q, 4 * kind + r], cst.at[slot, pl.ds(0, nr), pl.ds(0, kd)], zload.at[slot])

    def chunk(kind, s, r, half, q_add, first):
        i = 4 * half + r
        if q_add is not None:
            with sc("zrecv"):
                zcopy(q_add, kind, r, half, dev_a).wait_recv()
            zload_(q_add, kind, r, r % 2).start()
        if not first:
            with sc("zsend"):
                zcopy(0, kind, r, half, dev_a).wait_send()
        back(zs, (i, 0), kind, s, r)
        if q_add is not None:
            zload_(q_add, kind, r, r % 2).wait()
            zs[i] = zs[i] + cst[r % 2, pl.ds(0, nr), pl.ds(0, kd)]

    def jobs(*specs):
        with sc("job" + "_".join(f"{kind}{s}" for kind, s, *_ in specs)):
            @pl.loop(0, 4)
            def _(r):
                for kind, s, h, q_add, q_dst, dev, first in specs:
                    chunk(kind, s, r, h, q_add, first)
                    zcopy(q_dst, kind, r, h, dev).start()

    def last_part():
        back(cst, (0, kd), 1, 0, 3)
        at = (0, pl.ds(0, nr), pl.ds(kd, kd))
        cst[at] = cst[at] + dya[rows(0), pl.ds(3 * kd, kd)].astype(f32)
        cp = pltpu.make_async_copy(cst.at[at], zl.at[1, 7], zload.at[0])
        cp.start()
        cp.wait()

    def finish(kind, adds, lo=0, hi=4):
        res = (xa, dya)[kind]
        with sc(f"fin{kind}"):
            @pl.loop(lo, hi)
            def _(r):
                col = pl.ds(pl.multiple_of(r * kd, kd), kd)
                part = (pl.ds(0, nr), pl.ds(0, kd))
                temp = (0, pl.ds(0, nr), pl.ds(kd, kd))
                back(cst, (0, kd), kind, 0, r)
                for n, q in enumerate(adds):
                    with sc("finrecv"):
                        zcopy(q, kind, r, 0, dev_a).wait_recv()
                    zload_(q, kind, r, n).start()
                for n, q in enumerate(adds):
                    zload_(q, kind, r, n).wait()
                v = cst[temp] + res[rows(0), col].astype(f32)
                for n in range(len(adds)):
                    v = v + cst[n, *part]
                res[rows(1), col] = v.astype(bf)

    def unit(rc, rx, j, put):
        ryi, k, half = j // 6, ((j // 2) % 3 + 2) % 3, j % 2
        f0 = (1 - ryi) * kf

        @pl.when(k < 2)
        def _():
            a = xt[rc, pl.ds(pl.multiple_of(half * hd, hd), hd), :]
            for q in range(4):
                b = act[k, :, pl.ds(pl.multiple_of(f0 + q * hd, hd), hd)]
                put(pl.ds(q * hd, hd), mm(a, b))

        @pl.when(k == 2)
        def _():
            for q in range(4):
                b = dya[:, pl.ds((2 * rc + rx) * kd + q % 2 * hd, hd)]
                a = ht[pl.ds(pl.multiple_of(f0 + half * hf + q // 2 * hd, hd), hd), :]
                put(pl.ds(q * hd, hd), mm(a, b))

    def fcopy(u):
        return remote(fst.at[u % 3], far_r.at[u], fsend.at[u % 3], frecv.at[u], dev_c)

    def ncopy(u):
        return pltpu.make_async_copy(nst.at[(u + 1) % 2], near.at[u], nstore.at[(u + 1) % 2])

    def ccopy(u):
        return pltpu.make_async_copy(far_r.at[u], cst.at[(u + 1) % 2], cload.at[(u + 1) % 2])

    def xcopy1(i, u):
        return remote(near.at[u], xr1.at[i], xs1.at[i], xq1.at[i], dev_x)

    def ycopy1(i, u):
        return remote(near.at[u], yr1.at[i], ys1.at[i], yq1.at[i], dev_y)

    def nsend(rx, j):
        ryi, k, half = j // 6, (j // 2) % 3, j % 2
        u = 12 * (1 - rx) + j
        if rx:
            @pl.when(half == 0)
            def _():
                xcopy1(ryi * 3 + k, u).start()

        @pl.when((half == 1) & (ryi == 0))
        def _():
            ycopy1(3 * (1 - rx) + k, u).start()

    def far_unit(rx, j):
        u = 12 * (1 - rx) + j

        @pl.when(u > 2)
        def _():
            with sc("fsend"):
                fcopy(u).wait_send()

        def put(col, v):
            fst[u % 3, :, col] = v

        unit(1, rx, j, put)
        fcopy(u).start()

    def far_start(lo, hi):
        t = pl.ds(lo * nr, (hi - lo) * nr)
        with sc("farstart"):
            @pl.loop(0, 2)
            def _(j):
                for q in range(4):
                    a = ht[pl.ds(pl.multiple_of(kf + j * hf + q // 2 * hd, hd), hd), t]
                    v = mm(a, dya[t, pl.ds(3 * kd + q % 2 * hd, hd)])
                    at = (j, slice(None), pl.ds(q * hd, hd))
                    fst[at] = fst[at] + v if lo else v

                if lo:
                    fcopy(j).start()

    def near_load(rx, j):
        u = 12 * (1 - rx) + j
        with sc("frecv"):
            fcopy(u).wait_recv()
        ccopy(u).start()

    def near_unit(rx, j):
        u = 12 * (1 - rx) + j
        with sc("cwait"):
            ccopy(u).wait()

        def put(col, v):
            i = (u + 1) % 2
            nst[i, :, col] = v + cst[i, :, col]

        unit(0, rx, j, put)

    def near_done(rx, j):
        with sc("nwait"):
            ncopy(12 * (1 - rx) + j).wait()
        nsend(rx, j)

    def dw(rx, f0, n0):
        base = 12 * (1 - rx)

        with sc(f"dw{rx}"):
            @pl.loop(f0, 12 + LAG)
            def _(j):
                n = j - LAG

                @pl.when(j < 12)
                def _():
                    far_unit(rx, j)

                @pl.when((n + 1 >= n0) & (n < 11))
                def _():
                    near_load(rx, n + 1)

                @pl.when(n >= n0)
                def _():
                    near_unit(rx, n)

                    @pl.when(n > n0)
                    def _():
                        near_done(rx, n - 1)

                    ncopy(base + n).start()

            near_done(rx, 11)

    def add_pair(units, waits, arrived, dsts, after=(None, None)):
        cn = [pltpu.make_async_copy(near.at[u], fst.at[h], cin.at[h]) for h, u in enumerate(units)]
        cr = [pltpu.make_async_copy(v, cst.at[h], cload.at[h]) for h, v in enumerate(arrived)]
        cd = [pltpu.make_async_copy(nst.at[h], t, nstore.at[h]) for h, t in enumerate(dsts)]
        st = min(64, hd)
        for h in range(2):
            cn[h].start()
        for h in range(2):
            waits[h].wait_recv()
            cr[h].start()
        for h in range(2):
            cn[h].wait()
            cr[h].wait()

            @pl.loop(0, hd // st)
            def _(i):
                row = pl.ds(pl.multiple_of(i * st, st), st)
                nst[h, row, :] = fst[h, row, :] + cst[h, row, :]

            cd[h].start()
        for h in range(2):
            cd[h].wait()
            if after[h] is not None:
                after[h].start()

    def uid(rx, ry, k, half):
        return 12 * (1 - rx) + 6 * (1 - ry) + 2 * k + half

    def ycopy2(k):
        return remote(near.at[uid(0, 1, k, 0)], r2.at[2 * k], s2.at[2 * k], q2.at[2 * k], dev_y)

    def xcopy2(k):
        return remote(near.at[uid(1, 0, k, 1)], r2.at[2 * k + 1], s2.at[2 * k + 1], q2.at[2 * k + 1], dev_x)

    def second(k):
        ua, ub = uid(0, 1, k, 0), uid(1, 0, k, 1)
        with sc(f"second{k}"):
            add_pair(
                (ua, ub), (xcopy1(k, 0), ycopy1(k, 0)), (xr1.at[k], yr1.at[k]), (near.at[ua], near.at[ub]),
                (ycopy2(k), xcopy2(k)),
            )

    def third(k):
        ua, ub = uid(0, 0, k, 0), uid(0, 0, k, 1)
        with sc(f"third{k}"):
            add_pair(
                (ua, ub), (xcopy1(3 + k, 0), ycopy1(3 + k, 0)), (xr1.at[3 + k], yr1.at[3 + k]),
                (n00.at[2 * k], n00.at[2 * k + 1]),
            )

    def fourth(k):
        cn = [pltpu.make_async_copy(n00.at[2 * k + h], dwv.at[2 * k + h], cin.at[h]) for h in range(2)]
        cr = [pltpu.make_async_copy(r2.at[2 * k + h], cst.at[h], cload.at[h]) for h in range(2)]
        st = min(64, hd)
        with sc(f"fourth{k}"):
            for h in range(2):
                cn[h].start()
            for h in range(2):
                (ycopy2, xcopy2)[h](k).wait_recv()
                cr[h].start()
            for h in range(2):
                cn[h].wait()
                cr[h].wait()

                @pl.loop(0, hd // st)
                def _(i):
                    row = pl.ds(pl.multiple_of(i * st, st), st)
                    dwv[2 * k + h, row, :] = dwv[2 * k + h, row, :] + cst[h, row, :]

    with sc("own_in"):
        for k in range(3):
            local[k].wait()
            if k < 2:
                xo[k].start()
                yo[k].start()
        yd[0].start()
        for cp in local[3:]:
            cp.wait()
    for j in range(2):
        acopy(0, 1, j).start()

    @mid
    def _():
        for j in range(2):
            bcopy(0, 2, j).start()

    for k in range(3):
        co[k].start()

    eye[...] = (
        lax.broadcasted_iota(jnp.int32, (hd, hd), 0) == lax.broadcasted_iota(jnp.int32, (hd, hd), 1)
    ).astype(f32).astype(bf)

    with sc("xt0"):
        transpose_x(1, 0, 1)

    def pass_on(s, j):
        with sc(f"rows{s}_{j}"):
            got(s, j)
        if s == 1:
            bcopy(1, 3, j).start()
        else:
            acopy(s, s, j).start()

    with sc("gx0"):
        xo[0].wait_recv()
        cx[0].start()
        yo[0].wait_recv()
    rg.start()
    cy[0].start()

    @mid
    def _():
        pass_on(1, 0)
        pass_on(2, 0)

    with sc("gx1"):
        xo[1].wait_recv()
        for cp in rua:
            cp.start()
        yd[1].start()
        cx[1].start()
        yo[1].wait_recv()
    for cp in rub:
        cp.start()
    for h in range(2):
        xd[h].start()
    cy[1].start()

    @mid
    def _():
        pass_on(1, 1)
        pass_on(2, 1)

    @end
    def _():
        with sc("e_rows1"):
            got(1, 0)

    with sc("gc0"):
        for cp in (*co[:2], *cx):
            cp.wait_recv()
    part_ab(1, 0)
    part_ab(0, 0)
    with sc("gyd"):
        yd[0].wait_recv()
        cyd[0].start()
        rg.wait_recv()
        crg.start()
    with sc("gc1"):
        for cp in (*cy, crg):
            cp.wait_recv()
    part_ab(1, 1, 1)
    co[2].wait_recv()

    @end
    def _():
        @pl.loop(0, 2)
        def _(i):
            n = pl.ds(pl.multiple_of(2 * i * kd, kd), hd)
            zs[2 * i, :, pl.ds(0, hd)] = mm(act[2, rows(1), pl.ds(0, kf)], wd[pl.ds(0, kf), n])

    @mid
    def _():
        pass_on(3, 0)

    with sc("gru"):
        for cp, fwd in zip((*rua[:1], *rub[:1], *rua[1:], *rub[1:]), (*crua[:1], *crub[:1], *crua[1:], *crub[1:])):
            cp.wait_recv()
            fwd.start()
    with sc("gc2"):
        for cp in (*crua, *crub):
            cp.wait_recv()
    part_ab(1, 1, 2)
    with sc("gc3"):
        cyd[0].wait_recv()

    def early_half(h):
        with sc(f"early1_{h}"):
            @pl.loop(0, 2)
            def _(i):
                r = 2 * i
                col = pl.ds(h * hd, hd)
                n = pl.ds(pl.multiple_of(r * kd + h * hd, hd), hd)
                if h == 0:
                    v = zs[r, :, col] + mm(act[2, rows(1), pl.ds(kf, kf)], wd[pl.ds(kf, kf), n])
                else:
                    v = mm(act[2, rows(1), :], wd[:, n])
                zs[r, :, col] = v
                remote(zs.at[r, :, col], zl.at[0, r, :, col], zsend.at[r], zrecv.at[0, r], dev_a).start()

    def early(s, odd):
        with sc(f"early{s}_{odd}"):
            @pl.loop(0, 2)
            def _(i):
                r = 2 * i + odd
                chunk(0, s, r, s - 1, None, True)
                zcopy(s - 1, 0, r, s - 1, dev_a).start()

    @end
    def _():
        early_half(0)
        with sc("e_rows2"):
            got(2, 0)

    part_ab(2, 0)
    with sc("gd0"):
        yd[1].wait_recv()
        cyd[1].start()
        xd[0].wait_recv()
        rd[0].start()
        cxd[0].start()
        cyd[1].wait_recv()

    @end
    def _():
        early_half(1)

    part_ab(2, 1)

    @end
    def _():
        early(2, 0)

    @mid
    def _():
        pass_on(3, 1)

    with sc("gd1"):
        xd[1].wait_recv()
        rd[1].start()
        cxd[1].start()
    part_ab(0, 1)
    with sc("gd2"):
        rd[0].wait_recv()
        crd[0].start()
    transpose_x(1, 1, 3)
    keep_h(0, 3)
    with sc("gd3"):
        rd[1].wait_recv()
        crd[1].start()
        for cp in (*cxd, *crd):
            cp.wait_recv()

    @end
    def _():
        early(1, 1)
        early(2, 1)
        got(1, 1)
        got(2, 1)
        with sc("e_rows3"):
            got(3, 0)

    part_ab(3, 0)
    part_ab(3, 1)
    flush(0)
    flush(1)
    gload(1)
    transpose_x(1, 3, 4)
    keep_h(3, 4)
    front_g(1, 0)
    front_g(0, 2)
    front_g(2, 3)
    far_start(0, 3)

    @end
    def _():
        with sc("e_rows3"):
            got(3, 1)

    far_start(3, 4)
    half_g(3, 1, None)
    near_load(1, 0)
    half_g(3, 0, None)
    near_load(1, 1)

    @pl.loop(0, 2)
    def _(j):
        near_unit(1, j)
        ncopy(j).start()

    for j in range(2):
        near_done(1, j)
    dw(1, 2, 2)

    @end
    def _():
        jobs((0, 3, 0, None, 2, dev_a, False))

    @mid
    def _():
        jobs((0, 2, 0, 1, 3, dev_b, True))

    with sc("xtb"):
        transpose_x(0, 0, 4)
    dw(0, 0, 0)
    for u in range(3):
        fcopy(u).wait_send()
    for cp in wcopies:
        cp.wait_send()
    for j in range(2):
        acopy(0, 1, j).wait_send()

    @mid
    def _():
        for j in range(2):
            bcopy(0, 2, j).wait_send()
            bcopy(1, 3, j).wait_send()
            acopy(2, 2, j).wait_send()
            acopy(3, 3, j).wait_send()

    @end
    def _():
        jobs((1, 3, 1, None, 2, dev_a, False))
        second(0)
        second(1)
        second(2)
        jobs((1, 2, 0, None, 1, dev_a, False))
        third(0)
        third(1)
        jobs((1, 1, 1, None, 0, dev_a, False))
        third(2)
        finish(0, (0,))
        last_part()
        fourth(0)
        finish(1, (0,), 0, 2)
        fourth(1)
        finish(1, (0,), 2, 3)
        fourth(2)

    @mid
    def _():
        jobs((0, 3, 1, 2, 4, dev_b, True))
        second(0)
        second(1)
        second(2)
        jobs((0, 1, 0, 4, 0, dev_a, False), (1, 3, 1, 2, 4, dev_b, False))
        third(0)
        third(1)
        jobs((1, 1, 0, 4, 0, dev_a, False), (1, 2, 1, 1, 3, dev_b, False))
        third(2)
        finish(0, (0, 3))
        fourth(0)
        fourth(1)
        last_part()
        finish(1, (0, 3), 0, 3)
        fourth(2)

    with sc("drain"):
        for i in range(6):
            xcopy1(i, 0).wait_send()
            ycopy1(i, 0).wait_send()
        for k in range(3):
            ycopy2(k).wait_send()
            xcopy2(k).wait_send()
        for half in range(2):
            for r in range(4):
                zcopy(0, 0, r, half, dev_a).wait_send()

        @mid
        def _():
            zcopy(3, 1, 3, 0, dev_a).wait_recv()

        zcopy(0, 1, 3, 0, dev_a).wait_recv()


def fused(x, dy, wg, wu, wd):
    nr, d = x.shape
    kd, kf = wg.shape
    f, hd = 2 * kf, kd // 2
    hbm = pl.BlockSpec(memory_space=pl.ANY)
    sds = jax.ShapeDtypeStruct
    out_shape = (
        pltpu.VMEM((4 * nr, d), bf), pltpu.VMEM((4 * nr, d), bf), pltpu.VMEM((6, hd, kf), f32),
        sds((5, 8, nr, kd), f32), sds((6, hd, kf), f32), sds((6, hd, kf), f32),
        sds((24, hd, kf), f32), sds((24, hd, kf), f32),
        sds((6, hd, kf), f32), sds((6, hd, kf), f32), sds((4, 2, 2, nr, kf), f32),
    )
    dma = pltpu.SemaphoreType.DMA
    return pl.pallas_call(
        kernel,
        name="fused",
        out_shape=out_shape,
        in_specs=[hbm] * 5,
        out_specs=(pl.BlockSpec(memory_space=pltpu.VMEM),) * 3 + (hbm,) * (len(out_shape) - 3),
        scratch_shapes=[
            pltpu.VMEM((d, f), bf), pltpu.VMEM((d, f), bf), pltpu.VMEM((f, d), bf),
            pltpu.VMEM((3, 4 * nr, f), bf),
            pltpu.VMEM((8, nr, kd), f32), pltpu.VMEM((2, kd, 4 * nr), bf), pltpu.VMEM((f, 4 * nr), bf),
            pltpu.VMEM((hd, hd), bf),
            pltpu.VMEM((2, hd, kf), f32),
            dma((49,)), dma((41,)), dma((11,)), dma((8,)), dma((5, 8)), dma((2,)), dma((3,)), dma((24,)), dma((2,)),
            dma((2,)), dma((6,)), dma((6,)), dma((6,)), dma((6,)), dma((6,)), dma((6,)), dma((2,)), dma((4,)),
        ],
        compiler_params=pltpu.CompilerParams(collective_id=0, has_side_effects=True, vmem_limit_bytes=VMEM_LIMIT - 14 * 2**20),
    )(x, dy, wg, wu, wd)


def tail_kernel(xa, dya, dwv, zl, y, dx, dwg, dwu, dwd, buf, out, sem, lsem):
    dp = lax.axis_index("dp")
    z = lax.axis_index("tp") // 2
    is_mid = (z == 1) | (z == 2)
    nr, kd = y.shape[0], dwd.shape[1]
    hd = kd // 2
    srcs = (zl.at[1, 7], zl.at[0, 7], zl.at[3, 7])
    loads = [pltpu.make_async_copy(v, buf.at[i], lsem.at[i]) for i, v in enumerate(srcs)]
    loads[0].start()
    loads[1].start()

    @pl.when(is_mid)
    def _():
        loads[2].start()

    copies = []
    for k in range(3):
        for h in range(2):
            v = dwv.at[2 * k + h]
            if k > 0:
                copies.append((v, (dwg, dwu)[k - 1].at[pl.ds(h * hd, hd)]))
            else:
                for q in range(2):
                    copies.append((v.at[:, pl.ds(q * kd, kd)], dwd.at[pl.ds((2 * h + q) * hd, hd)]))
    for src, dst, n in ((xa, y, 4), (dya, dx, 3)):
        for r in range(n):
            copies.append((src.at[pl.ds(nr, nr), pl.ds(r * kd, kd)], dst.at[:, natural(dp, r, kd)]))
    copies.append((out, dx.at[:, natural(dp, 3, kd)]))
    copies = [pltpu.make_async_copy(s, t, sem.at[i]) for i, (s, t) in enumerate(copies)]
    for c in copies[:-1]:
        c.start()
    loads[0].wait()
    loads[1].wait()
    buf[0] = buf[0] + buf[1]

    @pl.when(is_mid)
    def _():
        loads[2].wait()
        buf[0] = buf[0] + buf[2]

    out[...] = buf[0].astype(bf)
    copies[-1].start()
    for c in copies:
        c.wait()


def tail(xa, dya, dwv, zl, nr, kd, kf):
    hbm = pl.BlockSpec(memory_space=pl.ANY)
    sds = jax.ShapeDtypeStruct
    d = xa.shape[1]
    dma = pltpu.SemaphoreType.DMA
    return pl.pallas_call(
        tail_kernel,
        name="tail",
        out_shape=(sds((nr, d), bf), sds((nr, d), bf), sds((kd, kf), f32), sds((kd, kf), f32), sds((kf, kd), f32)),
        in_specs=[hbm] * 4,
        out_specs=(hbm,) * 5,
        scratch_shapes=[pltpu.VMEM((3, nr, kd), f32), pltpu.VMEM((nr, kd), bf), dma((16,)), dma((3,))],
        compiler_params=pltpu.CompilerParams(vmem_limit_bytes=VMEM_LIMIT - 27 * 2**20),
    )(xa, dya, dwv, zl)


def solution(mesh):
    rows = P(("dp", "tp"), None)
    wsp = P("dp", "tp")
    dsp = P("tp", "dp")

    def local(x, w_gate, w_up, w_down, dy):
        return tail(*fused(x, dy, w_gate, w_up, w_down)[:4], x.shape[0], *w_gate.shape)

    return jax.shard_map(local, mesh=mesh, in_specs=(rows, wsp, wsp, dsp, rows), out_specs=(rows, rows, wsp, wsp, dsp), check_vma=False)
```
